32 devices in a mesh: dp: 8 (over z, core), expert: 4 (over y, x).
Axes of the slice: x: 2, y: 2, z: 4, core: 2. Of those that a mesh axis runs over, the one named last changes fastest.
Arguments:
- tokens: bfloat16 [24576, 768], P(('dp', 'expert')), may hold values from -6 to 6
- cotangent: bfloat16 [24576, 768], P(('dp', 'expert')), may hold values from -6 to 6
- expert_ids: int32 [24576, 2], P(('dp', 'expert')), may hold values from 0 to 15, all different within a row
- route_gates: float32 [24576, 2], P(('dp', 'expert')), may hold values from 0.25 to 1
- slot_order: int32 [32, 1536], P(('dp', 'expert')), may hold values from 0 to 1535, each once within a row
- prefix_len: int32 [32], P(('dp', 'expert')), may hold values from 1 to 767
- attention_gain: float32 [768], replicated, may hold values from 0.1 to 1.9
- qkv_weight: bfloat16 [768, 2304], replicated, may hold values from -0.21875 to 0.21875
- output_weight: bfloat16 [768, 768], replicated, may hold values from -0.875 to 0.875
- feedforward_gain: float32 [768], replicated, may hold values from 0.1 to 1.9
- shared_gate: bfloat16 [768, 2048], replicated, may hold values from -0.21875 to 0.21875
- shared_up: bfloat16 [768, 2048], replicated, may hold values from -0.21875 to 0.21875
- shared_down: bfloat16 [2048, 768], replicated, may hold values from -0.125 to 0.125
- expert_gate: bfloat16 [16, 768, 2048], P('expert'), may hold values from -0.21875 to 0.21875
- expert_up: bfloat16 [16, 768, 2048], P('expert'), may hold values from -0.21875 to 0.21875
- expert_down: bfloat16 [16, 2048, 768], P('expert'), may hold values from -0.125 to 0.125
Outputs:
- block_out: bfloat16 [24576, 768], P(('dp', 'expert'))
- tokens_grad: bfloat16 [24576, 768], P(('dp', 'expert'))
- attention_gain_grad: float32 [768], P('dp')
- qkv_weight_grad: float32 [768, 2304], P('dp')
- output_weight_grad: float32 [768, 768], P('dp')
- feedforward_gain_grad: float32 [768], P('dp')
- shared_gate_grad: float32 [768, 2048], P('dp')
- shared_up_grad: float32 [768, 2048], P('dp')
- shared_down_grad: float32 [2048, 768], P('dp')
- expert_gate_grad: float32 [16, 768, 2048], P('expert', 'dp')
- expert_up_grad: float32 [16, 768, 2048], P('expert', 'dp')
- expert_down_grad: float32 [16, 2048, 768], P('expert', 'dp')
The draws below stay inside these ranges and needn't reach their ends.
Inputs may be any that keep to these rules, and one draw needn't show every extreme that they name: `expert_ids`: each token names two different experts; every expert is named by some token. `slot_order`: each row is a permutation of its sequence's pair numbers 2 p + k.
All inputs are finite; a program needn't handle non-finite values.
Results may differ from the reference program's by a relative error of at most 0.023.
Values may be sent and summed in bfloat16 or wider, within the bound.
A program may use at most 320 MiB of HBM per device.

```python
import math
import jax
import jax.numpy as jnp
from jax import lax

D = 768
HEADS = 12
HEAD_DIM = 64
FF = 2048
E = 16
TOK_DEV = 768
CAP = 120
SEQS = 32
TOKENS = 24576


def with_ends(array, own_key, smallest, high):
    shape = array.shape
    spot = [jax.random.randint(jax.random.fold_in(own_key, axis), (), 0, shape[axis]) for axis in range(len(shape))]
    array = array.at[tuple(spot)].set(smallest)
    longest = shape.index(max(shape))
    spot[longest] = (spot[longest] + 1) % shape[longest]
    return array.at[tuple(spot)].set(high)


def raised(entries, rng, source, target, blocks, factor):
    def block_of(dim):
        return (jnp.arange(entries.shape[dim]) // (entries.shape[dim] // blocks)).reshape((-1,) + (1,) * (entries.ndim - 1 - dim))

    one_side = jax.random.permutation(rng, blocks)[block_of(target)]
    far = (block_of(target) + blocks // 2) % blocks
    return jnp.where((block_of(source) == one_side) | (block_of(source) == far), factor * entries, entries)


def block_scale(stream_key, extent, cuts, smallest, high):
    factor_of = 1.0
    for dim, blocks in cuts:
        heights = jax.random.uniform(jax.random.fold_in(jax.random.fold_in(stream_key, 6), dim), (blocks,), jnp.float32, smallest / len(cuts), high / len(cuts))
        factor_of = factor_of * jnp.repeat(jnp.exp(heights), extent[dim] // blocks).reshape((-1,) + (1,) * (len(extent) - 1 - dim))
    return factor_of


def picks_of(rng, rows, amount, top, lift):
    order = jax.random.permutation(jax.random.fold_in(rng, 1), amount)
    favour = order
    for power in range(3):
        favour = favour * favour // amount
    favour = favour * lift // amount
    lots = jax.random.randint(jax.random.fold_in(rng, 2), (rows, amount), 0, 4096) + favour
    fixed_rows = jax.random.permutation(jax.random.fold_in(rng, 3), rows)[jnp.arange(amount) % rows]
    lots = jnp.where(jnp.arange(rows)[:, None] == fixed_rows[None, :], 1 << 14, lots)
    priority = lots * amount + jnp.arange(amount)
    return lax.top_k(priority.astype(jnp.int32), top)[1].astype(jnp.int32)


def scatter_about(rng, shape, spread, bound, pieces=(), held_as=jnp.bfloat16):
    entries = jax.random.normal(rng, shape, jnp.float32) * spread
    if len(pieces) > 0:
        entries = block_scale(rng, shape, pieces, -0.22, 0.18) * entries
    return jnp.clip(entries, min=-bound, max=bound).astype(held_as)


def bell_draw_with(key, shape, scale, reach, split, heavy, held_as=jnp.bfloat16):
    entries = scale * jax.random.normal(key, shape, jnp.float32)
    if split:
        entries = entries * block_scale(key, shape, split, -0.22, 0.18)
    return jnp.clip(raised(entries, jax.random.fold_in(key, 3), *heavy), -reach, reach).astype(held_as)


def setup_inputs(seed: int = 0) -> dict:
    streams_of = jax.random.split(jax.random.key(seed), 17)
    tokens = bell_draw_with(streams_of[0], (TOKENS, D), 1.0, 6.0, ((0, 32),), (0, 1, 32, 2.75))
    cotangent = scatter_about(streams_of[1], (TOKENS, D), 1.0, 6.0, ((0, 32),))
    expert_ids = picks_of(streams_of[2], TOKENS, E, 2, 1024)
    route_gates = jnp.clip(jnp.exp(math.log(1.0) - 1.3862944 * jax.random.uniform(streams_of[3], (TOKENS, 2), jnp.float32) ** block_scale(streams_of[3], (TOKENS, 2), ((0, 32),), -0.2, 0.2)), 0.25, 1.0)
    slot_order = jax.vmap(lambda own: jax.random.permutation(own, 2 * TOK_DEV))(jax.random.split(streams_of[4], SEQS)).reshape((SEQS, 2 * TOK_DEV)).astype(jnp.int32)
    prefix_len = with_ends(jax.random.randint(streams_of[5], (SEQS,), 1, TOK_DEV), jax.random.fold_in(streams_of[5], 1), 1, TOK_DEV - 1).astype(jnp.int32)
    attention_gain = jnp.clip(1.0 + 0.18 * jax.random.normal(streams_of[6], (D,), jnp.float32), 0.1, 1.9)
    qkv_weight = scatter_about(streams_of[7], (D, 3 * D), D ** -0.5, 0.21875)
    output_weight = scatter_about(streams_of[8], (D, D), (D // 16) ** -0.5, 0.875)
    feedforward_gain = jnp.clip(1.0 + 0.18 * jax.random.normal(streams_of[9], (D,), jnp.float32), 0.1, 1.9)
    shared_gate = scatter_about(streams_of[10], (D, FF), D ** -0.5, 0.21875)
    shared_up = scatter_about(streams_of[11], (D, FF), D ** -0.5, 0.21875)
    shared_down = scatter_about(streams_of[12], (FF, D), FF ** -0.5, 0.125)
    expert_gate = scatter_about(streams_of[13], (E, D, FF), D ** -0.5, 0.21875, ((0, 4),))
    expert_up = scatter_about(streams_of[14], (E, D, FF), D ** -0.5, 0.21875, ((0, 4),))
    expert_down = scatter_about(streams_of[15], (E, FF, D), FF ** -0.5, 0.125, ((0, 4),))
    return {"tokens": tokens, "cotangent": cotangent, "expert_ids": expert_ids, "route_gates": route_gates, "slot_order": slot_order, "prefix_len": prefix_len, "attention_gain": attention_gain, "qkv_weight": qkv_weight, "output_weight": output_weight, "feedforward_gain": feedforward_gain, "shared_gate": shared_gate, "shared_up": shared_up, "shared_down": shared_down, "expert_gate": expert_gate, "expert_up": expert_up, "expert_down": expert_down}


epsilon = 1e-06
highest = lax.Precision.HIGHEST

@jax.custom_vjp
def low(v):
    return lax.optimization_barrier(v.astype(jnp.bfloat16)).astype(jnp.float32)

@jax.custom_vjp
def low_back(v):
    return v

def low_keep(v):
    return (low(v), None)

def low_pass(kept, grad):
    return (grad,)

def back_keep(v):
    return (v, None)

def back_low(kept, grad):
    return (low(grad),)
low.defvjp(low_keep, low_pass)
low_back.defvjp(back_keep, back_low)

def rms_norm(values, gain_vector):
    return values * lax.rsqrt(lax.optimization_barrier(jnp.mean(values * values, axis=-1, keepdims=True)) + epsilon) * gain_vector

def rope_tables(length, head_size):
    positions = jnp.arange(length, dtype=jnp.float32)
    frequency = 10000.0 ** (-jnp.arange(head_size // 2, dtype=jnp.float32) * 2.0 / head_size)
    angles = positions[:, None] * frequency[None, :]
    return (jnp.cos(angles)[:, None, :], jnp.sin(angles)[:, None, :])

def rotate(values, cosine, sine_table):
    half_size = values.shape[-1] // 2
    first_half = values[..., :half_size]
    second = values[..., half_size:]
    return jnp.concatenate([first_half * cosine - second * sine_table, second * cosine + first_half * sine_table], axis=-1)

def pick_rows(table_rows, indices):
    return table_rows[indices]

def slot_tables(expert_ids, slot_order):
    seq_count = slot_order.shape[0]
    pair_count = slot_order.shape[1]
    pair_expert = expert_ids.reshape(seq_count, pair_count).astype(jnp.int32)
    sorted_expert = jnp.take_along_axis(pair_expert, slot_order, axis=1)
    onehot = (sorted_expert[:, :, None] == jnp.arange(E, dtype=jnp.int32)[None, None, :]).astype(jnp.int32)
    before = jnp.cumsum(onehot, axis=1) - onehot
    sorted_slot = lax.optimization_barrier(jnp.sum(before * onehot, axis=2)).astype(jnp.int32)
    rowids = jnp.arange(seq_count, dtype=jnp.int32)[:, None]
    position = jnp.zeros((seq_count, pair_count), jnp.int32).at[rowids, slot_order].set(sorted_slot)
    slot_index = jnp.where(position < CAP, pair_expert * CAP + position, E * CAP).astype(jnp.int32)
    pair_ids = jnp.broadcast_to(jnp.arange(pair_count, dtype=jnp.int32)[None, :], (seq_count, pair_count))
    pair_table = jnp.full((seq_count, E * CAP + 1), pair_count, jnp.int32).at[rowids, slot_index].set(pair_ids)
    return (slot_index, pair_table[:, :E * CAP])

def attend(normed, prefix, qkv_matrix, output_matrix):
    length, features = normed.shape
    projected = low_back(jnp.dot(normed, qkv_matrix, precision=highest)).reshape(length, 3, HEADS, HEAD_DIM)
    cosine, sine_table = rope_tables(length, HEAD_DIM)
    queries = low(rotate(projected[:, 0], cosine, sine_table))
    key_rows = low(rotate(projected[:, 1], cosine, sine_table))
    values = low(projected[:, 2])
    scores = low_back(jnp.einsum('qhd,khd->hqk', queries, key_rows, precision=highest) * HEAD_DIM ** (-0.5))
    row_ids = jnp.arange(length)[:, None]
    col_ids = jnp.arange(length)[None, :]
    visible = (col_ids <= row_ids) | (col_ids < prefix)
    soft_probs = jax.nn.softmax(jnp.where(visible[None], scores, -1e+30), axis=-1)
    attended = jnp.einsum('hqk,khd->qhd', low(soft_probs), values, precision=highest).reshape(length, features)
    attended = low(low_back(attended))
    return low_back(jnp.dot(attended, output_matrix, precision=highest))

def expert_apply(packed):
    expert_rows, gate_matrix, up_matrix, down_matrix = packed
    gate_pre = low_back(jnp.dot(expert_rows, gate_matrix, precision=highest))
    up_pre = low_back(jnp.dot(expert_rows, up_matrix, precision=highest))
    hidden = low(jax.nn.silu(gate_pre) * up_pre)
    return low(low_back(jnp.dot(hidden, down_matrix, precision=highest)))

def reference(tokens, cotangent, expert_ids, route_gates, slot_order, prefix_len, attention_gain, qkv_weight, output_weight, feedforward_gain, shared_gate, shared_up, shared_down, expert_gate, expert_up, expert_down):
    seq_count = slot_order.shape[0]
    slot_index, pair_table = slot_tables(expert_ids, slot_order)
    token_table = (pair_table // 2).astype(jnp.int32)
    gates_seq = route_gates.astype(jnp.float32).reshape(seq_count, TOK_DEV, 2)

    def block_forward(tokens_f, attention_f, qkv_f, output_f, feedforward_f, shared_gate_f, shared_up_f, shared_down_f, expert_gate_f, expert_up_f, expert_down_f):
        features = tokens_f.shape[2]
        normed_one = low(rms_norm(tokens_f, attention_f))

        def attend_one(packed):
            return attend(packed[0], packed[1], qkv_f, output_f)
        attn_branch = lax.map(jax.checkpoint(attend_one), (normed_one, prefix_len))
        state = tokens_f + attn_branch
        normed_two = low(rms_norm(state, feedforward_f))
        flat_rows = normed_two.reshape(seq_count * TOK_DEV, features)
        gate_pre = low_back(jnp.dot(flat_rows, shared_gate_f, precision=highest))
        up_pre = low_back(jnp.dot(flat_rows, shared_up_f, precision=highest))
        shared_hidden = low(jax.nn.silu(gate_pre) * up_pre)
        shared_branch = low_back(jnp.dot(shared_hidden, shared_down_f, precision=highest)).reshape(seq_count, TOK_DEV, features)
        padded = jnp.concatenate([normed_two, jnp.zeros((seq_count, 1, features), jnp.float32)], axis=1)
        gathered = jax.vmap(pick_rows)(padded, token_table)
        dispatched = low_back(gathered).reshape(seq_count, E, CAP, features).transpose(1, 0, 2, 3).reshape(E, seq_count * CAP, features)
        results = lax.map(jax.checkpoint(expert_apply), (dispatched, expert_gate_f, expert_up_f, expert_down_f))
        results = results.reshape(E, seq_count, CAP, features).transpose(1, 0, 2, 3).reshape(seq_count, E * CAP, features)
        results = jnp.concatenate([results, jnp.zeros((seq_count, 1, features), jnp.float32)], axis=1)
        picked = jax.vmap(pick_rows)(results, slot_index).reshape(seq_count, TOK_DEV, 2, features)
        mixture = lax.optimization_barrier(jnp.sum(picked * gates_seq[:, :, :, None], axis=2))
        return state + shared_branch + mixture
    block_value, pullback = jax.vjp(block_forward, tokens.astype(jnp.float32).reshape(seq_count, TOK_DEV, D), attention_gain.astype(jnp.float32), qkv_weight.astype(jnp.float32), output_weight.astype(jnp.float32), feedforward_gain.astype(jnp.float32), shared_gate.astype(jnp.float32), shared_up.astype(jnp.float32), shared_down.astype(jnp.float32), expert_gate.astype(jnp.float32), expert_up.astype(jnp.float32), expert_down.astype(jnp.float32))
    gradients = pullback(cotangent.astype(jnp.float32).reshape(seq_count, TOK_DEV, D))
    return (block_value.reshape(seq_count * TOK_DEV, D).astype(jnp.bfloat16), gradients[0].reshape(seq_count * TOK_DEV, D).astype(jnp.bfloat16), gradients[1], gradients[2], gradients[3], gradients[4], gradients[5], gradients[6], gradients[7], gradients[8], gradients[9], gradients[10])
```

```python
import jax
import jax.numpy as jnp
from jax import lax
from jax.experimental import pallas as pl
from jax.experimental.pallas import tpu as pltpu
from jax.sharding import PartitionSpec as P

f32=jnp.float32; bf16=jnp.bfloat16
def nn(a,b): return lax.dot_general(a,b,(((1,),(0,)),((),())),preferred_element_type=f32)
def nt(a,b): return lax.dot_general(a,b,(((1,),(1,)),((),())),preferred_element_type=f32)
def tn(a,b): return lax.dot_general(a,b,(((0,),(0,)),((),())),preferred_element_type=f32)
EPS=1e-6
HD=64; GH=4; GW=GH*HD; QC=256
def lane_head(shape):
    return lax.broadcasted_iota(jnp.int32,shape,1)//HD
def swap_half(x):
    w=x.shape[1]
    first=(lax.broadcasted_iota(jnp.int32,x.shape,1)%HD)<HD//2
    return jnp.where(first,pltpu.roll(x,w-HD//2,1),pltpu.roll(x,HD//2,1))
def wide(t):
    return jnp.concatenate([t,t],axis=1)
def inv_rms(v):
    return lax.rsqrt(jnp.mean(v*v,axis=1,keepdims=True)+EPS)

def attn_fwd(tokens, prefix, again, wqkv, wo, fgain, cosw, sinw):
    T,D=tokens.shape
    ng=D//GW; nq=T//QC
    def kernel(pre,tok,ag,fg,wq,wk,wv,wor,cw,sw,qo,ko,vo,atto,lseo,stateo,ntwoo,normed,bias,q4,k4,vT,OT,acc):
        g=pl.program_id(0)
        @pl.when(g==0)
        def _():
            for c in range(nq):
                r=slice(c*QC,(c+1)*QC)
                x=tok[r,:].astype(f32)
                normed[r,:]=(x*inv_rms(x)*ag[...]).astype(bf16)
                j=lax.broadcasted_iota(jnp.int32,(T,QC),0)
                i=lax.broadcasted_iota(jnp.int32,(T,QC),1)+c*QC
                bias[c]=jnp.where((j<=i)|(j<pre[0]),0.0,-1e30)
        for c in range(nq):
            r=slice(c*QC,(c+1)*QC)
            n=normed[r,:]
            C=wide(cw[r,:]); S=wide(sw[r,:])
            q=nn(n,wq[...]); k=nn(n,wk[...]); v=nn(n,wv[...])
            qb=((q*C+swap_half(q)*S).astype(bf16)).astype(f32)*(HD**-0.5)
            qb=qb.astype(bf16)
            kb=(k*C+swap_half(k)*S).astype(bf16)
            q4[r,:]=qb; qo[r,:]=qb
            k4[r,:]=kb; ko[r,:]=kb
            vo[r,:]=v.astype(bf16)
            vT[:,r]=v.T.astype(bf16)
        lh=lane_head((QC,GW))
        @pl.loop(0,GH)
        def _(h):
            hr=pl.ds(pl.multiple_of(h*HD,HD),HD)
            for c in range(nq):
                r=slice(c*QC,(c+1)*QC)
                qm=jnp.where(lh==h,q4[r,:],jnp.zeros((),bf16))
                st=nt(k4[...],qm)+bias[c]
                m=jnp.max(st,axis=0,keepdims=True)
                p=jnp.exp(st-m)
                l=jnp.sum(p,axis=0,keepdims=True)
                ot=nn(vT[hr,:],p.astype(bf16))
                OT[c,hr,:]=ot*(1.0/l)
                lseo[0,pl.ds(h,1),r]=m+jnp.log(l)
        for c in range(nq):
            r=slice(c*QC,(c+1)*QC)
            a=OT[c].T.astype(bf16)
            atto[r,:]=a
            o=nn(a,wor[...])
            @pl.when(g==0)
            def _(): acc[r,:]=o+tok[r,:].astype(f32)
            @pl.when(g>0)
            def _(): acc[r,:]+=o
        @pl.when(g==ng-1)
        def _():
            for c in range(nq):
                r=slice(c*QC,(c+1)*QC)
                st=acc[r,:]
                stateo[r,:]=st
                ntwoo[r,:]=(st*inv_rms(st)*fg[...]).astype(bf16)
    full=lambda s: pl.BlockSpec(s,lambda g:(0,)*len(s))
    col=lambda off: pl.BlockSpec((D,GW),lambda g,off=off:(0,g+off))
    tcol=pl.BlockSpec((T,GW),lambda g:(0,g))
    return pl.pallas_call(kernel,grid=(ng,),
      in_specs=[pl.BlockSpec(memory_space=pltpu.SMEM),full((T,D)),full((1,D)),full((1,D)),col(0),col(ng),col(2*ng),pl.BlockSpec((GW,D),lambda g:(g,0)),full((T,128)),full((T,128))],
      out_specs=[tcol,tcol,tcol,tcol,pl.BlockSpec((1,8,T),lambda g:(g,0,0)),full((T,D)),full((T,D))],
      out_shape=[jax.ShapeDtypeStruct((T,D),bf16)]*4+[jax.ShapeDtypeStruct((ng,8,T),f32),jax.ShapeDtypeStruct((T,D),f32),jax.ShapeDtypeStruct((T,D),bf16)],
      scratch_shapes=[pltpu.VMEM((T,D),bf16),pltpu.VMEM((nq,T,QC),f32),pltpu.VMEM((T,GW),bf16),pltpu.VMEM((T,GW),bf16),pltpu.VMEM((GW,T),bf16),pltpu.VMEM((nq,GW,QC),f32),pltpu.VMEM((T,D),f32)],
      compiler_params=pltpu.CompilerParams(vmem_limit_bytes=56<<20,dimension_semantics=("arbitrary",)),
      cost_estimate=pl.CostEstimate(flops=2*T*D*4*D+4*T*T*D,bytes_accessed=16<<20,transcendentals=12*T*T),
      name="attn_fwd")(prefix,tokens,again[None],fgain[None],wqkv,wqkv,wqkv,wo,cosw,sinw)

def attn_bwd(sgrad, prefix, tokens, again, wqkv, wo, cosw, sinw, q, k, v, att, lse):
    T,D=tokens.shape
    ng=D//GW; nq=T//QC
    def kernel(pre,sg,tok,ag,wq,wk,wv,wor,cw,sw,qr,kr,vr,attr,lser,tgo,ggo,gq,gk,gv,gwo,normed,normedT,bg,bias,dO,kT,PB,DS,dv,dk,dqT,drow,acc):
        g=pl.program_id(0)
        @pl.when(g==0)
        def _():
            for c in range(nq):
                r=slice(c*QC,(c+1)*QC)
                x=tok[r,:].astype(f32)
                n=x*inv_rms(x)*ag[...]
                normedT[:,r]=n.T.astype(bf16)
                bg[r,:]=sg[r,:].astype(bf16)
                j=lax.broadcasted_iota(jnp.int32,(T,QC),0)
                i=lax.broadcasted_iota(jnp.int32,(T,QC),1)+c*QC
                bias[c]=jnp.where((j<=i)|(j<pre[0]),0.0,-1e30)
        hmask=(lax.broadcasted_iota(jnp.int32,(8,GW),0)==lane_head((8,GW))).astype(f32)
        for c in range(nq):
            r=slice(c*QC,(c+1)*QC)
            d=nt(bg[r,:],wor[...]).astype(bf16)
            dO[r,:]=d
            a=attr[r,:].astype(f32)
            drow[:,r]=lax.dot_general(hmask,d.astype(f32)*a,(((1,),(1,)),((),())),preferred_element_type=f32,precision=lax.Precision.HIGHEST)
            kT[:,r]=kr[r,:].astype(f32).T.astype(bf16)
        gwo[...]=tn(attr[...],bg[...]).astype(bf16)
        dv[...]=jnp.zeros_like(dv); dk[...]=jnp.zeros_like(dk)
        lh=lane_head((QC,GW)); lhT=lane_head((T,GW))
        @pl.loop(0,GH)
        def _(h):
            hr=pl.ds(pl.multiple_of(h*HD,HD),HD)
            zero=jnp.zeros((),bf16)
            for c in range(nq):
                r=slice(c*QC,(c+1)*QC)
                qm=jnp.where(lh==h,qr[r,:],zero)
                dOm=jnp.where(lh==h,dO[r,:],zero)
                st=nt(kr[...],qm)+bias[c]
                p=jnp.exp(st-lser[0,pl.ds(h,1),r])
                PB[:,r]=p.astype(bf16)
                dp=nt(vr[...],dOm)
                DS[:,r]=(p*(dp-drow[pl.ds(h,1),r])).astype(bf16)
            dv[...]+=nn(PB[...],jnp.where(lhT==h,dO[...],zero))
            dk[...]+=nn(DS[...],jnp.where(lhT==h,qr[...],zero))
            dqT[hr,:]=nn(kT[hr,:],DS[...])
        for c in range(nq):
            r=slice(c*QC,(c+1)*QC)
            C=wide(cw[r,:]); S=wide(sw[r,:])
            dq=dqT[:,r].T*(HD**-0.5)
            dq=dq*C-swap_half(dq)*S
            dkk=dk[r,:]
            dkk=dkk*C-swap_half(dkk)*S
            a=dq.astype(bf16); b=dkk.astype(bf16); e=dv[r,:].astype(bf16)
            PB[r,0:GW]=a; PB[r,GW:2*GW]=b; PB[r,2*GW:3*GW]=e
            o=nt(a,wq[...])+nt(b,wk[...])+nt(e,wv[...])
            @pl.when(g==0)
            def _(): acc[r,:]=o
            @pl.when(g>0)
            def _(): acc[r,:]+=o
        gq[...]=nn(normedT[...],PB[:,0:GW]).astype(bf16)
        gk[...]=nn(normedT[...],PB[:,GW:2*GW]).astype(bf16)
        gv[...]=nn(normedT[...],PB[:,2*GW:3*GW]).astype(bf16)
        @pl.when(g==ng-1)
        def _():
            gg=jnp.zeros((1,D),f32)
            for c in range(nq):
                r=slice(c*QC,(c+1)*QC)
                x=tok[r,:].astype(f32)
                inv=inv_rms(x); u=x*inv
                ngd=acc[r,:]
                gg=gg+jnp.sum(ngd*u,axis=0,keepdims=True)
                w=ngd*ag[...]
                tgo[r,:]=(sg[r,:]+inv*(w-u*jnp.mean(w*u,axis=1,keepdims=True))).astype(bf16)
            ggo[...]=jnp.broadcast_to(gg,(8,D))
    full=lambda s: pl.BlockSpec(s,lambda g:(0,)*len(s))
    col=lambda off: pl.BlockSpec((D,GW),lambda g,off=off:(0,g+off))
    tcol=pl.BlockSpec((T,GW),lambda g:(0,g))
    rowb=pl.BlockSpec((GW,D),lambda g:(g,0))
    return pl.pallas_call(kernel,grid=(ng,),
      in_specs=[pl.BlockSpec(memory_space=pltpu.SMEM),full((T,D)),full((T,D)),full((1,D)),col(0),col(ng),col(2*ng),rowb,full((T,128)),full((T,128)),tcol,tcol,tcol,tcol,pl.BlockSpec((1,8,T),lambda g:(g,0,0))],
      out_specs=[full((T,D)),full((8,D)),tcol,tcol,tcol,rowb],
      out_shape=[jax.ShapeDtypeStruct((T,D),bf16),jax.ShapeDtypeStruct((8,D),f32)]+[jax.ShapeDtypeStruct((D,D),bf16)]*4,
      scratch_shapes=[pltpu.VMEM((T,D),bf16),pltpu.VMEM((D,T),bf16),pltpu.VMEM((T,D),bf16),pltpu.VMEM((nq,T,QC),f32),pltpu.VMEM((T,GW),bf16),pltpu.VMEM((GW,T),bf16),
        pltpu.VMEM((T,T),bf16),pltpu.VMEM((T,T),bf16),pltpu.VMEM((T,GW),f32),pltpu.VMEM((T,GW),f32),pltpu.VMEM((GW,T),f32),pltpu.VMEM((8,T),f32),pltpu.VMEM((T,D),f32)],
      compiler_params=pltpu.CompilerParams(vmem_limit_bytes=60<<20,dimension_semantics=("arbitrary",)),
      cost_estimate=pl.CostEstimate(flops=2*T*D*8*D+10*T*T*D,bytes_accessed=24<<20,transcendentals=12*T*T),
      name="attn_bwd")(prefix,sgrad,tokens,again[None],wqkv,wqkv,wqkv,wo,cosw,sinw,q,k,v,att,lse)


def make_ffn(parts, G, L, cap, D, FF, FB, chunk, out_dt):
    R=parts*G*cap
    nf=FF//FB
    def kernel(*refs):
        xs=refs[:parts]; ss=refs[parts:2*parts]
        wg,wu,wd=refs[2*parts:2*parts+3]
        o=2*parts+3
        res=refs[o:o+parts]; dgr=refs[o+parts:o+2*parts]
        gG,gU,gD=refs[o+2*parts:o+2*parts+3]
        X,S,H,GB,UB,AR,AD=refs[o+2*parts+3:]
        f=pl.program_id(1)
        @pl.when(f==0)
        def _():
            for p in range(parts):
                for g in range(G):
                    r=(p*G+g)*cap
                    X[r:r+cap,:]=xs[p][g,0]
                    S[r:r+cap,:]=ss[p][g,0]
        @pl.loop(0,R//chunk)
        def _(i):
            rows=pl.ds(pl.multiple_of(i*chunk,chunk),chunk)
            x=X[rows,:]; s=S[rows,:]
            gate=nn(x,wg[0]); up=nn(x,wu[0]); hg=nt(s,wd[0])
            sig=1.0/(1.0+jnp.exp(-gate))
            sil=gate*sig
            h=(sil*up).astype(bf16)
            gb=(hg*up*(sig*(1.0+gate*(1.0-sig)))).astype(bf16)
            ub=(hg*sil).astype(bf16)
            H[rows,:]=h; GB[rows,:]=gb; UB[rows,:]=ub
            r=nn(h,wd[0]); d=nt(gb,wg[0])+nt(ub,wu[0])
            @pl.when(f==0)
            def _():
                AR[rows,:]=r; AD[rows,:]=d
            @pl.when(f>0)
            def _():
                AR[rows,:]+=r; AD[rows,:]+=d
        gG[0]=tn(X[...],GB[...]).astype(bf16)
        gU[0]=tn(X[...],UB[...]).astype(bf16)
        gD[0]=tn(H[...],S[...]).astype(bf16)
        @pl.when(f==nf-1)
        def _():
            for p in range(parts):
                for g in range(G):
                    r=(p*G+g)*cap
                    res[p][g,0]=AR[r:r+cap,:].astype(out_dt)
                    dgr[p][g,0]=AD[r:r+cap,:].astype(out_dt)
    rowspec=pl.BlockSpec((G,1,cap,D),lambda l,f:(0,l,0,0))
    wspec=pl.BlockSpec((1,D,FB),lambda l,f:(l,0,f))
    wdspec=pl.BlockSpec((1,FB,D),lambda l,f:(l,f,0))
    call=pl.pallas_call(kernel,
      out_shape=[jax.ShapeDtypeStruct((G,L,cap,D),out_dt)]*(2*parts)+[jax.ShapeDtypeStruct((L,D,FF),bf16)]*2+[jax.ShapeDtypeStruct((L,FF,D),bf16)],
      grid=(L,nf),
      in_specs=[rowspec]*(2*parts)+[wspec,wspec,wdspec],
      out_specs=[rowspec]*(2*parts)+[wspec,wspec,wdspec],
      scratch_shapes=[pltpu.VMEM((R,D),bf16)]*2+[pltpu.VMEM((R,FB),bf16)]*3+[pltpu.VMEM((R,D),f32)]*2,
      compiler_params=pltpu.CompilerParams(vmem_limit_bytes=60<<20,dimension_semantics=("arbitrary","arbitrary")),
      cost_estimate=pl.CostEstimate(flops=2*9*R*D*FF*L,bytes_accessed=L*(6*D*FF*2+4*R*D*2),transcendentals=R*FF*L),
      name="ffn")
    return call

E=16; CAP=120

def route(order, expert_ids, gates, cot, core, G, L, parts):
    T,D=cot.shape; P2=2*T
    LP=L//parts; S=G*LP*CAP
    big=E*CAP
    CH=480 if S%480==0 else CAP*4
    def kernel(core_ref,orow,ids,gts,ct,rowo,colo,*rest):
        sgs=rest[:parts]; PT,PG=rest[parts:]
        lane=lax.broadcasted_iota(jnp.int32,(T,128),1)
        e0=ids[:,0:1].astype(f32); e1=ids[:,1:2].astype(f32)
        er=jnp.where(lane==0,e0,jnp.where(lane==1,e1,0.0)).T[0:8,:]
        ecat=jnp.concatenate([er[0:1,:],er[1:2,:]],axis=1)
        eoh=(lax.broadcasted_iota(jnp.int32,(E,P2),0).astype(f32)==ecat)
        eohb=jnp.where(eoh,1.0,0.0).astype(bf16)
        o=orow[...]
        oj=(o&1)*T+(o>>1)
        CB=256
        for c in range(P2//CB):
            jj=lax.broadcasted_iota(jnp.int32,(CB,P2),0)+c*CB
            PT[c*CB:(c+1)*CB,:]=jnp.where(jj==oj,1.0,0.0).astype(bf16)
        soh=nn(eohb,PT[...])
        sohb=soh.astype(bf16)
        tri=jnp.where(lax.broadcasted_iota(jnp.int32,(CB,CB),0)<lax.broadcasted_iota(jnp.int32,(CB,CB),1),1.0,0.0).astype(bf16)
        run=jnp.zeros((E,1),f32)
        pos=[]
        for c in range(P2//CB):
            blk=soh[:,c*CB:(c+1)*CB]
            before=nn(sohb[:,c*CB:(c+1)*CB],tri)+run
            run=run+jnp.sum(blk,axis=1,keepdims=True)
            pos.append(jnp.sum(before*blk,axis=0,keepdims=True))
        posr=jnp.minimum(jnp.concatenate(pos,axis=1),127.0)
        posj=nt(jnp.broadcast_to(posr,(16,P2)).astype(bf16),PT[...])[0:1,:]
        e=ecat.astype(jnp.int32)
        l=lax.rem(e,L); j=lax.div(e,L)
        if parts==2:
            cc=lax.rem(lax.div(l,LP)+core_ref[0],2)
            base=((cc*G+j)*LP+lax.rem(l,LP))*CAP
        else:
            base=e*CAP
        p=posj.astype(jnp.int32)
        slot=jnp.where(p<CAP,base+p,big)
        s0=slot[:,0:T]; s1=slot[:,T:P2]
        r8=lax.broadcasted_iota(jnp.int32,(8,T),0)
        rows=jnp.where(r8==0,s0,jnp.where(r8==1,s1,big))
        rowo[...]=rows
        rep=jnp.concatenate([rows.astype(f32)]*16,axis=0).T
        colo[...]=rep[:,0:8].astype(jnp.int32)
        ctf=ct[...].astype(f32)
        PG[0:T,:]=(gts[:,0:1]*ctf).astype(bf16)
        PG[T:P2,:]=(gts[:,1:2]*ctf).astype(bf16)
        for pi in range(parts):
            @pl.loop(0,S//CH)
            def _(i):
                si=lax.broadcasted_iota(jnp.int32,(CH,T),0)+(i*CH+pi*S)
                d0=jnp.where(si==rowo[0:1,:],1.0,0.0).astype(bf16)
                d1=jnp.where(si==rowo[1:2,:],1.0,0.0).astype(bf16)
                sgs[pi][pl.ds(pl.multiple_of(i*CH,CH),CH),:]=(nn(d0,PG[0:T,:])+nn(d1,PG[T:P2,:])).astype(bf16)
    vm=pl.BlockSpec(memory_space=pltpu.VMEM)
    out=pl.pallas_call(kernel,
      in_specs=[pl.BlockSpec(memory_space=pltpu.SMEM)]+[vm]*4,out_specs=[vm]*(2+parts),
      out_shape=[jax.ShapeDtypeStruct((8,T),jnp.int32),jax.ShapeDtypeStruct((T,8),jnp.int32)]+[jax.ShapeDtypeStruct((S,D),bf16)]*parts,
      scratch_shapes=[pltpu.VMEM((P2,P2),bf16),pltpu.VMEM((P2,D),bf16)],
      compiler_params=pltpu.CompilerParams(vmem_limit_bytes=50<<20),
      cost_estimate=pl.CostEstimate(flops=4*S*parts*T*D+4*P2*P2*16,bytes_accessed=8<<20,transcendentals=0),
      name="route")(core,order,expert_ids,gates,cot)
    return out[0],out[1],out[2:]

def dispatch(rows, x, parts):
    T,D=x.shape; S=E*CAP//parts; CH=480
    def kernel(rowr,xr,*outs):
        for pi in range(parts):
            @pl.loop(0,S//CH)
            def _(i):
                si=lax.broadcasted_iota(jnp.int32,(CH,T),0)+(i*CH+pi*S)
                d=jnp.where((si==rowr[0:1,:])|(si==rowr[1:2,:]),1.0,0.0).astype(bf16)
                outs[pi][pl.ds(pl.multiple_of(i*CH,CH),CH),:]=nn(d,xr[...]).astype(bf16)
    vm=pl.BlockSpec(memory_space=pltpu.VMEM)
    return pl.pallas_call(kernel,in_specs=[vm]*2,out_specs=[vm]*parts,out_shape=[jax.ShapeDtypeStruct((S,D),bf16)]*parts,
      compiler_params=pltpu.CompilerParams(vmem_limit_bytes=50<<20),
      cost_estimate=pl.CostEstimate(flops=2*S*parts*T*D,bytes_accessed=6<<20,transcendentals=0),name="dispatch")(rows,x)

def combine(cols, gates, ret, state, shared):
    parts=len(ret); T,D=state.shape; S=ret[0].shape[0]
    def kernel(colr,g,*refs):
        rs=refs[:parts]; st,sh,out=refs[parts:]
        @pl.loop(0,T//QC)
        def _(i):
            r=pl.ds(pl.multiple_of(i*QC,QC),QC)
            acc=st[r,:]+sh[r,:]
            for k in range(2):
                pk=None
                for pi in range(parts):
                    si=lax.broadcasted_iota(jnp.int32,(QC,S),1)+pi*S
                    d=jnp.where(si==colr[r,k:k+1],1.0,0.0).astype(bf16)
                    q=nn(d,rs[pi][...])
                    pk=q if pk is None else pk+q
                acc=acc+g[r,k:k+1]*pk
            out[r,:]=acc.astype(bf16)
    vm=pl.BlockSpec(memory_space=pltpu.VMEM)
    return pl.pallas_call(kernel,in_specs=[vm]*(4+parts),out_specs=vm,out_shape=jax.ShapeDtypeStruct((T,D),bf16),
      compiler_params=pltpu.CompilerParams(vmem_limit_bytes=50<<20),
      cost_estimate=pl.CostEstimate(flops=4*S*parts*T*D,bytes_accessed=9<<20,transcendentals=0),name="combine")(cols,gates,*ret,state,shared)

def mid_bwd(cols, back, dsh, state, fgain, cot):
    parts=len(back); T,D=state.shape; S=back[0].shape[0]
    def kernel(colr,*refs):
        bs=refs[:parts]; ds,st,fg,ct,sgo,fgo=refs[parts:]
        fgo[...]=jnp.zeros_like(fgo)
        @pl.loop(0,T//QC)
        def _(i):
            r=pl.ds(pl.multiple_of(i*QC,QC),QC)
            n=ds[r,:]
            for pi in range(parts):
                si=lax.broadcasted_iota(jnp.int32,(QC,S),1)+pi*S
                d=jnp.where((si==colr[r,0:1])|(si==colr[r,1:2]),1.0,0.0).astype(bf16)
                n=n+nn(d,bs[pi][...])
            x=st[r,:]; inv=inv_rms(x); u=x*inv
            fgo[...]+=jnp.broadcast_to(jnp.sum(n*u,axis=0,keepdims=True),(8,D))
            w=n*fg[...]
            sgo[r,:]=ct[r,:].astype(f32)+inv*(w-u*jnp.mean(w*u,axis=1,keepdims=True))
    vm=pl.BlockSpec(memory_space=pltpu.VMEM)
    return pl.pallas_call(kernel,in_specs=[vm]*(5+parts),out_specs=[vm]*2,out_shape=[jax.ShapeDtypeStruct((T,D),f32),jax.ShapeDtypeStruct((8,D),f32)],
      compiler_params=pltpu.CompilerParams(vmem_limit_bytes=50<<20),
      cost_estimate=pl.CostEstimate(flops=2*S*parts*T*D,bytes_accessed=12<<20,transcendentals=0),name="mid_bwd")(cols,*back,dsh,state,fgain[None],cot)

HEADS = 12
HEAD_DIM = 64


def rope_wide(length):
    positions = jnp.arange(length, dtype=f32)
    frequency = 10000.0 ** (-jnp.arange(HEAD_DIM // 2, dtype=f32) * 2.0 / HEAD_DIM)
    angles = positions[:, None] * frequency[None, :]
    c = jnp.cos(angles)
    s = jnp.sin(angles)
    return jnp.concatenate([c, c, c, c], axis=1), jnp.concatenate([-s, s, -s, s], axis=1)


def shards(tokens, cotangent, expert_ids, route_gates, slot_order, prefix_len, attention_gain, qkv_weight,
           output_weight, feedforward_gain, shared_gate, shared_up, shared_down, expert_gate, expert_up, expert_down):
    T, D = tokens.shape
    L, _, FF = expert_gate.shape
    G = lax.axis_size("expert")
    DP = lax.axis_size("dp")
    Z = DP // 2
    parts = 2 if L % 2 == 0 else 1
    LP = L // parts
    dpi = lax.axis_index("dp")
    core = lax.rem(dpi, 2)
    swap_perm = [(i, i ^ 1) for i in range(DP)]
    zgroups = [[2 * z + c for z in range(Z)] for c in range(2)]

    def swap(x):
        return lax.ppermute(x, "dp", swap_perm)

    def a2a(x):
        return lax.all_to_all(x, "expert", split_axis=0, concat_axis=0, tiled=True)

    def to_experts(arrs):
        arrs = [a.reshape(G, LP, CAP, D) for a in arrs]
        if parts == 2:
            arrs = [arrs[0], swap(arrs[1])]
        return [a2a(a) for a in arrs]

    def from_experts(arrs):
        arrs = [a2a(a) for a in arrs]
        if parts == 2:
            arrs = [arrs[0], swap(arrs[1])]
        return [a.reshape(G * LP * CAP, D) for a in arrs]

    cosw, sinw = rope_wide(T)
    rows, cols, sgs = route(slot_order, expert_ids, route_gates, cotangent, core[None].astype(jnp.int32), G, L, parts)
    slot_in = to_experts(sgs)
    q, k, v, att, lse, state, ntwo = attn_fwd(tokens, prefix_len, attention_gain, qkv_weight, output_weight,
                                              feedforward_gain, cosw, sinw)
    xs = dispatch(rows, ntwo, parts)
    x_in = to_experts(xs)
    sh = make_ffn(1, 1, 1, T, D, FF, 512, T // 2, f32)(
        ntwo[None, None], cotangent[None, None], shared_gate[None], shared_up[None], shared_down[None])
    shared_branch = sh[0].reshape(T, D)
    dshared = sh[1].reshape(T, D)
    dense_shared = [sh[2][0], sh[3][0], sh[4][0]]

    res, dgr, eg = [], [], []
    one = make_ffn(parts, G, 1, CAP, D, FF, 512, parts * G * CAP // 2, bf16)
    for l in range(LP):
        o = one(*[a[:, l:l + 1] for a in x_in], *[a[:, l:l + 1] for a in slot_in],
                *[lax.dynamic_slice_in_dim(w, (core * LP if parts == 2 else 0) + l, 1, 0)
                  for w in (expert_gate, expert_up, expert_down)])
        res.append(o[:parts])
        dgr.append(o[parts:2 * parts])
        eg.append(o[2 * parts:])
    cat = lambda xs_: jnp.concatenate(xs_, axis=1) if len(xs_) > 1 else xs_[0]
    res = [cat([r[p] for r in res]) for p in range(parts)]
    dgr = [cat([r[p] for r in dgr]) for p in range(parts)]

    egr = []
    for l in range(LP):
        if parts == 2:
            egr.append([lax.psum_scatter(g[0], "dp", scatter_dimension=0, tiled=True, axis_index_groups=zgroups)
                        for g in eg[l]])
        else:
            egr.append([lax.psum_scatter(g[0], "dp", scatter_dimension=0, tiled=True) for g in eg[l]])

    back = from_experts(dgr)
    ret = from_experts(res)
    sgrad, fgg = mid_bwd(cols, back, dshared, state, feedforward_gain, cotangent)
    tokens_grad, agg, gq, gk, gv, gwo = attn_bwd(sgrad, prefix_len, tokens, attention_gain, qkv_weight, output_weight,
                                                 cosw, sinw, q, k, v, att, lse)
    block_out = combine(cols, route_gates, ret, state, shared_branch)

    def dense(g):
        r = g.shape[0] // DP
        h = g.reshape(Z, 2, r, g.shape[1])
        mine = lax.dynamic_index_in_dim(h, core, 1, keepdims=False)
        other = lax.dynamic_index_in_dim(h, 1 - core, 1, keepdims=False)
        s = (mine.astype(f32) + swap(other).astype(f32)).astype(bf16)
        quarter = s.reshape(Z, G, r // G, g.shape[1])
        quarter = jnp.swapaxes(quarter, 0, 1)
        got = lax.all_to_all(quarter, "expert", split_axis=0, concat_axis=0, tiled=True)
        s = jnp.sum(got.astype(f32), axis=0).astype(bf16)
        zs = lax.psum_scatter(s, "dp", scatter_dimension=0, tiled=True, axis_index_groups=zgroups)
        return lax.all_gather(zs[0], "expert", axis=0, tiled=True).astype(f32)

    def dense_simple(g):
        p = lax.psum_scatter(g, "dp", scatter_dimension=0, tiled=True)
        return lax.psum(p, "expert").astype(f32)

    if (qkv_weight.shape[0] // DP) % (8 * G) == 0 and parts == 2:
        dn = dense
    else:
        dn = dense_simple
    dsh = [dn(g) for g in dense_shared]
    dq, dk, dv, dwo = [dn(g) for g in (gq, gk, gv, gwo)]
    gains = lax.psum(jnp.stack([agg[0], fgg[0]]), ("dp", "expert"))
    gs = D // DP
    gains = lax.dynamic_slice_in_dim(gains, dpi * gs, gs, 1)

    def finish(t):
        a = [egr[l][t] for l in range(LP)]
        if parts == 1:
            return jnp.stack(a).astype(f32)
        b = jnp.stack(a)
        h = b.reshape(LP, 2, b.shape[1] // 2, b.shape[2])
        mine = lax.dynamic_index_in_dim(h, core, 1, keepdims=False)
        other = swap(lax.dynamic_index_in_dim(h, 1 - core, 1, keepdims=False))
        return jnp.concatenate([jnp.where(core == 0, mine, other), jnp.where(core == 0, other, mine)], axis=0).astype(f32)

    return (block_out, tokens_grad, gains[0], jnp.concatenate([dq, dk, dv], axis=1), dwo, gains[1],
            dsh[0], dsh[1], dsh[2], finish(0), finish(1), finish(2))


def solution(mesh):
    row = P(("dp", "expert"), None)
    return jax.shard_map(
        shards,
        mesh=mesh,
        in_specs=(row, row, row, row, row, P(("dp", "expert")), P(), P(), P(), P(), P(), P(), P(),
                  P("expert", None, None), P("expert", None, None), P("expert", None, None)),
        out_specs=(row, row, P("dp"), P("dp", None), P("dp", None), P("dp"), P("dp", None), P("dp", None),
                   P("dp", None), P("expert", "dp", None), P("expert", "dp", None), P("expert", "dp", None)),
        check_vma=False,
    )
```

```python
import jax
import jax.numpy as jnp
from jax import lax
from jax.experimental import pallas as pl
from jax.experimental.pallas import tpu as pltpu
from jax.sharding import PartitionSpec as P

f32=jnp.float32; bf16=jnp.bfloat16
def nn(a,b): return lax.dot_general(a,b,(((1,),(0,)),((),())),preferred_element_type=f32)
def nt(a,b): return lax.dot_general(a,b,(((1,),(1,)),((),())),preferred_element_type=f32)
def tn(a,b): return lax.dot_general(a,b,(((0,),(0,)),((),())),preferred_element_type=f32)
EPS=1e-6
E=16; CAP=120
HD=64; GH=4; GW=GH*HD; QC=256
def lane_head(shape):
    return lax.broadcasted_iota(jnp.int32,shape,1)//HD
def swap_half(x):
    w=x.shape[1]
    first=(lax.broadcasted_iota(jnp.int32,x.shape,1)%HD)<HD//2
    return jnp.where(first,pltpu.roll(x,w-HD//2,1),pltpu.roll(x,HD//2,1))
def wide(t):
    return jnp.concatenate([t,t],axis=1)
def inv_rms(v):
    return lax.rsqrt(jnp.mean(v*v,axis=1,keepdims=True)+EPS)

def plane_copies(src, dst, local_sem, send_sem, recv_sem):
    d=lax.axis_index("dp"); e=lax.axis_index("expert")
    c=lax.rem(d,2); z2=d-c; me=c*4+e
    own=pltpu.make_async_copy(src.at[me],dst.at[me],local_sem)
    out=[]
    for kk in range(1,8):
        pc=lax.rem(c+(kk>>2),2)
        pe=xor4(e,kk&3)
        out.append(pltpu.make_async_remote_copy(src_ref=src.at[pc*4+pe],dst_ref=dst.at[me],send_sem=send_sem.at[kk-1],recv_sem=recv_sem.at[kk-1],
            device_id=(z2+pc,pe),device_id_type=pl.DeviceIdType.MESH))
    return own,out

def xor4(e,k):
    lo=lax.rem(e,2); hi=lax.div(e,2)
    if k&1: lo=1-lo
    if k&2: hi=1-hi
    return hi*2+lo

def plane_barrier():
    d=lax.axis_index("dp"); e=lax.axis_index("expert")
    c=lax.rem(d,2); z2=d-c
    b=pltpu.get_barrier_semaphore()
    for kk in range(1,8):
        pl.semaphore_signal(b,inc=1,device_id=(z2+lax.rem(c+(kk>>2),2),xor4(e,kk&3)),device_id_type=pl.DeviceIdType.MESH)
    pl.semaphore_wait(b,7)

def attn_fwd(tokens, prefix, again, wqkv, wo, fgain, cosw, sinw, rows=None, sout=None):
    T,D=tokens.shape
    ng=D//GW; nq=T//QC
    fused=rows is not None
    NS=E*CAP; CH=480
    def kernel(pre,tok,ag,fg,wq,wk,wv,wor,cw,sw,*rest):
        if fused:
            rowr,so,qo,ko,vo,atto,lseo,stateo,ntwoo,xo,sino,normed,bias,q4,k4,vT,OT,acc,lsem,ssem,rsem=rest
        else:
            qo,ko,vo,atto,lseo,stateo,ntwoo,normed,bias,q4,k4,vT,OT,acc=rest
        g=pl.program_id(0)
        @pl.when(g==0)
        def _():
            if fused:
                plane_barrier()
                own,others=plane_copies(so,sino,lsem.at[0],ssem,rsem)
                own.start()
                for cpy in others: cpy.start()
            for c in range(nq):
                r=slice(c*QC,(c+1)*QC)
                x=tok[r,:].astype(f32)
                normed[r,:]=(x*inv_rms(x)*ag[...]).astype(bf16)
                j=lax.broadcasted_iota(jnp.int32,(T,QC),0)
                i=lax.broadcasted_iota(jnp.int32,(T,QC),1)+c*QC
                bias[c]=jnp.where((j<=i)|(j<pre[0]),0.0,-1e30)
        for c in range(nq):
            r=slice(c*QC,(c+1)*QC)
            n=normed[r,:]
            C=wide(cw[r,:]); S=wide(sw[r,:])
            q=nn(n,wq[...]); k=nn(n,wk[...]); v=nn(n,wv[...])
            qb=((q*C+swap_half(q)*S).astype(bf16)).astype(f32)*(HD**-0.5)
            qb=qb.astype(bf16)
            kb=(k*C+swap_half(k)*S).astype(bf16)
            q4[r,:]=qb; qo[r,:]=qb
            k4[r,:]=kb; ko[r,:]=kb
            vo[r,:]=v.astype(bf16)
            vT[:,r]=v.T.astype(bf16)
        lh=lane_head((QC,GW))
        @pl.loop(0,GH)
        def _(h):
            hr=pl.ds(pl.multiple_of(h*HD,HD),HD)
            for c in range(nq):
                r=slice(c*QC,(c+1)*QC)
                qm=jnp.where(lh==h,q4[r,:],jnp.zeros((),bf16))
                st=nt(k4[...],qm)+bias[c]
                m=jnp.max(st,axis=0,keepdims=True)
                p=jnp.exp(st-m)
                l=jnp.sum(p,axis=0,keepdims=True)
                ot=nn(vT[hr,:],p.astype(bf16))
                OT[c,hr,:]=ot*(1.0/l)
                lseo[0,pl.ds(h,1),r]=m+jnp.log(l)
        for c in range(nq):
            r=slice(c*QC,(c+1)*QC)
            a=OT[c].T.astype(bf16)
            atto[r,:]=a
            o=nn(a,wor[...])
            @pl.when(g==0)
            def _(): acc[r,:]=o+tok[r,:].astype(f32)
            @pl.when(g>0)
            def _(): acc[r,:]+=o
        @pl.when(g==ng-1)
        def _():
            for c in range(nq):
                r=slice(c*QC,(c+1)*QC)
                st=acc[r,:]
                stateo[r,:]=st
                ntwoo[r,:]=(st*inv_rms(st)*fg[...]).astype(bf16)
            if fused:
                for i in range(NS//CH):
                    si=lax.broadcasted_iota(jnp.int32,(CH,T),0)+i*CH
                    d=jnp.where((si==rowr[0:1,:])|(si==rowr[1:2,:]),1.0,0.0).astype(bf16)
                    xo[i*CH:(i+1)*CH,:]=nn(d,ntwoo[...]).astype(bf16)
                own,others=plane_copies(so,sino,lsem.at[0],ssem,rsem)
                own.wait()
                for cpy in others: cpy.wait()
    full=lambda s: pl.BlockSpec(s,lambda g:(0,)*len(s))
    col=lambda off: pl.BlockSpec((D,GW),lambda g,off=off:(0,g+off))
    tcol=pl.BlockSpec((T,GW),lambda g:(0,g))
    return pl.pallas_call(kernel,grid=(ng,),
      in_specs=[pl.BlockSpec(memory_space=pltpu.SMEM),full((T,D)),full((1,D)),full((1,D)),col(0),col(ng),col(2*ng),pl.BlockSpec((GW,D),lambda g:(g,0)),full((T,128)),full((T,128))]+([full((8,T)),pl.BlockSpec(memory_space=pl.ANY)] if fused else []),
      out_specs=[tcol,tcol,tcol,tcol,pl.BlockSpec((1,8,T),lambda g:(g,0,0)),full((T,D)),full((T,D))]+([full((NS,D)),pl.BlockSpec(memory_space=pl.ANY)] if fused else []),
      out_shape=[jax.ShapeDtypeStruct((T,D),bf16)]*4+[jax.ShapeDtypeStruct((ng,8,T),f32),jax.ShapeDtypeStruct((T,D),f32),jax.ShapeDtypeStruct((T,D),bf16)]+([jax.ShapeDtypeStruct((NS,D),bf16),jax.ShapeDtypeStruct((8,2*CAP,D),bf16)] if fused else []),
      scratch_shapes=[pltpu.VMEM((T,D),bf16),pltpu.VMEM((nq,T,QC),f32),pltpu.VMEM((T,GW),bf16),pltpu.VMEM((T,GW),bf16),pltpu.VMEM((GW,T),bf16),pltpu.VMEM((nq,GW,QC),f32),pltpu.VMEM((T,D),f32)]+([pltpu.SemaphoreType.DMA((1,)),pltpu.SemaphoreType.DMA((7,)),pltpu.SemaphoreType.DMA((7,))] if fused else []),
      compiler_params=pltpu.CompilerParams(vmem_limit_bytes=56<<20,dimension_semantics=("arbitrary",),**(dict(collective_id=0,has_side_effects=True) if fused else {})),
      cost_estimate=pl.CostEstimate(flops=2*T*D*4*D+4*T*T*D,bytes_accessed=16<<20,transcendentals=12*T*T),
      name="attn_fwd")(prefix,tokens,again[None],fgain[None],wqkv,wqkv,wqkv,wo,cosw,sinw,*([rows,sout] if fused else []))

def attn_bwd(sgrad, prefix, tokens, again, wqkv, wo, cosw, sinw, q, k, v, att, lse, place=None):
    T,D=tokens.shape
    ng=D//GW; nq=T//QC
    fast=place is not None
    if not fast:
        place=jnp.zeros((8,),jnp.int32)
    SH=D//8
    def kernel(pre,plc,sg,tok,ag,wq,wk,wv,wor,cw,sw,qr,kr,vr,attr,lser,tgo,ggo,*rest):
        if fast:
            at0,at1,normed,normedT,bg,bias,dO,kT,PB,DS,dv,dk,dqT,drow,acc,GS=rest
        else:
            gq,gk,gv,gwo,normed,normedT,bg,bias,dO,kT,PB,DS,dv,dk,dqT,drow,acc=rest
        g=pl.program_id(0)
        @pl.when(g==0)
        def _():
            for c in range(nq):
                r=slice(c*QC,(c+1)*QC)
                x=tok[r,:].astype(f32)
                n=x*inv_rms(x)*ag[...]
                normedT[:,r]=n.T.astype(bf16)
                bg[r,:]=sg[r,:].astype(bf16)
                j=lax.broadcasted_iota(jnp.int32,(T,QC),0)
                i=lax.broadcasted_iota(jnp.int32,(T,QC),1)+c*QC
                bias[c]=jnp.where((j<=i)|(j<pre[0]),0.0,-1e30)
        hmask=(lax.broadcasted_iota(jnp.int32,(8,GW),0)==lane_head((8,GW))).astype(f32)
        for c in range(nq):
            r=slice(c*QC,(c+1)*QC)
            d=nt(bg[r,:],wor[...]).astype(bf16)
            dO[r,:]=d
            a=attr[r,:].astype(f32)
            drow[:,r]=lax.dot_general(hmask,d.astype(f32)*a,(((1,),(1,)),((),())),preferred_element_type=f32,precision=lax.Precision.HIGHEST)
            kT[:,r]=kr[r,:].astype(f32).T.astype(bf16)
        gwv=tn(attr[...],bg[...]).astype(bf16)
        if fast:
            GS[3,pl.ds(pl.multiple_of(g*GW,GW),GW),:]=gwv
        else:
            gwo[...]=gwv
        dv[...]=jnp.zeros_like(dv); dk[...]=jnp.zeros_like(dk)
        lh=lane_head((QC,GW)); lhT=lane_head((T,GW))
        @pl.loop(0,GH)
        def _(h):
            hr=pl.ds(pl.multiple_of(h*HD,HD),HD)
            zero=jnp.zeros((),bf16)
            for c in range(nq):
                r=slice(c*QC,(c+1)*QC)
                qm=jnp.where(lh==h,qr[r,:],zero)
                dOm=jnp.where(lh==h,dO[r,:],zero)
                st=nt(kr[...],qm)+bias[c]
                p=jnp.exp(st-lser[0,pl.ds(h,1),r])
                PB[:,r]=p.astype(bf16)
                dp=nt(vr[...],dOm)
                DS[:,r]=(p*(dp-drow[pl.ds(h,1),r])).astype(bf16)
            dv[...]+=nn(PB[...],jnp.where(lhT==h,dO[...],zero))
            dk[...]+=nn(DS[...],jnp.where(lhT==h,qr[...],zero))
            dqT[hr,:]=nn(kT[hr,:],DS[...])
        for c in range(nq):
            r=slice(c*QC,(c+1)*QC)
            C=wide(cw[r,:]); S=wide(sw[r,:])
            dq=dqT[:,r].T*(HD**-0.5)
            dq=dq*C-swap_half(dq)*S
            dkk=dk[r,:]
            dkk=dkk*C-swap_half(dkk)*S
            a=dq.astype(bf16); b=dkk.astype(bf16); e=dv[r,:].astype(bf16)
            PB[r,0:GW]=a; PB[r,GW:2*GW]=b; PB[r,2*GW:3*GW]=e
            o=nt(a,wq[...])+nt(b,wk[...])+nt(e,wv[...])
            @pl.when(g==0)
            def _(): acc[r,:]=o
            @pl.when(g>0)
            def _(): acc[r,:]+=o
        for i in range(3):
            gval=nn(normedT[...],PB[:,i*GW:(i+1)*GW]).astype(bf16)
            if fast:
                GS[i,:,pl.ds(pl.multiple_of(g*GW,GW),GW)]=gval
            else:
                (gq,gk,gv)[i][...]=gval
        @pl.when(g==ng-1)
        def _():
            gg=jnp.zeros((1,D),f32)
            for c in range(nq):
                r=slice(c*QC,(c+1)*QC)
                x=tok[r,:].astype(f32)
                inv=inv_rms(x); u=x*inv
                ngd=acc[r,:]
                gg=gg+jnp.sum(ngd*u,axis=0,keepdims=True)
                w=ngd*ag[...]
                tgo[r,:]=(sg[r,:]+inv*(w-u*jnp.mean(w*u,axis=1,keepdims=True))).astype(bf16)
            ggo[...]=jnp.broadcast_to(gg,(8,D))
            if fast:
                for i in range(4):
                    for zr in range(4):
                        for cp in range(2):
                            src=pl.multiple_of(2*SH*plc[1+zr]+SH*((plc[0]+cp)&1),SH)
                            (at0,at1)[cp][i,zr]=GS[i,pl.ds(src,SH),:]
    full=lambda s: pl.BlockSpec(s,lambda g:(0,)*len(s))
    col=lambda off: pl.BlockSpec((D,GW),lambda g,off=off:(0,g+off))
    tcol=pl.BlockSpec((T,GW),lambda g:(0,g))
    if fast:
        outs=[full((4,4,SH,D))]*2
        oshape=[jax.ShapeDtypeStruct((4,4,SH,D),bf16)]*2
        extra=[pltpu.VMEM((4,D,D),bf16)]
    else:
        outs=[tcol,tcol,tcol,pl.BlockSpec((GW,D),lambda g:(g,0))]
        oshape=[jax.ShapeDtypeStruct((D,D),bf16)]*4
        extra=[]
    rowb=pl.BlockSpec((GW,D),lambda g:(g,0))
    return pl.pallas_call(kernel,grid=(ng,),
      in_specs=[pl.BlockSpec(memory_space=pltpu.SMEM)]*2+[full((T,D)),full((T,D)),full((1,D)),col(0),col(ng),col(2*ng),rowb,full((T,128)),full((T,128)),tcol,tcol,tcol,tcol,pl.BlockSpec((1,8,T),lambda g:(g,0,0))],
      out_specs=[full((T,D)),full((8,D))]+outs,
      out_shape=[jax.ShapeDtypeStruct((T,D),bf16),jax.ShapeDtypeStruct((8,D),f32)]+oshape,
      scratch_shapes=[pltpu.VMEM((T,D),bf16),pltpu.VMEM((D,T),bf16),pltpu.VMEM((T,D),bf16),pltpu.VMEM((nq,T,QC),f32),pltpu.VMEM((T,GW),bf16),pltpu.VMEM((GW,T),bf16),
        pltpu.VMEM((T,T),bf16),pltpu.VMEM((T,T),bf16),pltpu.VMEM((T,GW),f32),pltpu.VMEM((T,GW),f32),pltpu.VMEM((GW,T),f32),pltpu.VMEM((8,T),f32),pltpu.VMEM((T,D),f32)]+extra,
      compiler_params=pltpu.CompilerParams(vmem_limit_bytes=60<<20,dimension_semantics=("arbitrary",)),
      cost_estimate=pl.CostEstimate(flops=2*T*D*8*D+10*T*T*D,bytes_accessed=24<<20,transcendentals=12*T*T),
      name="attn_bwd")(prefix,place,sgrad,tokens,again[None],wqkv,wqkv,wqkv,wo,cosw,sinw,q,k,v,att,lse)


def make_ffn(parts, G, L, cap, D, FF, FB, chunk, out_dt):
    R=parts*G*cap
    nf=FF//FB
    def kernel(*refs):
        xs=refs[:parts]; ss=refs[parts:2*parts]
        wg,wu,wd=refs[2*parts:2*parts+3]
        o=2*parts+3
        res=refs[o:o+parts]; dgr=refs[o+parts:o+2*parts]
        gG,gU,gD=refs[o+2*parts:o+2*parts+3]
        X,S,H,GB,UB,AR,AD=refs[o+2*parts+3:]
        f=pl.program_id(1)
        @pl.when(f==0)
        def _():
            for p in range(parts):
                for g in range(G):
                    r=(p*G+g)*cap
                    X[r:r+cap,:]=xs[p][g,0]
                    S[r:r+cap,:]=ss[p][g,0]
        @pl.loop(0,R//chunk)
        def _(i):
            rows=pl.ds(pl.multiple_of(i*chunk,chunk),chunk)
            x=X[rows,:]; s=S[rows,:]
            gate=nn(x,wg[0]); up=nn(x,wu[0]); hg=nt(s,wd[0])
            sig=1.0/(1.0+jnp.exp(-gate))
            sil=gate*sig
            h=(sil*up).astype(bf16)
            gb=(hg*up*(sig*(1.0+gate*(1.0-sig)))).astype(bf16)
            ub=(hg*sil).astype(bf16)
            H[rows,:]=h; GB[rows,:]=gb; UB[rows,:]=ub
            r=nn(h,wd[0]); d=nt(gb,wg[0])+nt(ub,wu[0])
            @pl.when(f==0)
            def _():
                AR[rows,:]=r; AD[rows,:]=d
            @pl.when(f>0)
            def _():
                AR[rows,:]+=r; AD[rows,:]+=d
        gG[0]=tn(X[...],GB[...]).astype(bf16)
        gU[0]=tn(X[...],UB[...]).astype(bf16)
        gD[0]=tn(H[...],S[...]).astype(bf16)
        @pl.when(f==nf-1)
        def _():
            for p in range(parts):
                for g in range(G):
                    r=(p*G+g)*cap
                    res[p][g,0]=AR[r:r+cap,:].astype(out_dt)
                    dgr[p][g,0]=AD[r:r+cap,:].astype(out_dt)
    rowspec=pl.BlockSpec((G,1,cap,D),lambda l,f:(0,l,0,0))
    wspec=pl.BlockSpec((1,D,FB),lambda l,f:(l,0,f))
    wdspec=pl.BlockSpec((1,FB,D),lambda l,f:(l,f,0))
    call=pl.pallas_call(kernel,
      out_shape=[jax.ShapeDtypeStruct((G,L,cap,D),out_dt)]*(2*parts)+[jax.ShapeDtypeStruct((L,D,FF),bf16)]*2+[jax.ShapeDtypeStruct((L,FF,D),bf16)],
      grid=(L,nf),
      in_specs=[rowspec]*(2*parts)+[wspec,wspec,wdspec],
      out_specs=[rowspec]*(2*parts)+[wspec,wspec,wdspec],
      scratch_shapes=[pltpu.VMEM((R,D),bf16)]*2+[pltpu.VMEM((R,FB),bf16)]*3+[pltpu.VMEM((R,D),f32)]*2,
      compiler_params=pltpu.CompilerParams(vmem_limit_bytes=60<<20,dimension_semantics=("arbitrary","arbitrary")),
      cost_estimate=pl.CostEstimate(flops=2*9*R*D*FF*L,bytes_accessed=L*(6*D*FF*2+4*R*D*2),transcendentals=R*FF*L),
      name="ffn")
    return call


def ffn_rows(x,s,wg,wu,wd,H,GB,UB,rows):
    gate=nn(x,wg); up=nn(x,wu); hg=nt(s,wd)
    sig=1.0/(1.0+jnp.exp(-gate))
    sil=gate*sig
    h=(sil*up).astype(bf16)
    gb=(hg*up*(sig*(1.0+gate*(1.0-sig)))).astype(bf16)
    ub=(hg*sil).astype(bf16)
    H[rows,:]=h; GB[rows,:]=gb; UB[rows,:]=ub
    return nn(h,wd),nt(gb,wg)+nt(ub,wu)

def expert_ffn(place, xs, ss, wg, wu, wd, half, prev=(), FB=512, chunk=480):
    n=len(xs); RG,D=xs[0].shape; FF=wg.shape[2]; R=n*RG; nf=2; HB=nf*FB
    SR=D//4; np_=len(prev)
    def kernel(plc,*refs):
        xr=refs[:n]; sr=refs[n:2*n]; wgr,wur,wdr=refs[2*n:2*n+3]; o=2*n+3
        pv=refs[o:o+np_]; o+=np_
        res=refs[o:o+n]; dgr=refs[o+n:o+2*n]; o+=2*n
        gf,gi,go,dw,tok,XT,XN,H,GB,UB,AR,AD=refs[o:]
        f=pl.program_id(0)
        tok[...]=jnp.zeros_like(tok)
        @pl.when(f==0)
        def _():
            for a in range(n):
                for b in range(RG//chunk):
                    XN[...]=xr[a][b*chunk:(b+1)*chunk,:].astype(f32).T.astype(bf16)
                    for q in range(4):
                        XT[a*(RG//chunk)+b,q*SR:(q+1)*SR,:]=XN[pl.ds(pl.multiple_of(plc[1+q]*SR,SR),SR),:]
        for a in range(n):
            @pl.loop(0,RG//chunk)
            def _(i):
                src=pl.ds(pl.multiple_of(i*chunk,chunk),chunk)
                rows=pl.ds(pl.multiple_of(a*RG+i*chunk,chunk),chunk)
                r,d=ffn_rows(xr[a][src,:],sr[a][src,:],wgr[0],wur[0],wdr[0],H,GB,UB,rows)
                @pl.when(f==0)
                def _():
                    if np_:
                        AR[rows,:]=r+pv[a][src,:].astype(f32); AD[rows,:]=d+pv[n+a][src,:].astype(f32)
                    else:
                        AR[rows,:]=r; AD[rows,:]=d
                @pl.when(f>0)
                def _():
                    res[a][src,:]=(AR[rows,:]+r).astype(bf16); dgr[a][src,:]=(AD[rows,:]+d).astype(bf16)
        for t,Y in enumerate((GB,UB)):
            gv=None
            for b in range(R//chunk):
                p=nn(XT[b],Y[b*chunk:(b+1)*chunk,:])
                gv=p if gv is None else gv+p
            gv=gv.astype(bf16)
            cols=pl.ds(pl.multiple_of(t*HB+f*FB,FB),FB)
            gf[:,cols]=gv[0:2*SR]; gi[:,cols]=gv[2*SR:3*SR]; go[:,cols]=gv[3*SR:4*SR]
        dv=None
        for a in range(n):
            t=tn(H[a*RG:(a+1)*RG,:],sr[a][...])
            dv=t if dv is None else dv+t
        dw[...]=dv.astype(bf16)
    one=pl.Buffered(1)
    rowspec=pl.BlockSpec((RG,D),lambda f,p:(0,0),pipeline_mode=one)
    wspec=pl.BlockSpec((1,D,FB),lambda f,p:(p[5],0,f+nf*half))
    wdspec=pl.BlockSpec((1,FB,D),lambda f,p:(p[5],f+nf*half,0))
    full=lambda r,c: pl.BlockSpec((r,c),lambda f,p:(0,0),pipeline_mode=one)
    out=pl.pallas_call(kernel,
      grid_spec=pltpu.PrefetchScalarGridSpec(num_scalar_prefetch=1,grid=(nf,),
        in_specs=[rowspec]*(2*n)+[wspec,wspec,wdspec]+[rowspec]*np_,
        out_specs=[rowspec]*(2*n)+[full(2*SR,2*HB),full(SR,2*HB),full(SR,2*HB),pl.BlockSpec((FB,D),lambda f,p:((1-f) if half else f,0)),full(8,128)],
        scratch_shapes=[pltpu.VMEM((R//chunk,D,chunk),bf16),pltpu.VMEM((D,chunk),bf16)]+[pltpu.VMEM((R,FB),bf16)]*3+[pltpu.VMEM((R,D),f32)]*2),
      out_shape=[jax.ShapeDtypeStruct((RG,D),bf16)]*(2*n)+[jax.ShapeDtypeStruct((2*SR,2*HB),bf16)]+[jax.ShapeDtypeStruct((SR,2*HB),bf16)]*2+[jax.ShapeDtypeStruct((HB,D),bf16),jax.ShapeDtypeStruct((8,128),f32)],
      compiler_params=pltpu.CompilerParams(vmem_limit_bytes=62<<20,dimension_semantics=("arbitrary",)),
      cost_estimate=pl.CostEstimate(flops=9*R*D*FF,bytes_accessed=3*D*FF*2+4*R*D*2,transcendentals=R*FF//2),
      name=f"expert_ffn{n}_{half}")(place,*xs,*ss,wg,wu,wd,*prev)
    return out[:2*n],out[2*n:2*n+3],out[2*n+3],out[2*n+4]

def shared_ffn(place, x, s, wg, wu, wd, FB=512):
    T,D=x.shape; FF=wg.shape[1]; nf=FF//FB; chunk=T//2
    SG=D//8; SD=FB//8
    NR=2*SG*(FB//128)+SD*(D//128)
    def kernel(plc,xr,sr,wgr,wur,wdr,res,dgr,o0,o1,tok,XT,H,GB,UB,VG,VD):
        f=pl.program_id(0)
        tok[...]=jnp.zeros_like(tok)
        @pl.when(f==0)
        def _():
            for b in range(2):
                XT[:,b*chunk:(b+1)*chunk]=xr[b*chunk:(b+1)*chunk,:].astype(f32).T.astype(bf16)
        @pl.loop(0,T//chunk)
        def _(i):
            rows=pl.ds(pl.multiple_of(i*chunk,chunk),chunk)
            r,d=ffn_rows(xr[rows,:],sr[rows,:],wgr[...],wur[...],wdr[...],H,GB,UB,rows)
            @pl.when(f==0)
            def _():
                res[rows,:]=r; dgr[rows,:]=d
            @pl.when(f>0)
            def _():
                res[rows,:]+=r; dgr[rows,:]+=d
        for t,Y in enumerate((GB,UB)):
            VG[...]=nn(XT[...],Y[...]).astype(bf16)
            for zr in range(4):
                for cp in range(2):
                    src=pl.ds(pl.multiple_of(2*SG*plc[1+zr]+SG*((plc[0]+cp)&1),SG),SG)
                    for b in range(FB//128):
                        off=(t*(FB//128)+b)*SG
                        (o0,o1)[cp][f,zr,off:off+SG,:]=VG[src,b*128:(b+1)*128]
        VD[...]=tn(H[...],sr[...]).astype(bf16)
        zr=jnp.where(plc[1]==f,0,jnp.where(plc[2]==f,1,jnp.where(plc[3]==f,2,3)))
        for cp in range(2):
            for e in range(4):
                src=pl.ds(pl.multiple_of(((plc[0]+cp)&1)*4*SD+e*SD,SD),SD)
                for b in range(D//128):
                    off=2*SG*(FB//128)+b*SD
                    (o0,o1)[cp][e,zr,off:off+SD,:]=VD[src,b*128:(b+1)*128]
    full=lambda sh: pl.BlockSpec(sh,lambda f:(0,)*len(sh))
    return pl.pallas_call(kernel,grid=(nf,),
      in_specs=[pl.BlockSpec(memory_space=pltpu.SMEM),full((T,D)),full((T,D)),pl.BlockSpec((D,FB),lambda f:(0,f)),pl.BlockSpec((D,FB),lambda f:(0,f)),pl.BlockSpec((FB,D),lambda f:(f,0))],
      out_specs=[full((T,D)),full((T,D)),full((4,4,NR,128)),full((4,4,NR,128)),full((8,128))],
      out_shape=[jax.ShapeDtypeStruct((T,D),f32)]*2+[jax.ShapeDtypeStruct((4,4,NR,128),bf16)]*2+[jax.ShapeDtypeStruct((8,128),f32)],
      scratch_shapes=[pltpu.VMEM((D,T),bf16)]+[pltpu.VMEM((T,FB),bf16)]*3+[pltpu.VMEM((D,FB),bf16),pltpu.VMEM((FB,D),bf16)],
      compiler_params=pltpu.CompilerParams(vmem_limit_bytes=62<<20,dimension_semantics=("arbitrary",)),
      cost_estimate=pl.CostEstimate(flops=2*9*T*D*FF,bytes_accessed=6*D*FF*2+8*T*D*2,transcendentals=T*FF),
      name="shared_ffn")(place,x,s,wg,wu,wd)


def route(order, expert_ids, gates, cot, core, G, L, parts, plane=False):
    T,D=cot.shape; P2=2*T
    LP=L//parts; S=G*LP*CAP
    big=E*CAP
    CH=480 if S%480==0 else CAP*4
    def kernel(core_ref,orow,ids,gts,ct,rowo,colo,*rest):
        sgs=rest[:parts]; PT,PG=rest[parts:]
        lane=lax.broadcasted_iota(jnp.int32,(T,128),1)
        e0=ids[:,0:1].astype(f32); e1=ids[:,1:2].astype(f32)
        er=jnp.where(lane==0,e0,jnp.where(lane==1,e1,0.0)).T[0:8,:]
        ecat=jnp.concatenate([er[0:1,:],er[1:2,:]],axis=1)
        eoh=(lax.broadcasted_iota(jnp.int32,(E,P2),0).astype(f32)==ecat)
        eohb=jnp.where(eoh,1.0,0.0).astype(bf16)
        o=orow[...]
        oj=(o&1)*T+(o>>1)
        CB=256
        for c in range(P2//CB):
            jj=lax.broadcasted_iota(jnp.int32,(CB,P2),0)+c*CB
            PT[c*CB:(c+1)*CB,:]=jnp.where(jj==oj,1.0,0.0).astype(bf16)
        soh=nn(eohb,PT[...])
        sohb=soh.astype(bf16)
        tri=jnp.where(lax.broadcasted_iota(jnp.int32,(CB,CB),0)<lax.broadcasted_iota(jnp.int32,(CB,CB),1),1.0,0.0).astype(bf16)
        run=jnp.zeros((E,1),f32)
        pos=[]
        for c in range(P2//CB):
            blk=soh[:,c*CB:(c+1)*CB]
            before=nn(sohb[:,c*CB:(c+1)*CB],tri)+run
            run=run+jnp.sum(blk,axis=1,keepdims=True)
            pos.append(jnp.sum(before*blk,axis=0,keepdims=True))
        posr=jnp.minimum(jnp.concatenate(pos,axis=1),127.0)
        posj=nt(jnp.broadcast_to(posr,(16,P2)).astype(bf16),PT[...])[0:1,:]
        e=ecat.astype(jnp.int32)
        l=lax.rem(e,L); j=lax.div(e,L)
        if plane:
            base=((lax.div(l,2)*G+j)*2+lax.rem(l,2))*CAP
        elif parts==2:
            cc=lax.rem(lax.div(l,LP)+core_ref[0],2)
            base=((cc*G+j)*LP+lax.rem(l,LP))*CAP
        else:
            base=e*CAP
        p=posj.astype(jnp.int32)
        slot=jnp.where(p<CAP,base+p,big)
        s0=slot[:,0:T]; s1=slot[:,T:P2]
        r8=lax.broadcasted_iota(jnp.int32,(8,T),0)
        rows=jnp.where(r8==0,s0,jnp.where(r8==1,s1,big))
        rowo[...]=rows
        rep=jnp.concatenate([rows.astype(f32)]*16,axis=0).T
        colo[...]=rep[:,0:8].astype(jnp.int32)
        ctf=ct[...].astype(f32)
        PG[0:T,:]=(gts[:,0:1]*ctf).astype(bf16)
        PG[T:P2,:]=(gts[:,1:2]*ctf).astype(bf16)
        for pi in range(parts):
            @pl.loop(0,S//CH)
            def _(i):
                si=lax.broadcasted_iota(jnp.int32,(CH,T),0)+(i*CH+pi*S)
                d0=jnp.where(si==rowo[0:1,:],1.0,0.0).astype(bf16)
                d1=jnp.where(si==rowo[1:2,:],1.0,0.0).astype(bf16)
                sgs[pi][pl.ds(pl.multiple_of(i*CH,CH),CH),:]=(nn(d0,PG[0:T,:])+nn(d1,PG[T:P2,:])).astype(bf16)
    vm=pl.BlockSpec(memory_space=pltpu.VMEM)
    out=pl.pallas_call(kernel,
      in_specs=[pl.BlockSpec(memory_space=pltpu.SMEM)]+[vm]*4,out_specs=[vm]*(2+parts),
      out_shape=[jax.ShapeDtypeStruct((8,T),jnp.int32),jax.ShapeDtypeStruct((T,8),jnp.int32)]+[jax.ShapeDtypeStruct((S,D),bf16)]*parts,
      scratch_shapes=[pltpu.VMEM((P2,P2),bf16),pltpu.VMEM((P2,D),bf16)],
      compiler_params=pltpu.CompilerParams(vmem_limit_bytes=50<<20),
      cost_estimate=pl.CostEstimate(flops=4*S*parts*T*D+4*P2*P2*16,bytes_accessed=8<<20,transcendentals=0),
      name="route")(core,order,expert_ids,gates,cot)
    return out[0],out[1],out[2:]

def dispatch(rows, x, parts):
    T,D=x.shape; S=E*CAP//parts; CH=480
    def kernel(rowr,xr,*outs):
        for pi in range(parts):
            @pl.loop(0,S//CH)
            def _(i):
                si=lax.broadcasted_iota(jnp.int32,(CH,T),0)+(i*CH+pi*S)
                d=jnp.where((si==rowr[0:1,:])|(si==rowr[1:2,:]),1.0,0.0).astype(bf16)
                outs[pi][pl.ds(pl.multiple_of(i*CH,CH),CH),:]=nn(d,xr[...]).astype(bf16)
    vm=pl.BlockSpec(memory_space=pltpu.VMEM)
    return pl.pallas_call(kernel,in_specs=[vm]*2,out_specs=[vm]*parts,out_shape=[jax.ShapeDtypeStruct((S,D),bf16)]*parts,
      compiler_params=pltpu.CompilerParams(vmem_limit_bytes=50<<20),
      cost_estimate=pl.CostEstimate(flops=2*S*parts*T*D,bytes_accessed=6<<20,transcendentals=0),name="dispatch")(rows,x)

def combine(cols, gates, ret, state, shared):
    parts=len(ret); T,D=state.shape; S=ret[0].shape[0]
    def kernel(colr,g,*refs):
        rs=refs[:parts]; st,sh,out=refs[parts:]
        @pl.loop(0,T//QC)
        def _(i):
            r=pl.ds(pl.multiple_of(i*QC,QC),QC)
            acc=st[r,:]+sh[r,:]
            for k in range(2):
                pk=None
                for pi in range(parts):
                    si=lax.broadcasted_iota(jnp.int32,(QC,S),1)+pi*S
                    d=jnp.where(si==colr[r,k:k+1],1.0,0.0).astype(bf16)
                    q=nn(d,rs[pi][...])
                    pk=q if pk is None else pk+q
                acc=acc+g[r,k:k+1]*pk
            out[r,:]=acc.astype(bf16)
    vm=pl.BlockSpec(memory_space=pltpu.VMEM)
    return pl.pallas_call(kernel,in_specs=[vm]*(4+parts),out_specs=vm,out_shape=jax.ShapeDtypeStruct((T,D),bf16),
      compiler_params=pltpu.CompilerParams(vmem_limit_bytes=50<<20),
      cost_estimate=pl.CostEstimate(flops=4*S*parts*T*D,bytes_accessed=9<<20,transcendentals=0),name="combine")(cols,gates,*ret,state,shared)

def mid_bwd(cols, back, dsh, state, fgain, cot):
    parts=len(back); T,D=state.shape; S=back[0].shape[0]
    def kernel(colr,*refs):
        bs=refs[:parts]; ds,st,fg,ct,sgo,fgo=refs[parts:]
        fgo[...]=jnp.zeros_like(fgo)
        @pl.loop(0,T//QC)
        def _(i):
            r=pl.ds(pl.multiple_of(i*QC,QC),QC)
            n=ds[r,:]
            for pi in range(parts):
                si=lax.broadcasted_iota(jnp.int32,(QC,S),1)+pi*S
                d=jnp.where((si==colr[r,0:1])|(si==colr[r,1:2]),1.0,0.0).astype(bf16)
                n=n+nn(d,bs[pi][...])
            x=st[r,:]; inv=inv_rms(x); u=x*inv
            fgo[...]+=jnp.broadcast_to(jnp.sum(n*u,axis=0,keepdims=True),(8,D))
            w=n*fg[...]
            sgo[r,:]=ct[r,:].astype(f32)+inv*(w-u*jnp.mean(w*u,axis=1,keepdims=True))
    vm=pl.BlockSpec(memory_space=pltpu.VMEM)
    return pl.pallas_call(kernel,in_specs=[vm]*(5+parts),out_specs=[vm]*2,out_shape=[jax.ShapeDtypeStruct((T,D),f32),jax.ShapeDtypeStruct((8,D),f32)],
      compiler_params=pltpu.CompilerParams(vmem_limit_bytes=50<<20),
      cost_estimate=pl.CostEstimate(flops=2*S*parts*T*D,bytes_accessed=12<<20,transcendentals=0),name="mid_bwd")(cols,*back,dsh,state,fgain[None],cot)

HEADS = 12
HEAD_DIM = 64


def rope_wide(length):
    positions = jnp.arange(length, dtype=f32)
    frequency = 10000.0 ** (-jnp.arange(HEAD_DIM // 2, dtype=f32) * 2.0 / HEAD_DIM)
    angles = positions[:, None] * frequency[None, :]
    c = jnp.cos(angles)
    s = jnp.sin(angles)
    return jnp.concatenate([c, c, c, c], axis=1), jnp.concatenate([-s, s, -s, s], axis=1)


def shards_any(tokens, cotangent, expert_ids, route_gates, slot_order, prefix_len, attention_gain, qkv_weight,
           output_weight, feedforward_gain, shared_gate, shared_up, shared_down, expert_gate, expert_up, expert_down):
    T, D = tokens.shape
    L, _, FF = expert_gate.shape
    G = lax.axis_size("expert")
    DP = lax.axis_size("dp")
    Z = DP // 2
    parts = 2 if L % 2 == 0 else 1
    LP = L // parts
    dpi = lax.axis_index("dp")
    core = lax.rem(dpi, 2)
    swap_perm = [(i, i ^ 1) for i in range(DP)]
    zgroups = [[2 * z + c for z in range(Z)] for c in range(2)]

    def swap(x):
        return lax.ppermute(x, "dp", swap_perm)

    def a2a(x):
        return lax.all_to_all(x, "expert", split_axis=0, concat_axis=0, tiled=True)

    def to_experts(arrs):
        arrs = [a.reshape(G, LP, CAP, D) for a in arrs]
        if parts == 2:
            arrs = [arrs[0], swap(arrs[1])]
        return [a2a(a) for a in arrs]

    def from_experts(arrs):
        arrs = [a2a(a) for a in arrs]
        if parts == 2:
            arrs = [arrs[0], swap(arrs[1])]
        return [a.reshape(G * LP * CAP, D) for a in arrs]

    cosw, sinw = rope_wide(T)
    rows, cols, sgs = route(slot_order, expert_ids, route_gates, cotangent, core[None].astype(jnp.int32), G, L, parts)
    slot_in = to_experts(sgs)
    q, k, v, att, lse, state, ntwo = attn_fwd(tokens, prefix_len, attention_gain, qkv_weight, output_weight,
                                              feedforward_gain, cosw, sinw)
    xs = dispatch(rows, ntwo, parts)
    x_in = to_experts(xs)
    sh = make_ffn(1, 1, 1, T, D, FF, 512, T // 2, f32)(
        ntwo[None, None], cotangent[None, None], shared_gate[None], shared_up[None], shared_down[None])
    shared_branch = sh[0].reshape(T, D)
    dshared = sh[1].reshape(T, D)
    dense_shared = [sh[2][0], sh[3][0], sh[4][0]]

    res, dgr, eg = [], [], []
    one = make_ffn(parts, G, 1, CAP, D, FF, 512, parts * G * CAP // 2, bf16)
    for l in range(LP):
        o = one(*[a[:, l:l + 1] for a in x_in], *[a[:, l:l + 1] for a in slot_in],
                *[lax.dynamic_slice_in_dim(w, (core * LP if parts == 2 else 0) + l, 1, 0)
                  for w in (expert_gate, expert_up, expert_down)])
        res.append(o[:parts])
        dgr.append(o[parts:2 * parts])
        eg.append(o[2 * parts:])
    cat = lambda xs_: jnp.concatenate(xs_, axis=1) if len(xs_) > 1 else xs_[0]
    res = [cat([r[p] for r in res]) for p in range(parts)]
    dgr = [cat([r[p] for r in dgr]) for p in range(parts)]

    egr = []
    for l in range(LP):
        if parts == 2:
            egr.append([lax.psum_scatter(g[0], "dp", scatter_dimension=0, tiled=True, axis_index_groups=zgroups)
                        for g in eg[l]])
        else:
            egr.append([lax.psum_scatter(g[0], "dp", scatter_dimension=0, tiled=True) for g in eg[l]])

    back = from_experts(dgr)
    ret = from_experts(res)
    sgrad, fgg = mid_bwd(cols, back, dshared, state, feedforward_gain, cotangent)
    tokens_grad, agg, gq, gk, gv, gwo = attn_bwd(sgrad, prefix_len, tokens, attention_gain, qkv_weight, output_weight,
                                                 cosw, sinw, q, k, v, att, lse)
    block_out = combine(cols, route_gates, ret, state, shared_branch)

    def dense(g):
        r = g.shape[0] // DP
        h = g.reshape(Z, 2, r, g.shape[1])
        mine = lax.dynamic_index_in_dim(h, core, 1, keepdims=False)
        other = lax.dynamic_index_in_dim(h, 1 - core, 1, keepdims=False)
        s = (mine.astype(f32) + swap(other).astype(f32)).astype(bf16)
        quarter = s.reshape(Z, G, r // G, g.shape[1])
        quarter = jnp.swapaxes(quarter, 0, 1)
        got = lax.all_to_all(quarter, "expert", split_axis=0, concat_axis=0, tiled=True)
        s = jnp.sum(got.astype(f32), axis=0).astype(bf16)
        zs = lax.psum_scatter(s, "dp", scatter_dimension=0, tiled=True, axis_index_groups=zgroups)
        return lax.all_gather(zs[0], "expert", axis=0, tiled=True).astype(f32)

    def dense_simple(g):
        p = lax.psum_scatter(g, "dp", scatter_dimension=0, tiled=True)
        return lax.psum(p, "expert").astype(f32)

    if (qkv_weight.shape[0] // DP) % (8 * G) == 0 and parts == 2:
        dn = dense
    else:
        dn = dense_simple
    dsh = [dn(g) for g in dense_shared]
    dq, dk, dv, dwo = [dn(g) for g in (gq, gk, gv, gwo)]
    gains = lax.psum(jnp.stack([agg[0], fgg[0]]), ("dp", "expert"))
    gs = D // DP
    gains = lax.dynamic_slice_in_dim(gains, dpi * gs, gs, 1)

    def finish(t):
        a = [egr[l][t] for l in range(LP)]
        if parts == 1:
            return jnp.stack(a).astype(f32)
        b = jnp.stack(a)
        h = b.reshape(LP, 2, b.shape[1] // 2, b.shape[2])
        mine = lax.dynamic_index_in_dim(h, core, 1, keepdims=False)
        other = swap(lax.dynamic_index_in_dim(h, 1 - core, 1, keepdims=False))
        return jnp.concatenate([jnp.where(core == 0, mine, other), jnp.where(core == 0, other, mine)], axis=0).astype(f32)

    return (block_out, tokens_grad, gains[0], jnp.concatenate([dq, dk, dv], axis=1), dwo, gains[1],
            dsh[0], dsh[1], dsh[2], finish(0), finish(1), finish(2))


def shards_fast(tokens, cotangent, expert_ids, route_gates, slot_order, prefix_len, attention_gain, qkv_weight,
                output_weight, feedforward_gain, shared_gate, shared_up, shared_down, expert_gate, expert_up, expert_down):
    T, D = tokens.shape
    FF = expert_gate.shape[2]
    i32 = jnp.int32
    dpi = lax.axis_index("dp").astype(i32)
    ei = lax.axis_index("expert").astype(i32)
    core = lax.rem(dpi, 2)
    zi = lax.div(dpi, 2)
    outer = (zi == 0) | (zi == 3)
    low = zi < 2
    pick = lambda a, b: jnp.where(low, a, b).astype(i32)
    place = jnp.stack([core, pick(3, 0), pick(2, 1), pick(1, 2), pick(0, 3)])
    place_a = jnp.concatenate([place, (2 * core)[None]])
    place_b = jnp.concatenate([place, (2 * core + 1)[None]])
    plane = [[(2 * z + c) * 4 + e for c in range(2) for e in range(4)] for z in range(4)]

    def swap(x):
        return lax.ppermute(x, "dp", [(i, i ^ 1) for i in range(8)])

    def inward(x):
        return lax.ppermute(x, "dp", [(0, 2), (1, 3), (6, 4), (7, 5)])

    def outward(x):
        return lax.ppermute(x, "dp", [(2, 0), (3, 1), (4, 6), (5, 7)])

    def across(x):
        return lax.ppermute(x, "dp", [(2, 4), (3, 5), (4, 2), (5, 3)])

    def a2a(x):
        return lax.all_to_all(x.reshape(8, 2 * CAP, D), ("dp", "expert"), split_axis=0, concat_axis=0,
                              axis_index_groups=plane, tiled=True)

    def add(*xs):
        t = xs[0].astype(f32)
        for x in xs[1:]:
            t = t + x.astype(f32)
        return t.astype(bf16)

    def tie(x, token):
        return lax.optimization_barrier((x, token))[0]

    def zdense(far, inner, out):
        r = far.shape[0] // 2
        m = across(add(far, inward(far)))
        rin = inward(inner)
        ro = outward(add(out, m[:r]))
        return jnp.where(outer, add(out, ro), add(inner, m[r:], rin))

    cosw, sinw = rope_wide(T)
    rows, cols, (s_out,) = route(slot_order, expert_ids, route_gates, cotangent, core[None], 4, 4, 1, True)
    q, k, v, att, lse, state, ntwo, x_out, sab = attn_fwd(tokens, prefix_len, attention_gain, qkv_weight, output_weight,
                                                     feedforward_gain, cosw, sinw, rows,
                                                          s_out.reshape(8, 2 * CAP, D))
    xab = a2a(x_out)
    half_rows = lambda y, l: y.reshape(8, 2, CAP, D)[:, l].reshape(8 * CAP, D)
    sa, sb = half_rows(sab, 0), half_rows(sab, 1)
    sx = inward(sa)
    shared_branch, dshared, sh0, sh1, t_sh = shared_ffn(place, ntwo, cotangent, shared_gate, shared_up, shared_down)
    xa, xb = half_rows(xab, 0), half_rows(xab, 1)
    xx = inward(xa)
    ws = (expert_gate, expert_up, expert_down)
    p0, gb0, wb0, t_b0 = expert_ffn(tie(place_b, t_sh), [xb], [sb], *ws, 0)
    (rb, db), gb1, wb1, t_b1 = expert_ffn(place_b, [xb], [sb], *ws, 1, p0)
    rf0 = inward(gb0[0])
    p0, ga0, wa0, t_a0 = expert_ffn(tie(place_a, t_b1), [xa, xx], [sa, sx], *ws, 0)
    bs0 = add(gb0[0], tie(rf0, t_a0))
    (ra, rx, da, dx), ga1, wa1, t_a1 = expert_ffn(tie(place_a, bs0), [xa, xx], [sa, sx], *ws, 1, p0)

    far_w = lambda w0, w1: jnp.where(low, w1, w0)
    near_w = lambda w0, w1: jnp.where(low, w0, w1)
    hw = FF // 4
    bfar = [gb0[0], gb1[0], far_w(wb0, wb1)]
    bin_ = [gb0[1], gb1[1], near_w(wb0[hw:], wb1[hw:])]
    bout = [gb0[2], gb1[2], near_w(wb0[:hw], wb1[:hw])]
    afar = [ga0[0], ga1[0], far_w(wa0, wa1)]
    ain = [ga0[1], ga1[1], near_w(wa0[hw:], wa1[hw:])]
    aout = [ga0[2], ga1[2], near_w(wa0[:hw], wa1[:hw])]

    rf = [tie(inward(x), t_a1) for x in bfar[1:]]
    bm = [across(bs0)] + [across(add(x, r)) for x, r in zip(bfar[1:], rf)]
    am = [across(x) for x in afar]
    rin = [inward(x) for x in bin_]

    def both(b, a):
        return jnp.concatenate([b.reshape(8, 1, CAP, D), a.reshape(8, 1, CAP, D)], axis=1)

    da = jnp.where(outer, outward(dx), da)
    dback = a2a(both(da, db)).reshape(16 * CAP, D)
    sgrad, fgg = mid_bwd(cols, [dback], dshared, state, feedforward_gain, cotangent)
    tokens_grad, agg, at0, at1 = attn_bwd(sgrad, prefix_len, tokens, attention_gain, qkv_weight, output_weight,
                                          cosw, sinw, q, k, v, att, lse, place)
    ra = jnp.where(outer, outward(rx), ra)
    rback = a2a(both(ra, rb)).reshape(16 * CAP, D)
    block_out = combine(tie(cols, agg), route_gates, [rback], state, shared_branch)

    def last(m, inner, out, r=None):
        h = m.shape[0] // 2
        m = tie(m, agg)
        ro = outward(add(out, m[:h]))
        if r is None:
            return jnp.where(outer, ro, add(inner, m[h:]))
        return jnp.where(outer, add(out, ro), add(inner, m[h:], r))

    eb = [last(m, i, o, r) for m, i, o, r in zip(bm, bin_, bout, rin)]
    ea = [last(m, i, o) for m, i, o in zip(am, ain, aout)]

    def dense(mine, other):
        s = add(mine, swap(other))
        s = lax.all_to_all(s, "expert", split_axis=0, concat_axis=0, tiled=True)
        s = add(s[0], s[1], s[2], s[3])
        s = zdense(s[0:2].reshape(-1, s.shape[2]), s[2], s[3])
        p = [s] + [lax.ppermute(s, "expert", [(e, e ^ kk) for e in range(4)]) for kk in (1, 2, 3)]
        odd = lax.rem(ei, 2) == 1
        p = [jnp.where(odd, p[kk ^ 1], p[kk]) for kk in range(4)]
        return [jnp.where(ei >= 2, p[kk ^ 2], p[kk]) for kk in range(4)]

    shd = jnp.stack(dense(sh0, sh1))
    nb = FF // 4 // 128
    sg = D // 8
    sd = FF // 32
    cut = nb * sg

    def columns(x):
        return x.reshape(4, nb, sg, 128).transpose(2, 0, 1, 3).reshape(sg, FF).astype(f32)

    d_gate = columns(shd[:, :cut])
    d_up = columns(shd[:, cut:2 * cut])
    d_down = shd[:, 2 * cut:].reshape(4, D // 128, sd, 128).transpose(0, 2, 1, 3).reshape(4 * sd, D).astype(f32)
    dq, dk, dv, dwo = dense(at0, at1)

    gains = jnp.concatenate([agg[0:1], fgg[0:1]], axis=0)
    for kk in (1, 2, 4):
        gains = gains + lax.ppermute(gains, "dp", [(i, i ^ kk) for i in range(8)])
    for kk in (1, 2):
        gains = gains + lax.ppermute(gains, "expert", [(i, i ^ kk) for i in range(4)])
    gains = lax.dynamic_slice_in_dim(gains, dpi * sg, sg, 1)

    def finish(a, b):
        h = jnp.stack([a, b]).reshape(2, 2, a.shape[0] // 2, a.shape[1])
        mine = lax.dynamic_index_in_dim(h, core, 1, keepdims=False)
        other = swap(lax.dynamic_index_in_dim(h, 1 - core, 1, keepdims=False))
        return jnp.concatenate([jnp.where(core == 0, mine, other), jnp.where(core == 0, other, mine)], axis=0).astype(f32)

    full = [finish(a, b) for a, b in zip(ea, eb)]
    hc = FF // 2
    outs = [jnp.concatenate([full[0][:, :, :hc], full[1][:, :, :hc]], axis=2),
            jnp.concatenate([full[0][:, :, hc:], full[1][:, :, hc:]], axis=2), full[2]]
    return (block_out, tokens_grad, gains[0], jnp.concatenate([dq, dk, dv], axis=1).astype(f32), dwo.astype(f32), gains[1],
            d_gate, d_up, d_down, *outs)


def shards(*args):
    local = args[13].shape[0]
    if lax.axis_size("dp") == 8 and lax.axis_size("expert") == 4 and local == 4:
        return shards_fast(*args)
    return shards_any(*args)


def solution(mesh):
    row = P(("dp", "expert"), None)
    return jax.shard_map(
        shards,
        mesh=mesh,
        in_specs=(row, row, row, row, row, P(("dp", "expert")), P(), P(), P(), P(), P(), P(), P(),
                  P("expert", None, None), P("expert", None, None), P("expert", None, None)),
        out_specs=(row, row, P("dp"), P("dp", None), P("dp", None), P("dp"), P("dp", None), P("dp", None),
                   P("dp", None), P("expert", "dp", None), P("expert", "dp", None), P("expert", "dp", None)),
        check_vma=False,
    )
```

```python
import jax
import jax.numpy as jnp
from jax import lax
from jax.experimental import pallas as pl
from jax.experimental.pallas import tpu as pltpu
from jax.sharding import PartitionSpec as P


MESH_ID = pl.DeviceIdType.MESH

def xor4(e,k):
    lo=lax.rem(e,2); hi=lax.div(e,2)
    if k&1: lo=1-lo
    if k&2: hi=1-hi
    return hi*2+lo

def spot():
    d=lax.axis_index("dp"); e=lax.axis_index("expert")
    c=lax.rem(d,2)
    return c,lax.div(d,2),e

def shard_of(q):
    c,z,e=spot()
    return jnp.where(z<2,3-q,q).astype(jnp.int32)

def peer(z,kk):
    c,_,e=spot()
    return (2*z+lax.rem(c+(kk>>2),2),xor4(e,kk&3))

def block_of(kk):
    c,_,e=spot()
    return lax.rem(c+(kk>>2),2)*4+xor4(e,kk&3)

def plane_sems(n):
    return [pltpu.SemaphoreType.DMA((n,)),pltpu.SemaphoreType.DMA((n,7)),pltpu.SemaphoreType.DMA((n,7))]

def plane_barrier():
    c,z,e=spot()
    b=pltpu.get_barrier_semaphore()
    for kk in range(1,8):
        pl.semaphore_signal(b,inc=1,device_id=peer(z,kk),device_id_type=MESH_ID)
    pl.semaphore_wait(b,7)

def plane_copies(pairs, sems):
    local,send,recv=sems
    c,z,e=spot()
    me=block_of(0)
    out=[]
    for i,(src,dst) in enumerate(pairs):
        out.append(pltpu.make_async_copy(src.at[me],dst.at[me],local.at[i]))
        for kk in range(1,8):
            out.append(pltpu.make_async_remote_copy(src_ref=src.at[block_of(kk)],dst_ref=dst.at[me],send_sem=send.at[i,kk-1],
                recv_sem=recv.at[i,kk-1],device_id=peer(z,kk),device_id_type=MESH_ID))
    return out

def home_sems():
    return [pltpu.SemaphoreType.DMA((1,)),pltpu.SemaphoreType.DMA((8,)),pltpu.SemaphoreType.DMA((8,)),pltpu.SemaphoreType.DMA((8,))]

def home_barrier():
    c,z,e=spot()
    b=pltpu.get_barrier_semaphore()
    inner=(z==1)|(z==2)
    zo=jnp.where(z<2,0,3); zi=jnp.where(z<2,1,2)
    @pl.when(inner)
    def _():
        for kk in range(8):
            pl.semaphore_signal(b,inc=1,device_id=peer(zo,kk),device_id_type=MESH_ID)
            if kk:
                pl.semaphore_signal(b,inc=1,device_id=peer(z,kk),device_id_type=MESH_ID)
        pl.semaphore_wait(b,15)
    @pl.when(jnp.logical_not(inner))
    def _():
        for kk in range(8):
            pl.semaphore_signal(b,inc=1,device_id=peer(zi,kk),device_id_type=MESH_ID)
        pl.semaphore_wait(b,8)

def home_run(own, ext, dst, sems, start):
    local,send,send2,recv=sems
    c,z,e=spot()
    inner=(z==1)|(z==2)
    zo=jnp.where(z<2,0,3); zi=jnp.where(z<2,1,2)
    me=block_of(0)
    def remote(src,kk,zz,s):
        return pltpu.make_async_remote_copy(src_ref=src.at[block_of(kk)],dst_ref=dst.at[me],send_sem=s.at[kk],recv_sem=recv.at[kk],
            device_id=peer(zz,kk),device_id_type=MESH_ID)
    @pl.when(inner)
    def _():
        lc=pltpu.make_async_copy(own.at[me],dst.at[me],local.at[0])
        if start:
            lc.start()
            for kk in range(8):
                remote(ext,kk,zo,send2).start()
                if kk: remote(own,kk,z,send).start()
        else:
            lc.wait()
            for kk in range(8):
                remote(ext,kk,zo,send2).wait_send()
                if kk:
                    remote(own,kk,z,send).wait()
    if not start:
        @pl.when(jnp.logical_not(inner))
        def _():
            for kk in range(8):
                remote(own,kk,zi,send).wait_recv()


def addb(*refs):
    t=refs[0].astype(f32)
    for r in refs[1:]: t=t+r.astype(f32)
    return t.astype(bf16)

class Tail:
    KIND=("g","g","g","g","w","w")
    L2=(1,0,1,0,0,1)
    H=(0,0,1,1,0,0)
    def __init__(self, arrays, T, D, FF):
        self.names=list(arrays); self.arrays=[arrays[n] for n in self.names]
        self.T,self.D,self.FF=T,D,FF
        SG=D//8; self.SG=SG; self.SD=FF//32
        R2=2*SG; self.R2=R2; HW=FF//4
        self.gs=(R2,FF); self.ws=(HW,D)
        self.NR=arrays["msh"].shape[1]
        an=pl.BlockSpec(memory_space=pl.ANY)
        S=jax.ShapeDtypeStruct
        outs={"gate":S((4,SG,FF),f32),"up":S((4,SG,FF),f32),"down":S((4,FF//8,D),f32),
              "dgate":S((SG,FF),f32),"dup":S((SG,FF),f32),"ddown":S((FF//8,D),f32),
              "dqkv":S((SG,3*D),f32),"dwo":S((SG,D),f32),"gains":S((8,D),f32),
              "ra":S((8,CAP,D),bf16)}
        for i in range(2,6):
            outs[f"m{i}"]=S((2*R2,FF) if self.KIND[i]=="g" else (2*HW,D),bf16)
        for i in range(6):
            outs[f"ro{i}"]=S(self.shape(i),bf16)
        self.onames=list(outs); self.oshape=[outs[n] for n in self.onames]
        self.in_specs=[an]*len(self.names); self.out_specs=[an]*len(self.onames)
        V=pltpu.VMEM; DM=pltpu.SemaphoreType.DMA
        scr={"ga":V((3,)+self.gs,bf16),"wa":V((3,)+self.ws,bf16),
             "gto":V((2,)+self.gs,bf16),"wto":V((2,)+self.ws,bf16),
             "gfin":V((2,)+self.gs,bf16),"wfin":V((2,)+self.ws,bf16),
             "gfs":V((2,SG,FF),f32),"wfs":V((2,FF//8,D),f32),
             "gsw":V((4,SG,FF),bf16),"wsw":V((2,FF//8,D),bf16),
             "atr":V((4,4,SG,D),bf16),"sv":V((4,4,SG,D),bf16),"xr":V((3,4,SG,D),bf16),
             "za":V((4,SG,D),bf16),"zb":V((4,self.NR,128),bf16),
             "gn":V((8,8,D),f32),
             "s_x":DM((4,)),"r_x":DM((4,)),"s_o":DM((6,)),"r_o":DM((6,)),"s_w":DM((6,)),"r_w":DM((6,)),
             "ld":DM((3,)),"st":DM((8,)),"s_at":DM((16,)),"r_at":DM((16,)),"s_xr":DM((3,)),"r_xr":DM((3,)),
             "s_gn":DM((7,)),"r_gn":DM((7,)),"st2":DM((4,))}
        for nm,sh in (("a",(SG,D)),("b",(self.NR,128))):
            scr.update({"zr"+nm:V((2,)+sh,bf16),"zs"+nm:V((2,)+sh,bf16),"zm"+nm:V((2,)+sh,bf16),"zi"+nm:V(sh,bf16),"zt"+nm:V(sh,bf16),
                "zo"+nm:V(sh,bf16),"fi"+nm:V(sh,bf16),"ag"+nm:V((3,)+sh,bf16),
                "s_z"+nm:DM((4,)),"r_z"+nm:DM((4,)),"s_ag"+nm:DM((3,)),"r_ag"+nm:DM((3,))})
        scr.update({"oa":V((2,SG,D),f32),"og":V((2,SG,FF//4),f32),"od":V((self.SD,D),f32)})
        self.snames=list(scr)+[f"home{i}" for i in range(4)]
        self.scratch=[scr[n] for n in scr]+home_sems()
    def shape(self,i): return self.gs if self.KIND[i]=="g" else self.ws
    def bind(self,ins,outs,scr):
        self.r=dict(zip(self.names,ins)); self.r.update(zip(self.onames,outs)); self.r.update(zip(self.snames,scr))
        c,z,e=spot()
        self.c,self.z,self.e=c,z,e
        self.inner=(z==1)|(z==2); self.outer=jnp.logical_not(self.inner); self.low=z<2
        self.zo=jnp.where(z<2,0,3); self.zi=jnp.where(z<2,1,2); self.zx=3-z
        self.home=[self.r[f"home{i}"] for i in range(4)]
    def rcopy(self,src,dst,s,r,dev):
        return pltpu.make_async_remote_copy(src_ref=src,dst_ref=dst,send_sem=s,recv_sem=r,device_id=dev,device_id_type=MESH_ID)
    def barrier(self):
        b=pltpu.get_barrier_semaphore()
        def sig(dev): pl.semaphore_signal(b,inc=1,device_id=dev,device_id_type=MESH_ID)
        for kk in range(1,8): sig(peer(self.z,kk))
        @pl.when(self.inner)
        def _():
            for kk in range(8): sig(peer(self.zo,kk))
            sig(peer(self.zx,0))
            pl.semaphore_wait(b,16)
        @pl.when(self.outer)
        def _():
            for kk in range(8): sig(peer(self.zi,kk))
            pl.semaphore_wait(b,15)
    def far_src(self,i):
        return self.r[f"far{i}"]
    def across(self,i):
        return self.rcopy(self.far_src(i),self.r[f"m{i}"],self.r["s_x"].at[i-2],self.r["r_x"].at[i-2],peer(self.zx,0))
    def start(self):
        self.barrier()
        home_run(self.r["hown"],self.r["hext"],self.r["ra"],self.home,True)
        ld=pltpu.make_async_copy(self.r["msh"],self.r["zb"],self.r["st2"].at[0])
        ld.start(); ld.wait()
        self.z_inward("b")
        @pl.when(self.inner)
        def _():
            for i in (2,3): self.across(i).start()
    def load(self,pairs):
        cs=[pltpu.make_async_copy(s,d,self.r["ld"].at[k]) for k,(s,d) in enumerate(pairs)]
        for c in cs: c.start()
        for c in cs: c.wait()
    def near(self,i,which):
        if self.KIND[i]=="g":
            return self.r[f"n{which}{i}"]
        n=self.ws[0]
        return self.r[f"nw{i}"].at[pl.ds(0 if which=="o" else n,n)]
    def piece(self,i):
        g=self.KIND[i]=="g"; k="g" if g else "w"
        buf=self.r[k+"a"]; to=self.r[k+"to"]; fin=self.r[k+"fin"]; fs=self.r[k+"fs"]; sw=self.r[k+"sw"]
        n=self.shape(i)[0]; hn=n//2; b=self.L2[i]==1
        idx=i if g else i-4
        slot=idx%2
        o=self.rcopy(to.at[slot],self.r[f"ro{i}"],self.r["s_o"].at[i],self.r["r_o"].at[i],peer(self.zo,0))
        @pl.when(self.inner)
        def _():
            if i>=2: self.across(i).wait()
            m=self.r[f"m{i}"]
            self.load([(m.at[pl.ds(0,n)],buf.at[0]),(self.near(i,"o"),buf.at[1])])
            if g and idx>=2:
                self.rcopy(to.at[slot],self.r[f"ro{i-2}"],self.r["s_o"].at[i-2],self.r["r_o"].at[i-2],peer(self.zo,0)).wait_send()
            to[slot]=addb(buf[0],buf[1])
            o.start()
            self.load([(m.at[pl.ds(n,n)],buf.at[0]),(self.near(i,"i"),buf.at[1])]+([(self.r[f"rin{i}"],buf.at[2])] if b else []))
        @pl.when(self.outer)
        def _():
            self.rcopy(to.at[slot],self.r[f"ro{i}"],self.r["s_o"].at[i],self.r["r_o"].at[i],peer(self.zi,0)).wait_recv()
            self.load([(self.r[f"ro{i}"],buf.at[0])]+([(self.near(i,"o"),buf.at[1])] if b else []))
        if g and idx>=2:
            self.swap(i-2,fin,sw).wait_send()
        @pl.when(self.inner)
        def _():
            fin[slot]=addb(buf[0],buf[1],buf[2]) if b else addb(buf[0],buf[1])
        @pl.when(self.outer)
        def _():
            fin[slot]=addb(buf[0],buf[1]) if b else buf[0]
        self.swap(i,fin,sw).start()
        fs[slot]=fin[slot,pl.ds(pl.multiple_of(self.c*hn,hn),hn),:].astype(f32)
        for cp in self.store(i,fs,slot,self.c): cp.start()
    def swap(self,i,fin,sw):
        g=self.KIND[i]=="g"; n=self.shape(i)[0]; hn=n//2; idx=i if g else i-4
        return self.rcopy(fin.at[idx%2,pl.ds(pl.multiple_of((1-self.c)*hn,hn),hn)],sw.at[idx],self.r["s_w"].at[i],self.r["r_w"].at[i],peer(self.z,4))
    def store(self,i,fs,slot,core):
        ex=2*core+self.L2[i]; base=0 if self.KIND[i]=="g" else 4
        if self.KIND[i]=="g":
            hc=self.FF//2; h=self.H[i]
            return [pltpu.make_async_copy(fs.at[slot,:,pl.ds(t*hc,hc)],self.r[nm].at[ex,:,pl.ds(h*hc,hc)],self.r["st"].at[base+2*slot+t])
                    for t,nm in enumerate(("gate","up"))]
        return [pltpu.make_async_copy(fs.at[slot],self.r["down"].at[ex],self.r["st"].at[base+slot])]
    def store_wait(self,i,fs):
        idx=i if self.KIND[i]=="g" else i-4
        for cp in self.store(i,fs,idx%2,self.c): cp.wait()
    def other_half(self,i):
        g=self.KIND[i]=="g"; k="g" if g else "w"
        fin=self.r[k+"fin"]; sw=self.r[k+"sw"]; fs=self.r[k+"fs"]; idx=i if g else i-4; slot=idx%2
        self.store_wait(i,fs)
        self.swap(i,fin,sw).wait_recv()
        fs[slot]=sw[idx].astype(f32)
        for cp in self.store(i,fs,slot,1-self.c): cp.start()
        for cp in self.store(i,fs,slot,1-self.c): cp.wait()
    def zsem(self,nm,k): return self.r["s_z"+nm].at[k],self.r["r_z"+nm].at[k]
    def zc(self,nm,k):
        r=self.r; M=r["z"+nm]
        src,dst,dev={0:(M.at[pl.ds(0,2)],r["zr"+nm],peer(self.zi,0)),1:(M.at[2],r["zi"+nm],peer(self.zi,0)),
            2:(r["zs"+nm],r["zm"+nm],peer(self.zx,0)),3:(r["zt"+nm],r["zo"+nm],peer(self.zo,0))}[k]
        s,v=self.zsem(nm,k)
        return self.rcopy(src,dst,s,v,dev)
    def z_inward(self,nm):
        @pl.when(self.outer)
        def _():
            self.zc(nm,0).start(); self.zc(nm,1).start()
    def z_across(self,nm):
        r=self.r
        @pl.when(self.inner)
        def _():
            self.zrecv(nm,0)
            r["zs"+nm][...]=addb(r["z"+nm][0:2],r["zr"+nm][...])
            self.zc(nm,2).start()
    def zrecv(self,nm,k):
        r=self.r; M=r["z"+nm]
        dst={0:r["zr"+nm],1:r["zi"+nm],2:r["zm"+nm],3:r["zo"+nm]}[k]
        src={0:M.at[pl.ds(0,2)],1:M.at[2],2:r["zs"+nm],3:r["zt"+nm]}[k]
        s,v=self.zsem(nm,k)
        dev={0:peer(self.zo,0),1:peer(self.zo,0),2:peer(self.zx,0),3:peer(self.zi,0)}[k]
        self.rcopy(src,dst,s,v,dev).wait_recv()
    def z_last(self,nm):
        r=self.r; M=r["z"+nm]
        @pl.when(self.inner)
        def _():
            self.zrecv(nm,2)
            r["zt"+nm][...]=addb(M[3],r["zm"+nm][0])
            self.zc(nm,3).start()
            self.zrecv(nm,1)
            r["fi"+nm][...]=addb(M[2],r["zm"+nm][1],r["zi"+nm][...])
            self.zc(nm,2).wait_send()
        @pl.when(self.outer)
        def _():
            self.zrecv(nm,3)
            r["fi"+nm][...]=addb(M[3],r["zo"+nm][...])
            self.zc(nm,0).wait_send(); self.zc(nm,1).wait_send()
        for kk in (1,2,3): self.agc(nm,kk).start()
    def agc(self,nm,kk):
        r=self.r
        return self.rcopy(r["fi"+nm],r["ag"+nm].at[kk-1],r["s_ag"+nm].at[kk-1],r["r_ag"+nm].at[kk-1],peer(self.z,kk))
    def z_out(self,nm):
        r=self.r
        for kk in range(4):
            if kk: self.agc(nm,kk).wait()
            a=xor4(self.e,kk)
            v=(r["fi"+nm][...] if kk==0 else r["ag"+nm][kk-1]).astype(f32)
            if nm=="a":
                oa=r["oa"].at[kk%2]
                oa[...]=v
                cols=pl.ds(pl.multiple_of(jnp.minimum(a,2)*self.D,self.D),self.D)
                @pl.when(a<3)
                def _():
                    cp=pltpu.make_async_copy(oa,r["dqkv"].at[:,cols],r["st2"].at[0]); cp.start(); cp.wait()
                @pl.when(a==3)
                def _():
                    cp=pltpu.make_async_copy(oa,r["dwo"],r["st2"].at[0]); cp.start(); cp.wait()
            else:
                SG,SD,Q=self.SG,self.SD,self.FF//4; nb=Q//128
                for t in range(2):
                    for b in range(nb):
                        r["og"][t,:,b*128:(b+1)*128]=v[(t*nb+b)*SG:(t*nb+b+1)*SG,:]
                off=2*nb*SG
                for b in range(self.D//128):
                    r["od"][:,b*128:(b+1)*128]=v[off+b*SD:off+(b+1)*SD,:]
                cols=pl.ds(pl.multiple_of(a*Q,Q),Q)
                cps=[pltpu.make_async_copy(r["og"].at[0],r["dgate"].at[:,cols],r["st2"].at[0]),
                     pltpu.make_async_copy(r["og"].at[1],r["dup"].at[:,cols],r["st2"].at[1]),
                     pltpu.make_async_copy(r["od"],r["ddown"].at[pl.ds(pl.multiple_of(a*SD,SD),SD),:],r["st2"].at[2])]
                for cp in cps: cp.start()
                for cp in cps: cp.wait()
    def rows_of(self,core,zr):
        return pl.ds(pl.multiple_of(2*self.SG*shard_of(zr)+self.SG*core,self.SG),self.SG)
    def at_swap(self,GS):
        return [self.rcopy(GS.at[i,self.rows_of(1-self.c,zr)],self.r["atr"].at[i,zr],self.r["s_at"].at[4*i+zr],self.r["r_at"].at[4*i+zr],peer(self.z,4))
                for i in range(4) for zr in range(4)]
    def at_xy(self,kk):
        return self.rcopy(self.r["sv"].at[xor4(self.e,kk)],self.r["xr"].at[kk-1],self.r["s_xr"].at[kk-1],self.r["r_xr"].at[kk-1],peer(self.z,kk))
    def gcopy(self,k,dev):
        return self.rcopy(self.r["gn"].at[0] ,self.r["gn"].at[k+1],self.r["s_gn"].at[k],self.r["r_gn"].at[k],dev)
    def finish(self,GS,gg):
        r=self.r; gn=r["gn"]
        sw=self.at_swap(GS)
        for cp in sw: cp.start()
        row=lax.broadcasted_iota(jnp.int32,(8,self.D),0)
        ld=pltpu.make_async_copy(r["fgg"],gn.at[7],r["st2"].at[1]); ld.start(); ld.wait()
        gn[0]=jnp.where(row==0,gg,jnp.where(row==1,gn[7],0.0))
        self.gcopy(0,peer(self.z,4)).start()
        @pl.when(self.inner)
        def _(): self.across(4).start()
        self.z_across("b")
        self.piece(0)
        self.piece(1)
        self.gcopy(0,peer(self.z,4)).wait()
        gn[0]=gn[0]+gn[1]
        for kk in (1,2,3): self.gcopy(kk,peer(self.z,kk)).start()
        for cp in sw: cp.wait()
        for i in range(4):
            for zr in range(4):
                r["sv"][i,zr]=addb(GS[i,self.rows_of(self.c,zr),:],r["atr"][i,zr])
        for kk in (1,2,3): self.at_xy(kk).start()
        self.z_last("b")
        self.other_half(0)
        self.other_half(1)
        self.piece(2)
        for kk in (1,2,3): self.gcopy(kk,peer(self.z,kk)).wait()
        gn[0]=(gn[0]+gn[2])+(gn[3]+gn[4])
        @pl.when(self.outer)
        def _(): self.gcopy(4,peer(self.zi,0)).start()
        for kk in (1,2,3): self.at_xy(kk).wait()
        r["za"][...]=addb(r["sv"][self.e],r["xr"][0],r["xr"][1],r["xr"][2])
        self.z_inward("a")
        self.z_out("b")
        @pl.when(self.inner)
        def _():
            self.gcopy(4,peer(self.zo,0)).wait_recv()
            gn[0]=gn[0]+gn[5]
            self.gcopy(5,peer(self.zx,0)).start()
        self.piece(3)
        self.z_across("a")
        @pl.when(self.inner)
        def _():
            self.across(5).start()
            self.gcopy(5,peer(self.zx,0)).wait()
            gn[0]=gn[0]+gn[6]
            self.gcopy(6,peer(self.zo,0)).start()
        @pl.when(self.outer)
        def _():
            self.gcopy(4,peer(self.zi,0)).wait_send()
            self.gcopy(6,peer(self.zi,0)).wait_recv()
            gn[0]=gn[7]
        self.other_half(2)
        self.piece(4)
        self.z_last("a")
        self.other_half(3)
        self.z_out("a")
        self.piece(5)
        @pl.when(self.inner)
        def _(): self.gcopy(6,peer(self.zo,0)).wait_send()
        gcp=pltpu.make_async_copy(gn.at[0],r["gains"],r["st2"].at[1]); gcp.start()
        self.other_half(4); self.other_half(5)
        for i in (2,3): self.swap(i,r["gfin"],r["gsw"]).wait_send()
        for i in (4,5): self.swap(i,r["wfin"],r["wsw"]).wait_send()
        @pl.when(self.inner)
        def _():
            for i in (2,3,4,5):
                k="g" if self.KIND[i]=="g" else "w"; idx=i if k=="g" else i-4
                self.rcopy(r[k+"to"].at[idx%2],r[f"ro{i}"],r["s_o"].at[i],r["r_o"].at[i],peer(self.zo,0)).wait_send()
            self.zc("a",3).wait_send(); self.zc("b",3).wait_send()
        gcp.wait()
        home_run(r["hown"],r["hext"],r["ra"],self.home,False)

f32=jnp.float32; bf16=jnp.bfloat16
def nn(a,b): return lax.dot_general(a,b,(((1,),(0,)),((),())),preferred_element_type=f32)
def nt(a,b): return lax.dot_general(a,b,(((1,),(1,)),((),())),preferred_element_type=f32)
def tn(a,b): return lax.dot_general(a,b,(((0,),(0,)),((),())),preferred_element_type=f32)
EPS=1e-6
E=16; CAP=120
HD=64; GH=4; GW=GH*HD; QC=256
def lane_head(shape):
    return lax.broadcasted_iota(jnp.int32,shape,1)//HD
def swap_half(x):
    w=x.shape[1]
    first=(lax.broadcasted_iota(jnp.int32,x.shape,1)%HD)<HD//2
    return jnp.where(first,pltpu.roll(x,w-HD//2,1),pltpu.roll(x,HD//2,1))
def wide(t):
    return jnp.concatenate([t,t],axis=1)
def inv_rms(v):
    return lax.rsqrt(jnp.mean(v*v,axis=1,keepdims=True)+EPS)

def attn_fwd(tokens, prefix, again, wqkv, wo, fgain, cosw, sinw, rows=None, sout=None):
    T,D=tokens.shape
    ng=D//GW; nq=T//QC
    fused=rows is not None
    NS=E*CAP; CH=480
    def kernel(pre,tok,ag,fg,wq,wk,wv,wor,cw,sw,*rest):
        if fused:
            rowr,so,qo,ko,vo,atto,lseo,stateo,ntwoo,xo,sia,sib,normed,bias,q4,k4,vT,OT,acc,*sems=rest
        else:
            qo,ko,vo,atto,lseo,stateo,ntwoo,normed,bias,q4,k4,vT,OT,acc=rest
        g=pl.program_id(0)
        @pl.when(g==0)
        def _():
            if fused:
                plane_barrier()
                for cpy in plane_copies([(so.at[0],sia),(so.at[1],sib)],sems): cpy.start()
            for c in range(nq):
                r=slice(c*QC,(c+1)*QC)
                x=tok[r,:].astype(f32)
                normed[r,:]=(x*inv_rms(x)*ag[...]).astype(bf16)
                j=lax.broadcasted_iota(jnp.int32,(T,QC),0)
                i=lax.broadcasted_iota(jnp.int32,(T,QC),1)+c*QC
                bias[c]=jnp.where((j<=i)|(j<pre[0]),0.0,-1e30)
        for c in range(nq):
            r=slice(c*QC,(c+1)*QC)
            n=normed[r,:]
            C=wide(cw[r,:]); S=wide(sw[r,:])
            q=nn(n,wq[...]); k=nn(n,wk[...]); v=nn(n,wv[...])
            qb=((q*C+swap_half(q)*S).astype(bf16)).astype(f32)*(HD**-0.5)
            qb=qb.astype(bf16)
            kb=(k*C+swap_half(k)*S).astype(bf16)
            q4[r,:]=qb; qo[r,:]=qb
            k4[r,:]=kb; ko[r,:]=kb
            vo[r,:]=v.astype(bf16)
            vT[:,r]=v.T.astype(bf16)
        lh=lane_head((QC,GW))
        @pl.loop(0,GH)
        def _(h):
            hr=pl.ds(pl.multiple_of(h*HD,HD),HD)
            for c in range(nq):
                r=slice(c*QC,(c+1)*QC)
                qm=jnp.where(lh==h,q4[r,:],jnp.zeros((),bf16))
                st=nt(k4[...],qm)+bias[c]
                m=jnp.max(st,axis=0,keepdims=True)
                p=jnp.exp(st-m)
                l=jnp.sum(p,axis=0,keepdims=True)
                ot=nn(vT[hr,:],p.astype(bf16))
                OT[c,hr,:]=ot*(1.0/l)
                lseo[0,pl.ds(h,1),r]=m+jnp.log(l)
        for c in range(nq):
            r=slice(c*QC,(c+1)*QC)
            a=OT[c].T.astype(bf16)
            atto[r,:]=a
            o=nn(a,wor[...])
            @pl.when(g==0)
            def _(): acc[r,:]=o+tok[r,:].astype(f32)
            @pl.when(g>0)
            def _(): acc[r,:]+=o
        @pl.when(g==ng-1)
        def _():
            for c in range(nq):
                r=slice(c*QC,(c+1)*QC)
                st=acc[r,:]
                stateo[r,:]=st
                ntwoo[r,:]=(st*inv_rms(st)*fg[...]).astype(bf16)
            if fused:
                for i in range(NS//CH):
                    si=lax.broadcasted_iota(jnp.int32,(CH,T),0)+i*CH
                    d=jnp.where((si==rowr[0:1,:])|(si==rowr[1:2,:]),1.0,0.0).astype(bf16)
                    xo[i*CH:(i+1)*CH,:]=nn(d,ntwoo[...]).astype(bf16)
                for cpy in plane_copies([(so.at[0],sia),(so.at[1],sib)],sems): cpy.wait()
    full=lambda s: pl.BlockSpec(s,lambda g:(0,)*len(s))
    col=lambda off: pl.BlockSpec((D,GW),lambda g,off=off:(0,g+off))
    tcol=pl.BlockSpec((T,GW),lambda g:(0,g))
    return pl.pallas_call(kernel,grid=(ng,),
      in_specs=[pl.BlockSpec(memory_space=pltpu.SMEM),full((T,D)),full((1,D)),full((1,D)),col(0),col(ng),col(2*ng),pl.BlockSpec((GW,D),lambda g:(g,0)),full((T,128)),full((T,128))]+([full((8,T)),pl.BlockSpec(memory_space=pl.ANY)] if fused else []),
      out_specs=[tcol,tcol,tcol,tcol,pl.BlockSpec((1,8,T),lambda g:(g,0,0)),full((T,D)),full((T,D))]+([full((NS,D))]+[pl.BlockSpec(memory_space=pl.ANY)]*2 if fused else []),
      out_shape=[jax.ShapeDtypeStruct((T,D),bf16)]*4+[jax.ShapeDtypeStruct((ng,8,T),f32),jax.ShapeDtypeStruct((T,D),f32),jax.ShapeDtypeStruct((T,D),bf16)]+([jax.ShapeDtypeStruct((NS,D),bf16),*[jax.ShapeDtypeStruct((8,CAP,D),bf16)]*2] if fused else []),
      scratch_shapes=[pltpu.VMEM((T,D),bf16),pltpu.VMEM((nq,T,QC),f32),pltpu.VMEM((T,GW),bf16),pltpu.VMEM((T,GW),bf16),pltpu.VMEM((GW,T),bf16),pltpu.VMEM((nq,GW,QC),f32),pltpu.VMEM((T,D),f32)]+(plane_sems(2) if fused else []),
      compiler_params=pltpu.CompilerParams(vmem_limit_bytes=56<<20,dimension_semantics=("arbitrary",),**(dict(collective_id=0,has_side_effects=True) if fused else {})),
      cost_estimate=pl.CostEstimate(flops=2*T*D*4*D+4*T*T*D,bytes_accessed=16<<20,transcendentals=12*T*T),
      name="attn_fwd")(prefix,tokens,again[None],fgain[None],wqkv,wqkv,wqkv,wo,cosw,sinw,*([rows,sout] if fused else []))

def attn_bwd(sgrad, prefix, tokens, again, wqkv, wo, cosw, sinw, q, k, v, att, lse, tail=None):
    T,D=tokens.shape
    ng=D//GW; nq=T//QC
    fast=tail is not None
    def kernel(pre,sg,tok,ag,wq,wk,wv,wor,cw,sw,qr,kr,vr,attr,lser,*rest):
        if fast:
            ni,no=len(tail.in_specs),len(tail.out_specs)
            tgo,ggo=rest[ni:ni+2]
            tins,touts=rest[:ni],rest[ni+2:ni+2+no]
            normed,normedT,bg,bias,dO,kT,PB,DS,dv,dk,dqT,drow,acc,GS,*tscr=rest[ni+2+no:]
            tail.bind(tins,touts,tscr)
        else:
            tgo,ggo,gq,gk,gv,gwo,normed,normedT,bg,bias,dO,kT,PB,DS,dv,dk,dqT,drow,acc=rest
        g=pl.program_id(0)
        if fast:
            @pl.when(g==0)
            def _():
                tail.start()
        @pl.when(g==0)
        def _():
            for c in range(nq):
                r=slice(c*QC,(c+1)*QC)
                x=tok[r,:].astype(f32)
                n=x*inv_rms(x)*ag[...]
                normedT[:,r]=n.T.astype(bf16)
                bg[r,:]=sg[r,:].astype(bf16)
                j=lax.broadcasted_iota(jnp.int32,(T,QC),0)
                i=lax.broadcasted_iota(jnp.int32,(T,QC),1)+c*QC
                bias[c]=jnp.where((j<=i)|(j<pre[0]),0.0,-1e30)
        hmask=(lax.broadcasted_iota(jnp.int32,(8,GW),0)==lane_head((8,GW))).astype(f32)
        for c in range(nq):
            r=slice(c*QC,(c+1)*QC)
            d=nt(bg[r,:],wor[...]).astype(bf16)
            dO[r,:]=d
            a=attr[r,:].astype(f32)
            drow[:,r]=lax.dot_general(hmask,d.astype(f32)*a,(((1,),(1,)),((),())),preferred_element_type=f32,precision=lax.Precision.HIGHEST)
            kT[:,r]=kr[r,:].astype(f32).T.astype(bf16)
        gwv=tn(attr[...],bg[...]).astype(bf16)
        if fast:
            GS[3,pl.ds(pl.multiple_of(g*GW,GW),GW),:]=gwv
        else:
            gwo[...]=gwv
        dv[...]=jnp.zeros_like(dv); dk[...]=jnp.zeros_like(dk)
        lh=lane_head((QC,GW)); lhT=lane_head((T,GW))
        @pl.loop(0,GH)
        def _(h):
            hr=pl.ds(pl.multiple_of(h*HD,HD),HD)
            zero=jnp.zeros((),bf16)
            for c in range(nq):
                r=slice(c*QC,(c+1)*QC)
                qm=jnp.where(lh==h,qr[r,:],zero)
                dOm=jnp.where(lh==h,dO[r,:],zero)
                st=nt(kr[...],qm)+bias[c]
                p=jnp.exp(st-lser[0,pl.ds(h,1),r])
                PB[:,r]=p.astype(bf16)
                dp=nt(vr[...],dOm)
                DS[:,r]=(p*(dp-drow[pl.ds(h,1),r])).astype(bf16)
            dv[...]+=nn(PB[...],jnp.where(lhT==h,dO[...],zero))
            dk[...]+=nn(DS[...],jnp.where(lhT==h,qr[...],zero))
            dqT[hr,:]=nn(kT[hr,:],DS[...])
        for c in range(nq):
            r=slice(c*QC,(c+1)*QC)
            C=wide(cw[r,:]); S=wide(sw[r,:])
            dq=dqT[:,r].T*(HD**-0.5)
            dq=dq*C-swap_half(dq)*S
            dkk=dk[r,:]
            dkk=dkk*C-swap_half(dkk)*S
            a=dq.astype(bf16); b=dkk.astype(bf16); e=dv[r,:].astype(bf16)
            PB[r,0:GW]=a; PB[r,GW:2*GW]=b; PB[r,2*GW:3*GW]=e
            o=nt(a,wq[...])+nt(b,wk[...])+nt(e,wv[...])
            @pl.when(g==0)
            def _(): acc[r,:]=o
            @pl.when(g>0)
            def _(): acc[r,:]+=o
        for i in range(3):
            gval=nn(normedT[...],PB[:,i*GW:(i+1)*GW]).astype(bf16)
            if fast:
                GS[i,:,pl.ds(pl.multiple_of(g*GW,GW),GW)]=gval
            else:
                (gq,gk,gv)[i][...]=gval
        @pl.when(g==ng-1)
        def _():
            gg=jnp.zeros((1,D),f32)
            for c in range(nq):
                r=slice(c*QC,(c+1)*QC)
                x=tok[r,:].astype(f32)
                inv=inv_rms(x); u=x*inv
                ngd=acc[r,:]
                gg=gg+jnp.sum(ngd*u,axis=0,keepdims=True)
                w=ngd*ag[...]
                tgo[r,:]=(sg[r,:]+inv*(w-u*jnp.mean(w*u,axis=1,keepdims=True))).astype(bf16)
            ggo[...]=jnp.broadcast_to(gg,(8,D))
            if fast:
                tail.finish(GS,gg)
    full=lambda s: pl.BlockSpec(s,lambda g:(0,)*len(s),pipeline_mode=pl.Buffered(1))
    col=lambda off: pl.BlockSpec((D,GW),lambda g,off=off:(0,g+off))
    tcol=pl.BlockSpec((T,GW),lambda g:(0,g))
    if fast:
        outs=tail.out_specs; oshape=tail.oshape
        extra=[pltpu.VMEM((4,D,D),bf16)]+tail.scratch
    else:
        outs=[tcol,tcol,tcol,pl.BlockSpec((GW,D),lambda g:(g,0))]
        oshape=[jax.ShapeDtypeStruct((D,D),bf16)]*4
        extra=[]
    rowb=pl.BlockSpec((GW,D),lambda g:(g,0))
    return pl.pallas_call(kernel,grid=(ng,),
      in_specs=[pl.BlockSpec(memory_space=pltpu.SMEM)]+[full((T,D)),full((T,D)),full((1,D)),col(0),col(ng),col(2*ng),rowb,full((T,128)),full((T,128)),tcol,tcol,tcol,tcol,pl.BlockSpec((1,8,T),lambda g:(g,0,0))]+(tail.in_specs if fast else []),
      out_specs=[full((T,D)),full((8,D))]+outs,
      out_shape=[jax.ShapeDtypeStruct((T,D),bf16),jax.ShapeDtypeStruct((8,D),f32)]+oshape,
      scratch_shapes=[pltpu.VMEM((T,D),bf16),pltpu.VMEM((D,T),bf16),pltpu.VMEM((T,D),bf16),pltpu.VMEM((nq,T,QC),f32),pltpu.VMEM((T,GW),bf16),pltpu.VMEM((GW,T),bf16),
        pltpu.VMEM((T,T),bf16),pltpu.VMEM((T,T),bf16),pltpu.VMEM((T,GW),f32),pltpu.VMEM((T,GW),f32),pltpu.VMEM((GW,T),f32),pltpu.VMEM((8,T),f32),pltpu.VMEM((T,D),f32)]+extra,
      compiler_params=pltpu.CompilerParams(vmem_limit_bytes=63<<20,dimension_semantics=("arbitrary",),**(dict(collective_id=5,has_side_effects=True) if fast else {})),
      cost_estimate=pl.CostEstimate(flops=2*T*D*8*D+10*T*T*D,bytes_accessed=24<<20,transcendentals=12*T*T),
      name="attn_bwd")(prefix,sgrad,tokens,again[None],wqkv,wqkv,wqkv,wo,cosw,sinw,q,k,v,att,lse,*(tail.arrays if fast else ()))


def make_ffn(parts, G, L, cap, D, FF, FB, chunk, out_dt):
    R=parts*G*cap
    nf=FF//FB
    def kernel(*refs):
        xs=refs[:parts]; ss=refs[parts:2*parts]
        wg,wu,wd=refs[2*parts:2*parts+3]
        o=2*parts+3
        res=refs[o:o+parts]; dgr=refs[o+parts:o+2*parts]
        gG,gU,gD=refs[o+2*parts:o+2*parts+3]
        X,S,H,GB,UB,AR,AD=refs[o+2*parts+3:]
        f=pl.program_id(1)
        @pl.when(f==0)
        def _():
            for p in range(parts):
                for g in range(G):
                    r=(p*G+g)*cap
                    X[r:r+cap,:]=xs[p][g,0]
                    S[r:r+cap,:]=ss[p][g,0]
        @pl.loop(0,R//chunk)
        def _(i):
            rows=pl.ds(pl.multiple_of(i*chunk,chunk),chunk)
            x=X[rows,:]; s=S[rows,:]
            gate=nn(x,wg[0]); up=nn(x,wu[0]); hg=nt(s,wd[0])
            sig=1.0/(1.0+jnp.exp(-gate))
            sil=gate*sig
            h=(sil*up).astype(bf16)
            gb=(hg*up*(sig*(1.0+gate*(1.0-sig)))).astype(bf16)
            ub=(hg*sil).astype(bf16)
            H[rows,:]=h; GB[rows,:]=gb; UB[rows,:]=ub
            r=nn(h,wd[0]); d=nt(gb,wg[0])+nt(ub,wu[0])
            @pl.when(f==0)
            def _():
                AR[rows,:]=r; AD[rows,:]=d
            @pl.when(f>0)
            def _():
                AR[rows,:]+=r; AD[rows,:]+=d
        gG[0]=tn(X[...],GB[...]).astype(bf16)
        gU[0]=tn(X[...],UB[...]).astype(bf16)
        gD[0]=tn(H[...],S[...]).astype(bf16)
        @pl.when(f==nf-1)
        def _():
            for p in range(parts):
                for g in range(G):
                    r=(p*G+g)*cap
                    res[p][g,0]=AR[r:r+cap,:].astype(out_dt)
                    dgr[p][g,0]=AD[r:r+cap,:].astype(out_dt)
    rowspec=pl.BlockSpec((G,1,cap,D),lambda l,f:(0,l,0,0))
    wspec=pl.BlockSpec((1,D,FB),lambda l,f:(l,0,f))
    wdspec=pl.BlockSpec((1,FB,D),lambda l,f:(l,f,0))
    call=pl.pallas_call(kernel,
      out_shape=[jax.ShapeDtypeStruct((G,L,cap,D),out_dt)]*(2*parts)+[jax.ShapeDtypeStruct((L,D,FF),bf16)]*2+[jax.ShapeDtypeStruct((L,FF,D),bf16)],
      grid=(L,nf),
      in_specs=[rowspec]*(2*parts)+[wspec,wspec,wdspec],
      out_specs=[rowspec]*(2*parts)+[wspec,wspec,wdspec],
      scratch_shapes=[pltpu.VMEM((R,D),bf16)]*2+[pltpu.VMEM((R,FB),bf16)]*3+[pltpu.VMEM((R,D),f32)]*2,
      compiler_params=pltpu.CompilerParams(vmem_limit_bytes=60<<20,dimension_semantics=("arbitrary","arbitrary")),
      cost_estimate=pl.CostEstimate(flops=2*9*R*D*FF*L,bytes_accessed=L*(6*D*FF*2+4*R*D*2),transcendentals=R*FF*L),
      name="ffn")
    return call


def ffn_rows(x,s,wg,wu,wd,H,GB,UB,rows):
    gate=nn(x,wg); up=nn(x,wu); hg=nt(s,wd)
    sig=1.0/(1.0+jnp.exp(-gate))
    sil=gate*sig
    h=(sil*up).astype(bf16)
    gb=(hg*up*(sig*(1.0+gate*(1.0-sig)))).astype(bf16)
    ub=(hg*sil).astype(bf16)
    H[rows,:]=h; GB[rows,:]=gb; UB[rows,:]=ub
    return nn(h,wd),nt(gb,wg)+nt(ub,wu)

def expert_ffn(token, l2, xs, ss, wg, wu, wd, half, prev=(), carry=None, cid=None, FB=512, chunk=480):
    n=len(xs); RG,D=xs[0].shape; FF=wg.shape[2]; R=n*RG; nf=2; HB=nf*FB
    SR=D//4; np_=len(prev); nc=0 if carry is None else 1
    def kernel(tk,*refs):
        xr=refs[:n]; sr=refs[n:2*n]; wgr,wur,wdr=refs[2*n:2*n+3]; o=2*n+3
        pv=refs[o:o+np_]; o+=np_
        csrc=refs[o:o+nc]; o+=nc
        res=refs[o:o+n]; dgr=refs[o+n:o+2*n]; o+=2*n
        gf,gi,go,dw,tok=refs[o:o+5]; o+=5
        cdst=refs[o:o+nc]; o+=nc
        XT,XN,H,GB,UB,AR,AD=refs[o:o+7]; sems=refs[o+7:]
        f=pl.program_id(0)
        tok[...]=jnp.zeros_like(tok)
        if nc:
            @pl.when(f==0)
            def _():
                plane_barrier()
                for cpy in plane_copies([(csrc[0],cdst[0])],sems): cpy.start()
        @pl.when(f==0)
        def _():
            for a in range(n):
                for b in range(RG//chunk):
                    XN[...]=xr[a][b*chunk:(b+1)*chunk,:].astype(f32).T.astype(bf16)
                    for q in range(4):
                        XT[a*(RG//chunk)+b,q*SR:(q+1)*SR,:]=XN[pl.ds(pl.multiple_of(shard_of(q)*SR,SR),SR),:]
        for a in range(n):
            @pl.loop(0,RG//chunk)
            def _(i):
                src=pl.ds(pl.multiple_of(i*chunk,chunk),chunk)
                rows=pl.ds(pl.multiple_of(a*RG+i*chunk,chunk),chunk)
                r,d=ffn_rows(xr[a][src,:],sr[a][src,:],wgr[0],wur[0],wdr[0],H,GB,UB,rows)
                @pl.when(f==0)
                def _():
                    if np_:
                        AR[rows,:]=r+pv[a][src,:].astype(f32); AD[rows,:]=d+pv[n+a][src,:].astype(f32)
                    else:
                        AR[rows,:]=r; AD[rows,:]=d
                @pl.when(f>0)
                def _():
                    res[a][src,:]=(AR[rows,:]+r).astype(bf16); dgr[a][src,:]=(AD[rows,:]+d).astype(bf16)
        for t,Y in enumerate((GB,UB)):
            gv=None
            for b in range(R//chunk):
                p=nn(XT[b],Y[b*chunk:(b+1)*chunk,:])
                gv=p if gv is None else gv+p
            gv=gv.astype(bf16)
            cols=pl.ds(pl.multiple_of(t*HB+f*FB,FB),FB)
            gf[:,cols]=gv[0:2*SR]; gi[:,cols]=gv[2*SR:3*SR]; go[:,cols]=gv[3*SR:4*SR]
        dv=None
        for a in range(n):
            t=tn(H[a*RG:(a+1)*RG,:],sr[a][...])
            dv=t if dv is None else dv+t
        dw[...]=dv.astype(bf16)
        if nc:
            @pl.when(f==nf-1)
            def _():
                for cpy in plane_copies([(csrc[0],cdst[0])],sems): cpy.wait()
    one=pl.Buffered(1)
    rowspec=pl.BlockSpec((RG,D),lambda f:(0,0),pipeline_mode=one)
    wspec=pl.BlockSpec((1,D,FB),lambda f:(2*spot()[0]+l2,0,f+nf*half))
    wdspec=pl.BlockSpec((1,FB,D),lambda f:(2*spot()[0]+l2,f+nf*half,0))
    full=lambda r,c: pl.BlockSpec((r,c),lambda f:(0,0),pipeline_mode=one)
    anyspec=pl.BlockSpec(memory_space=pl.ANY)
    out=pl.pallas_call(kernel,grid=(nf,),
        in_specs=[pl.BlockSpec(memory_space=pltpu.SMEM)]+[rowspec]*(2*n)+[wspec,wspec,wdspec]+[rowspec]*np_+[anyspec]*nc,
        out_specs=[rowspec]*(2*n)+[full(2*SR,2*HB),full(SR,2*HB),full(SR,2*HB),pl.BlockSpec((FB,D),lambda f:((1-f) if half else f,0)),full(8,128)]+[anyspec]*nc,
        scratch_shapes=[pltpu.VMEM((R//chunk,D,chunk),bf16),pltpu.VMEM((D,chunk),bf16)]+[pltpu.VMEM((R,FB),bf16)]*3+[pltpu.VMEM((R,D),f32)]*2+(plane_sems(1) if nc else []),
      out_shape=[jax.ShapeDtypeStruct((RG,D),bf16)]*(2*n)+[jax.ShapeDtypeStruct((2*SR,2*HB),bf16)]+[jax.ShapeDtypeStruct((SR,2*HB),bf16)]*2+[jax.ShapeDtypeStruct((HB,D),bf16),jax.ShapeDtypeStruct((8,128),jnp.int32)]+[jax.ShapeDtypeStruct((8,RG//8,D),bf16)]*nc,
      compiler_params=pltpu.CompilerParams(vmem_limit_bytes=62<<20,dimension_semantics=("arbitrary",),**(dict(collective_id=cid,has_side_effects=True) if nc else {})),
      cost_estimate=pl.CostEstimate(flops=9*R*D*FF,bytes_accessed=3*D*FF*2+4*R*D*2,transcendentals=R*FF//2),
      name=f"expert_ffn{n}_{half}")(token,*xs,*ss,wg,wu,wd,*prev,*([carry] if nc else []))
    return (out[:2*n],out[2*n:2*n+3],out[2*n+3],out[2*n+4][0,0:1],*out[2*n+5:])

def shared_ffn(x, s, wg, wu, wd, xout, FB=512):
    T,D=x.shape; FF=wg.shape[1]; nf=FF//FB; chunk=T//2
    SG=D//8; SD=FB//8
    NR=2*SG*(FB//128)+SD*(D//128)
    def kernel(xr,sr,wgr,wur,wdr,xo,res,dgr,o0,o1,tok,xia,xib,XT,H,GB,UB,VG,VD,*sems):
        f=pl.program_id(0)
        tok[...]=jnp.zeros_like(tok)
        core=spot()[0]
        pairs=[(xo.at[0],xia),(xo.at[1],xib)]
        @pl.when(f==0)
        def _():
            plane_barrier()
            for cpy in plane_copies(pairs,sems): cpy.start()
        @pl.when(f==0)
        def _():
            for b in range(2):
                XT[:,b*chunk:(b+1)*chunk]=xr[b*chunk:(b+1)*chunk,:].astype(f32).T.astype(bf16)
        @pl.loop(0,T//chunk)
        def _(i):
            rows=pl.ds(pl.multiple_of(i*chunk,chunk),chunk)
            r,d=ffn_rows(xr[rows,:],sr[rows,:],wgr[...],wur[...],wdr[...],H,GB,UB,rows)
            @pl.when(f==0)
            def _():
                res[rows,:]=r; dgr[rows,:]=d
            @pl.when(f>0)
            def _():
                res[rows,:]+=r; dgr[rows,:]+=d
        for t,Y in enumerate((GB,UB)):
            VG[...]=nn(XT[...],Y[...]).astype(bf16)
            for zr in range(4):
                for cp in range(2):
                    src=pl.ds(pl.multiple_of(2*SG*shard_of(zr)+SG*lax.rem(core+cp,2),SG),SG)
                    for b in range(FB//128):
                        off=(t*(FB//128)+b)*SG
                        (o0,o1)[cp][f,zr,off:off+SG,:]=VG[src,b*128:(b+1)*128]
        VD[...]=tn(H[...],sr[...]).astype(bf16)
        zr=jnp.where(spot()[1]<2,3-f,f)
        for cp in range(2):
            for e in range(4):
                src=pl.ds(pl.multiple_of(lax.rem(core+cp,2)*4*SD+e*SD,SD),SD)
                for b in range(D//128):
                    off=2*SG*(FB//128)+b*SD
                    (o0,o1)[cp][e,zr,off:off+SD,:]=VD[src,b*128:(b+1)*128]
        @pl.when(f==nf-1)
        def _():
            for cpy in plane_copies(pairs,sems): cpy.wait()
    full=lambda sh: pl.BlockSpec(sh,lambda f:(0,)*len(sh))
    return pl.pallas_call(kernel,grid=(nf,),
      in_specs=[full((T,D)),full((T,D)),pl.BlockSpec((D,FB),lambda f:(0,f)),pl.BlockSpec((D,FB),lambda f:(0,f)),pl.BlockSpec((FB,D),lambda f:(f,0)),pl.BlockSpec(memory_space=pl.ANY)],
      out_specs=[full((T,D)),full((T,D)),full((4,4,NR,128)),full((4,4,NR,128)),full((8,128))]+[pl.BlockSpec(memory_space=pl.ANY)]*2,
      out_shape=[jax.ShapeDtypeStruct((T,D),f32)]*2+[jax.ShapeDtypeStruct((4,4,NR,128),bf16)]*2+[jax.ShapeDtypeStruct((8,128),jnp.int32)]+[jax.ShapeDtypeStruct(xout.shape[1:],bf16)]*2,
      scratch_shapes=[pltpu.VMEM((D,T),bf16)]+[pltpu.VMEM((T,FB),bf16)]*3+[pltpu.VMEM((D,FB),bf16),pltpu.VMEM((FB,D),bf16)]+plane_sems(2),
      compiler_params=pltpu.CompilerParams(vmem_limit_bytes=62<<20,dimension_semantics=("arbitrary",),collective_id=1,has_side_effects=True),
      cost_estimate=pl.CostEstimate(flops=2*9*T*D*FF,bytes_accessed=6*D*FF*2+8*T*D*2,transcendentals=T*FF),
      name="shared_ffn")(x,s,wg,wu,wd,xout)


def route(order, expert_ids, gates, cot, core, G, L, parts, plane=False):
    T,D=cot.shape; P2=2*T
    LP=L//parts; S=G*LP*CAP
    big=E*CAP
    CH=480 if S%480==0 else CAP*4
    def kernel(core_ref,orow,ids,gts,ct,rowo,colo,*rest):
        sgs=rest[:parts]; PT,PG=rest[parts:]
        lane=lax.broadcasted_iota(jnp.int32,(T,128),1)
        e0=ids[:,0:1].astype(f32); e1=ids[:,1:2].astype(f32)
        er=jnp.where(lane==0,e0,jnp.where(lane==1,e1,0.0)).T[0:8,:]
        ecat=jnp.concatenate([er[0:1,:],er[1:2,:]],axis=1)
        eoh=(lax.broadcasted_iota(jnp.int32,(E,P2),0).astype(f32)==ecat)
        eohb=jnp.where(eoh,1.0,0.0).astype(bf16)
        o=orow[...]
        oj=(o&1)*T+(o>>1)
        CB=256
        for c in range(P2//CB):
            jj=lax.broadcasted_iota(jnp.int32,(CB,P2),0)+c*CB
            PT[c*CB:(c+1)*CB,:]=jnp.where(jj==oj,1.0,0.0).astype(bf16)
        soh=nn(eohb,PT[...])
        sohb=soh.astype(bf16)
        tri=jnp.where(lax.broadcasted_iota(jnp.int32,(CB,CB),0)<lax.broadcasted_iota(jnp.int32,(CB,CB),1),1.0,0.0).astype(bf16)
        run=jnp.zeros((E,1),f32)
        pos=[]
        for c in range(P2//CB):
            blk=soh[:,c*CB:(c+1)*CB]
            before=nn(sohb[:,c*CB:(c+1)*CB],tri)+run
            run=run+jnp.sum(blk,axis=1,keepdims=True)
            pos.append(jnp.sum(before*blk,axis=0,keepdims=True))
        posr=jnp.minimum(jnp.concatenate(pos,axis=1),127.0)
        posj=nt(jnp.broadcast_to(posr,(16,P2)).astype(bf16),PT[...])[0:1,:]
        e=ecat.astype(jnp.int32)
        l=lax.rem(e,L); j=lax.div(e,L)
        if plane:
            base=((lax.rem(l,2)*2+lax.div(l,2))*G+j)*CAP
        elif parts==2:
            cc=lax.rem(lax.div(l,LP)+core_ref[0],2)
            base=((cc*G+j)*LP+lax.rem(l,LP))*CAP
        else:
            base=e*CAP
        p=posj.astype(jnp.int32)
        slot=jnp.where(p<CAP,base+p,big)
        s0=slot[:,0:T]; s1=slot[:,T:P2]
        r8=lax.broadcasted_iota(jnp.int32,(8,T),0)
        rows=jnp.where(r8==0,s0,jnp.where(r8==1,s1,big))
        rowo[...]=rows
        rep=jnp.concatenate([rows.astype(f32)]*16,axis=0).T
        colo[...]=rep[:,0:8].astype(jnp.int32)
        ctf=ct[...].astype(f32)
        PG[0:T,:]=(gts[:,0:1]*ctf).astype(bf16)
        PG[T:P2,:]=(gts[:,1:2]*ctf).astype(bf16)
        for pi in range(parts):
            @pl.loop(0,S//CH)
            def _(i):
                si=lax.broadcasted_iota(jnp.int32,(CH,T),0)+(i*CH+pi*S)
                d0=jnp.where(si==rowo[0:1,:],1.0,0.0).astype(bf16)
                d1=jnp.where(si==rowo[1:2,:],1.0,0.0).astype(bf16)
                sgs[pi][pl.ds(pl.multiple_of(i*CH,CH),CH),:]=(nn(d0,PG[0:T,:])+nn(d1,PG[T:P2,:])).astype(bf16)
    vm=pl.BlockSpec(memory_space=pltpu.VMEM)
    out=pl.pallas_call(kernel,
      in_specs=[pl.BlockSpec(memory_space=pltpu.SMEM)]+[vm]*4,out_specs=[vm]*(2+parts),
      out_shape=[jax.ShapeDtypeStruct((8,T),jnp.int32),jax.ShapeDtypeStruct((T,8),jnp.int32)]+[jax.ShapeDtypeStruct((S,D),bf16)]*parts,
      scratch_shapes=[pltpu.VMEM((P2,P2),bf16),pltpu.VMEM((P2,D),bf16)],
      compiler_params=pltpu.CompilerParams(vmem_limit_bytes=50<<20),
      cost_estimate=pl.CostEstimate(flops=4*S*parts*T*D+4*P2*P2*16,bytes_accessed=8<<20,transcendentals=0),
      name="route")(core,order,expert_ids,gates,cot)
    return out[0],out[1],out[2:]

def dispatch(rows, x, parts):
    T,D=x.shape; S=E*CAP//parts; CH=480
    def kernel(rowr,xr,*outs):
        for pi in range(parts):
            @pl.loop(0,S//CH)
            def _(i):
                si=lax.broadcasted_iota(jnp.int32,(CH,T),0)+(i*CH+pi*S)
                d=jnp.where((si==rowr[0:1,:])|(si==rowr[1:2,:]),1.0,0.0).astype(bf16)
                outs[pi][pl.ds(pl.multiple_of(i*CH,CH),CH),:]=nn(d,xr[...]).astype(bf16)
    vm=pl.BlockSpec(memory_space=pltpu.VMEM)
    return pl.pallas_call(kernel,in_specs=[vm]*2,out_specs=[vm]*parts,out_shape=[jax.ShapeDtypeStruct((S,D),bf16)]*parts,
      compiler_params=pltpu.CompilerParams(vmem_limit_bytes=50<<20),
      cost_estimate=pl.CostEstimate(flops=2*S*parts*T*D,bytes_accessed=6<<20,transcendentals=0),name="dispatch")(rows,x)

def combine(cols, gates, ret, state, shared):
    parts=len(ret); T,D=state.shape; S=ret[0].shape[0]
    def kernel(colr,g,*refs):
        rs=refs[:parts]; st,sh,out=refs[parts:]
        @pl.loop(0,T//QC)
        def _(i):
            r=pl.ds(pl.multiple_of(i*QC,QC),QC)
            acc=st[r,:]+sh[r,:]
            for k in range(2):
                pk=None
                for pi in range(parts):
                    si=lax.broadcasted_iota(jnp.int32,(QC,S),1)+pi*S
                    d=jnp.where(si==colr[r,k:k+1],1.0,0.0).astype(bf16)
                    q=nn(d,rs[pi][...])
                    pk=q if pk is None else pk+q
                acc=acc+g[r,k:k+1]*pk
            out[r,:]=acc.astype(bf16)
    vm=pl.BlockSpec(memory_space=pltpu.VMEM)
    return pl.pallas_call(kernel,in_specs=[vm]*(4+parts),out_specs=vm,out_shape=jax.ShapeDtypeStruct((T,D),bf16),
      compiler_params=pltpu.CompilerParams(vmem_limit_bytes=50<<20),
      cost_estimate=pl.CostEstimate(flops=4*S*parts*T*D,bytes_accessed=9<<20,transcendentals=0),name="combine")(cols,gates,*ret,state,shared)

def mid_bwd_home(cols, own, ext, back_b, dsh, state, fgain, cot):
    T,D=state.shape; S=8*CAP
    def kernel(colr,hown,hext,bb,ds,st,fg,ct,sgo,fgo,ba,BV,cs,*hsems):
        home_barrier()
        home_run(hown,hext,ba,hsems,True)
        fgo[...]=jnp.zeros_like(fgo)
        home_run(hown,hext,ba,hsems,False)
        cps=[pltpu.make_async_copy(ba.at[i],BV.at[i],cs.at[i]) for i in range(8)]
        for cp in cps: cp.start()
        for cp in cps: cp.wait()
        @pl.loop(0,T//QC)
        def _(i):
            r=pl.ds(pl.multiple_of(i*QC,QC),QC)
            n=ds[r,:]
            si=lax.broadcasted_iota(jnp.int32,(QC,S),1)+S
            d=jnp.where((si==colr[r,0:1])|(si==colr[r,1:2]),1.0,0.0).astype(bf16)
            n=n+nn(d,bb[...])
            for b in range(8):
                si=lax.broadcasted_iota(jnp.int32,(QC,128),1)
                si=jnp.where(si<CAP,si+b*CAP,-1)
                d=jnp.where((si==colr[r,0:1])|(si==colr[r,1:2]),1.0,0.0).astype(bf16)[:,0:CAP]
                n=n+nn(d,BV[b])
            x=st[r,:]; inv=inv_rms(x); u=x*inv
            fgo[...]+=jnp.broadcast_to(jnp.sum(n*u,axis=0,keepdims=True),(8,D))
            w=n*fg[...]
            sgo[r,:]=ct[r,:].astype(f32)+inv*(w-u*jnp.mean(w*u,axis=1,keepdims=True))
    vm=pl.BlockSpec(memory_space=pltpu.VMEM); an=pl.BlockSpec(memory_space=pl.ANY)
    return pl.pallas_call(kernel,in_specs=[vm,an,an]+[vm]*5,out_specs=[vm]*2+[an],
      out_shape=[jax.ShapeDtypeStruct((T,D),f32),jax.ShapeDtypeStruct((8,D),f32),jax.ShapeDtypeStruct((8,CAP,D),bf16)],
      scratch_shapes=[pltpu.VMEM((8,CAP,D),bf16),pltpu.SemaphoreType.DMA((8,))]+home_sems(),
      compiler_params=pltpu.CompilerParams(vmem_limit_bytes=50<<20,collective_id=4,has_side_effects=True),
      cost_estimate=pl.CostEstimate(flops=4*S*T*D,bytes_accessed=12<<20,transcendentals=0),name="mid_bwd")(cols,own,ext,back_b,dsh,state,fgain[None],cot)

def mid_bwd(cols, back, dsh, state, fgain, cot):
    parts=len(back); T,D=state.shape; S=back[0].shape[0]
    def kernel(colr,*refs):
        bs=refs[:parts]; ds,st,fg,ct,sgo,fgo=refs[parts:]
        fgo[...]=jnp.zeros_like(fgo)
        @pl.loop(0,T//QC)
        def _(i):
            r=pl.ds(pl.multiple_of(i*QC,QC),QC)
            n=ds[r,:]
            for pi in range(parts):
                si=lax.broadcasted_iota(jnp.int32,(QC,S),1)+pi*S
                d=jnp.where((si==colr[r,0:1])|(si==colr[r,1:2]),1.0,0.0).astype(bf16)
                n=n+nn(d,bs[pi][...])
            x=st[r,:]; inv=inv_rms(x); u=x*inv
            fgo[...]+=jnp.broadcast_to(jnp.sum(n*u,axis=0,keepdims=True),(8,D))
            w=n*fg[...]
            sgo[r,:]=ct[r,:].astype(f32)+inv*(w-u*jnp.mean(w*u,axis=1,keepdims=True))
    vm=pl.BlockSpec(memory_space=pltpu.VMEM)
    return pl.pallas_call(kernel,in_specs=[vm]*(5+parts),out_specs=[vm]*2,out_shape=[jax.ShapeDtypeStruct((T,D),f32),jax.ShapeDtypeStruct((8,D),f32)],
      compiler_params=pltpu.CompilerParams(vmem_limit_bytes=50<<20),
      cost_estimate=pl.CostEstimate(flops=2*S*parts*T*D,bytes_accessed=12<<20,transcendentals=0),name="mid_bwd")(cols,*back,dsh,state,fgain[None],cot)

HEADS = 12
HEAD_DIM = 64


def rope_wide(length):
    positions = jnp.arange(length, dtype=f32)
    frequency = 10000.0 ** (-jnp.arange(HEAD_DIM // 2, dtype=f32) * 2.0 / HEAD_DIM)
    angles = positions[:, None] * frequency[None, :]
    c = jnp.cos(angles)
    s = jnp.sin(angles)
    return jnp.concatenate([c, c, c, c], axis=1), jnp.concatenate([-s, s, -s, s], axis=1)


def shards_any(tokens, cotangent, expert_ids, route_gates, slot_order, prefix_len, attention_gain, qkv_weight,
           output_weight, feedforward_gain, shared_gate, shared_up, shared_down, expert_gate, expert_up, expert_down):
    T, D = tokens.shape
    L, _, FF = expert_gate.shape
    G = lax.axis_size("expert")
    DP = lax.axis_size("dp")
    Z = DP // 2
    parts = 2 if L % 2 == 0 else 1
    LP = L // parts
    dpi = lax.axis_index("dp")
    core = lax.rem(dpi, 2)
    swap_perm = [(i, i ^ 1) for i in range(DP)]
    zgroups = [[2 * z + c for z in range(Z)] for c in range(2)]

    def swap(x):
        return lax.ppermute(x, "dp", swap_perm)

    def a2a(x):
        return lax.all_to_all(x, "expert", split_axis=0, concat_axis=0, tiled=True)

    def to_experts(arrs):
        arrs = [a.reshape(G, LP, CAP, D) for a in arrs]
        if parts == 2:
            arrs = [arrs[0], swap(arrs[1])]
        return [a2a(a) for a in arrs]

    def from_experts(arrs):
        arrs = [a2a(a) for a in arrs]
        if parts == 2:
            arrs = [arrs[0], swap(arrs[1])]
        return [a.reshape(G * LP * CAP, D) for a in arrs]

    cosw, sinw = rope_wide(T)
    rows, cols, sgs = route(slot_order, expert_ids, route_gates, cotangent, core[None].astype(jnp.int32), G, L, parts)
    slot_in = to_experts(sgs)
    q, k, v, att, lse, state, ntwo = attn_fwd(tokens, prefix_len, attention_gain, qkv_weight, output_weight,
                                              feedforward_gain, cosw, sinw)
    xs = dispatch(rows, ntwo, parts)
    x_in = to_experts(xs)
    sh = make_ffn(1, 1, 1, T, D, FF, 512, T // 2, f32)(
        ntwo[None, None], cotangent[None, None], shared_gate[None], shared_up[None], shared_down[None])
    shared_branch = sh[0].reshape(T, D)
    dshared = sh[1].reshape(T, D)
    dense_shared = [sh[2][0], sh[3][0], sh[4][0]]

    res, dgr, eg = [], [], []
    one = make_ffn(parts, G, 1, CAP, D, FF, 512, parts * G * CAP // 2, bf16)
    for l in range(LP):
        o = one(*[a[:, l:l + 1] for a in x_in], *[a[:, l:l + 1] for a in slot_in],
                *[lax.dynamic_slice_in_dim(w, (core * LP if parts == 2 else 0) + l, 1, 0)
                  for w in (expert_gate, expert_up, expert_down)])
        res.append(o[:parts])
        dgr.append(o[parts:2 * parts])
        eg.append(o[2 * parts:])
    cat = lambda xs_: jnp.concatenate(xs_, axis=1) if len(xs_) > 1 else xs_[0]
    res = [cat([r[p] for r in res]) for p in range(parts)]
    dgr = [cat([r[p] for r in dgr]) for p in range(parts)]

    egr = []
    for l in range(LP):
        if parts == 2:
            egr.append([lax.psum_scatter(g[0], "dp", scatter_dimension=0, tiled=True, axis_index_groups=zgroups)
                        for g in eg[l]])
        else:
            egr.append([lax.psum_scatter(g[0], "dp", scatter_dimension=0, tiled=True) for g in eg[l]])

    back = from_experts(dgr)
    ret = from_experts(res)
    sgrad, fgg = mid_bwd(cols, back, dshared, state, feedforward_gain, cotangent)
    tokens_grad, agg, gq, gk, gv, gwo = attn_bwd(sgrad, prefix_len, tokens, attention_gain, qkv_weight, output_weight,
                                                 cosw, sinw, q, k, v, att, lse)
    block_out = combine(cols, route_gates, ret, state, shared_branch)

    def dense(g):
        r = g.shape[0] // DP
        h = g.reshape(Z, 2, r, g.shape[1])
        mine = lax.dynamic_index_in_dim(h, core, 1, keepdims=False)
        other = lax.dynamic_index_in_dim(h, 1 - core, 1, keepdims=False)
        s = (mine.astype(f32) + swap(other).astype(f32)).astype(bf16)
        quarter = s.reshape(Z, G, r // G, g.shape[1])
        quarter = jnp.swapaxes(quarter, 0, 1)
        got = lax.all_to_all(quarter, "expert", split_axis=0, concat_axis=0, tiled=True)
        s = jnp.sum(got.astype(f32), axis=0).astype(bf16)
        zs = lax.psum_scatter(s, "dp", scatter_dimension=0, tiled=True, axis_index_groups=zgroups)
        return lax.all_gather(zs[0], "expert", axis=0, tiled=True).astype(f32)

    def dense_simple(g):
        p = lax.psum_scatter(g, "dp", scatter_dimension=0, tiled=True)
        return lax.psum(p, "expert").astype(f32)

    if (qkv_weight.shape[0] // DP) % (8 * G) == 0 and parts == 2:
        dn = dense
    else:
        dn = dense_simple
    dsh = [dn(g) for g in dense_shared]
    dq, dk, dv, dwo = [dn(g) for g in (gq, gk, gv, gwo)]
    gains = lax.psum(jnp.stack([agg[0], fgg[0]]), ("dp", "expert"))
    gs = D // DP
    gains = lax.dynamic_slice_in_dim(gains, dpi * gs, gs, 1)

    def finish(t):
        a = [egr[l][t] for l in range(LP)]
        if parts == 1:
            return jnp.stack(a).astype(f32)
        b = jnp.stack(a)
        h = b.reshape(LP, 2, b.shape[1] // 2, b.shape[2])
        mine = lax.dynamic_index_in_dim(h, core, 1, keepdims=False)
        other = swap(lax.dynamic_index_in_dim(h, 1 - core, 1, keepdims=False))
        return jnp.concatenate([jnp.where(core == 0, mine, other), jnp.where(core == 0, other, mine)], axis=0).astype(f32)

    return (block_out, tokens_grad, gains[0], jnp.concatenate([dq, dk, dv], axis=1), dwo, gains[1],
            dsh[0], dsh[1], dsh[2], finish(0), finish(1), finish(2))


def shards_fast(tokens, cotangent, expert_ids, route_gates, slot_order, prefix_len, attention_gain, qkv_weight,
                output_weight, feedforward_gain, shared_gate, shared_up, shared_down, expert_gate, expert_up, expert_down):
    T, D = tokens.shape
    FF = expert_gate.shape[2]
    dpi = lax.axis_index("dp").astype(jnp.int32)
    ei = lax.axis_index("expert").astype(jnp.int32)
    core = lax.rem(dpi, 2)
    zi = lax.div(dpi, 2)
    outer = (zi == 0) | (zi == 3)
    low = zi < 2

    def swap(x):
        return lax.ppermute(x, "dp", [(i, i ^ 1) for i in range(8)])

    def inward(x):
        return lax.ppermute(x, "dp", [(0, 2), (1, 3), (6, 4), (7, 5)])

    def outward(x):
        return lax.ppermute(x, "dp", [(2, 0), (3, 1), (4, 6), (5, 7)])

    def across(x):
        return lax.ppermute(x, "dp", [(2, 4), (3, 5), (4, 2), (5, 3)])

    def add(*xs, after=None):
        t = xs[0].astype(f32)
        for x in xs[1:]:
            t = t + x.astype(f32)
        if after is not None:
            t = t + after[0].astype(f32)
        return t.astype(bf16)

    def mark(x):
        y = lax.slice(x, (0,) * x.ndim, (1,) * x.ndim).reshape(1).astype(f32)
        return jnp.minimum(y * y, 0.0).astype(jnp.int32)

    cosw, sinw = rope_wide(T)
    rows, cols, (s_out,) = route(slot_order, expert_ids, route_gates, cotangent, core[None], 4, 4, 1, True)
    q, k, v, att, lse, state, ntwo, x_out, sa, sb = attn_fwd(
        tokens, prefix_len, attention_gain, qkv_weight, output_weight, feedforward_gain, cosw, sinw, rows,
        s_out.reshape(2, 8, CAP, D))
    flat = lambda y: y.reshape(8 * CAP, D)
    sx = inward(flat(sa))
    shared_branch, dshared, sh0, sh1, tok, xa, xb = shared_ffn(ntwo, cotangent, shared_gate, shared_up, shared_down,
                                                               x_out.reshape(2, 8, CAP, D))
    sa, sb, xa, xb = flat(sa), flat(sb), flat(xa), flat(xb)
    xx = inward(xa)
    ws = (expert_gate, expert_up, expert_down)
    p0, gb0, wb0, tok = expert_ffn(tok[0, 0:1], 1, [xb], [sb], *ws, 0)
    (rb, db), gb1, wb1, tok = expert_ffn(tok, 1, [xb], [sb], *ws, 1, p0)

    far_w = lambda w0, w1: jnp.where(low, w1, w0)
    near_w = lambda w0, w1: jnp.where(low, w0, w1)
    hw = FF // 4
    blocks = lambda y: y.reshape(8, CAP, D)
    rf = [inward(gb0[0]), inward(gb1[0]), inward(far_w(wb0, wb1))]
    p0, ga0, wa0, tok, db = expert_ffn(tok, 0, [xa, xx], [sa, sx], *ws, 0, carry=blocks(db), cid=2)
    bs0 = add(gb0[0], rf[0], after=tok)
    m_b0 = across(bs0)
    m_a0 = across(ga0[0])
    (ra, rx, da, dx), ga1, wa1, tok, rb = expert_ffn(tok + mark(bs0), 0, [xa, xx], [sa, sx], *ws, 1, p0, carry=blocks(rb), cid=3)
    bs1 = add(gb1[0], rf[1], after=tok)
    sgrad, fgg, _ = mid_bwd_home(cols + mark(bs1), blocks(da), blocks(dx), flat(db), dshared, state, feedforward_gain, cotangent)
    tok = mark(fgg)
    far_wb = far_w(wb0, wb1)
    bs2 = add(far_wb, rf[2], after=tok)
    near_wb = near_w(wb0, wb1)
    rin = [inward(gb0[1]), inward(gb1[1]), inward(near_wb[hw:])]

    s = add(sh0, swap(sh1))
    s = lax.all_to_all(s, "expert", split_axis=0, concat_axis=0, tiled=True)
    msh = add(s[0], s[1], s[2], s[3])
    carried = {
        "hown": blocks(ra), "hext": blocks(rx), "fgg": fgg, "msh": msh,
        "m0": m_b0, "ni0": gb0[1], "no0": gb0[2], "rin0": rin[0],
        "m1": m_a0, "ni1": ga0[1], "no1": ga0[2],
        "far2": bs1, "ni2": gb1[1], "no2": gb1[2], "rin2": rin[1],
        "far3": ga1[0], "ni3": ga1[1], "no3": ga1[2],
        "far4": far_w(wa0, wa1), "nw4": near_w(wa0, wa1),
        "far5": bs2, "nw5": near_wb, "rin5": rin[2],
    }
    tail = Tail(carried, T, D, FF)
    tokens_grad, _, *rest = attn_bwd(sgrad, prefix_len + mark(bs2), tokens, attention_gain, qkv_weight, output_weight,
                                     cosw, sinw, q, k, v, att, lse, tail)
    o = dict(zip(tail.onames, rest))
    block_out = combine(cols, route_gates, [flat(o["ra"]), flat(rb)], state, shared_branch)
    sg = D // 8
    gains = lax.dynamic_slice_in_dim(o["gains"], dpi * sg, sg, 1)
    return (block_out, tokens_grad, gains[0], o["dqkv"], o["dwo"], gains[1], o["dgate"], o["dup"], o["ddown"],
            o["gate"], o["up"], o["down"])


def shards(*args):
    local = args[13].shape[0]
    if lax.axis_size("dp") == 8 and lax.axis_size("expert") == 4 and local == 4:
        return shards_fast(*args)
    return shards_any(*args)


def solution(mesh):
    row = P(("dp", "expert"), None)
    return jax.shard_map(
        shards,
        mesh=mesh,
        in_specs=(row, row, row, row, row, P(("dp", "expert")), P(), P(), P(), P(), P(), P(), P(),
                  P("expert", None, None), P("expert", None, None), P("expert", None, None)),
        out_specs=(row, row, P("dp"), P("dp", None), P("dp", None), P("dp"), P("dp", None), P("dp", None),
                   P("dp", None), P("expert", "dp", None), P("expert", "dp", None), P("expert", "dp", None)),
        check_vma=False,
    )
```

```python
import jax
import jax.numpy as jnp
from jax import lax
from jax.experimental import pallas as pl
from jax.experimental.pallas import tpu as pltpu
from jax.sharding import PartitionSpec as P


MESH_ID = pl.DeviceIdType.MESH

def xor4(e,k):
    lo=lax.rem(e,2); hi=lax.div(e,2)
    if k&1: lo=1-lo
    if k&2: hi=1-hi
    return hi*2+lo

def spot():
    d=lax.axis_index("dp"); e=lax.axis_index("expert")
    c=lax.rem(d,2)
    return c,lax.div(d,2),e

def shard_of(q):
    c,z,e=spot()
    return jnp.where(z<2,3-q,q).astype(jnp.int32)

def peer(z,kk):
    c,_,e=spot()
    return (2*z+lax.rem(c+(kk>>2),2),xor4(e,kk&3))

def block_of(kk):
    c,_,e=spot()
    return lax.rem(c+(kk>>2),2)*4+xor4(e,kk&3)

def plane_sems(n):
    return [pltpu.SemaphoreType.DMA((n,)),pltpu.SemaphoreType.DMA((n,7)),pltpu.SemaphoreType.DMA((n,7))]

def plane_barrier():
    c,z,e=spot()
    b=pltpu.get_barrier_semaphore()
    for kk in range(1,8):
        pl.semaphore_signal(b,inc=1,device_id=peer(z,kk),device_id_type=MESH_ID)
    pl.semaphore_wait(b,7)

def plane_z_barrier():
    c,z,e=spot()
    b=pltpu.get_barrier_semaphore()
    for kk in range(1,8):
        pl.semaphore_signal(b,inc=1,device_id=peer(z,kk),device_id_type=MESH_ID)
    pl.semaphore_signal(b,inc=1,device_id=(2*side()+c,e),device_id_type=MESH_ID)
    pl.semaphore_wait(b,8)

def side():
    c,z,e=spot()
    return z+1-2*lax.rem(z,2)

def inward_run(srcs, dst, sems, start):
    c,z,e=spot()
    end=(z==0)|(z==3)
    def cp(src): return pltpu.make_async_remote_copy(src_ref=src,dst_ref=dst,send_sem=sems[0].at[0],recv_sem=sems[1].at[0],
        device_id=(2*side()+c,e),device_id_type=MESH_ID)
    if start:
        @pl.when(z==0)
        def _(): cp(srcs[0]).start()
        @pl.when(z==3)
        def _(): cp(srcs[1]).start()
    else:
        @pl.when(end)
        def _(): cp(srcs[0]).wait_send()
        @pl.when(jnp.logical_not(end))
        def _(): cp(srcs[0]).wait_recv()

def plane_copies(pairs, sems):
    local,send,recv=sems
    c,z,e=spot()
    me=block_of(0)
    out=[]
    for i,(src,dst) in enumerate(pairs):
        out.append(pltpu.make_async_copy(src.at[me],dst.at[me],local.at[i]))
        for kk in range(1,8):
            out.append(pltpu.make_async_remote_copy(src_ref=src.at[block_of(kk)],dst_ref=dst.at[me],send_sem=send.at[i,kk-1],
                recv_sem=recv.at[i,kk-1],device_id=peer(z,kk),device_id_type=MESH_ID))
    return out

def home_sems():
    return [pltpu.SemaphoreType.DMA((1,)),pltpu.SemaphoreType.DMA((8,)),pltpu.SemaphoreType.DMA((8,)),pltpu.SemaphoreType.DMA((8,))]

def home_barrier():
    c,z,e=spot()
    b=pltpu.get_barrier_semaphore()
    inner=(z==1)|(z==2)
    zo=jnp.where(z<2,0,3); zi=jnp.where(z<2,1,2)
    @pl.when(inner)
    def _():
        for kk in range(8):
            pl.semaphore_signal(b,inc=1,device_id=peer(zo,kk),device_id_type=MESH_ID)
            if kk:
                pl.semaphore_signal(b,inc=1,device_id=peer(z,kk),device_id_type=MESH_ID)
        pl.semaphore_wait(b,15)
    @pl.when(jnp.logical_not(inner))
    def _():
        for kk in range(8):
            pl.semaphore_signal(b,inc=1,device_id=peer(zi,kk),device_id_type=MESH_ID)
        pl.semaphore_wait(b,8)

def home_run(own, ext, dst, sems, start):
    local,send,send2,recv=sems
    c,z,e=spot()
    inner=(z==1)|(z==2)
    zo=jnp.where(z<2,0,3); zi=jnp.where(z<2,1,2)
    me=block_of(0)
    def remote(src,kk,zz,s):
        return pltpu.make_async_remote_copy(src_ref=src.at[block_of(kk)],dst_ref=dst.at[me],send_sem=s.at[kk],recv_sem=recv.at[kk],
            device_id=peer(zz,kk),device_id_type=MESH_ID)
    @pl.when(inner)
    def _():
        lc=pltpu.make_async_copy(own.at[me],dst.at[me],local.at[0])
        if start:
            lc.start()
            for kk in range(8):
                remote(ext,kk,zo,send2).start()
                if kk: remote(own,kk,z,send).start()
        else:
            lc.wait()
            for kk in range(8):
                remote(ext,kk,zo,send2).wait_send()
                if kk:
                    remote(own,kk,z,send).wait()
    if not start:
        @pl.when(jnp.logical_not(inner))
        def _():
            for kk in range(8):
                remote(own,kk,zi,send).wait_recv()

def row_sems():
    return [pltpu.SemaphoreType.DMA((3,)),pltpu.SemaphoreType.DMA((3,))]

def row_copies(src, dst, part, sems):
    send,recv=sems
    c,z,e=spot()
    return [pltpu.make_async_remote_copy(src_ref=src.at[xor4(e,kk),part],dst_ref=dst.at[kk-1],send_sem=send.at[kk-1],recv_sem=recv.at[kk-1],
        device_id=peer(z,kk),device_id_type=MESH_ID) for kk in (1,2,3)]


def add_rows(dst, srcs, step=16):
    @pl.loop(0,dst.shape[0]//step)
    def _(i):
        r=pl.ds(pl.multiple_of(i*step,step),step)
        t=srcs[0][r,:].astype(f32)
        for s in srcs[1:]: t=t+s[r,:].astype(f32)
        dst[r,:]=t.astype(dst.dtype)

class Tail:
    KIND=("g","g","g","g","w","w")
    L2=(1,0,1,0,0,1)
    H=(0,0,1,1,0,0)
    def __init__(self, arrays, T, D, FF):
        self.names=list(arrays); self.arrays=[arrays[n] for n in self.names]
        self.T,self.D,self.FF=T,D,FF
        SG=D//8; self.SG=SG; self.SD=FF//32
        R2=2*SG; self.R2=R2; HW=FF//4
        self.gs=(R2,FF); self.ws=(HW,D)
        self.NR=arrays["msh"].shape[1]
        an=pl.BlockSpec(memory_space=pl.ANY)
        S=jax.ShapeDtypeStruct
        outs={"gate":S((4,SG,FF),bf16),"up":S((4,SG,FF),bf16),"down":S((4,FF//8,D),bf16),
              "dgate":S((SG,FF),f32),"dup":S((SG,FF),f32),"ddown":S((FF//8,D),f32),
              "dqkv":S((SG,3*D),f32),"dwo":S((SG,D),f32),"gains":S((8,D),f32),
              "ra":S((8,CAP,D),bf16),"rb":S((8,CAP,D),bf16)}
        for i in range(3,6):
            outs[f"m{i}"]=S((2*R2,FF) if self.KIND[i]=="g" else (2*HW,D),bf16)
        for i in (0,2,5):
            outs[f"rin{i}"]=S(self.shape(i),bf16)
        for i in range(6):
            outs[f"ro{i}"]=S(self.shape(i),bf16)
        self.onames=list(outs); self.oshape=[outs[n] for n in self.onames]
        self.in_specs=[an]*len(self.names); self.out_specs=[an]*len(self.onames)
        V=pltpu.VMEM; DM=pltpu.SemaphoreType.DMA
        scr={"ga":V((3,)+self.gs,bf16),"wa":V((3,)+self.ws,bf16),
             "gto":V((4,)+self.gs,bf16),"wto":V((2,)+self.ws,bf16),
             "gfin":V((2,)+self.gs,bf16),"wfin":V((2,)+self.ws,bf16),
             "gsw":V((4,SG,FF),bf16),"wsw":V((2,FF//8,D),bf16),
             "atr":V((4,4,SG,D),bf16),"sv":V((4,4,SG,D),bf16),"xr":V((3,4,SG,D),bf16),
             "za":V((4,SG,D),bf16),"zb":V((4,self.NR,128),bf16),
             "gn":V((8,8,D),f32),
             "s_x":DM((3,)),"r_x":DM((3,)),"s_o":DM((6,)),"r_o":DM((6,)),"s_w":DM((6,)),"r_w":DM((6,)),
             "ld":DM((3,)),"st":DM((8,)),"so":DM((2,)),"s_r":DM((3,)),"r_r":DM((3,)),"s_at":DM((16,)),"r_at":DM((16,)),"s_xr":DM((3,)),"r_xr":DM((3,)),
             "s_gn":DM((7,)),"r_gn":DM((7,)),"st2":DM((4,))}
        for nm,sh in (("a",(SG,D)),("b",(self.NR,128))):
            scr.update({"zr"+nm:V((2,)+sh,bf16),"zs"+nm:V((2,)+sh,bf16),"zm"+nm:V((2,)+sh,bf16),"zi"+nm:V(sh,bf16),"zt"+nm:V(sh,bf16),
                "zo"+nm:V(sh,bf16),"fi"+nm:V(sh,bf16),"ag"+nm:V((3,)+sh,bf16),
                "s_z"+nm:DM((4,)),"r_z"+nm:DM((4,)),"s_ag"+nm:DM((3,)),"r_ag"+nm:DM((3,))})
        scr.update({"oa":V((2,SG,D),f32),"og":V((2,SG,FF//4),f32),"od":V((self.SD,D),f32)})
        self.snames=list(scr)+[f"home{i}" for i in range(4)]+[f"plane{i}" for i in range(3)]
        self.scratch=[scr[n] for n in scr]+home_sems()+plane_sems(1)
    def shape(self,i): return self.gs if self.KIND[i]=="g" else self.ws
    def bind(self,ins,outs,scr):
        self.r=dict(zip(self.names,ins)); self.r.update(zip(self.onames,outs)); self.r.update(zip(self.snames,scr))
        c,z,e=spot()
        self.c,self.z,self.e=c,z,e
        self.inner=(z==1)|(z==2); self.outer=jnp.logical_not(self.inner); self.low=z<2
        self.zo=jnp.where(z<2,0,3); self.zi=jnp.where(z<2,1,2); self.zx=3-z
        self.home=[self.r[f"home{i}"] for i in range(4)]
        self.plane=[self.r[f"plane{i}"] for i in range(3)]
    def rcopy(self,src,dst,s,r,dev):
        return pltpu.make_async_remote_copy(src_ref=src,dst_ref=dst,send_sem=s,recv_sem=r,device_id=dev,device_id_type=MESH_ID)
    def barrier(self):
        b=pltpu.get_barrier_semaphore()
        def sig(dev): pl.semaphore_signal(b,inc=1,device_id=dev,device_id_type=MESH_ID)
        for kk in range(1,8): sig(peer(self.z,kk))
        @pl.when(self.inner)
        def _():
            for kk in range(8): sig(peer(self.zo,kk))
            sig(peer(self.zx,0))
            pl.semaphore_wait(b,16)
        @pl.when(self.outer)
        def _():
            for kk in range(8): sig(peer(self.zi,kk))
            pl.semaphore_wait(b,15)
    def across(self,i,src=None):
        src=self.r["wa0"] if i==4 and src is None else self.r[f"far{i}"] if src is None else src
        return self.rcopy(src,self.r[f"m{i}"],self.r["s_x"].at[i-3],self.r["r_x"].at[i-3],peer(self.zx,0))
    def across_start(self):
        @pl.when(self.inner)
        def _():
            self.across(3).start()
            @pl.when(self.low)
            def _(): self.across(4,self.r["wa1"]).start()
            @pl.when(jnp.logical_not(self.low))
            def _(): self.across(4,self.r["wa0"]).start()
            self.across(5).start()
    def start(self):
        self.barrier()
        home_run(self.r["hown"],self.r["hext"],self.r["ra"],self.home,True)
        ld=pltpu.make_async_copy(self.r["msh"],self.r["zb"],self.r["st2"].at[0])
        ld.start(); ld.wait()
        self.z_inward("b")
        self.across_start()
        for i in range(3): self.stage1(i)
        self.rin_start()
        for cp in plane_copies([(self.r["rbs"],self.r["rb"])],self.plane): cp.start()
    def load(self,pairs):
        cs=[]
        for k,(s,d) in enumerate(pairs):
            both=[pltpu.make_async_copy(x,d,self.r["ld"].at[k]) for x in (s if isinstance(s,tuple) else (s,))]
            if len(both)==2:
                pl.when(self.low)(lambda: both[0].start())
                pl.when(jnp.logical_not(self.low))(lambda: both[1].start())
            else: both[0].start()
            cs.append(both[0])
        for c in cs: c.wait()
    def near(self,i,which):
        if self.KIND[i]=="g":
            return self.r[f"n{which}{i}"]
        n=self.ws[0]
        x="a" if i==4 else "b"
        return tuple(self.r[f"w{x}{h}"].at[pl.ds(0 if which=="o" else n,n)] for h in (0,1))
    def rin(self,k,src=None):
        i=(0,2,5)[k]
        src=self.r[f"rin{i}"] if src is None else src
        return self.rcopy(src,self.r[f"rin{i}"],self.r["s_r"].at[k],self.r["r_r"].at[k],peer(self.zi,0))
    def rin_start(self):
        @pl.when(self.outer)
        def _():
            for k,i in enumerate((0,2)): self.rin(k,self.near(i,"i")).start()
            lo,hi=self.near(5,"i")
            @pl.when(self.low)
            def _(): self.rin(2,lo).start()
            @pl.when(jnp.logical_not(self.low))
            def _(): self.rin(2,hi).start()
    def parts_of(self,i):
        k="g" if self.KIND[i]=="g" else "w"
        idx=i if k=="g" else i-4
        return k,idx,self.shape(i)[0],self.L2[i]==1
    def ro(self,i):
        k,idx,n,b=self.parts_of(i)
        return self.rcopy(self.r[k+"to"].at[idx],self.r[f"ro{i}"],self.r["s_o"].at[i],self.r["r_o"].at[i],peer(self.zo,0))
    def stage1(self,i):
        k,idx,n,b=self.parts_of(i)
        buf=self.r[k+"a"]
        @pl.when(self.inner)
        def _():
            if i>=3: self.across(i).wait()
            self.load([(self.r[f"m{i}"].at[pl.ds(0,n)],buf.at[0]),(self.near(i,"o"),buf.at[1])])
            add_rows(self.r[k+"to"].at[idx],[buf.at[0],buf.at[1]])
            self.ro(i).start()
    def piece(self,i):
        k,idx,n,b=self.parts_of(i)
        slot=idx%2; buf=self.r[k+"a"]; fin=self.r[k+"fin"]
        @pl.when(self.inner)
        def _():
            if b: self.rin((0,2,5).index(i)).wait_recv()
            self.load([(self.r[f"m{i}"].at[pl.ds(n,n)],buf.at[0]),(self.near(i,"i"),buf.at[1])]+([(self.r[f"rin{i}"],buf.at[2])] if b else []))
            add_rows(fin.at[slot],[buf.at[q] for q in range(3 if b else 2)])
        @pl.when(self.outer)
        def _():
            self.ro(i).wait_recv()
            self.load([(self.r[f"ro{i}"],buf.at[0])]+([(self.near(i,"o"),buf.at[1])] if b else []))
            add_rows(fin.at[slot],[buf.at[q] for q in range(2 if b else 1)])
        self.swap(i).start()
        hn=n//2
        for cp in self.store(i,fin.at[slot,pl.ds(pl.multiple_of(self.c*hn,hn),hn)],self.c,False): cp.start()
    def swap(self,i):
        k,idx,n,b=self.parts_of(i); hn=n//2
        return self.rcopy(self.r[k+"fin"].at[idx%2,pl.ds(pl.multiple_of((1-self.c)*hn,hn),hn)],self.r[k+"sw"].at[idx],self.r["s_w"].at[i],self.r["r_w"].at[i],peer(self.z,4))
    def store(self,i,src,core,theirs):
        ex=2*core+self.L2[i]; k,idx,n,b=self.parts_of(i); slot=idx%2
        if k=="g":
            hc=self.FF//2; h=self.H[i]
            return [pltpu.make_async_copy(src.at[:,pl.ds(t*hc,hc)],self.r[nm].at[ex,:,pl.ds(h*hc,hc)],self.r["so"].at[t] if theirs else self.r["st"].at[2*slot+t])
                    for t,nm in enumerate(("gate","up"))]
        return [pltpu.make_async_copy(src,self.r["down"].at[ex],self.r["so"].at[0] if theirs else self.r["st"].at[4+slot])]
    def other_half(self,i):
        k,idx,n,b=self.parts_of(i); hn=n//2
        for cp in self.store(i,self.r[k+"fin"].at[idx%2,pl.ds(pl.multiple_of(self.c*hn,hn),hn)],self.c,False): cp.wait()
        self.swap(i).wait()
        cps=self.store(i,self.r[k+"sw"].at[idx],1-self.c,True)
        for cp in cps: cp.start()
        for cp in cps: cp.wait()
    def zsem(self,nm,k): return self.r["s_z"+nm].at[k],self.r["r_z"+nm].at[k]
    def zc(self,nm,k):
        r=self.r; M=r["z"+nm]
        src,dst,dev={0:(M.at[pl.ds(0,2)],r["zr"+nm],peer(self.zi,0)),1:(M.at[2],r["zi"+nm],peer(self.zi,0)),
            2:(r["zs"+nm],r["zm"+nm],peer(self.zx,0)),3:(r["zt"+nm],r["zo"+nm],peer(self.zo,0))}[k]
        s,v=self.zsem(nm,k)
        return self.rcopy(src,dst,s,v,dev)
    def z_inward(self,nm):
        @pl.when(self.outer)
        def _():
            self.zc(nm,0).start(); self.zc(nm,1).start()
    def z_across(self,nm):
        r=self.r
        @pl.when(self.inner)
        def _():
            self.zrecv(nm,0)
            for k in (0,1): add_rows(r["zs"+nm].at[k],[r["z"+nm].at[k],r["zr"+nm].at[k]])
            self.zc(nm,2).start()
    def zrecv(self,nm,k):
        r=self.r; M=r["z"+nm]
        dst={0:r["zr"+nm],1:r["zi"+nm],2:r["zm"+nm],3:r["zo"+nm]}[k]
        src={0:M.at[pl.ds(0,2)],1:M.at[2],2:r["zs"+nm],3:r["zt"+nm]}[k]
        s,v=self.zsem(nm,k)
        dev={0:peer(self.zo,0),1:peer(self.zo,0),2:peer(self.zx,0),3:peer(self.zi,0)}[k]
        self.rcopy(src,dst,s,v,dev).wait_recv()
    def z_last(self,nm):
        r=self.r; M=r["z"+nm]
        @pl.when(self.inner)
        def _():
            self.zrecv(nm,2)
            add_rows(r["zt"+nm],[M.at[3],r["zm"+nm].at[0]])
            self.zc(nm,3).start()
            self.zrecv(nm,1)
            add_rows(r["fi"+nm],[M.at[2],r["zm"+nm].at[1],r["zi"+nm]])
            self.zc(nm,2).wait_send()
        @pl.when(self.outer)
        def _():
            self.zrecv(nm,3)
            add_rows(r["fi"+nm],[M.at[3],r["zo"+nm]])
            self.zc(nm,0).wait_send(); self.zc(nm,1).wait_send()
        for kk in (1,2,3): self.agc(nm,kk).start()
    def agc(self,nm,kk):
        r=self.r
        return self.rcopy(r["fi"+nm],r["ag"+nm].at[kk-1],r["s_ag"+nm].at[kk-1],r["r_ag"+nm].at[kk-1],peer(self.z,kk))
    def z_out(self,nm):
        r=self.r
        for kk in range(4):
            if kk: self.agc(nm,kk).wait()
            a=xor4(self.e,kk)
            src=r["fi"+nm] if kk==0 else r["ag"+nm].at[kk-1]
            if nm=="a":
                oa=r["oa"].at[kk%2]
                add_rows(oa,[src])
                cols=pl.ds(pl.multiple_of(jnp.minimum(a,2)*self.D,self.D),self.D)
                @pl.when(a<3)
                def _():
                    cp=pltpu.make_async_copy(oa,r["dqkv"].at[:,cols],r["st2"].at[0]); cp.start(); cp.wait()
                @pl.when(a==3)
                def _():
                    cp=pltpu.make_async_copy(oa,r["dwo"],r["st2"].at[0]); cp.start(); cp.wait()
            else:
                SG,SD,Q=self.SG,self.SD,self.FF//4; nb=Q//128
                for t in range(2):
                    for b in range(nb):
                        r["og"][t,:,b*128:(b+1)*128]=src[(t*nb+b)*SG:(t*nb+b+1)*SG,:].astype(f32)
                off=2*nb*SG
                for b in range(self.D//128):
                    r["od"][:,b*128:(b+1)*128]=src[off+b*SD:off+(b+1)*SD,:].astype(f32)
                cols=pl.ds(pl.multiple_of(a*Q,Q),Q)
                cps=[pltpu.make_async_copy(r["og"].at[0],r["dgate"].at[:,cols],r["st2"].at[0]),
                     pltpu.make_async_copy(r["og"].at[1],r["dup"].at[:,cols],r["st2"].at[1]),
                     pltpu.make_async_copy(r["od"],r["ddown"].at[pl.ds(pl.multiple_of(a*SD,SD),SD),:],r["st2"].at[2])]
                for cp in cps: cp.start()
                for cp in cps: cp.wait()
    def rows_of(self,core,zr):
        return pl.ds(pl.multiple_of(2*self.SG*shard_of(zr)+self.SG*core,self.SG),self.SG)
    def at_swap(self,GS):
        return [self.rcopy(GS.at[i,self.rows_of(1-self.c,zr)],self.r["atr"].at[i,zr],self.r["s_at"].at[4*i+zr],self.r["r_at"].at[4*i+zr],peer(self.z,4))
                for i in range(4) for zr in range(4)]
    def at_xy(self,kk):
        return self.rcopy(self.r["sv"].at[xor4(self.e,kk)],self.r["xr"].at[kk-1],self.r["s_xr"].at[kk-1],self.r["r_xr"].at[kk-1],peer(self.z,kk))
    def gcopy(self,k,dev):
        return self.rcopy(self.r["gn"].at[0] ,self.r["gn"].at[k+1],self.r["s_gn"].at[k],self.r["r_gn"].at[k],dev)
    def middle(self):
        self.z_across("b")
        self.stage1(3)
    def finish(self,GS,gg):
        r=self.r; gn=r["gn"]
        sw=self.at_swap(GS)
        for cp in sw: cp.start()
        row=lax.broadcasted_iota(jnp.int32,(8,self.D),0)
        ld=pltpu.make_async_copy(r["fgg"],gn.at[7],r["st2"].at[1]); ld.start(); ld.wait()
        gn[0]=jnp.where(row==0,gg,jnp.where(row==1,gn[7],0.0))
        self.gcopy(0,peer(self.z,4)).start()
        self.piece(0)
        for cp in sw: cp.wait()
        for i in range(4):
            for zr in range(4):
                add_rows(r["sv"].at[i,zr],[GS.at[i,self.rows_of(self.c,zr)],r["atr"].at[i,zr]])
        for kk in (1,2,3): self.at_xy(kk).start()
        self.gcopy(0,peer(self.z,4)).wait()
        gn[0]=gn[0]+gn[1]
        for kk in (1,2,3): self.gcopy(kk,peer(self.z,kk)).start()
        self.z_last("b")
        self.piece(1)
        self.stage1(4)
        self.other_half(0)
        self.piece(2)
        self.other_half(1)
        for kk in (1,2,3): self.gcopy(kk,peer(self.z,kk)).wait()
        gn[0]=(gn[0]+gn[2])+(gn[3]+gn[4])
        @pl.when(self.outer)
        def _(): self.gcopy(4,peer(self.zi,0)).start()
        for kk in (1,2,3): self.at_xy(kk).wait()
        for zr in range(4): add_rows(r["za"].at[zr],[r["sv"].at[self.e,zr]]+[r["xr"].at[k,zr] for k in range(3)])
        self.z_inward("a")
        self.z_out("b")
        @pl.when(self.inner)
        def _():
            self.gcopy(4,peer(self.zo,0)).wait_recv()
            gn[0]=gn[0]+gn[5]
            self.gcopy(5,peer(self.zx,0)).start()
        self.z_across("a")
        self.stage1(5)
        self.piece(3)
        @pl.when(self.inner)
        def _():
            self.gcopy(5,peer(self.zx,0)).wait()
            gn[0]=gn[0]+gn[6]
            self.gcopy(6,peer(self.zo,0)).start()
        @pl.when(self.outer)
        def _():
            self.gcopy(4,peer(self.zi,0)).wait_send()
            self.gcopy(6,peer(self.zi,0)).wait_recv()
            gn[0]=gn[7]
        gcp=pltpu.make_async_copy(gn.at[0],r["gains"],r["st2"].at[3]); gcp.start()
        self.other_half(2)
        self.z_last("a")
        self.piece(4)
        self.other_half(3)
        self.z_out("a")
        self.piece(5)
        self.other_half(4); self.other_half(5)
        gcp.wait()
        @pl.when(self.inner)
        def _():
            self.gcopy(6,peer(self.zo,0)).wait_send()
            for i in range(6): self.ro(i).wait_send()
            self.zc("a",3).wait_send(); self.zc("b",3).wait_send()
        @pl.when(self.outer)
        def _():
            for k in range(3): self.rin(k).wait_send()
        home_run(r["hown"],r["hext"],r["ra"],self.home,False)
        for cp in plane_copies([(r["rbs"],r["rb"])],self.plane): cp.wait()

f32=jnp.float32; bf16=jnp.bfloat16
def nn(a,b): return lax.dot_general(a,b,(((1,),(0,)),((),())),preferred_element_type=f32)
def nt(a,b): return lax.dot_general(a,b,(((1,),(1,)),((),())),preferred_element_type=f32)
def tn(a,b): return lax.dot_general(a,b,(((0,),(0,)),((),())),preferred_element_type=f32)
EPS=1e-6
E=16; CAP=120
HD=64; GH=4; GW=GH*HD; QC=256
def lane_head(shape):
    return lax.broadcasted_iota(jnp.int32,shape,1)//HD
def swap_half(x):
    w=x.shape[1]
    first=(lax.broadcasted_iota(jnp.int32,x.shape,1)%HD)<HD//2
    return jnp.where(first,pltpu.roll(x,w-HD//2,1),pltpu.roll(x,HD//2,1))
def wide(t):
    return jnp.concatenate([t,t],axis=1)
def inv_rms(v):
    return lax.rsqrt(jnp.mean(v*v,axis=1,keepdims=True)+EPS)

def attn_fwd(tokens, prefix, again, wqkv, wo, fgain, cosw, sinw, rows=None, sout=None):
    T,D=tokens.shape
    ng=D//GW; nq=T//QC
    fused=rows is not None
    NS=E*CAP; CH=480
    def kernel(pre,tok,ag,fg,wq,wk,wv,wor,cw,sw,*rest):
        if fused:
            rowr,so,qo,ko,vo,atto,lseo,stateo,ntwoo,xo,sia,sib,normed,bias,q4,k4,vT,OT,acc,*sems=rest
        else:
            qo,ko,vo,atto,lseo,stateo,ntwoo,normed,bias,q4,k4,vT,OT,acc=rest
        g=pl.program_id(0)
        @pl.when(g==0)
        def _():
            if fused:
                plane_barrier()
                for cpy in plane_copies([(so.at[0],sia),(so.at[1],sib)],sems): cpy.start()
            for c in range(nq):
                r=slice(c*QC,(c+1)*QC)
                x=tok[r,:].astype(f32)
                normed[r,:]=(x*inv_rms(x)*ag[...]).astype(bf16)
                j=lax.broadcasted_iota(jnp.int32,(T,QC),0)
                i=lax.broadcasted_iota(jnp.int32,(T,QC),1)+c*QC
                bias[c]=jnp.where((j<=i)|(j<pre[0]),0.0,-1e30)
        for c in range(nq):
            r=slice(c*QC,(c+1)*QC)
            n=normed[r,:]
            C=wide(cw[r,:]); S=wide(sw[r,:])
            q=nn(n,wq[...]); k=nn(n,wk[...]); v=nn(n,wv[...])
            qb=((q*C+swap_half(q)*S).astype(bf16)).astype(f32)*(HD**-0.5)
            qb=qb.astype(bf16)
            kb=(k*C+swap_half(k)*S).astype(bf16)
            q4[r,:]=qb; qo[r,:]=qb
            k4[r,:]=kb; ko[r,:]=kb
            vo[r,:]=v.astype(bf16)
            vT[:,r]=v.T.astype(bf16)
        lh=lane_head((QC,GW))
        @pl.loop(0,GH)
        def _(h):
            hr=pl.ds(pl.multiple_of(h*HD,HD),HD)
            for c in range(nq):
                r=slice(c*QC,(c+1)*QC)
                qm=jnp.where(lh==h,q4[r,:],jnp.zeros((),bf16))
                st=nt(k4[...],qm)+bias[c]
                m=jnp.max(st,axis=0,keepdims=True)
                p=jnp.exp(st-m)
                l=jnp.sum(p,axis=0,keepdims=True)
                ot=nn(vT[hr,:],p.astype(bf16))
                OT[c,hr,:]=ot*(1.0/l)
                lseo[0,pl.ds(h,1),r]=m+jnp.log(l)
        for c in range(nq):
            r=slice(c*QC,(c+1)*QC)
            a=OT[c].T.astype(bf16)
            atto[r,:]=a
            o=nn(a,wor[...])
            @pl.when(g==0)
            def _(): acc[r,:]=o+tok[r,:].astype(f32)
            @pl.when(g>0)
            def _(): acc[r,:]+=o
        @pl.when(g==ng-1)
        def _():
            for c in range(nq):
                r=slice(c*QC,(c+1)*QC)
                st=acc[r,:]
                stateo[r,:]=st
                ntwoo[r,:]=(st*inv_rms(st)*fg[...]).astype(bf16)
            if fused:
                for i in range(NS//CH):
                    si=lax.broadcasted_iota(jnp.int32,(CH,T),0)+i*CH
                    d=jnp.where((si==rowr[0:1,:])|(si==rowr[1:2,:]),1.0,0.0).astype(bf16)
                    xo[i*CH:(i+1)*CH,:]=nn(d,ntwoo[...]).astype(bf16)
                for cpy in plane_copies([(so.at[0],sia),(so.at[1],sib)],sems): cpy.wait()
    full=lambda s: pl.BlockSpec(s,lambda g:(0,)*len(s))
    col=lambda off: pl.BlockSpec((D,GW),lambda g,off=off:(0,g+off))
    tcol=pl.BlockSpec((T,GW),lambda g:(0,g))
    return pl.pallas_call(kernel,grid=(ng,),
      in_specs=[pl.BlockSpec(memory_space=pltpu.SMEM),full((T,D)),full((1,D)),full((1,D)),col(0),col(ng),col(2*ng),pl.BlockSpec((GW,D),lambda g:(g,0)),full((T,128)),full((T,128))]+([full((8,T)),pl.BlockSpec(memory_space=pl.ANY)] if fused else []),
      out_specs=[tcol,tcol,tcol,tcol,pl.BlockSpec((1,8,T),lambda g:(g,0,0)),full((T,D)),full((T,D))]+([full((NS,D))]+[pl.BlockSpec(memory_space=pl.ANY)]*2 if fused else []),
      out_shape=[jax.ShapeDtypeStruct((T,D),bf16)]*4+[jax.ShapeDtypeStruct((ng,8,T),f32),jax.ShapeDtypeStruct((T,D),f32),jax.ShapeDtypeStruct((T,D),bf16)]+([jax.ShapeDtypeStruct((NS,D),bf16),*[jax.ShapeDtypeStruct((8,CAP,D),bf16)]*2] if fused else []),
      scratch_shapes=[pltpu.VMEM((T,D),bf16),pltpu.VMEM((nq,T,QC),f32),pltpu.VMEM((T,GW),bf16),pltpu.VMEM((T,GW),bf16),pltpu.VMEM((GW,T),bf16),pltpu.VMEM((nq,GW,QC),f32),pltpu.VMEM((T,D),f32)]+(plane_sems(2) if fused else []),
      compiler_params=pltpu.CompilerParams(vmem_limit_bytes=56<<20,dimension_semantics=("arbitrary",),**(dict(collective_id=0,has_side_effects=True) if fused else {})),
      cost_estimate=pl.CostEstimate(flops=2*T*D*4*D+4*T*T*D,bytes_accessed=16<<20,transcendentals=12*T*T),
      name="attn_fwd")(prefix,tokens,again[None],fgain[None],wqkv,wqkv,wqkv,wo,cosw,sinw,*([rows,sout] if fused else []))

def attn_bwd(sgrad, prefix, tokens, again, wqkv, wo, cosw, sinw, q, k, v, att, lse, tail=None):
    T,D=tokens.shape
    ng=D//GW; nq=T//QC
    fast=tail is not None
    def kernel(pre,sg,tok,ag,wq,wk,wv,wor,cw,sw,qr,kr,vr,attr,lser,*rest):
        if fast:
            ni,no=len(tail.in_specs),len(tail.out_specs)
            tgo,ggo=rest[ni:ni+2]
            tins,touts=rest[:ni],rest[ni+2:ni+2+no]
            normed,normedT,bg,bias,dO,kT,PB,DS,dv,dk,dqT,drow,acc,GS,*tscr=rest[ni+2+no:]
            tail.bind(tins,touts,tscr)
        else:
            tgo,ggo,gq,gk,gv,gwo,normed,normedT,bg,bias,dO,kT,PB,DS,dv,dk,dqT,drow,acc=rest
        g=pl.program_id(0)
        if fast:
            @pl.when(g==0)
            def _():
                tail.start()
            @pl.when(g==ng-1)
            def _():
                tail.middle()
        @pl.when(g==0)
        def _():
            for c in range(nq):
                r=slice(c*QC,(c+1)*QC)
                x=tok[r,:].astype(f32)
                n=x*inv_rms(x)*ag[...]
                normedT[:,r]=n.T.astype(bf16)
                bg[r,:]=sg[r,:].astype(bf16)
                j=lax.broadcasted_iota(jnp.int32,(T,QC),0)
                i=lax.broadcasted_iota(jnp.int32,(T,QC),1)+c*QC
                bias[c]=jnp.where((j<=i)|(j<pre[0]),0.0,-1e30)
        hmask=(lax.broadcasted_iota(jnp.int32,(8,GW),0)==lane_head((8,GW))).astype(f32)
        for c in range(nq):
            r=slice(c*QC,(c+1)*QC)
            d=nt(bg[r,:],wor[...]).astype(bf16)
            dO[r,:]=d
            a=attr[r,:].astype(f32)
            drow[:,r]=lax.dot_general(hmask,d.astype(f32)*a,(((1,),(1,)),((),())),preferred_element_type=f32,precision=lax.Precision.HIGHEST)
            kT[:,r]=kr[r,:].astype(f32).T.astype(bf16)
        gwv=tn(attr[...],bg[...]).astype(bf16)
        if fast:
            GS[3,pl.ds(pl.multiple_of(g*GW,GW),GW),:]=gwv
        else:
            gwo[...]=gwv
        dv[...]=jnp.zeros_like(dv); dk[...]=jnp.zeros_like(dk)
        lh=lane_head((QC,GW)); lhT=lane_head((T,GW))
        @pl.loop(0,GH)
        def _(h):
            hr=pl.ds(pl.multiple_of(h*HD,HD),HD)
            zero=jnp.zeros((),bf16)
            for c in range(nq):
                r=slice(c*QC,(c+1)*QC)
                qm=jnp.where(lh==h,qr[r,:],zero)
                dOm=jnp.where(lh==h,dO[r,:],zero)
                st=nt(kr[...],qm)+bias[c]
                p=jnp.exp(st-lser[0,pl.ds(h,1),r])
                PB[:,r]=p.astype(bf16)
                dp=nt(vr[...],dOm)
                DS[:,r]=(p*(dp-drow[pl.ds(h,1),r])).astype(bf16)
            dv[...]+=nn(PB[...],jnp.where(lhT==h,dO[...],zero))
            dk[...]+=nn(DS[...],jnp.where(lhT==h,qr[...],zero))
            dqT[hr,:]=nn(kT[hr,:],DS[...])
        for c in range(nq):
            r=slice(c*QC,(c+1)*QC)
            C=wide(cw[r,:]); S=wide(sw[r,:])
            dq=dqT[:,r].T*(HD**-0.5)
            dq=dq*C-swap_half(dq)*S
            dkk=dk[r,:]
            dkk=dkk*C-swap_half(dkk)*S
            a=dq.astype(bf16); b=dkk.astype(bf16); e=dv[r,:].astype(bf16)
            PB[r,0:GW]=a; PB[r,GW:2*GW]=b; PB[r,2*GW:3*GW]=e
            o=nt(a,wq[...])+nt(b,wk[...])+nt(e,wv[...])
            @pl.when(g==0)
            def _(): acc[r,:]=o
            @pl.when(g>0)
            def _(): acc[r,:]+=o
        for i in range(3):
            gval=nn(normedT[...],PB[:,i*GW:(i+1)*GW]).astype(bf16)
            if fast:
                GS[i,:,pl.ds(pl.multiple_of(g*GW,GW),GW)]=gval
            else:
                (gq,gk,gv)[i][...]=gval
        @pl.when(g==ng-1)
        def _():
            gg=jnp.zeros((1,D),f32)
            for c in range(nq):
                r=slice(c*QC,(c+1)*QC)
                x=tok[r,:].astype(f32)
                inv=inv_rms(x); u=x*inv
                ngd=acc[r,:]
                gg=gg+jnp.sum(ngd*u,axis=0,keepdims=True)
                w=ngd*ag[...]
                tgo[r,:]=(sg[r,:]+inv*(w-u*jnp.mean(w*u,axis=1,keepdims=True))).astype(bf16)
            ggo[...]=jnp.broadcast_to(gg,(8,D))
            if fast:
                tail.finish(GS,gg)
    full=lambda s: pl.BlockSpec(s,lambda g:(0,)*len(s),pipeline_mode=pl.Buffered(1))
    col=lambda off: pl.BlockSpec((D,GW),lambda g,off=off:(0,g+off))
    tcol=pl.BlockSpec((T,GW),lambda g:(0,g))
    if fast:
        outs=tail.out_specs; oshape=tail.oshape
        extra=[pltpu.VMEM((4,D,D),bf16)]+tail.scratch
    else:
        outs=[tcol,tcol,tcol,pl.BlockSpec((GW,D),lambda g:(g,0))]
        oshape=[jax.ShapeDtypeStruct((D,D),bf16)]*4
        extra=[]
    rowb=pl.BlockSpec((GW,D),lambda g:(g,0))
    return pl.pallas_call(kernel,grid=(ng,),
      in_specs=[pl.BlockSpec(memory_space=pltpu.SMEM)]+[full((T,D)),full((T,D)),full((1,D)),col(0),col(ng),col(2*ng),rowb,full((T,128)),full((T,128)),tcol,tcol,tcol,tcol,pl.BlockSpec((1,8,T),lambda g:(g,0,0))]+(tail.in_specs if fast else []),
      out_specs=[full((T,D)),full((8,D))]+outs,
      out_shape=[jax.ShapeDtypeStruct((T,D),bf16),jax.ShapeDtypeStruct((8,D),f32)]+oshape,
      scratch_shapes=[pltpu.VMEM((T,D),bf16),pltpu.VMEM((D,T),bf16),pltpu.VMEM((T,D),bf16),pltpu.VMEM((nq,T,QC),f32),pltpu.VMEM((T,GW),bf16),pltpu.VMEM((GW,T),bf16),
        pltpu.VMEM((T,T),bf16),pltpu.VMEM((T,T),bf16),pltpu.VMEM((T,GW),f32),pltpu.VMEM((T,GW),f32),pltpu.VMEM((GW,T),f32),pltpu.VMEM((8,T),f32),pltpu.VMEM((T,D),f32)]+extra,
      compiler_params=pltpu.CompilerParams(vmem_limit_bytes=63<<20,dimension_semantics=("arbitrary",),**(dict(collective_id=5,has_side_effects=True) if fast else {})),
      cost_estimate=pl.CostEstimate(flops=2*T*D*8*D+10*T*T*D,bytes_accessed=24<<20,transcendentals=12*T*T),
      name="attn_bwd")(prefix,sgrad,tokens,again[None],wqkv,wqkv,wqkv,wo,cosw,sinw,q,k,v,att,lse,*(tail.arrays if fast else ()))


def make_ffn(parts, G, L, cap, D, FF, FB, chunk, out_dt):
    R=parts*G*cap
    nf=FF//FB
    def kernel(*refs):
        xs=refs[:parts]; ss=refs[parts:2*parts]
        wg,wu,wd=refs[2*parts:2*parts+3]
        o=2*parts+3
        res=refs[o:o+parts]; dgr=refs[o+parts:o+2*parts]
        gG,gU,gD=refs[o+2*parts:o+2*parts+3]
        X,S,H,GB,UB,AR,AD=refs[o+2*parts+3:]
        f=pl.program_id(1)
        @pl.when(f==0)
        def _():
            for p in range(parts):
                for g in range(G):
                    r=(p*G+g)*cap
                    X[r:r+cap,:]=xs[p][g,0]
                    S[r:r+cap,:]=ss[p][g,0]
        @pl.loop(0,R//chunk)
        def _(i):
            rows=pl.ds(pl.multiple_of(i*chunk,chunk),chunk)
            x=X[rows,:]; s=S[rows,:]
            gate=nn(x,wg[0]); up=nn(x,wu[0]); hg=nt(s,wd[0])
            sig=1.0/(1.0+jnp.exp(-gate))
            sil=gate*sig
            h=(sil*up).astype(bf16)
            gb=(hg*up*(sig*(1.0+gate*(1.0-sig)))).astype(bf16)
            ub=(hg*sil).astype(bf16)
            H[rows,:]=h; GB[rows,:]=gb; UB[rows,:]=ub
            r=nn(h,wd[0]); d=nt(gb,wg[0])+nt(ub,wu[0])
            @pl.when(f==0)
            def _():
                AR[rows,:]=r; AD[rows,:]=d
            @pl.when(f>0)
            def _():
                AR[rows,:]+=r; AD[rows,:]+=d
        gG[0]=tn(X[...],GB[...]).astype(bf16)
        gU[0]=tn(X[...],UB[...]).astype(bf16)
        gD[0]=tn(H[...],S[...]).astype(bf16)
        @pl.when(f==nf-1)
        def _():
            for p in range(parts):
                for g in range(G):
                    r=(p*G+g)*cap
                    res[p][g,0]=AR[r:r+cap,:].astype(out_dt)
                    dgr[p][g,0]=AD[r:r+cap,:].astype(out_dt)
    rowspec=pl.BlockSpec((G,1,cap,D),lambda l,f:(0,l,0,0))
    wspec=pl.BlockSpec((1,D,FB),lambda l,f:(l,0,f))
    wdspec=pl.BlockSpec((1,FB,D),lambda l,f:(l,f,0))
    call=pl.pallas_call(kernel,
      out_shape=[jax.ShapeDtypeStruct((G,L,cap,D),out_dt)]*(2*parts)+[jax.ShapeDtypeStruct((L,D,FF),bf16)]*2+[jax.ShapeDtypeStruct((L,FF,D),bf16)],
      grid=(L,nf),
      in_specs=[rowspec]*(2*parts)+[wspec,wspec,wdspec],
      out_specs=[rowspec]*(2*parts)+[wspec,wspec,wdspec],
      scratch_shapes=[pltpu.VMEM((R,D),bf16)]*2+[pltpu.VMEM((R,FB),bf16)]*3+[pltpu.VMEM((R,D),f32)]*2,
      compiler_params=pltpu.CompilerParams(vmem_limit_bytes=60<<20,dimension_semantics=("arbitrary","arbitrary")),
      cost_estimate=pl.CostEstimate(flops=2*9*R*D*FF*L,bytes_accessed=L*(6*D*FF*2+4*R*D*2),transcendentals=R*FF*L),
      name="ffn")
    return call


def ffn_rows(x,s,wg,wu,wd,H,GB,UB,rows):
    gate=nn(x,wg); up=nn(x,wu); hg=nt(s,wd)
    sig=1.0/(1.0+jnp.exp(-gate))
    sil=gate*sig
    h=(sil*up).astype(bf16)
    gb=(hg*up*(sig*(1.0+gate*(1.0-sig)))).astype(bf16)
    ub=(hg*sil).astype(bf16)
    H[rows,:]=h; GB[rows,:]=gb; UB[rows,:]=ub
    return nn(h,wd),nt(gb,wg)+nt(ub,wu)

def expert_ffn(deps, l2, xs, ss, wg, wu, wd, f0, nf, prev=(), carry=None, dense=None, inw=None, cid=None, FB=512, chunk=480):
    n=len(xs); RG,D=xs[0].shape; FF=wg.shape[2]; R=n*RG; HB=2*FB; ng=nf//2
    SR=D//4; np_=len(prev); nc=0 if carry is None else 1; nd=0 if dense is None else 1
    part=pl.ds(dense[1],dense[2]) if nd else None
    nx=len(deps); nz=0 if inw is None else 2
    def kernel(*refs):
        refs=refs[nx:]
        xr=refs[:n]; sr=refs[n:2*n]; wgr,wur,wdr=refs[2*n:2*n+3]; o=2*n+3
        pv=refs[o:o+np_]; o+=np_
        csrc=refs[o:o+nc]; o+=nc
        dsrc=refs[o:o+nd]; o+=nd
        zsrc=refs[o:o+nz]; o+=nz
        res=refs[o:o+n]; dgr=refs[o+n:o+2*n]; o+=2*n
        gus=[refs[o+3*q:o+3*q+3] for q in range(ng)]; o+=3*ng
        dws=refs[o:o+ng]; o+=ng
        cdst=refs[o:o+nc]; o+=nc
        ddst=refs[o:o+nd]; o+=nd
        zdst=refs[o:o+nz//2]; o+=nz//2
        XT,XN,H,GB,UB,AR,AD=refs[o:o+7]; sems=refs[o+7:]
        f=pl.program_id(0)
        def copies():
            return (plane_copies([(csrc[0],cdst[0])],sems[2*nd+nz:]) if nc else [])+(row_copies(dsrc[0],ddst[0],part,sems[nz:nz+2]) if nd else [])
        if nc or nd or nz:
            @pl.when(f==0)
            def _():
                if nz:
                    plane_z_barrier()
                    inward_run(zsrc,zdst[0],sems[:2],True)
                else:
                    plane_barrier()
                for cpy in copies(): cpy.start()
        @pl.when(f==0)
        def _():
            for a in range(n):
                for b in range(RG//chunk):
                    XN[...]=xr[a][b*chunk:(b+1)*chunk,:].astype(f32).T.astype(bf16)
                    for q in range(4):
                        XT[a*(RG//chunk)+b,q*SR:(q+1)*SR,:]=XN[pl.ds(pl.multiple_of(shard_of(q)*SR,SR),SR),:]
        for a in range(n):
            @pl.loop(0,RG//chunk)
            def _(i):
                src=pl.ds(pl.multiple_of(i*chunk,chunk),chunk)
                rows=pl.ds(pl.multiple_of(a*RG+i*chunk,chunk),chunk)
                r,d=ffn_rows(xr[a][src,:],sr[a][src,:],wgr[0],wur[0],wdr[0],H,GB,UB,rows)
                @pl.when(f==0)
                def _():
                    if np_:
                        AR[rows,:]=r+pv[a][src,:].astype(f32); AD[rows,:]=d+pv[n+a][src,:].astype(f32)
                    else:
                        AR[rows,:]=r; AD[rows,:]=d
                if nf>2:
                    @pl.when((f>0)&(f<nf-1))
                    def _():
                        AR[rows,:]+=r; AD[rows,:]+=d
                @pl.when(f==nf-1)
                def _():
                    res[a][src,:]=(AR[rows,:]+r).astype(bf16); dgr[a][src,:]=(AD[rows,:]+d).astype(bf16)
        for t,Y in enumerate((GB,UB)):
            gv=None
            for b in range(R//chunk):
                p=nn(XT[b],Y[b*chunk:(b+1)*chunk,:])
                gv=p if gv is None else gv+p
            gv=gv.astype(bf16)
            cols=pl.ds(pl.multiple_of(t*HB+lax.rem(f,2)*FB,FB),FB)
            for q in range(ng):
                def put(gf=gus[q][0],gi=gus[q][1],go=gus[q][2],gv=gv,cols=cols):
                    gf[:,cols]=gv[0:2*SR]; gi[:,cols]=gv[2*SR:3*SR]; go[:,cols]=gv[3*SR:4*SR]
                if ng==1: put()
                else: pl.when(lax.div(f,2)==q)(put)
        dv=None
        for a in range(n):
            t=tn(H[a*RG:(a+1)*RG,:],sr[a][...])
            dv=t if dv is None else dv+t
        dv=dv.astype(bf16)
        for q in range(ng):
            def put(dw=dws[q],dv=dv): dw[...]=dv
            if ng==1: put()
            else: pl.when(lax.div(f,2)==q)(put)
        if nc or nd or nz:
            @pl.when(f==nf-1)
            def _():
                for cpy in copies(): cpy.wait()
                if nz: inward_run(zsrc,zdst[0],sems[:2],False)
    one=pl.Buffered(1)
    rowspec=pl.BlockSpec((RG,D),lambda f:(0,0),pipeline_mode=one)
    wspec=pl.BlockSpec((1,D,FB),lambda f:(2*spot()[0]+l2,0,f+f0))
    wdspec=pl.BlockSpec((1,FB,D),lambda f:(2*spot()[0]+l2,f+f0,0))
    full=lambda r,c: pl.BlockSpec((r,c),lambda f:(0,0),pipeline_mode=one)
    anyspec=pl.BlockSpec(memory_space=pl.ANY)
    wspecs=[pl.BlockSpec((FB,D),lambda f: ((1-f) if f0 else f,0))] if ng==1 else [
        pl.BlockSpec((FB,D),lambda f: (jnp.minimum(f,1),0)),pl.BlockSpec((FB,D),lambda f: (jnp.minimum(3-f,1),0))]
    out=pl.pallas_call(kernel,grid=(nf,),
        in_specs=[anyspec]*nx+[rowspec]*(2*n)+[wspec,wspec,wdspec]+[rowspec]*np_+[anyspec]*(nc+nd+nz),
        out_specs=[rowspec]*(2*n)+[full(2*SR,2*HB),full(SR,2*HB),full(SR,2*HB)]*ng+wspecs+[anyspec]*(nc+nd+nz//2),
        scratch_shapes=[pltpu.VMEM((R//chunk,D,chunk),bf16),pltpu.VMEM((D,chunk),bf16)]+[pltpu.VMEM((R,FB),bf16)]*3+[pltpu.VMEM((R,D),f32)]*2+([pltpu.SemaphoreType.DMA((1,)),pltpu.SemaphoreType.DMA((1,))] if nz else [])+(row_sems() if nd else [])+(plane_sems(1) if nc else []),
      out_shape=[jax.ShapeDtypeStruct((RG,D),bf16)]*(2*n)+([jax.ShapeDtypeStruct((2*SR,2*HB),bf16)]+[jax.ShapeDtypeStruct((SR,2*HB),bf16)]*2)*ng+[jax.ShapeDtypeStruct((HB,D),bf16)]*ng+[jax.ShapeDtypeStruct((8,RG//8,D),bf16)]*nc+([jax.ShapeDtypeStruct((3,dense[2])+dense[0].shape[2:],bf16)] if nd else [])+([jax.ShapeDtypeStruct(inw[0].shape,bf16)] if nz else []),
      compiler_params=pltpu.CompilerParams(vmem_limit_bytes=62<<20,dimension_semantics=("arbitrary",),**(dict(collective_id=cid,has_side_effects=True) if nc or nd or nz else {})),
      cost_estimate=pl.CostEstimate(flops=9*R*D*FF*ng,bytes_accessed=3*D*FF*2*ng+4*R*D*2,transcendentals=R*FF*ng//2),
      name=f"expert_ffn{n}_{f0}")(*deps,*xs,*ss,wg,wu,wd,*prev,*([carry] if nc else []),*([dense[0]] if nd else []),*(inw if nz else ()))
    o=2*n
    return (out[:o],*[out[o+3*q:o+3*q+3] for q in range(ng)],*out[o+3*ng:])

def shared_ffn(x, s, wg, wu, wd, xout, sa, FB=512):
    T,D=x.shape; FF=wg.shape[1]; nf=FF//FB; chunk=T//2
    SG=D//8; SD=FB//8
    NR=2*SG*(FB//128)+SD*(D//128)
    def kernel(xr,sr,wgr,wur,wdr,xo,zs,res,dgr,o0,o1,xia,xib,zd,XT,H,GB,UB,VG,VD,zs0,zs1,*sems):
        f=pl.program_id(0)
        core=spot()[0]
        pairs=[(xo.at[0],xia),(xo.at[1],xib)]
        @pl.when(f==0)
        def _():
            plane_z_barrier()
            for cpy in plane_copies(pairs,sems): cpy.start()
            inward_run((zs,zs),zd,(zs0,zs1),True)
        @pl.when(f==0)
        def _():
            for b in range(2):
                XT[:,b*chunk:(b+1)*chunk]=xr[b*chunk:(b+1)*chunk,:].astype(f32).T.astype(bf16)
        @pl.loop(0,T//chunk)
        def _(i):
            rows=pl.ds(pl.multiple_of(i*chunk,chunk),chunk)
            r,d=ffn_rows(xr[rows,:],sr[rows,:],wgr[...],wur[...],wdr[...],H,GB,UB,rows)
            @pl.when(f==0)
            def _():
                res[rows,:]=r; dgr[rows,:]=d
            @pl.when(f>0)
            def _():
                res[rows,:]+=r; dgr[rows,:]+=d
        for t,Y in enumerate((GB,UB)):
            VG[...]=nn(XT[...],Y[...]).astype(bf16)
            for zr in range(4):
                for cp in range(2):
                    src=pl.ds(pl.multiple_of(2*SG*shard_of(zr)+SG*lax.rem(core+cp,2),SG),SG)
                    for b in range(FB//128):
                        off=(t*(FB//128)+b)*SG
                        (o0,o1)[cp][f,zr,off:off+SG,:]=VG[src,b*128:(b+1)*128]
        VD[...]=tn(H[...],sr[...]).astype(bf16)
        zr=jnp.where(spot()[1]<2,3-f,f)
        for cp in range(2):
            for e in range(4):
                src=pl.ds(pl.multiple_of(lax.rem(core+cp,2)*4*SD+e*SD,SD),SD)
                for b in range(D//128):
                    off=2*SG*(FB//128)+b*SD
                    (o0,o1)[cp][e,zr,off:off+SD,:]=VD[src,b*128:(b+1)*128]
        @pl.when(f==nf-1)
        def _():
            for cpy in plane_copies(pairs,sems): cpy.wait()
            inward_run((zs,zs),zd,(zs0,zs1),False)
    full=lambda sh: pl.BlockSpec(sh,lambda f:(0,)*len(sh))
    return pl.pallas_call(kernel,grid=(nf,),
      in_specs=[full((T,D)),full((T,D)),pl.BlockSpec((D,FB),lambda f:(0,f)),pl.BlockSpec((D,FB),lambda f:(0,f)),pl.BlockSpec((FB,D),lambda f:(f,0))]+[pl.BlockSpec(memory_space=pl.ANY)]*2,
      out_specs=[full((T,D)),full((T,D)),full((4,4,NR,128)),full((4,4,NR,128))]+[pl.BlockSpec(memory_space=pl.ANY)]*3,
      out_shape=[jax.ShapeDtypeStruct((T,D),f32)]*2+[jax.ShapeDtypeStruct((4,4,NR,128),bf16)]*2+[jax.ShapeDtypeStruct(xout.shape[1:],bf16)]*3,
      scratch_shapes=[pltpu.VMEM((D,T),bf16)]+[pltpu.VMEM((T,FB),bf16)]*3+[pltpu.VMEM((D,FB),bf16),pltpu.VMEM((FB,D),bf16)]+[pltpu.SemaphoreType.DMA((1,))]*2+plane_sems(2),
      compiler_params=pltpu.CompilerParams(vmem_limit_bytes=62<<20,dimension_semantics=("arbitrary",),collective_id=1,has_side_effects=True),
      cost_estimate=pl.CostEstimate(flops=2*9*T*D*FF,bytes_accessed=6*D*FF*2+8*T*D*2,transcendentals=T*FF),
      name="shared_ffn")(x,s,wg,wu,wd,xout,sa)


def route(order, expert_ids, gates, cot, core, G, L, parts, plane=False):
    T,D=cot.shape; P2=2*T
    LP=L//parts; S=G*LP*CAP
    big=E*CAP
    CH=480 if S%480==0 else CAP*4
    def kernel(core_ref,orow,ids,gts,ct,rowo,colo,*rest):
        sgs=rest[:parts]; PT,PG=rest[parts:]
        lane=lax.broadcasted_iota(jnp.int32,(T,128),1)
        e0=ids[:,0:1].astype(f32); e1=ids[:,1:2].astype(f32)
        er=jnp.where(lane==0,e0,jnp.where(lane==1,e1,0.0)).T[0:8,:]
        ecat=jnp.concatenate([er[0:1,:],er[1:2,:]],axis=1)
        eoh=(lax.broadcasted_iota(jnp.int32,(E,P2),0).astype(f32)==ecat)
        eohb=jnp.where(eoh,1.0,0.0).astype(bf16)
        o=orow[...]
        oj=(o&1)*T+(o>>1)
        CB=256
        for c in range(P2//CB):
            jj=lax.broadcasted_iota(jnp.int32,(CB,P2),0)+c*CB
            PT[c*CB:(c+1)*CB,:]=jnp.where(jj==oj,1.0,0.0).astype(bf16)
        soh=nn(eohb,PT[...])
        sohb=soh.astype(bf16)
        tri=jnp.where(lax.broadcasted_iota(jnp.int32,(CB,CB),0)<lax.broadcasted_iota(jnp.int32,(CB,CB),1),1.0,0.0).astype(bf16)
        run=jnp.zeros((E,1),f32)
        pos=[]
        for c in range(P2//CB):
            blk=soh[:,c*CB:(c+1)*CB]
            before=nn(sohb[:,c*CB:(c+1)*CB],tri)+run
            run=run+jnp.sum(blk,axis=1,keepdims=True)
            pos.append(jnp.sum(before*blk,axis=0,keepdims=True))
        posr=jnp.minimum(jnp.concatenate(pos,axis=1),127.0)
        posj=nt(jnp.broadcast_to(posr,(16,P2)).astype(bf16),PT[...])[0:1,:]
        e=ecat.astype(jnp.int32)
        l=lax.rem(e,L); j=lax.div(e,L)
        if plane:
            base=((lax.rem(l,2)*2+lax.div(l,2))*G+j)*CAP
        elif parts==2:
            cc=lax.rem(lax.div(l,LP)+core_ref[0],2)
            base=((cc*G+j)*LP+lax.rem(l,LP))*CAP
        else:
            base=e*CAP
        p=posj.astype(jnp.int32)
        slot=jnp.where(p<CAP,base+p,big)
        s0=slot[:,0:T]; s1=slot[:,T:P2]
        r8=lax.broadcasted_iota(jnp.int32,(8,T),0)
        rows=jnp.where(r8==0,s0,jnp.where(r8==1,s1,big))
        rowo[...]=rows
        rep=jnp.concatenate([rows.astype(f32)]*16,axis=0).T
        colo[...]=rep[:,0:8].astype(jnp.int32)
        ctf=ct[...].astype(f32)
        PG[0:T,:]=(gts[:,0:1]*ctf).astype(bf16)
        PG[T:P2,:]=(gts[:,1:2]*ctf).astype(bf16)
        for pi in range(parts):
            @pl.loop(0,S//CH)
            def _(i):
                si=lax.broadcasted_iota(jnp.int32,(CH,T),0)+(i*CH+pi*S)
                d0=jnp.where(si==rowo[0:1,:],1.0,0.0).astype(bf16)
                d1=jnp.where(si==rowo[1:2,:],1.0,0.0).astype(bf16)
                sgs[pi][pl.ds(pl.multiple_of(i*CH,CH),CH),:]=(nn(d0,PG[0:T,:])+nn(d1,PG[T:P2,:])).astype(bf16)
    vm=pl.BlockSpec(memory_space=pltpu.VMEM)
    out=pl.pallas_call(kernel,
      in_specs=[pl.BlockSpec(memory_space=pltpu.SMEM)]+[vm]*4,out_specs=[vm]*(2+parts),
      out_shape=[jax.ShapeDtypeStruct((8,T),jnp.int32),jax.ShapeDtypeStruct((T,8),jnp.int32)]+[jax.ShapeDtypeStruct((S,D),bf16)]*parts,
      scratch_shapes=[pltpu.VMEM((P2,P2),bf16),pltpu.VMEM((P2,D),bf16)],
      compiler_params=pltpu.CompilerParams(vmem_limit_bytes=50<<20),
      cost_estimate=pl.CostEstimate(flops=4*S*parts*T*D+4*P2*P2*16,bytes_accessed=8<<20,transcendentals=0),
      name="route")(core,order,expert_ids,gates,cot)
    return out[0],out[1],out[2:]

def dispatch(rows, x, parts):
    T,D=x.shape; S=E*CAP//parts; CH=480
    def kernel(rowr,xr,*outs):
        for pi in range(parts):
            @pl.loop(0,S//CH)
            def _(i):
                si=lax.broadcasted_iota(jnp.int32,(CH,T),0)+(i*CH+pi*S)
                d=jnp.where((si==rowr[0:1,:])|(si==rowr[1:2,:]),1.0,0.0).astype(bf16)
                outs[pi][pl.ds(pl.multiple_of(i*CH,CH),CH),:]=nn(d,xr[...]).astype(bf16)
    vm=pl.BlockSpec(memory_space=pltpu.VMEM)
    return pl.pallas_call(kernel,in_specs=[vm]*2,out_specs=[vm]*parts,out_shape=[jax.ShapeDtypeStruct((S,D),bf16)]*parts,
      compiler_params=pltpu.CompilerParams(vmem_limit_bytes=50<<20),
      cost_estimate=pl.CostEstimate(flops=2*S*parts*T*D,bytes_accessed=6<<20,transcendentals=0),name="dispatch")(rows,x)

def combine(cols, gates, ret, state, shared):
    parts=len(ret); T,D=state.shape; S=ret[0].shape[0]
    def kernel(colr,g,*refs):
        rs=refs[:parts]; st,sh,out=refs[parts:]
        @pl.loop(0,T//QC)
        def _(i):
            r=pl.ds(pl.multiple_of(i*QC,QC),QC)
            acc=st[r,:]+sh[r,:]
            for k in range(2):
                pk=None
                for pi in range(parts):
                    si=lax.broadcasted_iota(jnp.int32,(QC,S),1)+pi*S
                    d=jnp.where(si==colr[r,k:k+1],1.0,0.0).astype(bf16)
                    q=nn(d,rs[pi][...])
                    pk=q if pk is None else pk+q
                acc=acc+g[r,k:k+1]*pk
            out[r,:]=acc.astype(bf16)
    vm=pl.BlockSpec(memory_space=pltpu.VMEM)
    return pl.pallas_call(kernel,in_specs=[vm]*(4+parts),out_specs=vm,out_shape=jax.ShapeDtypeStruct((T,D),bf16),
      compiler_params=pltpu.CompilerParams(vmem_limit_bytes=50<<20),
      cost_estimate=pl.CostEstimate(flops=4*S*parts*T*D,bytes_accessed=9<<20,transcendentals=0),name="combine")(cols,gates,*ret,state,shared)

def mid_bwd_home(deps, inw, cols, own, ext, back_b, dsh, state, fgain, cot):
    T,D=state.shape; S=8*CAP; nx=len(deps)
    def kernel(*refs):
        body(*refs[nx:])
    def body(z0,z1,colr,hown,hext,bb,ds,st,fg,ct,sgo,fgo,ba,zd,BV,cs,zs0,zs1,*hsems):
        home_barrier()
        home_run(hown,hext,ba,hsems,True)
        inward_run((z0,z1),zd,(zs0,zs1),True)
        fgo[...]=jnp.zeros_like(fgo)
        home_run(hown,hext,ba,hsems,False)
        cps=[pltpu.make_async_copy(ba.at[i],BV.at[i],cs.at[i]) for i in range(8)]
        for cp in cps: cp.start()
        for cp in cps: cp.wait()
        @pl.loop(0,T//QC)
        def _(i):
            r=pl.ds(pl.multiple_of(i*QC,QC),QC)
            n=ds[r,:]
            si=lax.broadcasted_iota(jnp.int32,(QC,S),1)+S
            d=jnp.where((si==colr[r,0:1])|(si==colr[r,1:2]),1.0,0.0).astype(bf16)
            n=n+nn(d,bb[...])
            for b in range(8):
                si=lax.broadcasted_iota(jnp.int32,(QC,128),1)
                si=jnp.where(si<CAP,si+b*CAP,-1)
                d=jnp.where((si==colr[r,0:1])|(si==colr[r,1:2]),1.0,0.0).astype(bf16)[:,0:CAP]
                n=n+nn(d,BV[b])
            x=st[r,:]; inv=inv_rms(x); u=x*inv
            fgo[...]+=jnp.broadcast_to(jnp.sum(n*u,axis=0,keepdims=True),(8,D))
            w=n*fg[...]
            sgo[r,:]=ct[r,:].astype(f32)+inv*(w-u*jnp.mean(w*u,axis=1,keepdims=True))
        inward_run((z0,z1),zd,(zs0,zs1),False)
    vm=pl.BlockSpec(memory_space=pltpu.VMEM); an=pl.BlockSpec(memory_space=pl.ANY)
    return pl.pallas_call(kernel,in_specs=[an]*(nx+2)+[vm,an,an]+[vm]*5,out_specs=[vm]*2+[an]*2,
      out_shape=[jax.ShapeDtypeStruct((T,D),f32),jax.ShapeDtypeStruct((8,D),f32),jax.ShapeDtypeStruct((8,CAP,D),bf16),jax.ShapeDtypeStruct(inw[0].shape,bf16)],
      scratch_shapes=[pltpu.VMEM((8,CAP,D),bf16),pltpu.SemaphoreType.DMA((8,))]+[pltpu.SemaphoreType.DMA((1,))]*2+home_sems(),
      compiler_params=pltpu.CompilerParams(vmem_limit_bytes=50<<20,collective_id=4,has_side_effects=True),
      cost_estimate=pl.CostEstimate(flops=4*S*T*D,bytes_accessed=12<<20,transcendentals=0),name="mid_bwd")(*deps,*inw,cols,own,ext,back_b,dsh,state,fgain[None],cot)

def mid_bwd(cols, back, dsh, state, fgain, cot):
    parts=len(back); T,D=state.shape; S=back[0].shape[0]
    def kernel(colr,*refs):
        bs=refs[:parts]; ds,st,fg,ct,sgo,fgo=refs[parts:]
        fgo[...]=jnp.zeros_like(fgo)
        @pl.loop(0,T//QC)
        def _(i):
            r=pl.ds(pl.multiple_of(i*QC,QC),QC)
            n=ds[r,:]
            for pi in range(parts):
                si=lax.broadcasted_iota(jnp.int32,(QC,S),1)+pi*S
                d=jnp.where((si==colr[r,0:1])|(si==colr[r,1:2]),1.0,0.0).astype(bf16)
                n=n+nn(d,bs[pi][...])
            x=st[r,:]; inv=inv_rms(x); u=x*inv
            fgo[...]+=jnp.broadcast_to(jnp.sum(n*u,axis=0,keepdims=True),(8,D))
            w=n*fg[...]
            sgo[r,:]=ct[r,:].astype(f32)+inv*(w-u*jnp.mean(w*u,axis=1,keepdims=True))
    vm=pl.BlockSpec(memory_space=pltpu.VMEM)
    return pl.pallas_call(kernel,in_specs=[vm]*(5+parts),out_specs=[vm]*2,out_shape=[jax.ShapeDtypeStruct((T,D),f32),jax.ShapeDtypeStruct((8,D),f32)],
      compiler_params=pltpu.CompilerParams(vmem_limit_bytes=50<<20),
      cost_estimate=pl.CostEstimate(flops=2*S*parts*T*D,bytes_accessed=12<<20,transcendentals=0),name="mid_bwd")(cols,*back,dsh,state,fgain[None],cot)

HEADS = 12
HEAD_DIM = 64


def rope_wide(length):
    positions = jnp.arange(length, dtype=f32)
    frequency = 10000.0 ** (-jnp.arange(HEAD_DIM // 2, dtype=f32) * 2.0 / HEAD_DIM)
    angles = positions[:, None] * frequency[None, :]
    c = jnp.cos(angles)
    s = jnp.sin(angles)
    return jnp.concatenate([c, c, c, c], axis=1), jnp.concatenate([-s, s, -s, s], axis=1)


def shards_any(tokens, cotangent, expert_ids, route_gates, slot_order, prefix_len, attention_gain, qkv_weight,
           output_weight, feedforward_gain, shared_gate, shared_up, shared_down, expert_gate, expert_up, expert_down):
    T, D = tokens.shape
    L, _, FF = expert_gate.shape
    G = lax.axis_size("expert")
    DP = lax.axis_size("dp")
    Z = DP // 2
    parts = 2 if L % 2 == 0 else 1
    LP = L // parts
    dpi = lax.axis_index("dp")
    core = lax.rem(dpi, 2)
    swap_perm = [(i, i ^ 1) for i in range(DP)]
    zgroups = [[2 * z + c for z in range(Z)] for c in range(2)]

    def swap(x):
        return lax.ppermute(x, "dp", swap_perm)

    def a2a(x):
        return lax.all_to_all(x, "expert", split_axis=0, concat_axis=0, tiled=True)

    def to_experts(arrs):
        arrs = [a.reshape(G, LP, CAP, D) for a in arrs]
        if parts == 2:
            arrs = [arrs[0], swap(arrs[1])]
        return [a2a(a) for a in arrs]

    def from_experts(arrs):
        arrs = [a2a(a) for a in arrs]
        if parts == 2:
            arrs = [arrs[0], swap(arrs[1])]
        return [a.reshape(G * LP * CAP, D) for a in arrs]

    cosw, sinw = rope_wide(T)
    rows, cols, sgs = route(slot_order, expert_ids, route_gates, cotangent, core[None].astype(jnp.int32), G, L, parts)
    slot_in = to_experts(sgs)
    q, k, v, att, lse, state, ntwo = attn_fwd(tokens, prefix_len, attention_gain, qkv_weight, output_weight,
                                              feedforward_gain, cosw, sinw)
    xs = dispatch(rows, ntwo, parts)
    x_in = to_experts(xs)
    sh = make_ffn(1, 1, 1, T, D, FF, 512, T // 2, f32)(
        ntwo[None, None], cotangent[None, None], shared_gate[None], shared_up[None], shared_down[None])
    shared_branch = sh[0].reshape(T, D)
    dshared = sh[1].reshape(T, D)
    dense_shared = [sh[2][0], sh[3][0], sh[4][0]]

    res, dgr, eg = [], [], []
    one = make_ffn(parts, G, 1, CAP, D, FF, 512, parts * G * CAP // 2, bf16)
    for l in range(LP):
        o = one(*[a[:, l:l + 1] for a in x_in], *[a[:, l:l + 1] for a in slot_in],
                *[lax.dynamic_slice_in_dim(w, (core * LP if parts == 2 else 0) + l, 1, 0)
                  for w in (expert_gate, expert_up, expert_down)])
        res.append(o[:parts])
        dgr.append(o[parts:2 * parts])
        eg.append(o[2 * parts:])
    cat = lambda xs_: jnp.concatenate(xs_, axis=1) if len(xs_) > 1 else xs_[0]
    res = [cat([r[p] for r in res]) for p in range(parts)]
    dgr = [cat([r[p] for r in dgr]) for p in range(parts)]

    egr = []
    for l in range(LP):
        if parts == 2:
            egr.append([lax.psum_scatter(g[0], "dp", scatter_dimension=0, tiled=True, axis_index_groups=zgroups)
                        for g in eg[l]])
        else:
            egr.append([lax.psum_scatter(g[0], "dp", scatter_dimension=0, tiled=True) for g in eg[l]])

    back = from_experts(dgr)
    ret = from_experts(res)
    sgrad, fgg = mid_bwd(cols, back, dshared, state, feedforward_gain, cotangent)
    tokens_grad, agg, gq, gk, gv, gwo = attn_bwd(sgrad, prefix_len, tokens, attention_gain, qkv_weight, output_weight,
                                                 cosw, sinw, q, k, v, att, lse)
    block_out = combine(cols, route_gates, ret, state, shared_branch)

    def dense(g):
        r = g.shape[0] // DP
        h = g.reshape(Z, 2, r, g.shape[1])
        mine = lax.dynamic_index_in_dim(h, core, 1, keepdims=False)
        other = lax.dynamic_index_in_dim(h, 1 - core, 1, keepdims=False)
        s = (mine.astype(f32) + swap(other).astype(f32)).astype(bf16)
        quarter = s.reshape(Z, G, r // G, g.shape[1])
        quarter = jnp.swapaxes(quarter, 0, 1)
        got = lax.all_to_all(quarter, "expert", split_axis=0, concat_axis=0, tiled=True)
        s = jnp.sum(got.astype(f32), axis=0).astype(bf16)
        zs = lax.psum_scatter(s, "dp", scatter_dimension=0, tiled=True, axis_index_groups=zgroups)
        return lax.all_gather(zs[0], "expert", axis=0, tiled=True).astype(f32)

    def dense_simple(g):
        p = lax.psum_scatter(g, "dp", scatter_dimension=0, tiled=True)
        return lax.psum(p, "expert").astype(f32)

    if (qkv_weight.shape[0] // DP) % (8 * G) == 0 and parts == 2:
        dn = dense
    else:
        dn = dense_simple
    dsh = [dn(g) for g in dense_shared]
    dq, dk, dv, dwo = [dn(g) for g in (gq, gk, gv, gwo)]
    gains = lax.psum(jnp.stack([agg[0], fgg[0]]), ("dp", "expert"))
    gs = D // DP
    gains = lax.dynamic_slice_in_dim(gains, dpi * gs, gs, 1)

    def finish(t):
        a = [egr[l][t] for l in range(LP)]
        if parts == 1:
            return jnp.stack(a).astype(f32)
        b = jnp.stack(a)
        h = b.reshape(LP, 2, b.shape[1] // 2, b.shape[2])
        mine = lax.dynamic_index_in_dim(h, core, 1, keepdims=False)
        other = swap(lax.dynamic_index_in_dim(h, 1 - core, 1, keepdims=False))
        return jnp.concatenate([jnp.where(core == 0, mine, other), jnp.where(core == 0, other, mine)], axis=0).astype(f32)

    return (block_out, tokens_grad, gains[0], jnp.concatenate([dq, dk, dv], axis=1), dwo, gains[1],
            dsh[0], dsh[1], dsh[2], finish(0), finish(1), finish(2))


def shards_fast(tokens, cotangent, expert_ids, route_gates, slot_order, prefix_len, attention_gain, qkv_weight,
                output_weight, feedforward_gain, shared_gate, shared_up, shared_down, expert_gate, expert_up, expert_down):
    T, D = tokens.shape
    FF = expert_gate.shape[2]
    dpi = lax.axis_index("dp").astype(jnp.int32)
    ei = lax.axis_index("expert").astype(jnp.int32)
    core = lax.rem(dpi, 2)
    zi = lax.div(dpi, 2)
    outer = (zi == 0) | (zi == 3)
    low = zi < 2

    def swap(x):
        return lax.ppermute(x, "dp", [(i, i ^ 1) for i in range(8)])

    def across(x):
        return lax.ppermute(x, "dp", [(2, 4), (3, 5), (4, 2), (5, 3)])

    def add(*xs):
        t = xs[0].astype(f32)
        for x in xs[1:]:
            t = t + x.astype(f32)
        return t.astype(bf16)

    cosw, sinw = rope_wide(T)
    rows, cols, (s_out,) = route(slot_order, expert_ids, route_gates, cotangent, core[None], 4, 4, 1, True)
    q, k, v, att, lse, state, ntwo, x_out, sa, sb = attn_fwd(
        tokens, prefix_len, attention_gain, qkv_weight, output_weight, feedforward_gain, cosw, sinw, rows,
        s_out.reshape(2, 8, CAP, D))
    flat = lambda y: y.reshape(8 * CAP, D)
    shared_branch, dshared, sh0, sh1, xa, xb, sx = shared_ffn(ntwo, cotangent, shared_gate, shared_up, shared_down,
                                                              x_out.reshape(2, 8, CAP, D), sa)
    ws = (expert_gate, expert_up, expert_down)
    blocks = lambda y: y.reshape(8, CAP, D)
    dsum = add(sh0, swap(sh1))
    (rb, db), gb0, gb1, wb0, wb1, xx = expert_ffn([], 1, [flat(xb)], [flat(sb)], *ws, 0, 4, inw=(xa, xa), cid=6)
    sa, sx, xa, xx = flat(sa), flat(sx), flat(xa), flat(xx)
    p0, ga0, wa0, db, r0, rf0 = expert_ffn([], 0, [xa, xx], [sa, sx], *ws, 0, 2, carry=blocks(db), dense=(dsum, 0, 1),
                                           inw=(gb0[0], gb0[0]), cid=2)
    bs0 = add(gb0[0], rf0)
    m_b0 = across(bs0)
    m_a0 = across(ga0[0])
    (ra, rx, da, dx), ga1, wa1, r1, rf1 = expert_ffn([bs0], 0, [xa, xx], [sa, sx], *ws, 2, 2, p0, dense=(dsum, 1, 3),
                                                     inw=(gb1[0], gb1[0]), cid=3)
    bs1 = add(gb1[0], rf1)
    m_b1 = across(bs1)
    sgrad, fgg, _, rf2 = mid_bwd_home([bs1], (wb1, wb0), cols, blocks(da), blocks(dx), flat(db), dshared, state,
                                      feedforward_gain, cotangent)
    bs2 = add(jnp.where(low, wb1, wb0), rf2)
    mine = lax.dynamic_index_in_dim(dsum, ei, 0, keepdims=False)
    msh = jnp.concatenate([add(mine[:1], r0[0], r0[1], r0[2]), add(mine[1:], r1[0], r1[1], r1[2])])
    carried = {
        "hown": blocks(ra), "hext": blocks(rx), "rbs": blocks(rb), "fgg": fgg, "msh": msh,
        "m0": m_b0, "ni0": gb0[1], "no0": gb0[2],
        "m1": m_a0, "ni1": ga0[1], "no1": ga0[2],
        "m2": m_b1, "ni2": gb1[1], "no2": gb1[2],
        "far3": ga1[0], "ni3": ga1[1], "no3": ga1[2],
        "wa0": wa0, "wa1": wa1, "wb0": wb0, "wb1": wb1,
        "far5": bs2,
    }
    tail = Tail(carried, T, D, FF)
    tokens_grad, _, *rest = attn_bwd(sgrad, prefix_len, tokens, attention_gain, qkv_weight, output_weight,
                                     cosw, sinw, q, k, v, att, lse, tail)
    o = dict(zip(tail.onames, rest))
    block_out = combine(cols, route_gates, [flat(o["ra"]), flat(o["rb"])], state, shared_branch)
    sg = D // 8
    gains = lax.dynamic_slice_in_dim(o["gains"], dpi * sg, sg, 1)
    return (block_out, tokens_grad, gains[0], o["dqkv"], o["dwo"], gains[1], o["dgate"], o["dup"], o["ddown"],
            o["gate"].astype(f32), o["up"].astype(f32), o["down"].astype(f32))


def shards(*args):
    local = args[13].shape[0]
    if lax.axis_size("dp") == 8 and lax.axis_size("expert") == 4 and local == 4:
        return shards_fast(*args)
    return shards_any(*args)


def solution(mesh):
    row = P(("dp", "expert"), None)
    return jax.shard_map(
        shards,
        mesh=mesh,
        in_specs=(row, row, row, row, row, P(("dp", "expert")), P(), P(), P(), P(), P(), P(), P(),
                  P("expert", None, None), P("expert", None, None), P("expert", None, None)),
        out_specs=(row, row, P("dp"), P("dp", None), P("dp", None), P("dp"), P("dp", None), P("dp", None),
                   P("dp", None), P("expert", "dp", None), P("expert", "dp", None), P("expert", "dp", None)),
        check_vma=False,
    )
```

```python
import jax
import jax.numpy as jnp
import numpy as np
from jax import lax
from jax.experimental import pallas as pl
from jax.experimental.pallas import tpu as pltpu
from jax.sharding import PartitionSpec as P


MESH_ID = pl.DeviceIdType.MESH

def xor4(e,k):
    lo=lax.rem(e,2); hi=lax.div(e,2)
    if k&1: lo=1-lo
    if k&2: hi=1-hi
    return hi*2+lo

def spot():
    d=lax.axis_index("dp"); e=lax.axis_index("expert")
    c=lax.rem(d,2)
    return c,lax.div(d,2),e

def shard_of(q):
    c,z,e=spot()
    return jnp.where(z<2,3-q,q).astype(jnp.int32)

def peer(z,kk):
    c,_,e=spot()
    return (2*z+lax.rem(c+(kk>>2),2),xor4(e,kk&3))

def block_of(kk):
    c,_,e=spot()
    return lax.rem(c+(kk>>2),2)*4+xor4(e,kk&3)

def plane_sems(n):
    return [pltpu.SemaphoreType.DMA((n,)),pltpu.SemaphoreType.DMA((n,7)),pltpu.SemaphoreType.DMA((n,7))]

def plane_barrier():
    c,z,e=spot()
    b=pltpu.get_barrier_semaphore()
    for kk in range(1,8):
        pl.semaphore_signal(b,inc=1,device_id=peer(z,kk),device_id_type=MESH_ID)
    pl.semaphore_wait(b,7)

def plane_z_barrier():
    c,z,e=spot()
    b=pltpu.get_barrier_semaphore()
    for kk in range(1,8):
        pl.semaphore_signal(b,inc=1,device_id=peer(z,kk),device_id_type=MESH_ID)
    pl.semaphore_signal(b,inc=1,device_id=(2*side()+c,e),device_id_type=MESH_ID)
    pl.semaphore_wait(b,8)

def side():
    c,z,e=spot()
    return z+1-2*lax.rem(z,2)

def inward_run(srcs, dst, sems, start):
    c,z,e=spot()
    end=(z==0)|(z==3)
    def cp(src): return pltpu.make_async_remote_copy(src_ref=src,dst_ref=dst,send_sem=sems[0].at[0],recv_sem=sems[1].at[0],
        device_id=(2*side()+c,e),device_id_type=MESH_ID)
    if start:
        @pl.when(z==0)
        def _(): cp(srcs[0]).start()
        @pl.when(z==3)
        def _(): cp(srcs[1]).start()
    else:
        @pl.when(end)
        def _(): cp(srcs[0]).wait_send()
        @pl.when(jnp.logical_not(end))
        def _(): cp(srcs[0]).wait_recv()

def plane_copies(pairs, sems):
    local,send,recv=sems
    c,z,e=spot()
    me=block_of(0)
    out=[]
    for i,(src,dst) in enumerate(pairs):
        out.append(pltpu.make_async_copy(src.at[me],dst.at[me],local.at[i]))
        for kk in range(1,8):
            out.append(pltpu.make_async_remote_copy(src_ref=src.at[block_of(kk)],dst_ref=dst.at[me],send_sem=send.at[i,kk-1],
                recv_sem=recv.at[i,kk-1],device_id=peer(z,kk),device_id_type=MESH_ID))
    return out

def home_barrier():
    c,z,e=spot()
    b=pltpu.get_barrier_semaphore()
    inner=(z==1)|(z==2)
    zo=jnp.where(z<2,0,3); zi=jnp.where(z<2,1,2)
    @pl.when(inner)
    def _():
        for kk in range(8):
            pl.semaphore_signal(b,inc=1,device_id=peer(zo,kk),device_id_type=MESH_ID)
            if kk:
                pl.semaphore_signal(b,inc=1,device_id=peer(z,kk),device_id_type=MESH_ID)
        pl.semaphore_wait(b,15)
    @pl.when(jnp.logical_not(inner))
    def _():
        for kk in range(8):
            pl.semaphore_signal(b,inc=1,device_id=peer(zi,kk),device_id_type=MESH_ID)
            if kk:
                pl.semaphore_signal(b,inc=1,device_id=peer(z,kk),device_id_type=MESH_ID)
        pl.semaphore_wait(b,15)

def is_inner():
    c,z,e=spot()
    return (z==1)|(z==2)

def ext_sems():
    return [pltpu.SemaphoreType.DMA((8,)),pltpu.SemaphoreType.DMA((8,))]

def ext_run(src, dst, sems, start):
    send,recv=sems
    me=block_of(0)
    c,z,e=spot()
    def remote(kk,zz):
        return pltpu.make_async_remote_copy(src_ref=src.at[block_of(kk)],dst_ref=dst.at[me],send_sem=send.at[kk],recv_sem=recv.at[kk],
            device_id=peer(zz,kk),device_id_type=MESH_ID)
    @pl.when(is_inner())
    def _():
        for kk in range(8):
            if start: remote(kk,side()).start()
            else: remote(kk,side()).wait_send()
    if not start:
        @pl.when(jnp.logical_not(is_inner()))
        def _():
            for kk in range(8): remote(kk,side()).wait_recv()

def own_run(src, dst, sems, start):
    @pl.when(is_inner())
    def _():
        for cp in plane_copies([(src,dst)],sems):
            if start: cp.start()
            else: cp.wait()

def row_sems():
    return [pltpu.SemaphoreType.DMA((3,)),pltpu.SemaphoreType.DMA((3,))]

def row_copies(src, dst, part, sems):
    send,recv=sems
    c,z,e=spot()
    return [pltpu.make_async_remote_copy(src_ref=src.at[xor4(e,kk),part],dst_ref=dst.at[kk-1],send_sem=send.at[kk-1],recv_sem=recv.at[kk-1],
        device_id=peer(z,kk),device_id_type=MESH_ID) for kk in (1,2,3)]


def add_rows(dst, srcs):
    rows,cols=dst.shape
    step=max(s for s in range(16,rows+1,16) if rows%s==0 and s*cols<=40000)
    @pl.loop(0,dst.shape[0]//step)
    def _(i):
        r=pl.ds(pl.multiple_of(i*step,step),step)
        t=srcs[0][r,:].astype(f32)
        for s in srcs[1:]: t=t+s[r,:].astype(f32)
        dst[r,:]=t.astype(dst.dtype)

class Tail:
    KIND=("g","g","g","g","w","w")
    L2=(1,1,0,0,0,1)
    H=(0,1,0,1,0,0)
    RIN=(0,1,5)
    MID=((3,"o"),(4,"o"),(5,"o"),(2,"i"),(3,"i"),(4,"i"),(5,"i"))
    def __init__(self, arrays, T, D, FF):
        self.names=list(arrays); self.arrays=[arrays[n] for n in self.names]
        self.T,self.D,self.FF=T,D,FF
        SG=D//8; self.SG=SG; self.SD=FF//32
        R2=2*SG; self.R2=R2; HW=FF//4
        self.gs=(R2,FF); self.ws=(HW,D)
        self.NR=arrays["msh"].shape[1]
        an=pl.BlockSpec(memory_space=pl.ANY)
        S=jax.ShapeDtypeStruct
        outs={"gate":S((4,SG,FF),bf16),"up":S((4,SG,FF),bf16),"down":S((4,FF//8,D),bf16),
              "dgate":S((SG,FF),f32),"dup":S((SG,FF),f32),"ddown":S((FF//8,D),f32),
              "dqkv":S((SG,3*D),f32),"dwo":S((SG,D),f32),"gains":S((8,D),f32),
              "ra":S((8,CAP,D),bf16),"rb":S((8,CAP,D),bf16)}
        for i,w in self.MID:
            outs[f"m{i}{w}"]=S(self.shape(i),bf16)
        for i in self.RIN:
            outs[f"rin{i}"]=S(self.shape(i),bf16)
        for i in range(6):
            outs[f"ro{i}"]=S(self.shape(i),bf16)
        self.onames=list(outs); self.oshape=[outs[n] for n in self.onames]
        self.in_specs=[an]*len(self.names); self.out_specs=[an]*len(self.onames)
        V=pltpu.VMEM; DM=pltpu.SemaphoreType.DMA
        scr={"ga":V((2,3)+self.gs,bf16),"wa":V((2,3)+self.ws,bf16),
             "gto":V((3,)+self.gs,bf16),"wto":V((1,)+self.ws,bf16),
             "gfin":V((2,)+self.gs,bf16),"wfin":V((1,)+self.ws,bf16),
             "gsw":V((4,SG,FF),bf16),"wsw":V((2,FF//8,D),bf16),
             "atr":V((4,4,SG,D),bf16),"sv":V((4,4,SG,D),bf16),"xr":V((3,4,SG,D),bf16),
             "za":V((4,SG,D),bf16),"zb":V((4,self.NR,128),bf16),
             "gn":V((8,8,D),f32),
             "s_x":DM((7,)),"r_x":DM((7,)),"lra":DM((1,)),"s_o":DM((6,)),"r_o":DM((6,)),"s_w":DM((6,)),"r_w":DM((6,)),
             "ld":DM((2,2,3)),"st":DM((8,)),"so":DM((6,2)),"s_r":DM((3,)),"r_r":DM((3,)),"s_at":DM((16,)),"r_at":DM((16,)),"s_xr":DM((3,)),"r_xr":DM((3,)),
             "s_gn":DM((7,)),"r_gn":DM((7,)),"st2":DM((4,)),"sz":DM((2,3))}
        for nm,sh in (("a",(SG,D)),("b",(self.NR,128))):
            scr.update({"zr"+nm:V((2,)+sh,bf16),"zs"+nm:V((2,)+sh,bf16),"zm"+nm:V((2,)+sh,bf16),"zi"+nm:V(sh,bf16),"zt"+nm:V(sh,bf16),
                "zo"+nm:V(sh,bf16),"fi"+nm:V(sh,bf16),"ag"+nm:V((3,)+sh,bf16),
                "s_z"+nm:DM((4,)),"r_z"+nm:DM((4,)),"s_ag"+nm:DM((3,)),"r_ag"+nm:DM((3,))})
        scr.update({"oa":V((2,SG,D),f32),"og":V((2,2,SG,FF//4),f32),"od":V((2,self.SD,D),f32)})
        self.snames=list(scr)+[f"own{i}" for i in range(3)]+[f"plane{i}" for i in range(3)]
        self.scratch=[scr[n] for n in scr]+plane_sems(1)+plane_sems(1)
    def shape(self,i): return self.gs if self.KIND[i]=="g" else self.ws
    def bind(self,ins,outs,scr):
        self.r=dict(zip(self.names,ins)); self.r.update(zip(self.onames,outs)); self.r.update(zip(self.snames,scr))
        c,z,e=spot()
        self.c,self.z,self.e=c,z,e
        self.inner=(z==1)|(z==2); self.outer=jnp.logical_not(self.inner); self.low=z<2
        self.zo=jnp.where(z<2,0,3); self.zi=jnp.where(z<2,1,2); self.zx=3-z
        self.own=[self.r[f"own{i}"] for i in range(3)]
        self.plane=[self.r[f"plane{i}"] for i in range(3)]
    def rcopy(self,src,dst,s,r,dev):
        return pltpu.make_async_remote_copy(src_ref=src,dst_ref=dst,send_sem=s,recv_sem=r,device_id=dev,device_id_type=MESH_ID)
    def barrier(self):
        b=pltpu.get_barrier_semaphore()
        def sig(dev): pl.semaphore_signal(b,inc=1,device_id=dev,device_id_type=MESH_ID)
        for kk in range(1,8): sig(peer(self.z,kk))
        @pl.when(self.inner)
        def _():
            for kk in range(8): sig(peer(self.zo,kk))
            sig(peer(self.zx,0))
            pl.semaphore_wait(b,16)
        @pl.when(self.outer)
        def _():
            for kk in range(8): sig(peer(self.zi,kk))
            pl.semaphore_wait(b,15)
    def across(self,q,high=False):
        i,w=self.MID[q]; n=self.shape(i)[0]
        src={2:self.r["far2"],3:self.r["far3"],4:self.r["wa0" if high else "wa1"],5:self.r["far5"]}[i]
        return self.rcopy(src.at[pl.ds(0 if w=="o" else n,n)],self.r[f"m{i}{w}"],self.r["s_x"].at[q],self.r["r_x"].at[q],peer(self.zx,0))
    def across_start(self,qs):
        @pl.when(self.inner)
        def _():
            for q in qs:
                if self.MID[q][0]==4:
                    @pl.when(self.low)
                    def _(q=q): self.across(q).start()
                    @pl.when(jnp.logical_not(self.low))
                    def _(q=q): self.across(q,True).start()
                else: self.across(q).start()
    def rows_home(self,start):
        own_run(self.r["hown"],self.r["ra"],self.own,start)
        @pl.when(self.outer)
        def _():
            cp=pltpu.make_async_copy(self.r["rxl"],self.r["ra"],self.r["lra"].at[0])
            if start: cp.start()
            else: cp.wait()
    def start(self):
        self.barrier()
        self.across_start((0,1,2))
        self.stage1(0,1)
        ld=pltpu.make_async_copy(self.r["msh"],self.r["zb"],self.r["st2"].at[0])
        ld.start(); ld.wait()
        self.z_inward("b")
        self.rin_start()
        for cp in plane_copies([(self.r["rbs"],self.r["rb"])],self.plane): cp.start()
        self.rows_home(True)
        self.stage1(2)
    def load(self,pairs,kind,slot,go):
        buf=self.r[kind+"a"]; ki=0 if kind=="g" else 1
        for k,s in enumerate(pairs):
            def cp(x,k=k): return pltpu.make_async_copy(x,buf.at[slot,k],self.r["ld"].at[ki,slot,k])
            two=isinstance(s,tuple)
            if not go: cp(s[0] if two else s).wait()
            elif two:
                pl.when(self.low)(lambda cp=cp,s=s: cp(s[0]).start())
                pl.when(jnp.logical_not(self.low))(lambda cp=cp,s=s: cp(s[1]).start())
            else: cp(s).start()
    def near(self,i,which):
        if self.KIND[i]=="g":
            return self.r[f"n{which}{i}"]
        n=self.ws[0]
        x="a" if i==4 else "b"
        return tuple(self.r[f"w{x}{h}"].at[pl.ds(0 if which=="o" else n,n)] for h in (0,1))
    def rin(self,k,src=None):
        i=self.RIN[k]
        src=self.r[f"rin{i}"] if src is None else src
        return self.rcopy(src,self.r[f"rin{i}"],self.r["s_r"].at[k],self.r["r_r"].at[k],peer(self.zi,0))
    def rin_start(self):
        @pl.when(self.outer)
        def _():
            for k,i in enumerate((0,1)): self.rin(k,self.near(i,"i")).start()
            lo,hi=self.near(5,"i")
            @pl.when(self.low)
            def _(): self.rin(2,lo).start()
            @pl.when(jnp.logical_not(self.low))
            def _(): self.rin(2,hi).start()
    def parts_of(self,i):
        k="g" if self.KIND[i]=="g" else "w"
        idx=i if k=="g" else i-4
        return k,idx,self.shape(i)[0],self.L2[i]==1
    def ro(self,i):
        k,idx,n,b=self.parts_of(i)
        return self.rcopy(self.r[k+"to"].at[idx%3 if k=="g" else 0],self.r[f"ro{i}"],self.r["s_o"].at[i],self.r["r_o"].at[i],peer(self.zo,0))
    def view(self,i,w):
        if i<2:
            n=self.shape(i)[0]
            return self.r[f"m{i}"].at[pl.ds(0 if w=="o" else n,n)]
        return self.r[f"m{i}{w}"]
    def outward_load(self,i,go=True):
        k,idx,n,b=self.parts_of(i)
        if go and (i,"o") in self.MID: self.across(self.MID.index((i,"o"))).wait()
        self.load([self.view(i,"o"),self.near(i,"o")],k,idx%2,go)
    def outward_load_start(self,i):
        @pl.when(self.inner)
        def _(): self.outward_load(i)
    def outward_send(self,i):
        k,idx,n,b=self.parts_of(i); buf=self.r[k+"a"]
        @pl.when(self.inner)
        def _():
            self.outward_load(i,False)
            if i==3: self.ro(0).wait_send()
            if i==5: self.ro(4).wait_send()
            add_rows(self.r[k+"to"].at[idx%3 if k=="g" else 0],[buf.at[idx%2,0],buf.at[idx%2,1]])
            self.ro(i).start()
    def stage1(self,*pieces):
        for p,i in enumerate(pieces):
            self.outward_load_start(i)
            if p: self.outward_send(pieces[p-1])
        self.outward_send(pieces[-1])
    def sources(self,i):
        b=self.L2[i]==1
        return ([self.view(i,"i"),self.near(i,"i")]+([self.r[f"rin{i}"]] if b else []),
                [self.r[f"ro{i}"]]+([self.near(i,"o")] if b else []))
    def piece_load(self,i):
        k,idx,n,b=self.parts_of(i); s=self.sources(i)
        @pl.when(self.inner)
        def _():
            if (i,"i") in self.MID: self.across(self.MID.index((i,"i"))).wait()
            if b: self.rin(self.RIN.index(i)).wait_recv()
            self.load(s[0],k,idx%2,True)
        @pl.when(self.outer)
        def _():
            self.ro(i).wait_recv()
            self.load(s[1],k,idx%2,True)
    def fin_of(self,i):
        k,idx,n,b=self.parts_of(i)
        return self.r[k+"fin"].at[idx%2 if k=="g" else 0]
    def piece(self,i):
        k,idx,n,b=self.parts_of(i)
        slot=idx%2; buf=self.r[k+"a"]; fin=self.fin_of(i); s=self.sources(i); hn=n//2
        for who,src in ((self.inner,s[0]),(self.outer,s[1])):
            @pl.when(who)
            def _(src=src):
                self.load(src,k,slot,False)
                add_rows(fin,[buf.at[slot,q] for q in range(len(src))])
        self.swap(i).start()
        for cp in self.store(i,fin.at[pl.ds(pl.multiple_of(self.c*hn,hn),hn)],self.c,False): cp.start()
    def swap(self,i):
        k,idx,n,b=self.parts_of(i); hn=n//2
        return self.rcopy(self.fin_of(i).at[pl.ds(pl.multiple_of((1-self.c)*hn,hn),hn)],self.r[k+"sw"].at[idx],self.r["s_w"].at[i],self.r["r_w"].at[i],peer(self.z,4))
    def store(self,i,src,core,theirs):
        ex=2*core+self.L2[i]; k,idx,n,b=self.parts_of(i); slot=idx%2
        if k=="g":
            hc=self.FF//2; h=self.H[i]
            return [pltpu.make_async_copy(src.at[:,pl.ds(t*hc,hc)],self.r[nm].at[ex,:,pl.ds(h*hc,hc)],self.r["so"].at[i,t] if theirs else self.r["st"].at[2*slot+t])
                    for t,nm in enumerate(("gate","up"))]
        return [pltpu.make_async_copy(src,self.r["down"].at[ex],self.r["so"].at[i,0] if theirs else self.r["st"].at[4+slot])]
    def other_half(self,i):
        k,idx,n,b=self.parts_of(i); hn=n//2
        for cp in self.store(i,self.fin_of(i).at[pl.ds(pl.multiple_of(self.c*hn,hn),hn)],self.c,False): cp.wait()
        self.swap(i).wait()
        for cp in self.store(i,self.r[k+"sw"].at[idx],1-self.c,True): cp.start()
    def stores_end(self):
        for i in range(6):
            k,idx,n,b=self.parts_of(i)
            for cp in self.store(i,self.r[k+"sw"].at[idx],1-self.c,True): cp.wait()
    def zsem(self,nm,k): return self.r["s_z"+nm].at[k],self.r["r_z"+nm].at[k]
    def zc(self,nm,k):
        r=self.r; M=r["z"+nm]
        src,dst,dev={0:(M.at[pl.ds(0,2)],r["zr"+nm],peer(self.zi,0)),1:(M.at[2],r["zi"+nm],peer(self.zi,0)),
            2:(r["zs"+nm],r["zm"+nm],peer(self.zx,0)),3:(r["zt"+nm],r["zo"+nm],peer(self.zo,0))}[k]
        s,v=self.zsem(nm,k)
        return self.rcopy(src,dst,s,v,dev)
    def z_inward(self,nm):
        @pl.when(self.outer)
        def _():
            self.zc(nm,0).start(); self.zc(nm,1).start()
    def z_across(self,nm):
        r=self.r
        @pl.when(self.inner)
        def _():
            self.zrecv(nm,0)
            for k in (0,1): add_rows(r["zs"+nm].at[k],[r["z"+nm].at[k],r["zr"+nm].at[k]])
            self.zc(nm,2).start()
    def zrecv(self,nm,k):
        r=self.r; M=r["z"+nm]
        dst={0:r["zr"+nm],1:r["zi"+nm],2:r["zm"+nm],3:r["zo"+nm]}[k]
        src={0:M.at[pl.ds(0,2)],1:M.at[2],2:r["zs"+nm],3:r["zt"+nm]}[k]
        s,v=self.zsem(nm,k)
        dev={0:peer(self.zo,0),1:peer(self.zo,0),2:peer(self.zx,0),3:peer(self.zi,0)}[k]
        self.rcopy(src,dst,s,v,dev).wait_recv()
    def z_last(self,nm):
        r=self.r; M=r["z"+nm]
        @pl.when(self.inner)
        def _():
            self.zrecv(nm,2)
            add_rows(r["zt"+nm],[M.at[3],r["zm"+nm].at[0]])
            self.zc(nm,3).start()
            self.zrecv(nm,1)
            add_rows(r["fi"+nm],[M.at[2],r["zm"+nm].at[1],r["zi"+nm]])
            self.zc(nm,2).wait_send()
        @pl.when(self.outer)
        def _():
            self.zrecv(nm,3)
            add_rows(r["fi"+nm],[M.at[3],r["zo"+nm]])
            self.zc(nm,0).wait_send(); self.zc(nm,1).wait_send()
        for kk in (1,2,3): self.agc(nm,kk).start()
    def agc(self,nm,kk):
        r=self.r
        return self.rcopy(r["fi"+nm],r["ag"+nm].at[kk-1],r["s_ag"+nm].at[kk-1],r["r_ag"+nm].at[kk-1],peer(self.z,kk))
    def z_out(self,nm):
        r=self.r; SG,SD,Q=self.SG,self.SD,self.FF//4; nb=Q//128
        def stores(kk):
            a=xor4(self.e,kk); s=kk%2
            cols=pl.ds(pl.multiple_of(a*Q,Q),Q)
            return [pltpu.make_async_copy(r["og"].at[s,0],r["dgate"].at[:,cols],r["sz"].at[s,0]),
                    pltpu.make_async_copy(r["og"].at[s,1],r["dup"].at[:,cols],r["sz"].at[s,1]),
                    pltpu.make_async_copy(r["od"].at[s],r["ddown"].at[pl.ds(pl.multiple_of(a*SD,SD),SD),:],r["sz"].at[s,2])]
        def store_a(kk,go):
            a=xor4(self.e,kk); s=kk%2
            cols=pl.ds(pl.multiple_of(jnp.minimum(a,2)*self.D,self.D),self.D)
            one=pltpu.make_async_copy(r["oa"].at[s],r["dqkv"].at[:,cols],r["sz"].at[s,0])
            if not go: one.wait(); return
            pl.when(a<3)(lambda: one.start())
            pl.when(a==3)(lambda: pltpu.make_async_copy(r["oa"].at[s],r["dwo"],r["sz"].at[s,0]).start())
        def done(kk):
            if nm=="a": store_a(kk,False)
            else:
                for cp in stores(kk): cp.wait()
        for kk in range(4):
            if kk: self.agc(nm,kk).wait()
            if kk>=2: done(kk-2)
            src=r["fi"+nm] if kk==0 else r["ag"+nm].at[kk-1]
            if nm=="a":
                add_rows(r["oa"].at[kk%2],[src])
                store_a(kk,True)
            else:
                for t in range(2):
                    for b in range(nb):
                        r["og"][kk%2,t,:,b*128:(b+1)*128]=src[(t*nb+b)*SG:(t*nb+b+1)*SG,:].astype(f32)
                off=2*nb*SG
                for b in range(self.D//128):
                    r["od"][kk%2,:,b*128:(b+1)*128]=src[off+b*SD:off+(b+1)*SD,:].astype(f32)
                for cp in stores(kk): cp.start()
        done(2); done(3)
    def rows_of(self,core,zr):
        return pl.ds(pl.multiple_of(2*self.SG*shard_of(zr)+self.SG*core,self.SG),self.SG)
    def at_swap(self,GS):
        return [self.rcopy(GS.at[i,self.rows_of(1-self.c,zr)],self.r["atr"].at[i,zr],self.r["s_at"].at[4*i+zr],self.r["r_at"].at[4*i+zr],peer(self.z,4))
                for i in range(4) for zr in range(4)]
    def at_xy(self,kk):
        return self.rcopy(self.r["sv"].at[xor4(self.e,kk)],self.r["xr"].at[kk-1],self.r["s_xr"].at[kk-1],self.r["r_xr"].at[kk-1],peer(self.z,kk))
    def gcopy(self,k,dev):
        return self.rcopy(self.r["gn"].at[0] ,self.r["gn"].at[k+1],self.r["s_gn"].at[k],self.r["r_gn"].at[k],dev)
    def middle(self):
        self.z_across("b")
        self.across_start((3,4,5,6))
        self.stage1(3,4)
    def finish(self,GS,gg):
        r=self.r; gn=r["gn"]
        sw=self.at_swap(GS)
        for cp in sw: cp.start()
        row=lax.broadcasted_iota(jnp.int32,(8,self.D),0)
        ld=pltpu.make_async_copy(r["fgg"],gn.at[7],r["st2"].at[1]); ld.start(); ld.wait()
        gn[0]=jnp.where(row==0,gg,jnp.where(row==1,gn[7],0.0))
        self.gcopy(0,peer(self.z,4)).start()
        self.piece_load(0)
        self.piece_load(1)
        self.outward_load_start(5)
        self.piece(0)
        for cp in sw: cp.wait()
        for i in range(4):
            for zr in range(4):
                add_rows(r["sv"].at[i,zr],[GS.at[i,self.rows_of(self.c,zr)],r["atr"].at[i,zr]])
        for kk in (1,2,3): self.at_xy(kk).start()
        self.outward_send(5)
        self.gcopy(0,peer(self.z,4)).wait()
        gn[0]=gn[0]+gn[1]
        for kk in (1,2,3): self.gcopy(kk,peer(self.z,kk)).start()
        self.z_last("b")
        self.piece(1)
        self.other_half(0)
        self.piece_load(2)
        self.other_half(1)
        self.piece(2)
        self.piece_load(3)
        for kk in (1,2,3): self.gcopy(kk,peer(self.z,kk)).wait()
        gn[0]=(gn[0]+gn[2])+(gn[3]+gn[4])
        @pl.when(self.outer)
        def _(): self.gcopy(4,peer(self.zi,0)).start()
        self.z_out("b")
        for kk in (1,2,3): self.at_xy(kk).wait()
        for zr in range(4): add_rows(r["za"].at[zr],[r["sv"].at[self.e,zr]]+[r["xr"].at[k,zr] for k in range(3)])
        self.z_inward("a")
        @pl.when(self.inner)
        def _():
            self.gcopy(4,peer(self.zo,0)).wait_recv()
            gn[0]=gn[0]+gn[5]
            self.gcopy(5,peer(self.zx,0)).start()
        self.piece(3)
        self.z_across("a")
        self.other_half(2)
        self.piece_load(4)
        @pl.when(self.inner)
        def _():
            self.gcopy(5,peer(self.zx,0)).wait()
            gn[0]=gn[0]+gn[6]
            self.gcopy(6,peer(self.zo,0)).start()
        self.other_half(3)
        self.z_last("a")
        self.piece(4)
        self.piece_load(5)
        @pl.when(self.outer)
        def _():
            self.gcopy(4,peer(self.zi,0)).wait_send()
            self.gcopy(6,peer(self.zi,0)).wait_recv()
            gn[0]=gn[7]
        gcp=pltpu.make_async_copy(gn.at[0],r["gains"],r["st2"].at[3]); gcp.start()
        self.other_half(4)
        self.piece(5)
        self.z_out("a")
        self.other_half(5)
        self.stores_end()
        gcp.wait()
        @pl.when(self.inner)
        def _():
            self.gcopy(6,peer(self.zo,0)).wait_send()
            for i in (1,2,3,5): self.ro(i).wait_send()
            self.zc("a",3).wait_send(); self.zc("b",3).wait_send()
        @pl.when(self.outer)
        def _():
            for k in range(3): self.rin(k).wait_send()
        self.rows_home(False)
        for cp in plane_copies([(r["rbs"],r["rb"])],self.plane): cp.wait()

f32=jnp.float32; bf16=jnp.bfloat16
def nn(a,b): return lax.dot_general(a,b,(((1,),(0,)),((),())),preferred_element_type=f32)
def nt(a,b): return lax.dot_general(a,b,(((1,),(1,)),((),())),preferred_element_type=f32)
def tn(a,b): return lax.dot_general(a,b,(((0,),(0,)),((),())),preferred_element_type=f32)
EPS=1e-6
E=16; CAP=120
HD=64; GH=4; GW=GH*HD; QC=256
def lane_head(shape):
    return lax.broadcasted_iota(jnp.int32,shape,1)//HD
def swap_half(x):
    w=x.shape[1]
    first=(lax.broadcasted_iota(jnp.int32,x.shape,1)%HD)<HD//2
    return jnp.where(first,pltpu.roll(x,w-HD//2,1),pltpu.roll(x,HD//2,1))
def wide(t):
    return jnp.concatenate([t,t],axis=1)
def inv_rms(v):
    return lax.rsqrt(jnp.mean(v*v,axis=1,keepdims=True)+EPS)

def attn_fwd(tokens, prefix, again, wqkv, wo, fgain, cosw, sinw, rows=None, sout=None):
    T,D=tokens.shape
    ng=D//GW; nq=T//QC
    fused=rows is not None
    NS=E*CAP; CH=480
    def kernel(pre,tok,ag,fg,wq,wk,wv,wor,cw,sw,*rest):
        if fused:
            rowr,so,qo,ko,vo,atto,lseo,stateo,ntwoo,xo,sia,sib,normed,bias,q4,k4,vT,OT,acc,*sems=rest
        else:
            qo,ko,vo,atto,lseo,stateo,ntwoo,normed,bias,q4,k4,vT,OT,acc=rest
        g=pl.program_id(0)
        @pl.when(g==0)
        def _():
            if fused:
                plane_barrier()
                for cpy in plane_copies([(so.at[0],sia),(so.at[1],sib)],sems): cpy.start()
            for c in range(nq):
                r=slice(c*QC,(c+1)*QC)
                x=tok[r,:].astype(f32)
                normed[r,:]=(x*inv_rms(x)*ag[...]).astype(bf16)
                j=lax.broadcasted_iota(jnp.int32,(T,QC),0)
                i=lax.broadcasted_iota(jnp.int32,(T,QC),1)+c*QC
                bias[c]=jnp.where((j<=i)|(j<pre[0]),0.0,-1e30)
        for c in range(nq):
            r=slice(c*QC,(c+1)*QC)
            n=normed[r,:]
            C=wide(cw[r,:]); S=wide(sw[r,:])
            q=nn(n,wq[...]); k=nn(n,wk[...]); v=nn(n,wv[...])
            qb=((q*C+swap_half(q)*S).astype(bf16)).astype(f32)*(HD**-0.5)
            qb=qb.astype(bf16)
            kb=(k*C+swap_half(k)*S).astype(bf16)
            q4[r,:]=qb; qo[r,:]=qb
            k4[r,:]=kb; ko[r,:]=kb
            vo[r,:]=v.astype(bf16)
            vT[:,r]=v.T.astype(bf16)
        lh=lane_head((QC,GW))
        @pl.loop(0,GH)
        def _(h):
            hr=pl.ds(pl.multiple_of(h*HD,HD),HD)
            for c in range(nq):
                r=slice(c*QC,(c+1)*QC)
                qm=jnp.where(lh==h,q4[r,:],jnp.zeros((),bf16))
                st=nt(k4[...],qm)+bias[c]
                m=jnp.max(st,axis=0,keepdims=True)
                p=jnp.exp(st-m)
                l=jnp.sum(p,axis=0,keepdims=True)
                ot=nn(vT[hr,:],p.astype(bf16))
                OT[c,hr,:]=ot*(1.0/l)
                lseo[0,pl.ds(h,1),r]=m+jnp.log(l)
        for c in range(nq):
            r=slice(c*QC,(c+1)*QC)
            a=OT[c].T.astype(bf16)
            atto[r,:]=a
            o=nn(a,wor[...])
            @pl.when(g==0)
            def _(): acc[r,:]=o+tok[r,:].astype(f32)
            @pl.when(g>0)
            def _(): acc[r,:]+=o
        @pl.when(g==ng-1)
        def _():
            for c in range(nq):
                r=slice(c*QC,(c+1)*QC)
                st=acc[r,:]
                stateo[r,:]=st
                ntwoo[r,:]=(st*inv_rms(st)*fg[...]).astype(bf16)
            if fused:
                for i in range(NS//CH):
                    si=lax.broadcasted_iota(jnp.int32,(CH,T),0)+i*CH
                    d=jnp.where((si==rowr[0:1,:])|(si==rowr[1:2,:]),1.0,0.0).astype(bf16)
                    xo[i*CH:(i+1)*CH,:]=nn(d,ntwoo[...]).astype(bf16)
                for cpy in plane_copies([(so.at[0],sia),(so.at[1],sib)],sems): cpy.wait()
    full=lambda s: pl.BlockSpec(s,lambda g:(0,)*len(s))
    col=lambda off: pl.BlockSpec((D,GW),lambda g,off=off:(0,g+off))
    tcol=pl.BlockSpec((T,GW),lambda g:(0,g))
    return pl.pallas_call(kernel,grid=(ng,),
      in_specs=[pl.BlockSpec(memory_space=pltpu.SMEM),full((T,D)),full((1,D)),full((1,D)),col(0),col(ng),col(2*ng),pl.BlockSpec((GW,D),lambda g:(g,0)),full((T,128)),full((T,128))]+([full((8,T)),pl.BlockSpec(memory_space=pl.ANY)] if fused else []),
      out_specs=[tcol,tcol,tcol,tcol,pl.BlockSpec((1,8,T),lambda g:(g,0,0)),full((T,D)),full((T,D))]+([full((NS,D))]+[pl.BlockSpec(memory_space=pl.ANY)]*2 if fused else []),
      out_shape=[jax.ShapeDtypeStruct((T,D),bf16)]*4+[jax.ShapeDtypeStruct((ng,8,T),f32),jax.ShapeDtypeStruct((T,D),f32),jax.ShapeDtypeStruct((T,D),bf16)]+([jax.ShapeDtypeStruct((NS,D),bf16),*[jax.ShapeDtypeStruct((8,CAP,D),bf16)]*2] if fused else []),
      scratch_shapes=[pltpu.VMEM((T,D),bf16),pltpu.VMEM((nq,T,QC),f32),pltpu.VMEM((T,GW),bf16),pltpu.VMEM((T,GW),bf16),pltpu.VMEM((GW,T),bf16),pltpu.VMEM((nq,GW,QC),f32),pltpu.VMEM((T,D),f32)]+(plane_sems(2) if fused else []),
      compiler_params=pltpu.CompilerParams(vmem_limit_bytes=56<<20,dimension_semantics=("arbitrary",),**(dict(collective_id=0,has_side_effects=True) if fused else {})),
      cost_estimate=pl.CostEstimate(flops=2*T*D*4*D+4*T*T*D,bytes_accessed=16<<20,transcendentals=12*T*T),
      name="attn_fwd")(prefix,tokens,again[None],fgain[None],wqkv,wqkv,wqkv,wo,cosw,sinw,*([rows,sout] if fused else []))

def attn_bwd(sgrad, prefix, tokens, again, wqkv, wo, cosw, sinw, q, k, v, att, lse, tail=None):
    T,D=tokens.shape
    ng=D//GW; nq=T//QC
    fast=tail is not None
    def kernel(pre,sg,tok,ag,wq,wk,wv,wor,cw,sw,qr,kr,vr,attr,lser,*rest):
        if fast:
            ni,no=len(tail.in_specs),len(tail.out_specs)
            tgo,ggo=rest[ni:ni+2]
            tins,touts=rest[:ni],rest[ni+2:ni+2+no]
            normedT,bg,bias,dO,kT,PB,DS,dv,dk,dqT,drow,acc,GS,*tscr=rest[ni+2+no:]
            tail.bind(tins,touts,tscr)
        else:
            tgo,ggo,gq,gk,gv,gwo,normedT,bg,bias,dO,kT,PB,DS,dv,dk,dqT,drow,acc=rest
        g=pl.program_id(0)
        if fast:
            @pl.when(g==0)
            def _():
                tail.start()
            @pl.when(g==ng-1)
            def _():
                tail.middle()
        @pl.when(g==0)
        def _():
            for c in range(nq):
                r=slice(c*QC,(c+1)*QC)
                x=tok[r,:].astype(f32)
                n=x*inv_rms(x)*ag[...]
                normedT[:,r]=n.T.astype(bf16)
                bg[r,:]=sg[r,:].astype(bf16)
                j=lax.broadcasted_iota(jnp.int32,(T,QC),0)
                i=lax.broadcasted_iota(jnp.int32,(T,QC),1)+c*QC
                bias[c]=jnp.where((j<=i)|(j<pre[0]),0.0,-1e30).astype(bf16)
        hmask=(lax.broadcasted_iota(jnp.int32,(8,GW),0)==lane_head((8,GW))).astype(f32)
        for c in range(nq):
            r=slice(c*QC,(c+1)*QC)
            d=nt(bg[r,:],wor[...]).astype(bf16)
            dO[r,:]=d
            a=attr[r,:].astype(f32)
            drow[:,r]=lax.dot_general(hmask,d.astype(f32)*a,(((1,),(1,)),((),())),preferred_element_type=f32,precision=lax.Precision.HIGHEST)
            kT[:,r]=kr[r,:].astype(f32).T.astype(bf16)
        gwv=tn(attr[...],bg[...]).astype(bf16)
        if fast:
            GS[3,pl.ds(pl.multiple_of(g*GW,GW),GW),:]=gwv
        else:
            gwo[...]=gwv
        dv[...]=jnp.zeros_like(dv); dk[...]=jnp.zeros_like(dk)
        lh=lane_head((QC,GW)); lhT=lane_head((T,GW))
        @pl.loop(0,GH)
        def _(h):
            hr=pl.ds(pl.multiple_of(h*HD,HD),HD)
            zero=jnp.zeros((),bf16)
            for c in range(nq):
                r=slice(c*QC,(c+1)*QC)
                qm=jnp.where(lh==h,qr[r,:],zero)
                dOm=jnp.where(lh==h,dO[r,:],zero)
                st=nt(kr[...],qm)+bias[c].astype(f32)
                p=jnp.exp(st-lser[0,pl.ds(h,1),r])
                PB[:,r]=p.astype(bf16)
                dp=nt(vr[...],dOm)
                DS[:,r]=(p*(dp-drow[pl.ds(h,1),r])).astype(bf16)
            dv[...]+=nn(PB[...],jnp.where(lhT==h,dO[...],zero))
            dk[...]+=nn(DS[...],jnp.where(lhT==h,qr[...],zero))
            dqT[hr,:]=nn(kT[hr,:],DS[...])
        for c in range(nq):
            r=slice(c*QC,(c+1)*QC)
            C=wide(cw[r,:]); S=wide(sw[r,:])
            dq=dqT[:,r].T*(HD**-0.5)
            dq=dq*C-swap_half(dq)*S
            dkk=dk[r,:]
            dkk=dkk*C-swap_half(dkk)*S
            a=dq.astype(bf16); b=dkk.astype(bf16); e=dv[r,:].astype(bf16)
            PB[r,0:GW]=a; PB[r,GW:2*GW]=b; PB[r,2*GW:3*GW]=e
            o=nt(a,wq[...])+nt(b,wk[...])+nt(e,wv[...])
            @pl.when(g==0)
            def _(): acc[r,:]=o
            @pl.when(g>0)
            def _(): acc[r,:]+=o
        for i in range(3):
            gval=nn(normedT[...],PB[:,i*GW:(i+1)*GW]).astype(bf16)
            if fast:
                GS[i,:,pl.ds(pl.multiple_of(g*GW,GW),GW)]=gval
            else:
                (gq,gk,gv)[i][...]=gval
        @pl.when(g==ng-1)
        def _():
            gg=jnp.zeros((1,D),f32)
            for c in range(nq):
                r=slice(c*QC,(c+1)*QC)
                x=tok[r,:].astype(f32)
                inv=inv_rms(x); u=x*inv
                ngd=acc[r,:]
                gg=gg+jnp.sum(ngd*u,axis=0,keepdims=True)
                w=ngd*ag[...]
                tgo[r,:]=(sg[r,:]+inv*(w-u*jnp.mean(w*u,axis=1,keepdims=True))).astype(bf16)
            ggo[...]=jnp.broadcast_to(gg,(8,D))
            if fast:
                tail.finish(GS,gg)
    full=lambda s: pl.BlockSpec(s,lambda g:(0,)*len(s),pipeline_mode=pl.Buffered(1))
    col=lambda off: pl.BlockSpec((D,GW),lambda g,off=off:(0,g+off))
    tcol=pl.BlockSpec((T,GW),lambda g:(0,g))
    if fast:
        outs=tail.out_specs; oshape=tail.oshape
        extra=[pltpu.VMEM((4,D,D),bf16)]+tail.scratch
    else:
        outs=[tcol,tcol,tcol,pl.BlockSpec((GW,D),lambda g:(g,0))]
        oshape=[jax.ShapeDtypeStruct((D,D),bf16)]*4
        extra=[]
    rowb=pl.BlockSpec((GW,D),lambda g:(g,0))
    return pl.pallas_call(kernel,grid=(ng,),
      in_specs=[pl.BlockSpec(memory_space=pltpu.SMEM)]+[full((T,D)),full((T,D)),full((1,D)),col(0),col(ng),col(2*ng),rowb,full((T,128)),full((T,128)),tcol,tcol,tcol,tcol,pl.BlockSpec((1,8,T),lambda g:(g,0,0))]+(tail.in_specs if fast else []),
      out_specs=[full((T,D)),full((8,D))]+outs,
      out_shape=[jax.ShapeDtypeStruct((T,D),bf16),jax.ShapeDtypeStruct((8,D),f32)]+oshape,
      scratch_shapes=[pltpu.VMEM((D,T),bf16),pltpu.VMEM((T,D),bf16),pltpu.VMEM((nq,T,QC),bf16),pltpu.VMEM((T,GW),bf16),pltpu.VMEM((GW,T),bf16),
        pltpu.VMEM((T,T),bf16),pltpu.VMEM((T,T),bf16),pltpu.VMEM((T,GW),f32),pltpu.VMEM((T,GW),f32),pltpu.VMEM((GW,T),f32),pltpu.VMEM((8,T),f32),pltpu.VMEM((T,D),f32)]+extra,
      compiler_params=pltpu.CompilerParams(vmem_limit_bytes=63<<20,dimension_semantics=("arbitrary",),**(dict(collective_id=5,has_side_effects=True) if fast else {})),
      cost_estimate=pl.CostEstimate(flops=2*T*D*8*D+10*T*T*D,bytes_accessed=24<<20,transcendentals=12*T*T),
      name="attn_bwd")(prefix,sgrad,tokens,again[None],wqkv,wqkv,wqkv,wo,cosw,sinw,q,k,v,att,lse,*(tail.arrays if fast else ()))


def make_ffn(parts, G, L, cap, D, FF, FB, chunk, out_dt):
    R=parts*G*cap
    nf=FF//FB
    def kernel(*refs):
        xs=refs[:parts]; ss=refs[parts:2*parts]
        wg,wu,wd=refs[2*parts:2*parts+3]
        o=2*parts+3
        res=refs[o:o+parts]; dgr=refs[o+parts:o+2*parts]
        gG,gU,gD=refs[o+2*parts:o+2*parts+3]
        X,S,H,GB,UB,AR,AD=refs[o+2*parts+3:]
        f=pl.program_id(1)
        @pl.when(f==0)
        def _():
            for p in range(parts):
                for g in range(G):
                    r=(p*G+g)*cap
                    X[r:r+cap,:]=xs[p][g,0]
                    S[r:r+cap,:]=ss[p][g,0]
        @pl.loop(0,R//chunk)
        def _(i):
            rows=pl.ds(pl.multiple_of(i*chunk,chunk),chunk)
            x=X[rows,:]; s=S[rows,:]
            gate=nn(x,wg[0]); up=nn(x,wu[0]); hg=nt(s,wd[0])
            sig=1.0/(1.0+jnp.exp(-gate))
            sil=gate*sig
            h=(sil*up).astype(bf16)
            gb=(hg*up*(sig*(1.0+gate*(1.0-sig)))).astype(bf16)
            ub=(hg*sil).astype(bf16)
            H[rows,:]=h; GB[rows,:]=gb; UB[rows,:]=ub
            r=nn(h,wd[0]); d=nt(gb,wg[0])+nt(ub,wu[0])
            @pl.when(f==0)
            def _():
                AR[rows,:]=r; AD[rows,:]=d
            @pl.when(f>0)
            def _():
                AR[rows,:]+=r; AD[rows,:]+=d
        gG[0]=tn(X[...],GB[...]).astype(bf16)
        gU[0]=tn(X[...],UB[...]).astype(bf16)
        gD[0]=tn(H[...],S[...]).astype(bf16)
        @pl.when(f==nf-1)
        def _():
            for p in range(parts):
                for g in range(G):
                    r=(p*G+g)*cap
                    res[p][g,0]=AR[r:r+cap,:].astype(out_dt)
                    dgr[p][g,0]=AD[r:r+cap,:].astype(out_dt)
    rowspec=pl.BlockSpec((G,1,cap,D),lambda l,f:(0,l,0,0))
    wspec=pl.BlockSpec((1,D,FB),lambda l,f:(l,0,f))
    wdspec=pl.BlockSpec((1,FB,D),lambda l,f:(l,f,0))
    call=pl.pallas_call(kernel,
      out_shape=[jax.ShapeDtypeStruct((G,L,cap,D),out_dt)]*(2*parts)+[jax.ShapeDtypeStruct((L,D,FF),bf16)]*2+[jax.ShapeDtypeStruct((L,FF,D),bf16)],
      grid=(L,nf),
      in_specs=[rowspec]*(2*parts)+[wspec,wspec,wdspec],
      out_specs=[rowspec]*(2*parts)+[wspec,wspec,wdspec],
      scratch_shapes=[pltpu.VMEM((R,D),bf16)]*2+[pltpu.VMEM((R,FB),bf16)]*3+[pltpu.VMEM((R,D),f32)]*2,
      compiler_params=pltpu.CompilerParams(vmem_limit_bytes=60<<20,dimension_semantics=("arbitrary","arbitrary")),
      cost_estimate=pl.CostEstimate(flops=2*9*R*D*FF*L,bytes_accessed=L*(6*D*FF*2+4*R*D*2),transcendentals=R*FF*L),
      name="ffn")
    return call


def ffn_rows(x,s,wg,wu,wd,H,GB,UB,rows):
    gate=nn(x,wg); up=nn(x,wu); hg=nt(s,wd)
    sig=1.0/(1.0+jnp.exp(-gate))
    sil=gate*sig
    h=(sil*up).astype(bf16)
    gb=(hg*up*(sig*(1.0+gate*(1.0-sig)))).astype(bf16)
    ub=(hg*sil).astype(bf16)
    H[rows,:]=h; GB[rows,:]=gb; UB[rows,:]=ub
    return nn(h,wd),nt(gb,wg)+nt(ub,wu)

def expert_ffn(deps, l2, xs, ss, wg, wu, wd, f0, nf, prev=(), carry=None, dense=None, inw=None, ext=None, gprev=None, cid=None, FB=512, chunk=480):
    n=len(xs); RG,D=xs[0].shape; FF=wg.shape[2]; R=n*RG; HB=2*FB; ng=nf//2
    SR=D//4; np_=len(prev); nc=0 if carry is None else 1; nd=0 if dense is None else 1
    part=pl.ds(dense[1],dense[2]) if nd else None
    nx=len(deps); nz=0 if inw is None else 2; ne=0 if ext is None else 1; ngp=0 if gprev is None else 6*ng+ng
    def kernel(*refs):
        refs=refs[nx:]
        xr=refs[:n]; sr=refs[n:2*n]; wgr,wur,wdr=refs[2*n:2*n+3]; o=2*n+3
        pv=refs[o:o+np_]; o+=np_
        csrc=refs[o:o+nc]; o+=nc
        dsrc=refs[o:o+nd]; o+=nd
        zsrc=refs[o:o+nz]; o+=nz
        esrc=refs[o:o+ne]; o+=ne
        gp=refs[o:o+ngp]; o+=ngp
        res=refs[o:o+n]; dgr=refs[o+n:o+2*n]; o+=2*n
        gus=[refs[o+3*q:o+3*q+3] for q in range(ng)]; o+=3*ng
        dws=refs[o:o+ng]; o+=ng
        cdst=refs[o:o+nc]; o+=nc
        ddst=refs[o:o+nd]; o+=nd
        zdst=refs[o:o+nz//2]; o+=nz//2
        edst=refs[o:o+ne]; o+=ne
        XT,XN,H,GB,UB,AR,AD=refs[o:o+7]; sems=refs[o+7:]
        f=pl.program_id(0)
        def copies():
            return (plane_copies([(csrc[0],cdst[0])],sems[2*nd+nz+2*ne:]) if nc else [])+(row_copies(dsrc[0],ddst[0],part,sems[nz+2*ne:nz+2*ne+2]) if nd else [])
        if nc or nd or nz:
            @pl.when(f==0)
            def _():
                if nz:
                    if ne: home_barrier()
                    else: plane_z_barrier()
                    inward_run(zsrc,zdst[0],sems[:2],True)
                else:
                    plane_barrier()
                if ne: ext_run(esrc[0],edst[0],sems[nz:nz+2],True)
                for cpy in copies(): cpy.start()
        @pl.when(f==0)
        def _():
            for a in range(n):
                for b in range(RG//chunk):
                    XN[...]=xr[a][b*chunk:(b+1)*chunk,:].astype(f32).T.astype(bf16)
                    for q in range(4):
                        XT[a*(RG//chunk)+b,q*SR:(q+1)*SR,:]=XN[pl.ds(pl.multiple_of(shard_of(q)*SR,SR),SR),:]
        for a in range(n):
            @pl.loop(0,RG//chunk)
            def _(i):
                src=pl.ds(pl.multiple_of(i*chunk,chunk),chunk)
                rows=pl.ds(pl.multiple_of(a*RG+i*chunk,chunk),chunk)
                r,d=ffn_rows(xr[a][src,:],sr[a][src,:],wgr[0],wur[0],wdr[0],H,GB,UB,rows)
                @pl.when(f==0)
                def _():
                    if np_:
                        AR[rows,:]=r+pv[a][src,:].astype(f32); AD[rows,:]=d+pv[n+a][src,:].astype(f32)
                    else:
                        AR[rows,:]=r; AD[rows,:]=d
                if nf>2:
                    @pl.when((f>0)&(f<nf-1))
                    def _():
                        AR[rows,:]+=r; AD[rows,:]+=d
                @pl.when(f==nf-1)
                def _():
                    res[a][src,:]=(AR[rows,:]+r).astype(bf16); dgr[a][src,:]=(AD[rows,:]+d).astype(bf16)
        for t,Y in enumerate((GB,UB)):
            gv=None
            for b in range(R//chunk):
                p=nn(XT[b],Y[b*chunk:(b+1)*chunk,:])
                gv=p if gv is None else gv+p
            cols=pl.ds(pl.multiple_of(t*HB+lax.rem(f,2)*FB,FB),FB)
            for q in range(ng):
                def put(q=q,t=t,gv=gv,cols=cols):
                    for s,(ref,lo,hi) in enumerate(zip(gus[q],(0,2*SR,3*SR),(2*SR,3*SR,4*SR))):
                        v=gv[lo:hi]
                        if ngp: v=v+gp[6*q+3*t+s][...].astype(f32)
                        ref[:,cols]=v.astype(bf16)
                if ng==1: put()
                else: pl.when(lax.div(f,2)==q)(put)
        dv=None
        for a in range(n):
            t=tn(H[a*RG:(a+1)*RG,:],sr[a][...])
            dv=t if dv is None else dv+t
        for q in range(ng):
            def put(q=q,dv=dv):
                dws[q][...]=((dv+gp[6*ng+q][...].astype(f32)) if ngp else dv).astype(bf16)
            if ng==1: put()
            else: pl.when(lax.div(f,2)==q)(put)
        if nc or nd or nz:
            @pl.when(f==nf-1)
            def _():
                for cpy in copies(): cpy.wait()
                if nz: inward_run(zsrc,zdst[0],sems[:2],False)
                if ne: ext_run(esrc[0],edst[0],sems[nz:nz+2],False)
    one=pl.Buffered(1)
    rowspec=pl.BlockSpec((RG,D),lambda f:(0,0),pipeline_mode=one)
    wspec=pl.BlockSpec((1,D,FB),lambda f:(2*spot()[0]+l2,0,f+f0))
    wdspec=pl.BlockSpec((1,FB,D),lambda f:(2*spot()[0]+l2,f+f0,0))
    full=lambda r,c: pl.BlockSpec((r,c),lambda f:(0,0),pipeline_mode=one)
    anyspec=pl.BlockSpec(memory_space=pl.ANY)
    wspecs=[pl.BlockSpec((FB,D),lambda f: ((1-f) if f0 else f,0))] if ng==1 else [
        pl.BlockSpec((FB,D),lambda f: (jnp.minimum(f,1),0)),pl.BlockSpec((FB,D),lambda f: (jnp.minimum(3-f,1),0))]
    gpspecs=[]; gpargs=[]
    if ngp:
        for q in range(ng):
            for t in range(2):
                for s,rr in enumerate((2*SR,SR,SR)):
                    gpspecs.append(pl.BlockSpec((rr,FB),lambda f,q=q,t=t: (0,2*t+jnp.clip(f-2*q,0,1))))
                    gpargs.append(gprev[q][s])
        gpspecs+=wspecs; gpargs+=list(gprev[ng:])
    out=pl.pallas_call(kernel,grid=(nf,),
        in_specs=[anyspec]*nx+[rowspec]*(2*n)+[wspec,wspec,wdspec]+[rowspec]*np_+[anyspec]*(nc+nd+nz+ne)+gpspecs,
        out_specs=[rowspec]*(2*n)+[full(2*SR,2*HB),full(SR,2*HB),full(SR,2*HB)]*ng+wspecs+[anyspec]*(nc+nd+nz//2+ne),
        scratch_shapes=[pltpu.VMEM((R//chunk,D,chunk),bf16),pltpu.VMEM((D,chunk),bf16)]+[pltpu.VMEM((R,FB),bf16)]*3+[pltpu.VMEM((R,D),f32)]*2+([pltpu.SemaphoreType.DMA((1,)),pltpu.SemaphoreType.DMA((1,))] if nz else [])+(ext_sems() if ne else [])+(row_sems() if nd else [])+(plane_sems(1) if nc else []),
      out_shape=[jax.ShapeDtypeStruct((RG,D),bf16)]*(2*n)+([jax.ShapeDtypeStruct((2*SR,2*HB),bf16)]+[jax.ShapeDtypeStruct((SR,2*HB),bf16)]*2)*ng+[jax.ShapeDtypeStruct((HB,D),bf16)]*ng+[jax.ShapeDtypeStruct((8,RG//8,D),bf16)]*nc+([jax.ShapeDtypeStruct((3,dense[2])+dense[0].shape[2:],bf16)] if nd else [])+([jax.ShapeDtypeStruct(inw[0].shape,bf16)] if nz else [])+([jax.ShapeDtypeStruct(ext.shape,bf16)] if ne else []),
      compiler_params=pltpu.CompilerParams(vmem_limit_bytes=62<<20,dimension_semantics=("arbitrary",),**(dict(collective_id=cid,has_side_effects=True) if nc or nd or nz else {})),
      cost_estimate=pl.CostEstimate(flops=9*R*D*FF*ng,bytes_accessed=3*D*FF*2*ng+4*R*D*2,transcendentals=R*FF*ng//2),
      name=f"expert_ffn{n}_{f0}")(*deps,*xs,*ss,wg,wu,wd,*prev,*([carry] if nc else []),*([dense[0]] if nd else []),*(inw if nz else ()),*([ext] if ne else []),*gpargs)
    o=2*n
    return (out[:o],*[out[o+3*q:o+3*q+3] for q in range(ng)],*out[o+3*ng:])

def shared_ffn(x, s, wg, wu, wd, xout, sa, FB=512):
    T,D=x.shape; FF=wg.shape[1]; nf=FF//FB; chunk=T//2
    SG=D//8; SD=FB//8
    NR=2*SG*(FB//128)+SD*(D//128)
    def kernel(xr,sr,wgr,wur,wdr,xo,zs,res,dgr,o0,o1,xia,xib,zd,XT,H,GB,UB,VG,VD,zs0,zs1,*sems):
        f=pl.program_id(0)
        core=spot()[0]
        pairs=[(xo.at[0],xia),(xo.at[1],xib)]
        @pl.when(f==0)
        def _():
            plane_z_barrier()
            for cpy in plane_copies(pairs,sems): cpy.start()
            inward_run((zs,zs),zd,(zs0,zs1),True)
        @pl.when(f==0)
        def _():
            for b in range(2):
                XT[:,b*chunk:(b+1)*chunk]=xr[b*chunk:(b+1)*chunk,:].astype(f32).T.astype(bf16)
        @pl.loop(0,T//chunk)
        def _(i):
            rows=pl.ds(pl.multiple_of(i*chunk,chunk),chunk)
            r,d=ffn_rows(xr[rows,:],sr[rows,:],wgr[...],wur[...],wdr[...],H,GB,UB,rows)
            @pl.when(f==0)
            def _():
                res[rows,:]=r; dgr[rows,:]=d
            @pl.when(f>0)
            def _():
                res[rows,:]+=r; dgr[rows,:]+=d
        for t,Y in enumerate((GB,UB)):
            VG[...]=nn(XT[...],Y[...]).astype(bf16)
            for zr in range(4):
                for cp in range(2):
                    src=pl.ds(pl.multiple_of(2*SG*shard_of(zr)+SG*lax.rem(core+cp,2),SG),SG)
                    for b in range(FB//128):
                        off=(t*(FB//128)+b)*SG
                        (o0,o1)[cp][f,zr,off:off+SG,:]=VG[src,b*128:(b+1)*128]
        VD[...]=tn(H[...],sr[...]).astype(bf16)
        zr=jnp.where(spot()[1]<2,3-f,f)
        for cp in range(2):
            for e in range(4):
                src=pl.ds(pl.multiple_of(lax.rem(core+cp,2)*4*SD+e*SD,SD),SD)
                for b in range(D//128):
                    off=2*SG*(FB//128)+b*SD
                    (o0,o1)[cp][e,zr,off:off+SD,:]=VD[src,b*128:(b+1)*128]
        @pl.when(f==nf-1)
        def _():
            for cpy in plane_copies(pairs,sems): cpy.wait()
            inward_run((zs,zs),zd,(zs0,zs1),False)
    full=lambda sh: pl.BlockSpec(sh,lambda f:(0,)*len(sh))
    return pl.pallas_call(kernel,grid=(nf,),
      in_specs=[full((T,D)),full((T,D)),pl.BlockSpec((D,FB),lambda f:(0,f)),pl.BlockSpec((D,FB),lambda f:(0,f)),pl.BlockSpec((FB,D),lambda f:(f,0))]+[pl.BlockSpec(memory_space=pl.ANY)]*2,
      out_specs=[full((T,D)),full((T,D)),full((4,4,NR,128)),full((4,4,NR,128))]+[pl.BlockSpec(memory_space=pl.ANY)]*3,
      out_shape=[jax.ShapeDtypeStruct((T,D),f32)]*2+[jax.ShapeDtypeStruct((4,4,NR,128),bf16)]*2+[jax.ShapeDtypeStruct(xout.shape[1:],bf16)]*3,
      scratch_shapes=[pltpu.VMEM((D,T),bf16)]+[pltpu.VMEM((T,FB),bf16)]*3+[pltpu.VMEM((D,FB),bf16),pltpu.VMEM((FB,D),bf16)]+[pltpu.SemaphoreType.DMA((1,))]*2+plane_sems(2),
      compiler_params=pltpu.CompilerParams(vmem_limit_bytes=62<<20,dimension_semantics=("arbitrary",),collective_id=1,has_side_effects=True),
      cost_estimate=pl.CostEstimate(flops=2*9*T*D*FF,bytes_accessed=6*D*FF*2+8*T*D*2,transcendentals=T*FF),
      name="shared_ffn")(x,s,wg,wu,wd,xout,sa)


def route(order, expert_ids, gates, cot, core, G, L, parts, plane=False):
    T,D=cot.shape; P2=2*T
    LP=L//parts; S=G*LP*CAP
    big=E*CAP
    CH=480 if S%480==0 else CAP*4
    def kernel(core_ref,orow,ids,gts,ct,rowo,colo,*rest):
        sgs=rest[:parts]; PT,PG=rest[parts:]
        lane=lax.broadcasted_iota(jnp.int32,(T,128),1)
        e0=ids[:,0:1].astype(f32); e1=ids[:,1:2].astype(f32)
        er=jnp.where(lane==0,e0,jnp.where(lane==1,e1,0.0)).T[0:8,:]
        ecat=jnp.concatenate([er[0:1,:],er[1:2,:]],axis=1)
        eoh=(lax.broadcasted_iota(jnp.int32,(E,P2),0).astype(f32)==ecat)
        eohb=jnp.where(eoh,1.0,0.0).astype(bf16)
        o=orow[...]
        oj=(o&1)*T+(o>>1)
        CB=256
        for c in range(P2//CB):
            jj=lax.broadcasted_iota(jnp.int32,(CB,P2),0)+c*CB
            PT[c*CB:(c+1)*CB,:]=jnp.where(jj==oj,1.0,0.0).astype(bf16)
        soh=nn(eohb,PT[...])
        sohb=soh.astype(bf16)
        tri=jnp.where(lax.broadcasted_iota(jnp.int32,(CB,CB),0)<lax.broadcasted_iota(jnp.int32,(CB,CB),1),1.0,0.0).astype(bf16)
        run=jnp.zeros((E,1),f32)
        pos=[]
        for c in range(P2//CB):
            blk=soh[:,c*CB:(c+1)*CB]
            before=nn(sohb[:,c*CB:(c+1)*CB],tri)+run
            run=run+jnp.sum(blk,axis=1,keepdims=True)
            pos.append(jnp.sum(before*blk,axis=0,keepdims=True))
        posr=jnp.minimum(jnp.concatenate(pos,axis=1),127.0)
        posj=nt(jnp.broadcast_to(posr,(16,P2)).astype(bf16),PT[...])[0:1,:]
        e=ecat.astype(jnp.int32)
        l=lax.rem(e,L); j=lax.div(e,L)
        if plane:
            base=((lax.rem(l,2)*2+lax.div(l,2))*G+j)*CAP
        elif parts==2:
            cc=lax.rem(lax.div(l,LP)+core_ref[0],2)
            base=((cc*G+j)*LP+lax.rem(l,LP))*CAP
        else:
            base=e*CAP
        p=posj.astype(jnp.int32)
        slot=jnp.where(p<CAP,base+p,big)
        s0=slot[:,0:T]; s1=slot[:,T:P2]
        r8=lax.broadcasted_iota(jnp.int32,(8,T),0)
        rows=jnp.where(r8==0,s0,jnp.where(r8==1,s1,big))
        rowo[...]=rows
        rep=jnp.concatenate([rows.astype(f32)]*16,axis=0).T
        colo[...]=rep[:,0:8].astype(jnp.int32)
        ctf=ct[...].astype(f32)
        PG[0:T,:]=(gts[:,0:1]*ctf).astype(bf16)
        PG[T:P2,:]=(gts[:,1:2]*ctf).astype(bf16)
        for pi in range(parts):
            @pl.loop(0,S//CH)
            def _(i):
                si=lax.broadcasted_iota(jnp.int32,(CH,T),0)+(i*CH+pi*S)
                d0=jnp.where(si==rowo[0:1,:],1.0,0.0).astype(bf16)
                d1=jnp.where(si==rowo[1:2,:],1.0,0.0).astype(bf16)
                sgs[pi][pl.ds(pl.multiple_of(i*CH,CH),CH),:]=(nn(d0,PG[0:T,:])+nn(d1,PG[T:P2,:])).astype(bf16)
    vm=pl.BlockSpec(memory_space=pltpu.VMEM)
    out=pl.pallas_call(kernel,
      in_specs=[pl.BlockSpec(memory_space=pltpu.SMEM)]+[vm]*4,out_specs=[vm]*(2+parts),
      out_shape=[jax.ShapeDtypeStruct((8,T),jnp.int32),jax.ShapeDtypeStruct((T,8),jnp.int32)]+[jax.ShapeDtypeStruct((S,D),bf16)]*parts,
      scratch_shapes=[pltpu.VMEM((P2,P2),bf16),pltpu.VMEM((P2,D),bf16)],
      compiler_params=pltpu.CompilerParams(vmem_limit_bytes=50<<20),
      cost_estimate=pl.CostEstimate(flops=4*S*parts*T*D+4*P2*P2*16,bytes_accessed=8<<20,transcendentals=0),
      name="route")(core,order,expert_ids,gates,cot)
    return out[0],out[1],out[2:]

def dispatch(rows, x, parts):
    T,D=x.shape; S=E*CAP//parts; CH=480
    def kernel(rowr,xr,*outs):
        for pi in range(parts):
            @pl.loop(0,S//CH)
            def _(i):
                si=lax.broadcasted_iota(jnp.int32,(CH,T),0)+(i*CH+pi*S)
                d=jnp.where((si==rowr[0:1,:])|(si==rowr[1:2,:]),1.0,0.0).astype(bf16)
                outs[pi][pl.ds(pl.multiple_of(i*CH,CH),CH),:]=nn(d,xr[...]).astype(bf16)
    vm=pl.BlockSpec(memory_space=pltpu.VMEM)
    return pl.pallas_call(kernel,in_specs=[vm]*2,out_specs=[vm]*parts,out_shape=[jax.ShapeDtypeStruct((S,D),bf16)]*parts,
      compiler_params=pltpu.CompilerParams(vmem_limit_bytes=50<<20),
      cost_estimate=pl.CostEstimate(flops=2*S*parts*T*D,bytes_accessed=6<<20,transcendentals=0),name="dispatch")(rows,x)

def combine(cols, gates, ret, state, shared):
    parts=len(ret); T,D=state.shape; S=ret[0].shape[0]
    def kernel(colr,g,*refs):
        rs=refs[:parts]; st,sh,out=refs[parts:]
        @pl.loop(0,T//QC)
        def _(i):
            r=pl.ds(pl.multiple_of(i*QC,QC),QC)
            acc=st[r,:]+sh[r,:]
            for k in range(2):
                pk=None
                for pi in range(parts):
                    si=lax.broadcasted_iota(jnp.int32,(QC,S),1)+pi*S
                    d=jnp.where(si==colr[r,k:k+1],1.0,0.0).astype(bf16)
                    q=nn(d,rs[pi][...])
                    pk=q if pk is None else pk+q
                acc=acc+g[r,k:k+1]*pk
            out[r,:]=acc.astype(bf16)
    vm=pl.BlockSpec(memory_space=pltpu.VMEM)
    return pl.pallas_call(kernel,in_specs=[vm]*(4+parts),out_specs=vm,out_shape=jax.ShapeDtypeStruct((T,D),bf16),
      compiler_params=pltpu.CompilerParams(vmem_limit_bytes=50<<20),
      cost_estimate=pl.CostEstimate(flops=4*S*parts*T*D,bytes_accessed=9<<20,transcendentals=0),name="combine")(cols,gates,*ret,state,shared)

def mid_bwd_home(deps, inw, dsum, rext, cols, own, ext, back_b, dsh, state, fgain, cot):
    T,D=state.shape; S=8*CAP; nx=len(deps)
    def kernel(*refs):
        body(*refs[nx:])
    def body(z0,z1,dsrc,rsrc,colr,hown,hext,bb,ds,st,fg,ct,sgo,fgo,ba,zd,dd,rd,BV,cs,zs0,zs1,rs0,rs1,es0,es1,*osems):
        home_barrier()
        own_run(hown,ba,osems,True)
        ext_run(rsrc,rd,(es0,es1),True)
        inward_run((z0,z1),zd,(zs0,zs1),True)
        rows=lambda: row_copies(dsrc,dd,pl.ds(3,1),(rs0,rs1))
        for cp in rows(): cp.start()
        fgo[...]=jnp.zeros_like(fgo)
        @pl.loop(0,T//QC)
        def _(i):
            r=pl.ds(pl.multiple_of(i*QC,QC),QC)
            si=lax.broadcasted_iota(jnp.int32,(QC,S),1)+S
            d=jnp.where((si==colr[r,0:1])|(si==colr[r,1:2]),1.0,0.0).astype(bf16)
            sgo[r,:]=ds[r,:]+nn(d,bb[...])
        own_run(hown,ba,osems,False)
        def fetch(src):
            cps=[pltpu.make_async_copy(src.at[i],BV.at[i],cs.at[i]) for i in range(8)]
            for cp in cps: cp.start()
            for cp in cps: cp.wait()
        pl.when(is_inner())(lambda: fetch(ba))
        pl.when(jnp.logical_not(is_inner()))(lambda: fetch(hext))
        @pl.loop(0,T//QC)
        def _(i):
            r=pl.ds(pl.multiple_of(i*QC,QC),QC)
            n=sgo[r,:]
            for b in range(8):
                si=lax.broadcasted_iota(jnp.int32,(QC,128),1)
                si=jnp.where(si<CAP,si+b*CAP,-1)
                d=jnp.where((si==colr[r,0:1])|(si==colr[r,1:2]),1.0,0.0).astype(bf16)[:,0:CAP]
                n=n+nn(d,BV[b])
            x=st[r,:]; inv=inv_rms(x); u=x*inv
            fgo[...]+=jnp.broadcast_to(jnp.sum(n*u,axis=0,keepdims=True),(8,D))
            w=n*fg[...]
            sgo[r,:]=ct[r,:].astype(f32)+inv*(w-u*jnp.mean(w*u,axis=1,keepdims=True))
        inward_run((z0,z1),zd,(zs0,zs1),False)
        for cp in rows(): cp.wait()
        ext_run(rsrc,rd,(es0,es1),False)
    vm=pl.BlockSpec(memory_space=pltpu.VMEM); an=pl.BlockSpec(memory_space=pl.ANY)
    SD=jax.ShapeDtypeStruct
    return pl.pallas_call(kernel,in_specs=[an]*(nx+4)+[vm,an,an]+[vm]*5,out_specs=[vm]*2+[an]*4,
      out_shape=[SD((T,D),f32),SD((8,D),f32),SD((8,CAP,D),bf16),SD(inw[0].shape,bf16),SD((3,1)+dsum.shape[2:],bf16),SD((8,CAP,D),bf16)],
      scratch_shapes=[pltpu.VMEM((8,CAP,D),bf16),pltpu.SemaphoreType.DMA((8,))]+[pltpu.SemaphoreType.DMA((1,))]*2+row_sems()+ext_sems()+plane_sems(1),
      compiler_params=pltpu.CompilerParams(vmem_limit_bytes=50<<20,collective_id=4,has_side_effects=True),
      cost_estimate=pl.CostEstimate(flops=4*S*T*D,bytes_accessed=12<<20,transcendentals=0),name="mid_bwd")(*deps,*inw,dsum,rext,cols,own,ext,back_b,dsh,state,fgain[None],cot)

def mid_bwd(cols, back, dsh, state, fgain, cot):
    parts=len(back); T,D=state.shape; S=back[0].shape[0]
    def kernel(colr,*refs):
        bs=refs[:parts]; ds,st,fg,ct,sgo,fgo=refs[parts:]
        fgo[...]=jnp.zeros_like(fgo)
        @pl.loop(0,T//QC)
        def _(i):
            r=pl.ds(pl.multiple_of(i*QC,QC),QC)
            n=ds[r,:]
            for pi in range(parts):
                si=lax.broadcasted_iota(jnp.int32,(QC,S),1)+pi*S
                d=jnp.where((si==colr[r,0:1])|(si==colr[r,1:2]),1.0,0.0).astype(bf16)
                n=n+nn(d,bs[pi][...])
            x=st[r,:]; inv=inv_rms(x); u=x*inv
            fgo[...]+=jnp.broadcast_to(jnp.sum(n*u,axis=0,keepdims=True),(8,D))
            w=n*fg[...]
            sgo[r,:]=ct[r,:].astype(f32)+inv*(w-u*jnp.mean(w*u,axis=1,keepdims=True))
    vm=pl.BlockSpec(memory_space=pltpu.VMEM)
    return pl.pallas_call(kernel,in_specs=[vm]*(5+parts),out_specs=[vm]*2,out_shape=[jax.ShapeDtypeStruct((T,D),f32),jax.ShapeDtypeStruct((8,D),f32)],
      compiler_params=pltpu.CompilerParams(vmem_limit_bytes=50<<20),
      cost_estimate=pl.CostEstimate(flops=2*S*parts*T*D,bytes_accessed=12<<20,transcendentals=0),name="mid_bwd")(cols,*back,dsh,state,fgain[None],cot)

HEADS = 12
HEAD_DIM = 64


def rope_wide(length):
    positions = np.arange(length, dtype=np.float32)
    frequency = (10000.0 ** (-np.arange(HEAD_DIM // 2) * 2.0 / HEAD_DIM)).astype(np.float32)
    angles = (positions[:, None] * frequency[None, :]).astype(np.float64)
    c = np.cos(angles).astype(np.float32)
    s = np.sin(angles).astype(np.float32)
    return np.concatenate([c, c, c, c], axis=1), np.concatenate([-s, s, -s, s], axis=1)


def shards_any(tokens, cotangent, expert_ids, route_gates, slot_order, prefix_len, attention_gain, qkv_weight,
           output_weight, feedforward_gain, shared_gate, shared_up, shared_down, expert_gate, expert_up, expert_down):
    T, D = tokens.shape
    L, _, FF = expert_gate.shape
    G = lax.axis_size("expert")
    DP = lax.axis_size("dp")
    Z = DP // 2
    parts = 2 if L % 2 == 0 else 1
    LP = L // parts
    dpi = lax.axis_index("dp")
    core = lax.rem(dpi, 2)
    swap_perm = [(i, i ^ 1) for i in range(DP)]
    zgroups = [[2 * z + c for z in range(Z)] for c in range(2)]

    def swap(x):
        return lax.ppermute(x, "dp", swap_perm)

    def a2a(x):
        return lax.all_to_all(x, "expert", split_axis=0, concat_axis=0, tiled=True)

    def to_experts(arrs):
        arrs = [a.reshape(G, LP, CAP, D) for a in arrs]
        if parts == 2:
            arrs = [arrs[0], swap(arrs[1])]
        return [a2a(a) for a in arrs]

    def from_experts(arrs):
        arrs = [a2a(a) for a in arrs]
        if parts == 2:
            arrs = [arrs[0], swap(arrs[1])]
        return [a.reshape(G * LP * CAP, D) for a in arrs]

    cosw, sinw = rope_wide(T)
    rows, cols, sgs = route(slot_order, expert_ids, route_gates, cotangent, core[None].astype(jnp.int32), G, L, parts)
    slot_in = to_experts(sgs)
    q, k, v, att, lse, state, ntwo = attn_fwd(tokens, prefix_len, attention_gain, qkv_weight, output_weight,
                                              feedforward_gain, cosw, sinw)
    xs = dispatch(rows, ntwo, parts)
    x_in = to_experts(xs)
    sh = make_ffn(1, 1, 1, T, D, FF, 512, T // 2, f32)(
        ntwo[None, None], cotangent[None, None], shared_gate[None], shared_up[None], shared_down[None])
    shared_branch = sh[0].reshape(T, D)
    dshared = sh[1].reshape(T, D)
    dense_shared = [sh[2][0], sh[3][0], sh[4][0]]

    res, dgr, eg = [], [], []
    one = make_ffn(parts, G, 1, CAP, D, FF, 512, parts * G * CAP // 2, bf16)
    for l in range(LP):
        o = one(*[a[:, l:l + 1] for a in x_in], *[a[:, l:l + 1] for a in slot_in],
                *[lax.dynamic_slice_in_dim(w, (core * LP if parts == 2 else 0) + l, 1, 0)
                  for w in (expert_gate, expert_up, expert_down)])
        res.append(o[:parts])
        dgr.append(o[parts:2 * parts])
        eg.append(o[2 * parts:])
    cat = lambda xs_: jnp.concatenate(xs_, axis=1) if len(xs_) > 1 else xs_[0]
    res = [cat([r[p] for r in res]) for p in range(parts)]
    dgr = [cat([r[p] for r in dgr]) for p in range(parts)]

    egr = []
    for l in range(LP):
        if parts == 2:
            egr.append([lax.psum_scatter(g[0], "dp", scatter_dimension=0, tiled=True, axis_index_groups=zgroups)
                        for g in eg[l]])
        else:
            egr.append([lax.psum_scatter(g[0], "dp", scatter_dimension=0, tiled=True) for g in eg[l]])

    back = from_experts(dgr)
    ret = from_experts(res)
    sgrad, fgg = mid_bwd(cols, back, dshared, state, feedforward_gain, cotangent)
    tokens_grad, agg, gq, gk, gv, gwo = attn_bwd(sgrad, prefix_len, tokens, attention_gain, qkv_weight, output_weight,
                                                 cosw, sinw, q, k, v, att, lse)
    block_out = combine(cols, route_gates, ret, state, shared_branch)

    def dense(g):
        r = g.shape[0] // DP
        h = g.reshape(Z, 2, r, g.shape[1])
        mine = lax.dynamic_index_in_dim(h, core, 1, keepdims=False)
        other = lax.dynamic_index_in_dim(h, 1 - core, 1, keepdims=False)
        s = (mine.astype(f32) + swap(other).astype(f32)).astype(bf16)
        quarter = s.reshape(Z, G, r // G, g.shape[1])
        quarter = jnp.swapaxes(quarter, 0, 1)
        got = lax.all_to_all(quarter, "expert", split_axis=0, concat_axis=0, tiled=True)
        s = jnp.sum(got.astype(f32), axis=0).astype(bf16)
        zs = lax.psum_scatter(s, "dp", scatter_dimension=0, tiled=True, axis_index_groups=zgroups)
        return lax.all_gather(zs[0], "expert", axis=0, tiled=True).astype(f32)

    def dense_simple(g):
        p = lax.psum_scatter(g, "dp", scatter_dimension=0, tiled=True)
        return lax.psum(p, "expert").astype(f32)

    if (qkv_weight.shape[0] // DP) % (8 * G) == 0 and parts == 2:
        dn = dense
    else:
        dn = dense_simple
    dsh = [dn(g) for g in dense_shared]
    dq, dk, dv, dwo = [dn(g) for g in (gq, gk, gv, gwo)]
    gains = lax.psum(jnp.stack([agg[0], fgg[0]]), ("dp", "expert"))
    gs = D // DP
    gains = lax.dynamic_slice_in_dim(gains, dpi * gs, gs, 1)

    def finish(t):
        a = [egr[l][t] for l in range(LP)]
        if parts == 1:
            return jnp.stack(a).astype(f32)
        b = jnp.stack(a)
        h = b.reshape(LP, 2, b.shape[1] // 2, b.shape[2])
        mine = lax.dynamic_index_in_dim(h, core, 1, keepdims=False)
        other = swap(lax.dynamic_index_in_dim(h, 1 - core, 1, keepdims=False))
        return jnp.concatenate([jnp.where(core == 0, mine, other), jnp.where(core == 0, other, mine)], axis=0).astype(f32)

    return (block_out, tokens_grad, gains[0], jnp.concatenate([dq, dk, dv], axis=1), dwo, gains[1],
            dsh[0], dsh[1], dsh[2], finish(0), finish(1), finish(2))


def shards_fast(tokens, cotangent, expert_ids, route_gates, slot_order, prefix_len, attention_gain, qkv_weight,
                output_weight, feedforward_gain, shared_gate, shared_up, shared_down, expert_gate, expert_up, expert_down):
    T, D = tokens.shape
    FF = expert_gate.shape[2]
    dpi = lax.axis_index("dp").astype(jnp.int32)
    ei = lax.axis_index("expert").astype(jnp.int32)
    core = lax.rem(dpi, 2)
    zi = lax.div(dpi, 2)
    outer = (zi == 0) | (zi == 3)
    low = zi < 2

    def swap(x):
        return lax.ppermute(x, "dp", [(i, i ^ 1) for i in range(8)])

    def across(x):
        return lax.ppermute(x, "dp", [(2, 4), (3, 5), (4, 2), (5, 3)])

    def add(*xs):
        t = xs[0].astype(f32)
        for x in xs[1:]:
            t = t + x.astype(f32)
        return t.astype(bf16)

    cosw, sinw = rope_wide(T)
    rows, cols, (s_out,) = route(slot_order, expert_ids, route_gates, cotangent, core[None], 4, 4, 1, True)
    q, k, v, att, lse, state, ntwo, x_out, sa, sb = attn_fwd(
        tokens, prefix_len, attention_gain, qkv_weight, output_weight, feedforward_gain, cosw, sinw, rows,
        s_out.reshape(2, 8, CAP, D))
    flat = lambda y: y.reshape(8 * CAP, D)
    shared_branch, dshared, sh0, sh1, xa, xb, sx = shared_ffn(ntwo, cotangent, shared_gate, shared_up, shared_down,
                                                              x_out.reshape(2, 8, CAP, D), sa)
    ws = (expert_gate, expert_up, expert_down)
    blocks = lambda y: y.reshape(8, CAP, D)
    dsum = add(sh0, swap(sh1))
    (rb, db), gb0, gb1, wb0, wb1, xx = expert_ffn([], 1, [flat(xb)], [flat(sb)], *ws, 0, 4, inw=(xa, xa), cid=6)
    sa, sx, xa, xx = flat(sa), flat(sx), flat(xa), flat(xx)
    (rx, dx), gx0, gx1, wx0, wx1, db, r0, rf0 = expert_ffn([], 0, [xx], [sx], *ws, 0, 4, carry=blocks(db), dense=(dsum, 0, 1),
                                                           inw=(gb0[0], gb0[0]), cid=2)
    bs0 = add(gb0[0], rf0)
    m_b0 = across(bs0)
    (ra, da), ga0, ga1, wa0, wa1, r1, rf1, dxl = expert_ffn([bs0], 0, [xa], [sa], *ws, 0, 4, dense=(dsum, 1, 2),
                                                            inw=(gb1[0], gb1[0]), ext=blocks(dx),
                                                            gprev=(gx0, gx1, wx0, wx1), cid=3)
    bs1 = add(gb1[0], rf1)
    m_b1 = across(bs1)
    m_a0o = across(ga0[0][:D // 4])
    sgrad, fgg, _, rf2, r2, rxl = mid_bwd_home([bs1], (wb1, wb0), dsum, blocks(rx), cols, blocks(da), dxl, flat(db), dshared,
                                               state, feedforward_gain, cotangent)
    bs2 = add(jnp.where(low, wb1, wb0), rf2)
    mine = lax.dynamic_index_in_dim(dsum, ei, 0, keepdims=False)
    got = jnp.concatenate([r0, r1, r2], axis=1)
    msh = add(mine, got[0], got[1], got[2])
    carried = {
        "hown": blocks(ra), "rxl": rxl, "rbs": blocks(rb), "fgg": fgg, "msh": msh,
        "m0": m_b0, "ni0": gb0[1], "no0": gb0[2],
        "m1": m_b1, "m2o": m_a0o, "ni1": gb1[1], "no1": gb1[2],
        "far2": ga0[0], "ni2": ga0[1], "no2": ga0[2],
        "far3": ga1[0], "ni3": ga1[1], "no3": ga1[2],
        "wa0": wa0, "wa1": wa1, "wb0": wb0, "wb1": wb1,
        "far5": bs2,
    }
    tail = Tail(carried, T, D, FF)
    tokens_grad, _, *rest = attn_bwd(sgrad, prefix_len, tokens, attention_gain, qkv_weight, output_weight,
                                     cosw, sinw, q, k, v, att, lse, tail)
    o = dict(zip(tail.onames, rest))
    block_out = combine(cols, route_gates, [flat(o["ra"]), flat(o["rb"])], state, shared_branch)
    sg = D // 8
    gains = lax.dynamic_slice_in_dim(o["gains"], dpi * sg, sg, 1)
    return (block_out, tokens_grad, gains[0], o["dqkv"], o["dwo"], gains[1], o["dgate"], o["dup"], o["ddown"],
            o["gate"].astype(f32), o["up"].astype(f32), o["down"].astype(f32))


def shards(*args):
    local = args[13].shape[0]
    if lax.axis_size("dp") == 8 and lax.axis_size("expert") == 4 and local == 4:
        return shards_fast(*args)
    return shards_any(*args)


def solution(mesh):
    row = P(("dp", "expert"), None)
    return jax.shard_map(
        shards,
        mesh=mesh,
        in_specs=(row, row, row, row, row, P(("dp", "expert")), P(), P(), P(), P(), P(), P(), P(),
                  P("expert", None, None), P("expert", None, None), P("expert", None, None)),
        out_specs=(row, row, P("dp"), P("dp", None), P("dp", None), P("dp"), P("dp", None), P("dp", None),
                   P("dp", None), P("expert", "dp", None), P("expert", "dp", None), P("expert", "dp", None)),
        check_vma=False,
    )
```

```python
import jax
import jax.numpy as jnp
import numpy as np
from jax import lax
from jax.experimental import pallas as pl
from jax.experimental.pallas import tpu as pltpu
from jax.sharding import PartitionSpec as P

EX = "expert"
DX = "dp"
ARB = "arbitrary"


MESH_ID = pl.DeviceIdType.MESH

def xor4(e,k):
    lo=lax.rem(e,2); hi=lax.div(e,2)
    if k&1: lo=1-lo
    if k&2: hi=1-hi
    return hi*2+lo

def spot():
    d=lax.axis_index(DX); e=lax.axis_index(EX)
    c=lax.rem(d,2)
    return c,lax.div(d,2),e

def shard_of(q):
    c,z,e=spot()
    return jnp.where(z<2,3-q,q).astype(jnp.int32)

def peer(z,kk):
    c,_,e=spot()
    return (2*z+lax.rem(c+(kk>>2),2),xor4(e,kk&3))

def block_of(kk):
    c,_,e=spot()
    return lax.rem(c+(kk>>2),2)*4+xor4(e,kk&3)

def plane_sems(n):
    return [pltpu.SemaphoreType.DMA((n,)),pltpu.SemaphoreType.DMA((n,7)),pltpu.SemaphoreType.DMA((n,7))]

def plane_barrier():
    c,z,e=spot()
    b=pltpu.get_barrier_semaphore()
    for kk in range(1,8):
        pl.semaphore_signal(b,inc=1,device_id=peer(z,kk),device_id_type=MESH_ID)
    pl.semaphore_wait(b,7)

def plane_z_barrier():
    c,z,e=spot()
    b=pltpu.get_barrier_semaphore()
    for kk in range(1,8):
        pl.semaphore_signal(b,inc=1,device_id=peer(z,kk),device_id_type=MESH_ID)
    pl.semaphore_signal(b,inc=1,device_id=(2*side()+c,e),device_id_type=MESH_ID)
    pl.semaphore_wait(b,8)

def side():
    c,z,e=spot()
    return z+1-2*lax.rem(z,2)

def inward_run(srcs, dst, sems, start):
    c,z,e=spot()
    end=(z==0)|(z==3)
    def cp(src): return pltpu.make_async_remote_copy(src_ref=src,dst_ref=dst,send_sem=sems[0].at[0],recv_sem=sems[1].at[0],
        device_id=(2*side()+c,e),device_id_type=MESH_ID)
    if start:
        @pl.when(z==0)
        def _(): cp(srcs[0]).start()
        @pl.when(z==3)
        def _(): cp(srcs[1]).start()
    else:
        @pl.when(end)
        def _(): cp(srcs[0]).wait_send()
        @pl.when(jnp.logical_not(end))
        def _(): cp(srcs[0]).wait_recv()

def plane_copies(pairs, sems):
    local,send,recv=sems
    c,z,e=spot()
    me=block_of(0)
    out=[]
    for i,(src,dst) in enumerate(pairs):
        out.append(pltpu.make_async_copy(src.at[me],dst.at[me],local.at[i]))
        for kk in range(1,8):
            out.append(pltpu.make_async_remote_copy(src_ref=src.at[block_of(kk)],dst_ref=dst.at[me],send_sem=send.at[i,kk-1],
                recv_sem=recv.at[i,kk-1],device_id=peer(z,kk),device_id_type=MESH_ID))
    return out

def home_barrier():
    c,z,e=spot()
    b=pltpu.get_barrier_semaphore()
    inner=(z==1)|(z==2)
    zo=jnp.where(z<2,0,3); zi=jnp.where(z<2,1,2)
    @pl.when(inner)
    def _():
        for kk in range(8):
            pl.semaphore_signal(b,inc=1,device_id=peer(zo,kk),device_id_type=MESH_ID)
            if kk:
                pl.semaphore_signal(b,inc=1,device_id=peer(z,kk),device_id_type=MESH_ID)
        pl.semaphore_wait(b,15)
    @pl.when(jnp.logical_not(inner))
    def _():
        for kk in range(8):
            pl.semaphore_signal(b,inc=1,device_id=peer(zi,kk),device_id_type=MESH_ID)
            if kk:
                pl.semaphore_signal(b,inc=1,device_id=peer(z,kk),device_id_type=MESH_ID)
        pl.semaphore_wait(b,15)

def is_inner():
    c,z,e=spot()
    return (z==1)|(z==2)

def ext_sems():
    return [pltpu.SemaphoreType.DMA((8,)),pltpu.SemaphoreType.DMA((8,))]

def ext_run(src, dst, sems, start):
    send,recv=sems
    me=block_of(0)
    c,z,e=spot()
    def remote(kk,zz):
        return pltpu.make_async_remote_copy(src_ref=src.at[block_of(kk)],dst_ref=dst.at[me],send_sem=send.at[kk],recv_sem=recv.at[kk],
            device_id=peer(zz,kk),device_id_type=MESH_ID)
    @pl.when(is_inner())
    def _():
        for kk in range(8):
            if start: remote(kk,side()).start()
            else: remote(kk,side()).wait_send()
    if not start:
        @pl.when(jnp.logical_not(is_inner()))
        def _():
            for kk in range(8): remote(kk,side()).wait_recv()

def own_run(src, dst, sems, start):
    @pl.when(is_inner())
    def _():
        for cp in plane_copies([(src,dst)],sems):
            if start: cp.start()
            else: cp.wait()

def row_sems():
    return [pltpu.SemaphoreType.DMA((3,)),pltpu.SemaphoreType.DMA((3,))]

def row_copies(src, dst, part, sems):
    send,recv=sems
    c,z,e=spot()
    return [pltpu.make_async_remote_copy(src_ref=src.at[xor4(e,kk),part],dst_ref=dst.at[kk-1],send_sem=send.at[kk-1],recv_sem=recv.at[kk-1],
        device_id=peer(z,kk),device_id_type=MESH_ID) for kk in (1,2,3)]


def add_rows(dst, srcs):
    rows,cols=dst.shape
    step=max(s for s in range(16,rows+1,16) if rows%s==0 and s*cols<=40000)
    @pl.loop(0,dst.shape[0]//step)
    def _(i):
        r=pl.ds(pl.multiple_of(i*step,step),step)
        t=srcs[0][r,:].astype(f32)
        for s in srcs[1:]: t=t+s[r,:].astype(f32)
        dst[r,:]=t.astype(dst.dtype)

class Tail:
    KIND=("g","g","g","g","w","w")
    L2=(1,1,0,0,0,1)
    H=(0,1,0,1,0,0)
    RIN=(0,1,5)
    MID=((3,"o"),(4,"o"),(5,"o"),(2,"i"),(3,"i"),(4,"i"),(5,"i"))
    def __init__(self, arrays, T, D, FF):
        self.names=list(arrays); self.arrays=[arrays[n] for n in self.names]
        self.T,self.D,self.FF=T,D,FF
        SG=D//8; self.SG=SG; self.SD=FF//32
        R2=2*SG; self.R2=R2; HW=FF//4
        self.gs=(R2,FF); self.ws=(HW,D)
        self.NR=arrays["msh"].shape[1]
        an=pl.BlockSpec(memory_space=pl.ANY)
        S=jax.ShapeDtypeStruct
        outs={"gate":S((4,SG,FF),bf16),"up":S((4,SG,FF),bf16),"down":S((4,FF//8,D),bf16),
              "dgate":S((SG,FF),f32),"dup":S((SG,FF),f32),"ddown":S((FF//8,D),f32),
              "dqkv":S((SG,3*D),f32),"dwo":S((SG,D),f32),"gains":S((8,D),f32),
              "ra":S((8,CAP,D),bf16),"rb":S((8,CAP,D),bf16),"block":S((T,D),bf16)}
        for i,w in self.MID:
            outs[f"m{i}{w}"]=S(self.shape(i),bf16)
        for i in self.RIN:
            outs[f"rin{i}"]=S(self.shape(i),bf16)
        for i in range(6):
            outs[f"ro{i}"]=S(self.shape(i),bf16)
        self.onames=list(outs); self.oshape=[outs[n] for n in self.onames]
        self.in_specs=[pl.BlockSpec(memory_space=pltpu.VMEM) if n in ("cols","gates") else an for n in self.names]; self.out_specs=[an]*len(self.onames)
        V=pltpu.VMEM; DM=pltpu.SemaphoreType.DMA
        scr={"ga":V((2,3)+self.gs,bf16),"wa":V((2,3)+self.ws,bf16),
             "gto":V((3,)+self.gs,bf16),"wto":V((1,)+self.ws,bf16),
             "gfin":V((2,)+self.gs,bf16),"wfin":V((1,)+self.ws,bf16),
             "gsw":V((4,SG,FF),bf16),"wsw":V((2,FF//8,D),bf16),
             "atr":V((4,4,SG,D),bf16),"sv":V((4,4,SG,D),bf16),"xr":V((3,4,SG,D),bf16),
             "za":V((4,SG,D),bf16),"zb":V((4,self.NR,128),bf16),
             "gn":V((8,8,D),f32),
             "s_x":DM((7,)),"r_x":DM((7,)),"lra":DM((1,)),"cb":DM((18,)),"s_o":DM((6,)),"r_o":DM((6,)),"s_w":DM((6,)),"r_w":DM((6,)),
             "ld":DM((2,2,3)),"st":DM((8,)),"so":DM((6,2)),"s_r":DM((3,)),"r_r":DM((3,)),"s_at":DM((16,)),"r_at":DM((16,)),"s_xr":DM((3,)),"r_xr":DM((3,)),
             "s_gn":DM((7,)),"r_gn":DM((7,)),"st2":DM((4,)),"sz":DM((2,3))}
        for nm,sh in (("a",(SG,D)),("b",(self.NR,128))):
            scr.update({"zr"+nm:V((2,)+sh,bf16),"zs"+nm:V((2,)+sh,bf16),"zm"+nm:V((2,)+sh,bf16),"zi"+nm:V(sh,bf16),"zt"+nm:V(sh,bf16),
                "zo"+nm:V(sh,bf16),"fi"+nm:V(sh,bf16),"ag"+nm:V((3,)+sh,bf16),
                "s_z"+nm:DM((4,)),"r_z"+nm:DM((4,)),"s_ag"+nm:DM((3,)),"r_ag"+nm:DM((3,))})
        scr.update({"og":V((2,2,SG,FF//4),f32),"od":V((2,self.SD,D),f32)})
        self.snames=list(scr)+[f"own{i}" for i in range(3)]+[f"plane{i}" for i in range(3)]
        self.scratch=[scr[n] for n in scr]+plane_sems(1)+plane_sems(1)
    def shape(self,i): return self.gs if self.KIND[i]=="g" else self.ws
    def bind(self,ins,outs,scr):
        self.r=dict(zip(self.names,ins)); self.r.update(zip(self.onames,outs)); self.r.update(zip(self.snames,scr))
        c,z,e=spot()
        self.c,self.z,self.e=c,z,e
        self.inner=(z==1)|(z==2); self.outer=jnp.logical_not(self.inner); self.low=z<2
        self.zo=jnp.where(z<2,0,3); self.zi=jnp.where(z<2,1,2); self.zx=3-z
        self.own=[self.r[f"own{i}"] for i in range(3)]
        self.plane=[self.r[f"plane{i}"] for i in range(3)]
    def rcopy(self,src,dst,s,r,dev):
        return pltpu.make_async_remote_copy(src_ref=src,dst_ref=dst,send_sem=s,recv_sem=r,device_id=dev,device_id_type=MESH_ID)
    def barrier(self):
        b=pltpu.get_barrier_semaphore()
        def sig(dev): pl.semaphore_signal(b,inc=1,device_id=dev,device_id_type=MESH_ID)
        for kk in range(1,8): sig(peer(self.z,kk))
        @pl.when(self.inner)
        def _():
            for kk in range(8): sig(peer(self.zo,kk))
            sig(peer(self.zx,0))
            pl.semaphore_wait(b,16)
        @pl.when(self.outer)
        def _():
            for kk in range(8): sig(peer(self.zi,kk))
            pl.semaphore_wait(b,15)
    def across(self,q,high=False):
        i,w=self.MID[q]; n=self.shape(i)[0]
        src={2:self.r["far2"],3:self.r["far3"],4:self.r["wa0" if high else "wa1"],5:self.r["far5"]}[i]
        return self.rcopy(src.at[pl.ds(0 if w=="o" else n,n)],self.r[f"m{i}{w}"],self.r["s_x"].at[q],self.r["r_x"].at[q],peer(self.zx,0))
    def across_start(self,qs):
        @pl.when(self.inner)
        def _():
            for q in qs:
                if self.MID[q][0]==4:
                    @pl.when(self.low)
                    def _(q=q): self.across(q).start()
                    @pl.when(jnp.logical_not(self.low))
                    def _(q=q): self.across(q,True).start()
                else: self.across(q).start()
    def rows_home(self,start):
        own_run(self.r["hown"],self.r["ra"],self.own,start)
        @pl.when(self.outer)
        def _():
            cp=pltpu.make_async_copy(self.r["rxl"],self.r["ra"],self.r["lra"].at[0])
            if start: cp.start()
            else: cp.wait()
    def start(self):
        self.barrier()
        self.across_start((0,1,2))
        self.stage1(0,1)
        ld=pltpu.make_async_copy(self.r["msh"],self.r["zb"],self.r["st2"].at[0])
        ld.start(); ld.wait()
        self.z_inward("b")
        self.rin_start()
        for cp in plane_copies([(self.r["rbs"],self.r["rb"])],self.plane): cp.start()
        self.rows_home(True)
        self.stage1(2)
    def load(self,pairs,kind,slot,go):
        buf=self.r[kind+"a"]; ki=0 if kind=="g" else 1
        for k,s in enumerate(pairs):
            def cp(x,k=k): return pltpu.make_async_copy(x,buf.at[slot,k],self.r["ld"].at[ki,slot,k])
            two=isinstance(s,tuple)
            if not go: cp(s[0] if two else s).wait()
            elif two:
                pl.when(self.low)(lambda cp=cp,s=s: cp(s[0]).start())
                pl.when(jnp.logical_not(self.low))(lambda cp=cp,s=s: cp(s[1]).start())
            else: cp(s).start()
    def near(self,i,which):
        if self.KIND[i]=="g":
            return self.r[f"n{which}{i}"]
        n=self.ws[0]
        x="a" if i==4 else "b"
        return tuple(self.r[f"w{x}{h}"].at[pl.ds(0 if which=="o" else n,n)] for h in (0,1))
    def rin(self,k,src=None):
        i=self.RIN[k]
        src=self.r[f"rin{i}"] if src is None else src
        return self.rcopy(src,self.r[f"rin{i}"],self.r["s_r"].at[k],self.r["r_r"].at[k],peer(self.zi,0))
    def rin_start(self):
        @pl.when(self.outer)
        def _():
            for k,i in enumerate((0,1)): self.rin(k,self.near(i,"i")).start()
            lo,hi=self.near(5,"i")
            @pl.when(self.low)
            def _(): self.rin(2,lo).start()
            @pl.when(jnp.logical_not(self.low))
            def _(): self.rin(2,hi).start()
    def parts_of(self,i):
        k="g" if self.KIND[i]=="g" else "w"
        idx=i if k=="g" else i-4
        return k,idx,self.shape(i)[0],self.L2[i]==1
    def ro(self,i):
        k,idx,n,b=self.parts_of(i)
        return self.rcopy(self.r[k+"to"].at[idx%3 if k=="g" else 0],self.r[f"ro{i}"],self.r["s_o"].at[i],self.r["r_o"].at[i],peer(self.zo,0))
    def view(self,i,w):
        if i<2:
            n=self.shape(i)[0]
            return self.r[f"m{i}"].at[pl.ds(0 if w=="o" else n,n)]
        return self.r[f"m{i}{w}"]
    def outward_load(self,i,go=True):
        k,idx,n,b=self.parts_of(i)
        if go and (i,"o") in self.MID: self.across(self.MID.index((i,"o"))).wait()
        self.load([self.view(i,"o"),self.near(i,"o")],k,idx%2,go)
    def outward_load_start(self,i):
        @pl.when(self.inner)
        def _(): self.outward_load(i)
    def outward_send(self,i):
        k,idx,n,b=self.parts_of(i); buf=self.r[k+"a"]
        @pl.when(self.inner)
        def _():
            self.outward_load(i,False)
            if i==3: self.ro(0).wait_send()
            if i==5: self.ro(4).wait_send()
            add_rows(self.r[k+"to"].at[idx%3 if k=="g" else 0],[buf.at[idx%2,0],buf.at[idx%2,1]])
            self.ro(i).start()
    def stage1(self,*pieces):
        for p,i in enumerate(pieces):
            self.outward_load_start(i)
            if p: self.outward_send(pieces[p-1])
        self.outward_send(pieces[-1])
    def sources(self,i):
        b=self.L2[i]==1
        return ([self.view(i,"i"),self.near(i,"i")]+([self.r[f"rin{i}"]] if b else []),
                [self.r[f"ro{i}"]]+([self.near(i,"o")] if b else []))
    def piece_load(self,i):
        k,idx,n,b=self.parts_of(i); s=self.sources(i)
        @pl.when(self.inner)
        def _():
            if (i,"i") in self.MID: self.across(self.MID.index((i,"i"))).wait()
            if b: self.rin(self.RIN.index(i)).wait_recv()
            self.load(s[0],k,idx%2,True)
        @pl.when(self.outer)
        def _():
            self.ro(i).wait_recv()
            self.load(s[1],k,idx%2,True)
    def fin_of(self,i):
        k,idx,n,b=self.parts_of(i)
        return self.r[k+"fin"].at[idx%2 if k=="g" else 0]
    def piece(self,i):
        k,idx,n,b=self.parts_of(i)
        slot=idx%2; buf=self.r[k+"a"]; fin=self.fin_of(i); s=self.sources(i); hn=n//2
        for who,src in ((self.inner,s[0]),(self.outer,s[1])):
            @pl.when(who)
            def _(src=src):
                self.load(src,k,slot,False)
                add_rows(fin,[buf.at[slot,q] for q in range(len(src))])
        self.swap(i).start()
        for cp in self.store(i,fin.at[pl.ds(pl.multiple_of(self.c*hn,hn),hn)],self.c,False): cp.start()
    def swap(self,i):
        k,idx,n,b=self.parts_of(i); hn=n//2
        return self.rcopy(self.fin_of(i).at[pl.ds(pl.multiple_of((1-self.c)*hn,hn),hn)],self.r[k+"sw"].at[idx],self.r["s_w"].at[i],self.r["r_w"].at[i],peer(self.z,4))
    def store(self,i,src,core,theirs):
        ex=2*core+self.L2[i]; k,idx,n,b=self.parts_of(i); slot=idx%2
        if k=="g":
            hc=self.FF//2; h=self.H[i]
            return [pltpu.make_async_copy(src.at[:,pl.ds(t*hc,hc)],self.r[nm].at[ex,:,pl.ds(h*hc,hc)],self.r["so"].at[i,t] if theirs else self.r["st"].at[2*slot+t])
                    for t,nm in enumerate(("gate","up"))]
        return [pltpu.make_async_copy(src,self.r["down"].at[ex],self.r["so"].at[i,0] if theirs else self.r["st"].at[4+slot])]
    def other_half(self,i):
        k,idx,n,b=self.parts_of(i); hn=n//2
        for cp in self.store(i,self.fin_of(i).at[pl.ds(pl.multiple_of(self.c*hn,hn),hn)],self.c,False): cp.wait()
        self.swap(i).wait()
        for cp in self.store(i,self.r[k+"sw"].at[idx],1-self.c,True): cp.start()
    def stores_end(self):
        for i in range(6):
            k,idx,n,b=self.parts_of(i)
            for cp in self.store(i,self.r[k+"sw"].at[idx],1-self.c,True): cp.wait()
    def zsem(self,nm,k): return self.r["s_z"+nm].at[k],self.r["r_z"+nm].at[k]
    def zc(self,nm,k):
        r=self.r; M=r["z"+nm]
        src,dst,dev={0:(M.at[pl.ds(0,2)],r["zr"+nm],peer(self.zi,0)),1:(M.at[2],r["zi"+nm],peer(self.zi,0)),
            2:(r["zs"+nm],r["zm"+nm],peer(self.zx,0)),3:(r["zt"+nm],r["zo"+nm],peer(self.zo,0))}[k]
        s,v=self.zsem(nm,k)
        return self.rcopy(src,dst,s,v,dev)
    def z_inward(self,nm):
        @pl.when(self.outer)
        def _():
            self.zc(nm,0).start(); self.zc(nm,1).start()
    def z_across(self,nm):
        r=self.r
        @pl.when(self.inner)
        def _():
            self.zrecv(nm,0)
            for k in (0,1): add_rows(r["zs"+nm].at[k],[r["z"+nm].at[k],r["zr"+nm].at[k]])
            self.zc(nm,2).start()
    def zrecv(self,nm,k):
        r=self.r; M=r["z"+nm]
        dst={0:r["zr"+nm],1:r["zi"+nm],2:r["zm"+nm],3:r["zo"+nm]}[k]
        src={0:M.at[pl.ds(0,2)],1:M.at[2],2:r["zs"+nm],3:r["zt"+nm]}[k]
        s,v=self.zsem(nm,k)
        dev={0:peer(self.zo,0),1:peer(self.zo,0),2:peer(self.zx,0),3:peer(self.zi,0)}[k]
        self.rcopy(src,dst,s,v,dev).wait_recv()
    def z_last(self,nm):
        r=self.r; M=r["z"+nm]
        @pl.when(self.inner)
        def _():
            self.zrecv(nm,2)
            add_rows(r["zt"+nm],[M.at[3],r["zm"+nm].at[0]])
            self.zc(nm,3).start()
            self.zrecv(nm,1)
            add_rows(r["fi"+nm],[M.at[2],r["zm"+nm].at[1],r["zi"+nm]])
            self.zc(nm,2).wait_send()
        @pl.when(self.outer)
        def _():
            self.zrecv(nm,3)
            add_rows(r["fi"+nm],[M.at[3],r["zo"+nm]])
            self.zc(nm,0).wait_send(); self.zc(nm,1).wait_send()
        for kk in (1,2,3): self.agc(nm,kk).start()
    def agc(self,nm,kk):
        r=self.r
        return self.rcopy(r["fi"+nm],r["ag"+nm].at[kk-1],r["s_ag"+nm].at[kk-1],r["r_ag"+nm].at[kk-1],peer(self.z,kk))
    def z_out(self,nm):
        r=self.r; SG,SD,Q=self.SG,self.SD,self.FF//4; nb=Q//128
        def stores(kk):
            a=xor4(self.e,kk); s=kk%2
            cols=pl.ds(pl.multiple_of(a*Q,Q),Q)
            return [pltpu.make_async_copy(r["og"].at[s,0],r["dgate"].at[:,cols],r["sz"].at[s,0]),
                    pltpu.make_async_copy(r["og"].at[s,1],r["dup"].at[:,cols],r["sz"].at[s,1]),
                    pltpu.make_async_copy(r["od"].at[s],r["ddown"].at[pl.ds(pl.multiple_of(a*SD,SD),SD),:],r["sz"].at[s,2])]
        def store_a(kk,go):
            a=xor4(self.e,kk); s=kk%2
            cols=pl.ds(pl.multiple_of(jnp.minimum(a,2)*self.D,self.D),self.D)
            one=pltpu.make_async_copy(self.oa.at[pl.ds(kk*self.SG,self.SG)],r["dqkv"].at[:,cols],r["sz"].at[s,0])
            if not go: one.wait(); return
            pl.when(a<3)(lambda: one.start())
            pl.when(a==3)(lambda: pltpu.make_async_copy(self.oa.at[pl.ds(kk*self.SG,self.SG)],r["dwo"],r["sz"].at[s,0]).start())
        def done(kk):
            if nm=="a": store_a(kk,False)
            else:
                for cp in stores(kk): cp.wait()
        for kk in range(4):
            if kk: self.agc(nm,kk).wait()
            if kk>=2: done(kk-2)
            src=r["fi"+nm] if kk==0 else r["ag"+nm].at[kk-1]
            if nm=="a":
                add_rows(self.oa.at[pl.ds(kk*self.SG,self.SG)],[src])
                store_a(kk,True)
            else:
                for t in range(2):
                    for b in range(nb):
                        r["og"][kk%2,t,:,b*128:(b+1)*128]=src[(t*nb+b)*SG:(t*nb+b+1)*SG,:].astype(f32)
                off=2*nb*SG
                for b in range(self.D//128):
                    r["od"][kk%2,:,b*128:(b+1)*128]=src[off+b*SD:off+(b+1)*SD,:].astype(f32)
                for cp in stores(kk): cp.start()
        done(2); done(3)
    def rows_of(self,core,zr):
        return pl.ds(pl.multiple_of(2*self.SG*shard_of(zr)+self.SG*core,self.SG),self.SG)
    def at_swap(self,GS):
        return [self.rcopy(GS.at[i,self.rows_of(1-self.c,zr)],self.r["atr"].at[i,zr],self.r["s_at"].at[4*i+zr],self.r["r_at"].at[4*i+zr],peer(self.z,4))
                for i in range(4) for zr in range(4)]
    def at_xy(self,kk):
        return self.rcopy(self.r["sv"].at[xor4(self.e,kk)],self.r["xr"].at[kk-1],self.r["s_xr"].at[kk-1],self.r["r_xr"].at[kk-1],peer(self.z,kk))
    def combine(self,GS,acc,chunk_in,chunks_out):
        r=self.r; T=self.T; Q=chunk_in.shape[0]; self.oa=acc
        self.rows_home(False)
        for cp in plane_copies([(r["rbs"],r["rb"])],self.plane): cp.wait()
        B=T//128
        cps=[pltpu.make_async_copy((r["ra"] if b<8 else r["rb"]).at[b%8],GS.at[b//B,pl.ds((b%B)*128,CAP)],r["cb"].at[b]) for b in range(16)]
        cps.append(pltpu.make_async_copy(r["state"],acc,r["cb"].at[16]))
        for cp in cps: cp.start()
        for cp in cps: cp.wait()
        for c in range(T//Q):
            rows=slice(c*Q,(c+1)*Q)
            cp=pltpu.make_async_copy(r["shared"].at[pl.ds(c*Q,Q)],chunk_in,r["cb"].at[17]); cp.start(); cp.wait()
            out=acc[rows,:]+chunk_in[...]
            for k in range(2):
                s=r["cols"][rows,k:k+1]
                s=s+8*((s*34953)>>22)
                pk=None
                for g in range(3):
                    w=min(T,16*128-g*T)
                    d=jnp.where(lax.broadcasted_iota(jnp.int32,(Q,w),1)+g*T==s,1.0,0.0).astype(bf16)
                    q=lax.dot_general(d,GS[g,0:w,:],(((1,),(0,)),((),())),preferred_element_type=f32)
                    pk=q if pk is None else pk+q
                out=out+r["gates"][rows,k:k+1]*pk
            chunks_out[rows,:]=out.astype(bf16)
        pltpu.make_async_copy(chunks_out,r["block"],r["cb"].at[17]).start()
    def combine_end(self,chunks_out):
        pltpu.make_async_copy(chunks_out,self.r["block"],self.r["cb"].at[17]).wait()
    def gcopy(self,k,dev):
        return self.rcopy(self.r["gn"].at[0] ,self.r["gn"].at[k+1],self.r["s_gn"].at[k],self.r["r_gn"].at[k],dev)
    def middle(self):
        self.z_across("b")
        self.across_start((3,4,5,6))
        self.stage1(3,4)
    def finish(self,GS,gg,acc,chunk_in,chunks_out):
        r=self.r; gn=r["gn"]
        sw=self.at_swap(GS)
        for cp in sw: cp.start()
        row=lax.broadcasted_iota(jnp.int32,(8,self.D),0)
        ld=pltpu.make_async_copy(r["fgg"],gn.at[7],r["st2"].at[1]); ld.start(); ld.wait()
        gn[0]=jnp.where(row==0,gg,jnp.where(row==1,gn[7],0.0))
        self.gcopy(0,peer(self.z,4)).start()
        self.piece_load(0)
        self.piece_load(1)
        self.outward_load_start(5)
        self.piece(0)
        for cp in sw: cp.wait()
        for i in range(4):
            for zr in range(4):
                add_rows(r["sv"].at[i,zr],[GS.at[i,self.rows_of(self.c,zr)],r["atr"].at[i,zr]])
        for kk in (1,2,3): self.at_xy(kk).start()
        self.outward_send(5)
        self.combine(GS,acc,chunk_in,chunks_out)
        self.gcopy(0,peer(self.z,4)).wait()
        gn[0]=gn[0]+gn[1]
        for kk in (1,2,3): self.gcopy(kk,peer(self.z,kk)).start()
        self.z_last("b")
        self.piece(1)
        self.other_half(0)
        self.piece_load(2)
        self.other_half(1)
        self.piece(2)
        self.piece_load(3)
        for kk in (1,2,3): self.gcopy(kk,peer(self.z,kk)).wait()
        gn[0]=(gn[0]+gn[2])+(gn[3]+gn[4])
        @pl.when(self.outer)
        def _(): self.gcopy(4,peer(self.zi,0)).start()
        self.z_out("b")
        for kk in (1,2,3): self.at_xy(kk).wait()
        for zr in range(4): add_rows(r["za"].at[zr],[r["sv"].at[self.e,zr]]+[r["xr"].at[k,zr] for k in range(3)])
        self.z_inward("a")
        @pl.when(self.inner)
        def _():
            self.gcopy(4,peer(self.zo,0)).wait_recv()
            gn[0]=gn[0]+gn[5]
            self.gcopy(5,peer(self.zx,0)).start()
        self.piece(3)
        self.z_across("a")
        self.other_half(2)
        self.piece_load(4)
        @pl.when(self.inner)
        def _():
            self.gcopy(5,peer(self.zx,0)).wait()
            gn[0]=gn[0]+gn[6]
            self.gcopy(6,peer(self.zo,0)).start()
        self.other_half(3)
        self.z_last("a")
        self.piece(4)
        self.piece_load(5)
        @pl.when(self.outer)
        def _():
            self.gcopy(4,peer(self.zi,0)).wait_send()
            self.gcopy(6,peer(self.zi,0)).wait_recv()
            gn[0]=gn[7]
        gcp=pltpu.make_async_copy(gn.at[0],r["gains"],r["st2"].at[3]); gcp.start()
        self.other_half(4)
        self.piece(5)
        self.z_out("a")
        self.other_half(5)
        self.stores_end()
        gcp.wait()
        @pl.when(self.inner)
        def _():
            self.gcopy(6,peer(self.zo,0)).wait_send()
            for i in (1,2,3,5): self.ro(i).wait_send()
            self.zc("a",3).wait_send(); self.zc("b",3).wait_send()
        @pl.when(self.outer)
        def _():
            for k in range(3): self.rin(k).wait_send()
        self.combine_end(chunks_out)

f32=jnp.float32; bf16=jnp.bfloat16
def nn(a,b): return lax.dot_general(a,b,(((1,),(0,)),((),())),preferred_element_type=f32)
def nt(a,b): return lax.dot_general(a,b,(((1,),(1,)),((),())),preferred_element_type=f32)
def tn(a,b): return lax.dot_general(a,b,(((0,),(0,)),((),())),preferred_element_type=f32)
EPS=1e-6
E=16; CAP=120
HD=64; GH=4; GW=GH*HD; QC=256
def lane_head(shape):
    return lax.broadcasted_iota(jnp.int32,shape,1)//HD
def swap_half(x):
    w=x.shape[1]
    first=(lax.broadcasted_iota(jnp.int32,x.shape,1)%HD)<HD//2
    return jnp.where(first,pltpu.roll(x,w-HD//2,1),pltpu.roll(x,HD//2,1))
def wide(t):
    return jnp.concatenate([t,t],axis=1)
def inv_rms(v):
    return lax.rsqrt(jnp.mean(v*v,axis=1,keepdims=True)+EPS)

def attn_fwd(tokens, prefix, again, wqkv, wo, fgain, cosw, sinw, rows=None, sout=None):
    T,D=tokens.shape
    ng=D//GW; nq=T//QC
    fused=rows is not None
    NS=E*CAP; CH=480
    def kernel(pre,tok,ag,fg,wq,wk,wv,wor,cw,sw,*rest):
        if fused:
            rowr,so,qo,ko,vo,atto,lseo,stateo,ntwoo,xo,sia,sib,normed,bias,q4,k4,vT,OT,acc,*sems=rest
        else:
            qo,ko,vo,atto,lseo,stateo,ntwoo,normed,bias,q4,k4,vT,OT,acc=rest
        g=pl.program_id(0)
        @pl.when(g==0)
        def _():
            if fused:
                plane_barrier()
                for cpy in plane_copies([(so.at[0],sia),(so.at[1],sib)],sems): cpy.start()
            for c in range(nq):
                r=slice(c*QC,(c+1)*QC)
                x=tok[r,:].astype(f32)
                normed[r,:]=(x*inv_rms(x)*ag[...]).astype(bf16)
                j=lax.broadcasted_iota(jnp.int32,(T,QC),0)
                i=lax.broadcasted_iota(jnp.int32,(T,QC),1)+c*QC
                bias[c]=jnp.where((j<=i)|(j<pre[0]),0.0,-1e30)
        for c in range(nq):
            r=slice(c*QC,(c+1)*QC)
            n=normed[r,:]
            C=wide(cw[r,:]); S=wide(sw[r,:])
            q=nn(n,wq[...]); k=nn(n,wk[...]); v=nn(n,wv[...])
            qb=((q*C+swap_half(q)*S).astype(bf16)).astype(f32)*(HD**-0.5)
            qb=qb.astype(bf16)
            kb=(k*C+swap_half(k)*S).astype(bf16)
            q4[r,:]=qb; qo[r,:]=qb
            k4[r,:]=kb; ko[r,:]=kb
            vo[r,:]=v.astype(bf16)
            vT[:,r]=v.T.astype(bf16)
        lh=lane_head((QC,GW))
        @pl.loop(0,GH)
        def _(h):
            hr=pl.ds(pl.multiple_of(h*HD,HD),HD)
            for c in range(nq):
                r=slice(c*QC,(c+1)*QC)
                qm=jnp.where(lh==h,q4[r,:],jnp.zeros((),bf16))
                st=nt(k4[...],qm)+bias[c]
                m=jnp.max(st,axis=0,keepdims=True)
                p=jnp.exp(st-m)
                l=jnp.sum(p,axis=0,keepdims=True)
                ot=nn(vT[hr,:],p.astype(bf16))
                OT[c,hr,:]=ot*(1.0/l)
                lseo[0,pl.ds(h,1),r]=m+jnp.log(l)
        for c in range(nq):
            r=slice(c*QC,(c+1)*QC)
            a=OT[c].T.astype(bf16)
            atto[r,:]=a
            o=nn(a,wor[...])
            @pl.when(g==0)
            def _(): acc[r,:]=o+tok[r,:].astype(f32)
            @pl.when(g>0)
            def _(): acc[r,:]+=o
        @pl.when(g==ng-1)
        def _():
            for c in range(nq):
                r=slice(c*QC,(c+1)*QC)
                st=acc[r,:]
                stateo[r,:]=st
                ntwoo[r,:]=(st*inv_rms(st)*fg[...]).astype(bf16)
            if fused:
                for i in range(NS//CH):
                    si=lax.broadcasted_iota(jnp.int32,(CH,T),0)+i*CH
                    d=jnp.where((si==rowr[0:1,:])|(si==rowr[1:2,:]),1.0,0.0).astype(bf16)
                    xo[i*CH:(i+1)*CH,:]=nn(d,ntwoo[...]).astype(bf16)
                for cpy in plane_copies([(so.at[0],sia),(so.at[1],sib)],sems): cpy.wait()
    full=lambda s: pl.BlockSpec(s,lambda g:(0,)*len(s))
    col=lambda off: pl.BlockSpec((D,GW),lambda g,off=off:(0,g+off))
    tcol=pl.BlockSpec((T,GW),lambda g:(0,g))
    return pl.pallas_call(kernel,grid=(ng,),
      in_specs=[pl.BlockSpec(memory_space=pltpu.SMEM),full((T,D)),full((1,D)),full((1,D)),col(0),col(ng),col(2*ng),pl.BlockSpec((GW,D),lambda g:(g,0)),full((T,128)),full((T,128))]+([full((8,T)),pl.BlockSpec(memory_space=pl.ANY)] if fused else []),
      out_specs=[tcol,tcol,tcol,tcol,pl.BlockSpec((1,8,T),lambda g:(g,0,0)),full((T,D)),full((T,D))]+([full((NS,D))]+[pl.BlockSpec(memory_space=pl.ANY)]*2 if fused else []),
      out_shape=[jax.ShapeDtypeStruct((T,D),bf16)]*4+[jax.ShapeDtypeStruct((ng,8,T),f32),jax.ShapeDtypeStruct((T,D),f32),jax.ShapeDtypeStruct((T,D),bf16)]+([jax.ShapeDtypeStruct((NS,D),bf16),*[jax.ShapeDtypeStruct((8,CAP,D),bf16)]*2] if fused else []),
      scratch_shapes=[pltpu.VMEM((T,D),bf16),pltpu.VMEM((nq,T,QC),f32),pltpu.VMEM((T,GW),bf16),pltpu.VMEM((T,GW),bf16),pltpu.VMEM((GW,T),bf16),pltpu.VMEM((nq,GW,QC),f32),pltpu.VMEM((T,D),f32)]+(plane_sems(2) if fused else []),
      compiler_params=pltpu.CompilerParams(vmem_limit_bytes=56<<20,dimension_semantics=(ARB,),**(dict(collective_id=0,has_side_effects=True) if fused else {})),
      cost_estimate=pl.CostEstimate(flops=2*T*D*4*D+4*T*T*D,bytes_accessed=16<<20,transcendentals=12*T*T),
      name="attn_fwd")(prefix,tokens,again[None],fgain[None],wqkv,wqkv,wqkv,wo,cosw,sinw,*([rows,sout] if fused else []))

def attn_bwd(sgrad, prefix, tokens, again, wqkv, wo, cosw, sinw, q, k, v, att, lse, tail=None):
    T,D=tokens.shape
    ng=D//GW; nq=T//QC
    fast=tail is not None
    def kernel(pre,sg,tok,ag,wq,wk,wv,wor,cw,sw,qr,kr,vr,attr,lser,*rest):
        if fast:
            ni,no=len(tail.in_specs),len(tail.out_specs)
            tgo,ggo=rest[ni:ni+2]
            tins,touts=rest[:ni],rest[ni+2:ni+2+no]
            normedT,bg,bias,dO,kT,PB,DS,dv,dk,dqT,drow,acc,GS,*tscr=rest[ni+2+no:]
            tail.bind(tins,touts,tscr)
        else:
            tgo,ggo,gq,gk,gv,gwo,normedT,bg,bias,dO,kT,PB,DS,dv,dk,dqT,drow,acc=rest
        g=pl.program_id(0)
        if fast:
            @pl.when(g==0)
            def _():
                tail.start()
            @pl.when(g==ng-1)
            def _():
                tail.middle()
        @pl.when(g==0)
        def _():
            for c in range(nq):
                r=slice(c*QC,(c+1)*QC)
                x=tok[r,:].astype(f32)
                n=x*inv_rms(x)*ag[...]
                normedT[:,r]=n.T.astype(bf16)
                bg[r,:]=sg[r,:].astype(bf16)
                j=lax.broadcasted_iota(jnp.int32,(T,QC),0)
                i=lax.broadcasted_iota(jnp.int32,(T,QC),1)+c*QC
                bias[c]=jnp.where((j<=i)|(j<pre[0]),0.0,-1e30).astype(bf16)
        hmask=(lax.broadcasted_iota(jnp.int32,(8,GW),0)==lane_head((8,GW))).astype(f32)
        for c in range(nq):
            r=slice(c*QC,(c+1)*QC)
            d=nt(bg[r,:],wor[...]).astype(bf16)
            dO[r,:]=d
            a=attr[r,:].astype(f32)
            drow[:,r]=lax.dot_general(hmask,d.astype(f32)*a,(((1,),(1,)),((),())),preferred_element_type=f32,precision=lax.Precision.HIGHEST)
            kT[:,r]=kr[r,:].astype(f32).T.astype(bf16)
        gwv=tn(attr[...],bg[...]).astype(bf16)
        if fast:
            GS[3,pl.ds(pl.multiple_of(g*GW,GW),GW),:]=gwv
        else:
            gwo[...]=gwv
        dv[...]=jnp.zeros_like(dv); dk[...]=jnp.zeros_like(dk)
        lh=lane_head((QC,GW)); lhT=lane_head((T,GW))
        @pl.loop(0,GH)
        def _(h):
            hr=pl.ds(pl.multiple_of(h*HD,HD),HD)
            zero=jnp.zeros((),bf16)
            for c in range(nq):
                r=slice(c*QC,(c+1)*QC)
                qm=jnp.where(lh==h,qr[r,:],zero)
                dOm=jnp.where(lh==h,dO[r,:],zero)
                st=nt(kr[...],qm)+bias[c].astype(f32)
                p=jnp.exp(st-lser[0,pl.ds(h,1),r])
                PB[:,r]=p.astype(bf16)
                dp=nt(vr[...],dOm)
                DS[:,r]=(p*(dp-drow[pl.ds(h,1),r])).astype(bf16)
            dv[...]+=nn(PB[...],jnp.where(lhT==h,dO[...],zero))
            dk[...]+=nn(DS[...],jnp.where(lhT==h,qr[...],zero))
            dqT[hr,:]=nn(kT[hr,:],DS[...])
        for c in range(nq):
            r=slice(c*QC,(c+1)*QC)
            C=wide(cw[r,:]); S=wide(sw[r,:])
            dq=dqT[:,r].T*(HD**-0.5)
            dq=dq*C-swap_half(dq)*S
            dkk=dk[r,:]
            dkk=dkk*C-swap_half(dkk)*S
            a=dq.astype(bf16); b=dkk.astype(bf16); e=dv[r,:].astype(bf16)
            PB[r,0:GW]=a; PB[r,GW:2*GW]=b; PB[r,2*GW:3*GW]=e
            o=nt(a,wq[...])+nt(b,wk[...])+nt(e,wv[...])
            @pl.when(g==0)
            def _(): acc[r,:]=o
            @pl.when(g>0)
            def _(): acc[r,:]+=o
        for i in range(3):
            gval=nn(normedT[...],PB[:,i*GW:(i+1)*GW]).astype(bf16)
            if fast:
                GS[i,:,pl.ds(pl.multiple_of(g*GW,GW),GW)]=gval
            else:
                (gq,gk,gv)[i][...]=gval
        @pl.when(g==ng-1)
        def _():
            gg=jnp.zeros((1,D),f32)
            for c in range(nq):
                r=slice(c*QC,(c+1)*QC)
                x=tok[r,:].astype(f32)
                inv=inv_rms(x); u=x*inv
                ngd=acc[r,:]
                gg=gg+jnp.sum(ngd*u,axis=0,keepdims=True)
                w=ngd*ag[...]
                tgo[r,:]=(sg[r,:]+inv*(w-u*jnp.mean(w*u,axis=1,keepdims=True))).astype(bf16)
            ggo[...]=jnp.broadcast_to(gg,(8,D))
            if fast:
                tail.finish(GS,gg,acc,dqT,PB)
    full=lambda s: pl.BlockSpec(s,lambda g:(0,)*len(s),pipeline_mode=pl.Buffered(1))
    col=lambda off: pl.BlockSpec((D,GW),lambda g,off=off:(0,g+off))
    tcol=pl.BlockSpec((T,GW),lambda g:(0,g))
    if fast:
        outs=tail.out_specs; oshape=tail.oshape
        extra=[pltpu.VMEM((4,D,D),bf16)]+tail.scratch
    else:
        outs=[tcol,tcol,tcol,pl.BlockSpec((GW,D),lambda g:(g,0))]
        oshape=[jax.ShapeDtypeStruct((D,D),bf16)]*4
        extra=[]
    rowb=pl.BlockSpec((GW,D),lambda g:(g,0))
    return pl.pallas_call(kernel,grid=(ng,),
      in_specs=[pl.BlockSpec(memory_space=pltpu.SMEM)]+[full((T,D)),full((T,D)),full((1,D)),col(0),col(ng),col(2*ng),rowb,full((T,128)),full((T,128)),tcol,tcol,tcol,tcol,pl.BlockSpec((1,8,T),lambda g:(g,0,0))]+(tail.in_specs if fast else []),
      out_specs=[full((T,D)),full((8,D))]+outs,
      out_shape=[jax.ShapeDtypeStruct((T,D),bf16),jax.ShapeDtypeStruct((8,D),f32)]+oshape,
      scratch_shapes=[pltpu.VMEM((D,T),bf16),pltpu.VMEM((T,D),bf16),pltpu.VMEM((nq,T,QC),bf16),pltpu.VMEM((T,GW),bf16),pltpu.VMEM((GW,T),bf16),
        pltpu.VMEM((T,T),bf16),pltpu.VMEM((T,T),bf16),pltpu.VMEM((T,GW),f32),pltpu.VMEM((T,GW),f32),pltpu.VMEM((GW,T),f32),pltpu.VMEM((8,T),f32),pltpu.VMEM((T,D),f32)]+extra,
      compiler_params=pltpu.CompilerParams(vmem_limit_bytes=63<<20,dimension_semantics=(ARB,),**(dict(collective_id=5,has_side_effects=True) if fast else {})),
      cost_estimate=pl.CostEstimate(flops=2*T*D*8*D+10*T*T*D,bytes_accessed=24<<20,transcendentals=12*T*T),
      name="attn_bwd")(prefix,sgrad,tokens,again[None],wqkv,wqkv,wqkv,wo,cosw,sinw,q,k,v,att,lse,*(tail.arrays if fast else ()))


def make_ffn(parts, G, L, cap, D, FF, FB, chunk, out_dt):
    R=parts*G*cap
    nf=FF//FB
    def kernel(*refs):
        xs=refs[:parts]; ss=refs[parts:2*parts]
        wg,wu,wd=refs[2*parts:2*parts+3]
        o=2*parts+3
        res=refs[o:o+parts]; dgr=refs[o+parts:o+2*parts]
        gG,gU,gD=refs[o+2*parts:o+2*parts+3]
        X,S,H,GB,UB,AR,AD=refs[o+2*parts+3:]
        f=pl.program_id(1)
        @pl.when(f==0)
        def _():
            for p in range(parts):
                for g in range(G):
                    r=(p*G+g)*cap
                    X[r:r+cap,:]=xs[p][g,0]
                    S[r:r+cap,:]=ss[p][g,0]
        @pl.loop(0,R//chunk)
        def _(i):
            rows=pl.ds(pl.multiple_of(i*chunk,chunk),chunk)
            x=X[rows,:]; s=S[rows,:]
            gate=nn(x,wg[0]); up=nn(x,wu[0]); hg=nt(s,wd[0])
            sig=1.0/(1.0+jnp.exp(-gate))
            sil=gate*sig
            h=(sil*up).astype(bf16)
            gb=(hg*up*(sig*(1.0+gate*(1.0-sig)))).astype(bf16)
            ub=(hg*sil).astype(bf16)
            H[rows,:]=h; GB[rows,:]=gb; UB[rows,:]=ub
            r=nn(h,wd[0]); d=nt(gb,wg[0])+nt(ub,wu[0])
            @pl.when(f==0)
            def _():
                AR[rows,:]=r; AD[rows,:]=d
            @pl.when(f>0)
            def _():
                AR[rows,:]+=r; AD[rows,:]+=d
        gG[0]=tn(X[...],GB[...]).astype(bf16)
        gU[0]=tn(X[...],UB[...]).astype(bf16)
        gD[0]=tn(H[...],S[...]).astype(bf16)
        @pl.when(f==nf-1)
        def _():
            for p in range(parts):
                for g in range(G):
                    r=(p*G+g)*cap
                    res[p][g,0]=AR[r:r+cap,:].astype(out_dt)
                    dgr[p][g,0]=AD[r:r+cap,:].astype(out_dt)
    rowspec=pl.BlockSpec((G,1,cap,D),lambda l,f:(0,l,0,0))
    wspec=pl.BlockSpec((1,D,FB),lambda l,f:(l,0,f))
    wdspec=pl.BlockSpec((1,FB,D),lambda l,f:(l,f,0))
    call=pl.pallas_call(kernel,
      out_shape=[jax.ShapeDtypeStruct((G,L,cap,D),out_dt)]*(2*parts)+[jax.ShapeDtypeStruct((L,D,FF),bf16)]*2+[jax.ShapeDtypeStruct((L,FF,D),bf16)],
      grid=(L,nf),
      in_specs=[rowspec]*(2*parts)+[wspec,wspec,wdspec],
      out_specs=[rowspec]*(2*parts)+[wspec,wspec,wdspec],
      scratch_shapes=[pltpu.VMEM((R,D),bf16)]*2+[pltpu.VMEM((R,FB),bf16)]*3+[pltpu.VMEM((R,D),f32)]*2,
      compiler_params=pltpu.CompilerParams(vmem_limit_bytes=60<<20,dimension_semantics=(ARB,ARB)),
      cost_estimate=pl.CostEstimate(flops=2*9*R*D*FF*L,bytes_accessed=L*(6*D*FF*2+4*R*D*2),transcendentals=R*FF*L),
      name="ffn")
    return call


def ffn_rows(x,s,wg,wu,wd,H,GB,UB,rows):
    gate=nn(x,wg); up=nn(x,wu); hg=nt(s,wd)
    sig=1.0/(1.0+jnp.exp(-gate))
    sil=gate*sig
    h=(sil*up).astype(bf16)
    gb=(hg*up*(sig*(1.0+gate*(1.0-sig)))).astype(bf16)
    ub=(hg*sil).astype(bf16)
    H[rows,:]=h; GB[rows,:]=gb; UB[rows,:]=ub
    return nn(h,wd),nt(gb,wg)+nt(ub,wu)

def expert_ffn(deps, l2, xs, ss, wg, wu, wd, f0, nf, prev=(), carry=None, dense=None, inw=None, ext=None, gprev=None, cid=None, FB=512, chunk=480):
    n=len(xs); RG,D=xs[0].shape; FF=wg.shape[2]; R=n*RG; HB=2*FB; ng=nf//2
    SR=D//4; np_=len(prev); nc=0 if carry is None else 1; nd=0 if dense is None else 1
    part=pl.ds(dense[1],dense[2]) if nd else None
    nx=len(deps); nz=0 if inw is None else 2; ne=0 if ext is None else 1; ngp=0 if gprev is None else 6*ng+ng
    def kernel(*refs):
        refs=refs[nx:]
        xr=refs[:n]; sr=refs[n:2*n]; wgr,wur,wdr=refs[2*n:2*n+3]; o=2*n+3
        pv=refs[o:o+np_]; o+=np_
        csrc=refs[o:o+nc]; o+=nc
        dsrc=refs[o:o+nd]; o+=nd
        zsrc=refs[o:o+nz]; o+=nz
        esrc=refs[o:o+ne]; o+=ne
        gp=refs[o:o+ngp]; o+=ngp
        res=refs[o:o+n]; dgr=refs[o+n:o+2*n]; o+=2*n
        gus=[refs[o+3*q:o+3*q+3] for q in range(ng)]; o+=3*ng
        dws=refs[o:o+ng]; o+=ng
        cdst=refs[o:o+nc]; o+=nc
        ddst=refs[o:o+nd]; o+=nd
        zdst=refs[o:o+nz//2]; o+=nz//2
        edst=refs[o:o+ne]; o+=ne
        XT,XN,H,GB,UB,AR,AD=refs[o:o+7]; sems=refs[o+7:]
        f=pl.program_id(0)
        def copies():
            return (plane_copies([(csrc[0],cdst[0])],sems[2*nd+nz+2*ne:]) if nc else [])+(row_copies(dsrc[0],ddst[0],part,sems[nz+2*ne:nz+2*ne+2]) if nd else [])
        if nc or nd or nz:
            @pl.when(f==0)
            def _():
                if nz:
                    if ne: home_barrier()
                    else: plane_z_barrier()
                    inward_run(zsrc,zdst[0],sems[:2],True)
                else:
                    plane_barrier()
                if ne: ext_run(esrc[0],edst[0],sems[nz:nz+2],True)
                for cpy in copies(): cpy.start()
        @pl.when(f==0)
        def _():
            for a in range(n):
                for b in range(RG//chunk):
                    XN[...]=xr[a][b*chunk:(b+1)*chunk,:].astype(f32).T.astype(bf16)
                    for q in range(4):
                        XT[a*(RG//chunk)+b,q*SR:(q+1)*SR,:]=XN[pl.ds(pl.multiple_of(shard_of(q)*SR,SR),SR),:]
        for a in range(n):
            @pl.loop(0,RG//chunk)
            def _(i):
                src=pl.ds(pl.multiple_of(i*chunk,chunk),chunk)
                rows=pl.ds(pl.multiple_of(a*RG+i*chunk,chunk),chunk)
                r,d=ffn_rows(xr[a][src,:],sr[a][src,:],wgr[0],wur[0],wdr[0],H,GB,UB,rows)
                @pl.when(f==0)
                def _():
                    if np_:
                        AR[rows,:]=r+pv[a][src,:].astype(f32); AD[rows,:]=d+pv[n+a][src,:].astype(f32)
                    else:
                        AR[rows,:]=r; AD[rows,:]=d
                if nf>2:
                    @pl.when((f>0)&(f<nf-1))
                    def _():
                        AR[rows,:]+=r; AD[rows,:]+=d
                @pl.when(f==nf-1)
                def _():
                    res[a][src,:]=(AR[rows,:]+r).astype(bf16); dgr[a][src,:]=(AD[rows,:]+d).astype(bf16)
        for t,Y in enumerate((GB,UB)):
            gv=None
            for b in range(R//chunk):
                p=nn(XT[b],Y[b*chunk:(b+1)*chunk,:])
                gv=p if gv is None else gv+p
            cols=pl.ds(pl.multiple_of(t*HB+lax.rem(f,2)*FB,FB),FB)
            for q in range(ng):
                def put(q=q,t=t,gv=gv,cols=cols):
                    for s,(ref,lo,hi) in enumerate(zip(gus[q],(0,2*SR,3*SR),(2*SR,3*SR,4*SR))):
                        v=gv[lo:hi]
                        if ngp: v=v+gp[6*q+3*t+s][...].astype(f32)
                        ref[:,cols]=v.astype(bf16)
                if ng==1: put()
                else: pl.when(lax.div(f,2)==q)(put)
        dv=None
        for a in range(n):
            t=tn(H[a*RG:(a+1)*RG,:],sr[a][...])
            dv=t if dv is None else dv+t
        for q in range(ng):
            def put(q=q,dv=dv):
                dws[q][...]=((dv+gp[6*ng+q][...].astype(f32)) if ngp else dv).astype(bf16)
            if ng==1: put()
            else: pl.when(lax.div(f,2)==q)(put)
        if nc or nd or nz:
            @pl.when(f==nf-1)
            def _():
                for cpy in copies(): cpy.wait()
                if nz: inward_run(zsrc,zdst[0],sems[:2],False)
                if ne: ext_run(esrc[0],edst[0],sems[nz:nz+2],False)
    one=pl.Buffered(1)
    rowspec=pl.BlockSpec((RG,D),lambda f:(0,0),pipeline_mode=one)
    wspec=pl.BlockSpec((1,D,FB),lambda f:(2*spot()[0]+l2,0,f+f0))
    wdspec=pl.BlockSpec((1,FB,D),lambda f:(2*spot()[0]+l2,f+f0,0))
    full=lambda r,c: pl.BlockSpec((r,c),lambda f:(0,0),pipeline_mode=one)
    anyspec=pl.BlockSpec(memory_space=pl.ANY)
    wspecs=[pl.BlockSpec((FB,D),lambda f: ((1-f) if f0 else f,0))] if ng==1 else [
        pl.BlockSpec((FB,D),lambda f: (jnp.minimum(f,1),0)),pl.BlockSpec((FB,D),lambda f: (jnp.minimum(3-f,1),0))]
    gpspecs=[]; gpargs=[]
    if ngp:
        for q in range(ng):
            for t in range(2):
                for s,rr in enumerate((2*SR,SR,SR)):
                    gpspecs.append(pl.BlockSpec((rr,FB),lambda f,q=q,t=t: (0,2*t+jnp.clip(f-2*q,0,1))))
                    gpargs.append(gprev[q][s])
        gpspecs+=wspecs; gpargs+=list(gprev[ng:])
    out=pl.pallas_call(kernel,grid=(nf,),
        in_specs=[anyspec]*nx+[rowspec]*(2*n)+[wspec,wspec,wdspec]+[rowspec]*np_+[anyspec]*(nc+nd+nz+ne)+gpspecs,
        out_specs=[rowspec]*(2*n)+[full(2*SR,2*HB),full(SR,2*HB),full(SR,2*HB)]*ng+wspecs+[anyspec]*(nc+nd+nz//2+ne),
        scratch_shapes=[pltpu.VMEM((R//chunk,D,chunk),bf16),pltpu.VMEM((D,chunk),bf16)]+[pltpu.VMEM((R,FB),bf16)]*3+[pltpu.VMEM((R,D),f32)]*2+([pltpu.SemaphoreType.DMA((1,)),pltpu.SemaphoreType.DMA((1,))] if nz else [])+(ext_sems() if ne else [])+(row_sems() if nd else [])+(plane_sems(1) if nc else []),
      out_shape=[jax.ShapeDtypeStruct((RG,D),bf16)]*(2*n)+([jax.ShapeDtypeStruct((2*SR,2*HB),bf16)]+[jax.ShapeDtypeStruct((SR,2*HB),bf16)]*2)*ng+[jax.ShapeDtypeStruct((HB,D),bf16)]*ng+[jax.ShapeDtypeStruct((8,RG//8,D),bf16)]*nc+([jax.ShapeDtypeStruct((3,dense[2])+dense[0].shape[2:],bf16)] if nd else [])+([jax.ShapeDtypeStruct(inw[0].shape,bf16)] if nz else [])+([jax.ShapeDtypeStruct(ext.shape,bf16)] if ne else []),
      compiler_params=pltpu.CompilerParams(vmem_limit_bytes=62<<20,dimension_semantics=(ARB,),**(dict(collective_id=cid,has_side_effects=True) if nc or nd or nz else {})),
      cost_estimate=pl.CostEstimate(flops=9*R*D*FF*ng,bytes_accessed=3*D*FF*2*ng+4*R*D*2,transcendentals=R*FF*ng//2),
      name=f"expert_ffn{n}_{f0}")(*deps,*xs,*ss,wg,wu,wd,*prev,*([carry] if nc else []),*([dense[0]] if nd else []),*(inw if nz else ()),*([ext] if ne else []),*gpargs)
    o=2*n
    return (out[:o],*[out[o+3*q:o+3*q+3] for q in range(ng)],*out[o+3*ng:])

def shared_ffn(x, s, wg, wu, wd, xout, sa, FB=512):
    T,D=x.shape; FF=wg.shape[1]; nf=FF//FB; chunk=T//2
    SG=D//8; SD=FB//8
    NR=2*SG*(FB//128)+SD*(D//128)
    def kernel(xr,sr,wgr,wur,wdr,xo,zs,res,dgr,o0,o1,xia,xib,zd,XT,H,GB,UB,VG,VD,zs0,zs1,*sems):
        f=pl.program_id(0)
        core=spot()[0]
        pairs=[(xo.at[0],xia),(xo.at[1],xib)]
        @pl.when(f==0)
        def _():
            plane_z_barrier()
            for cpy in plane_copies(pairs,sems): cpy.start()
            inward_run((zs,zs),zd,(zs0,zs1),True)
        @pl.when(f==0)
        def _():
            for b in range(2):
                XT[:,b*chunk:(b+1)*chunk]=xr[b*chunk:(b+1)*chunk,:].astype(f32).T.astype(bf16)
        @pl.loop(0,T//chunk)
        def _(i):
            rows=pl.ds(pl.multiple_of(i*chunk,chunk),chunk)
            r,d=ffn_rows(xr[rows,:],sr[rows,:],wgr[...],wur[...],wdr[...],H,GB,UB,rows)
            @pl.when(f==0)
            def _():
                res[rows,:]=r; dgr[rows,:]=d
            @pl.when(f>0)
            def _():
                res[rows,:]+=r; dgr[rows,:]+=d
        for t,Y in enumerate((GB,UB)):
            VG[...]=nn(XT[...],Y[...]).astype(bf16)
            for zr in range(4):
                for cp in range(2):
                    src=pl.ds(pl.multiple_of(2*SG*shard_of(zr)+SG*lax.rem(core+cp,2),SG),SG)
                    for b in range(FB//128):
                        off=(t*(FB//128)+b)*SG
                        (o0,o1)[cp][f,zr,off:off+SG,:]=VG[src,b*128:(b+1)*128]
        VD[...]=tn(H[...],sr[...]).astype(bf16)
        zr=jnp.where(spot()[1]<2,3-f,f)
        for cp in range(2):
            for e in range(4):
                src=pl.ds(pl.multiple_of(lax.rem(core+cp,2)*4*SD+e*SD,SD),SD)
                for b in range(D//128):
                    off=2*SG*(FB//128)+b*SD
                    (o0,o1)[cp][e,zr,off:off+SD,:]=VD[src,b*128:(b+1)*128]
        @pl.when(f==nf-1)
        def _():
            for cpy in plane_copies(pairs,sems): cpy.wait()
            inward_run((zs,zs),zd,(zs0,zs1),False)
    full=lambda sh: pl.BlockSpec(sh,lambda f:(0,)*len(sh))
    return pl.pallas_call(kernel,grid=(nf,),
      in_specs=[full((T,D)),full((T,D)),pl.BlockSpec((D,FB),lambda f:(0,f)),pl.BlockSpec((D,FB),lambda f:(0,f)),pl.BlockSpec((FB,D),lambda f:(f,0))]+[pl.BlockSpec(memory_space=pl.ANY)]*2,
      out_specs=[full((T,D)),full((T,D)),full((4,4,NR,128)),full((4,4,NR,128))]+[pl.BlockSpec(memory_space=pl.ANY)]*3,
      out_shape=[jax.ShapeDtypeStruct((T,D),f32)]*2+[jax.ShapeDtypeStruct((4,4,NR,128),bf16)]*2+[jax.ShapeDtypeStruct(xout.shape[1:],bf16)]*3,
      scratch_shapes=[pltpu.VMEM((D,T),bf16)]+[pltpu.VMEM((T,FB),bf16)]*3+[pltpu.VMEM((D,FB),bf16),pltpu.VMEM((FB,D),bf16)]+[pltpu.SemaphoreType.DMA((1,))]*2+plane_sems(2),
      compiler_params=pltpu.CompilerParams(vmem_limit_bytes=62<<20,dimension_semantics=(ARB,),collective_id=1,has_side_effects=True),
      cost_estimate=pl.CostEstimate(flops=2*9*T*D*FF,bytes_accessed=6*D*FF*2+8*T*D*2,transcendentals=T*FF),
      name="shared_ffn")(x,s,wg,wu,wd,xout,sa)


def route(order, expert_ids, gates, cot, core, G, L, parts, plane=False):
    T,D=cot.shape; P2=2*T
    LP=L//parts; S=G*LP*CAP
    big=E*CAP
    CH=480 if S%480==0 else CAP*4
    def kernel(core_ref,orow,ids,gts,ct,rowo,colo,*rest):
        sgs=rest[:parts]; PT,PG=rest[parts:]
        lane=lax.broadcasted_iota(jnp.int32,(T,128),1)
        e0=ids[:,0:1].astype(f32); e1=ids[:,1:2].astype(f32)
        er=jnp.where(lane==0,e0,jnp.where(lane==1,e1,0.0)).T[0:8,:]
        ecat=jnp.concatenate([er[0:1,:],er[1:2,:]],axis=1)
        eoh=(lax.broadcasted_iota(jnp.int32,(E,P2),0).astype(f32)==ecat)
        eohb=jnp.where(eoh,1.0,0.0).astype(bf16)
        o=orow[...]
        oj=(o&1)*T+(o>>1)
        CB=256
        for c in range(P2//CB):
            jj=lax.broadcasted_iota(jnp.int32,(CB,P2),0)+c*CB
            PT[c*CB:(c+1)*CB,:]=jnp.where(jj==oj,1.0,0.0).astype(bf16)
        soh=nn(eohb,PT[...])
        sohb=soh.astype(bf16)
        tri=jnp.where(lax.broadcasted_iota(jnp.int32,(CB,CB),0)<lax.broadcasted_iota(jnp.int32,(CB,CB),1),1.0,0.0).astype(bf16)
        run=jnp.zeros((E,1),f32)
        pos=[]
        for c in range(P2//CB):
            blk=soh[:,c*CB:(c+1)*CB]
            before=nn(sohb[:,c*CB:(c+1)*CB],tri)+run
            run=run+jnp.sum(blk,axis=1,keepdims=True)
            pos.append(jnp.sum(before*blk,axis=0,keepdims=True))
        posr=jnp.minimum(jnp.concatenate(pos,axis=1),127.0)
        posj=nt(jnp.broadcast_to(posr,(16,P2)).astype(bf16),PT[...])[0:1,:]
        e=ecat.astype(jnp.int32)
        l=lax.rem(e,L); j=lax.div(e,L)
        if plane:
            base=((lax.rem(l,2)*2+lax.div(l,2))*G+j)*CAP
        elif parts==2:
            cc=lax.rem(lax.div(l,LP)+core_ref[0],2)
            base=((cc*G+j)*LP+lax.rem(l,LP))*CAP
        else:
            base=e*CAP
        p=posj.astype(jnp.int32)
        slot=jnp.where(p<CAP,base+p,big)
        s0=slot[:,0:T]; s1=slot[:,T:P2]
        r8=lax.broadcasted_iota(jnp.int32,(8,T),0)
        rows=jnp.where(r8==0,s0,jnp.where(r8==1,s1,big))
        rowo[...]=rows
        rep=jnp.concatenate([rows.astype(f32)]*16,axis=0).T
        colo[...]=rep[:,0:8].astype(jnp.int32)
        ctf=ct[...].astype(f32)
        PG[0:T,:]=(gts[:,0:1]*ctf).astype(bf16)
        PG[T:P2,:]=(gts[:,1:2]*ctf).astype(bf16)
        for pi in range(parts):
            @pl.loop(0,S//CH)
            def _(i):
                si=lax.broadcasted_iota(jnp.int32,(CH,T),0)+(i*CH+pi*S)
                d0=jnp.where(si==rowo[0:1,:],1.0,0.0).astype(bf16)
                d1=jnp.where(si==rowo[1:2,:],1.0,0.0).astype(bf16)
                sgs[pi][pl.ds(pl.multiple_of(i*CH,CH),CH),:]=(nn(d0,PG[0:T,:])+nn(d1,PG[T:P2,:])).astype(bf16)
    vm=pl.BlockSpec(memory_space=pltpu.VMEM)
    out=pl.pallas_call(kernel,
      in_specs=[pl.BlockSpec(memory_space=pltpu.SMEM)]+[vm]*4,out_specs=[vm]*(2+parts),
      out_shape=[jax.ShapeDtypeStruct((8,T),jnp.int32),jax.ShapeDtypeStruct((T,8),jnp.int32)]+[jax.ShapeDtypeStruct((S,D),bf16)]*parts,
      scratch_shapes=[pltpu.VMEM((P2,P2),bf16),pltpu.VMEM((P2,D),bf16)],
      compiler_params=pltpu.CompilerParams(vmem_limit_bytes=50<<20),
      cost_estimate=pl.CostEstimate(flops=4*S*parts*T*D+4*P2*P2*16,bytes_accessed=8<<20,transcendentals=0),
      name="route")(core,order,expert_ids,gates,cot)
    return out[0],out[1],out[2:]

def dispatch(rows, x, parts):
    T,D=x.shape; S=E*CAP//parts; CH=480
    def kernel(rowr,xr,*outs):
        for pi in range(parts):
            @pl.loop(0,S//CH)
            def _(i):
                si=lax.broadcasted_iota(jnp.int32,(CH,T),0)+(i*CH+pi*S)
                d=jnp.where((si==rowr[0:1,:])|(si==rowr[1:2,:]),1.0,0.0).astype(bf16)
                outs[pi][pl.ds(pl.multiple_of(i*CH,CH),CH),:]=nn(d,xr[...]).astype(bf16)
    vm=pl.BlockSpec(memory_space=pltpu.VMEM)
    return pl.pallas_call(kernel,in_specs=[vm]*2,out_specs=[vm]*parts,out_shape=[jax.ShapeDtypeStruct((S,D),bf16)]*parts,
      compiler_params=pltpu.CompilerParams(vmem_limit_bytes=50<<20),
      cost_estimate=pl.CostEstimate(flops=2*S*parts*T*D,bytes_accessed=6<<20,transcendentals=0),name="dispatch")(rows,x)

def combine(cols, gates, ret, state, shared):
    parts=len(ret); T,D=state.shape; S=ret[0].shape[0]
    def kernel(colr,g,*refs):
        rs=refs[:parts]; st,sh,out=refs[parts:]
        @pl.loop(0,T//QC)
        def _(i):
            r=pl.ds(pl.multiple_of(i*QC,QC),QC)
            acc=st[r,:]+sh[r,:]
            for k in range(2):
                pk=None
                for pi in range(parts):
                    si=lax.broadcasted_iota(jnp.int32,(QC,S),1)+pi*S
                    d=jnp.where(si==colr[r,k:k+1],1.0,0.0).astype(bf16)
                    q=nn(d,rs[pi][...])
                    pk=q if pk is None else pk+q
                acc=acc+g[r,k:k+1]*pk
            out[r,:]=acc.astype(bf16)
    vm=pl.BlockSpec(memory_space=pltpu.VMEM)
    return pl.pallas_call(kernel,in_specs=[vm]*(4+parts),out_specs=vm,out_shape=jax.ShapeDtypeStruct((T,D),bf16),
      compiler_params=pltpu.CompilerParams(vmem_limit_bytes=50<<20),
      cost_estimate=pl.CostEstimate(flops=4*S*parts*T*D,bytes_accessed=9<<20,transcendentals=0),name="combine")(cols,gates,*ret,state,shared)

def mid_bwd_home(deps, inw, dsum, rext, cols, own, ext, back_b, dsh, state, fgain, cot):
    T,D=state.shape; S=8*CAP; nx=len(deps)
    def kernel(*refs):
        body(*refs[nx:])
    def body(z0,z1,dsrc,rsrc,colr,hown,hext,bb,ds,st,fg,ct,sgo,fgo,ba,zd,dd,rd,BV,cs,zs0,zs1,rs0,rs1,es0,es1,*osems):
        home_barrier()
        own_run(hown,ba,osems,True)
        ext_run(rsrc,rd,(es0,es1),True)
        inward_run((z0,z1),zd,(zs0,zs1),True)
        rows=lambda: row_copies(dsrc,dd,pl.ds(3,1),(rs0,rs1))
        for cp in rows(): cp.start()
        fgo[...]=jnp.zeros_like(fgo)
        @pl.loop(0,T//QC)
        def _(i):
            r=pl.ds(pl.multiple_of(i*QC,QC),QC)
            si=lax.broadcasted_iota(jnp.int32,(QC,S),1)+S
            d=jnp.where((si==colr[r,0:1])|(si==colr[r,1:2]),1.0,0.0).astype(bf16)
            sgo[r,:]=ds[r,:]+nn(d,bb[...])
        own_run(hown,ba,osems,False)
        def fetch(src):
            cps=[pltpu.make_async_copy(src.at[i],BV.at[i],cs.at[i]) for i in range(8)]
            for cp in cps: cp.start()
            for cp in cps: cp.wait()
        pl.when(is_inner())(lambda: fetch(ba))
        pl.when(jnp.logical_not(is_inner()))(lambda: fetch(hext))
        @pl.loop(0,T//QC)
        def _(i):
            r=pl.ds(pl.multiple_of(i*QC,QC),QC)
            n=sgo[r,:]
            for b in range(8):
                si=lax.broadcasted_iota(jnp.int32,(QC,128),1)
                si=jnp.where(si<CAP,si+b*CAP,-1)
                d=jnp.where((si==colr[r,0:1])|(si==colr[r,1:2]),1.0,0.0).astype(bf16)[:,0:CAP]
                n=n+nn(d,BV[b])
            x=st[r,:]; inv=inv_rms(x); u=x*inv
            fgo[...]+=jnp.broadcast_to(jnp.sum(n*u,axis=0,keepdims=True),(8,D))
            w=n*fg[...]
            sgo[r,:]=ct[r,:].astype(f32)+inv*(w-u*jnp.mean(w*u,axis=1,keepdims=True))
        inward_run((z0,z1),zd,(zs0,zs1),False)
        for cp in rows(): cp.wait()
        ext_run(rsrc,rd,(es0,es1),False)
    vm=pl.BlockSpec(memory_space=pltpu.VMEM); an=pl.BlockSpec(memory_space=pl.ANY)
    SD=jax.ShapeDtypeStruct
    return pl.pallas_call(kernel,in_specs=[an]*(nx+4)+[vm,an,an]+[vm]*5,out_specs=[vm]*2+[an]*4,
      out_shape=[SD((T,D),f32),SD((8,D),f32),SD((8,CAP,D),bf16),SD(inw[0].shape,bf16),SD((3,1)+dsum.shape[2:],bf16),SD((8,CAP,D),bf16)],
      scratch_shapes=[pltpu.VMEM((8,CAP,D),bf16),pltpu.SemaphoreType.DMA((8,))]+[pltpu.SemaphoreType.DMA((1,))]*2+row_sems()+ext_sems()+plane_sems(1),
      compiler_params=pltpu.CompilerParams(vmem_limit_bytes=50<<20,collective_id=4,has_side_effects=True),
      cost_estimate=pl.CostEstimate(flops=4*S*T*D,bytes_accessed=12<<20,transcendentals=0),name="mid_bwd")(*deps,*inw,dsum,rext,cols,own,ext,back_b,dsh,state,fgain[None],cot)

def mid_bwd(cols, back, dsh, state, fgain, cot):
    parts=len(back); T,D=state.shape; S=back[0].shape[0]
    def kernel(colr,*refs):
        bs=refs[:parts]; ds,st,fg,ct,sgo,fgo=refs[parts:]
        fgo[...]=jnp.zeros_like(fgo)
        @pl.loop(0,T//QC)
        def _(i):
            r=pl.ds(pl.multiple_of(i*QC,QC),QC)
            n=ds[r,:]
            for pi in range(parts):
                si=lax.broadcasted_iota(jnp.int32,(QC,S),1)+pi*S
                d=jnp.where((si==colr[r,0:1])|(si==colr[r,1:2]),1.0,0.0).astype(bf16)
                n=n+nn(d,bs[pi][...])
            x=st[r,:]; inv=inv_rms(x); u=x*inv
            fgo[...]+=jnp.broadcast_to(jnp.sum(n*u,axis=0,keepdims=True),(8,D))
            w=n*fg[...]
            sgo[r,:]=ct[r,:].astype(f32)+inv*(w-u*jnp.mean(w*u,axis=1,keepdims=True))
    vm=pl.BlockSpec(memory_space=pltpu.VMEM)
    return pl.pallas_call(kernel,in_specs=[vm]*(5+parts),out_specs=[vm]*2,out_shape=[jax.ShapeDtypeStruct((T,D),f32),jax.ShapeDtypeStruct((8,D),f32)],
      compiler_params=pltpu.CompilerParams(vmem_limit_bytes=50<<20),
      cost_estimate=pl.CostEstimate(flops=2*S*parts*T*D,bytes_accessed=12<<20,transcendentals=0),name="mid_bwd")(cols,*back,dsh,state,fgain[None],cot)

HEADS = 12
HEAD_DIM = 64


def rope_wide(length):
    positions = np.arange(length, dtype=np.float32)
    frequency = (10000.0 ** (-np.arange(HEAD_DIM // 2) * 2.0 / HEAD_DIM)).astype(np.float32)
    angles = (positions[:, None] * frequency[None, :]).astype(np.float64)
    c = np.cos(angles).astype(np.float32)
    s = np.sin(angles).astype(np.float32)
    return np.concatenate([c, c, c, c], axis=1), np.concatenate([-s, s, -s, s], axis=1)


def shards_any(tokens, cotangent, expert_ids, route_gates, slot_order, prefix_len, attention_gain, qkv_weight,
           output_weight, feedforward_gain, shared_gate, shared_up, shared_down, expert_gate, expert_up, expert_down):
    T, D = tokens.shape
    L, _, FF = expert_gate.shape
    G = lax.axis_size(EX)
    DP = lax.axis_size(DX)
    Z = DP // 2
    parts = 2 if L % 2 == 0 else 1
    LP = L // parts
    dpi = lax.axis_index(DX)
    core = lax.rem(dpi, 2)
    swap_perm = [(i, i ^ 1) for i in range(DP)]
    zgroups = [[2 * z + c for z in range(Z)] for c in range(2)]

    def swap(x):
        return lax.ppermute(x, DX, swap_perm)

    def a2a(x):
        return lax.all_to_all(x, EX, split_axis=0, concat_axis=0, tiled=True)

    def to_experts(arrs):
        arrs = [a.reshape(G, LP, CAP, D) for a in arrs]
        if parts == 2:
            arrs = [arrs[0], swap(arrs[1])]
        return [a2a(a) for a in arrs]

    def from_experts(arrs):
        arrs = [a2a(a) for a in arrs]
        if parts == 2:
            arrs = [arrs[0], swap(arrs[1])]
        return [a.reshape(G * LP * CAP, D) for a in arrs]

    cosw, sinw = rope_wide(T)
    rows, cols, sgs = route(slot_order, expert_ids, route_gates, cotangent, core[None].astype(jnp.int32), G, L, parts)
    slot_in = to_experts(sgs)
    q, k, v, att, lse, state, ntwo = attn_fwd(tokens, prefix_len, attention_gain, qkv_weight, output_weight,
                                              feedforward_gain, cosw, sinw)
    xs = dispatch(rows, ntwo, parts)
    x_in = to_experts(xs)
    sh = make_ffn(1, 1, 1, T, D, FF, 512, T // 2, f32)(
        ntwo[None, None], cotangent[None, None], shared_gate[None], shared_up[None], shared_down[None])
    shared_branch = sh[0].reshape(T, D)
    dshared = sh[1].reshape(T, D)
    dense_shared = [sh[2][0], sh[3][0], sh[4][0]]

    res, dgr, eg = [], [], []
    one = make_ffn(parts, G, 1, CAP, D, FF, 512, parts * G * CAP // 2, bf16)
    for l in range(LP):
        o = one(*[a[:, l:l + 1] for a in x_in], *[a[:, l:l + 1] for a in slot_in],
                *[lax.dynamic_slice_in_dim(w, (core * LP if parts == 2 else 0) + l, 1, 0)
                  for w in (expert_gate, expert_up, expert_down)])
        res.append(o[:parts])
        dgr.append(o[parts:2 * parts])
        eg.append(o[2 * parts:])
    cat = lambda xs_: jnp.concatenate(xs_, axis=1) if len(xs_) > 1 else xs_[0]
    res = [cat([r[p] for r in res]) for p in range(parts)]
    dgr = [cat([r[p] for r in dgr]) for p in range(parts)]

    egr = []
    for l in range(LP):
        if parts == 2:
            egr.append([lax.psum_scatter(g[0], DX, scatter_dimension=0, tiled=True, axis_index_groups=zgroups)
                        for g in eg[l]])
        else:
            egr.append([lax.psum_scatter(g[0], DX, scatter_dimension=0, tiled=True) for g in eg[l]])

    back = from_experts(dgr)
    ret = from_experts(res)
    sgrad, fgg = mid_bwd(cols, back, dshared, state, feedforward_gain, cotangent)
    tokens_grad, agg, gq, gk, gv, gwo = attn_bwd(sgrad, prefix_len, tokens, attention_gain, qkv_weight, output_weight,
                                                 cosw, sinw, q, k, v, att, lse)
    block_out = combine(cols, route_gates, ret, state, shared_branch)

    def dense(g):
        r = g.shape[0] // DP
        h = g.reshape(Z, 2, r, g.shape[1])
        mine = lax.dynamic_index_in_dim(h, core, 1, keepdims=False)
        other = lax.dynamic_index_in_dim(h, 1 - core, 1, keepdims=False)
        s = (mine.astype(f32) + swap(other).astype(f32)).astype(bf16)
        quarter = s.reshape(Z, G, r // G, g.shape[1])
        quarter = jnp.swapaxes(quarter, 0, 1)
        got = lax.all_to_all(quarter, EX, split_axis=0, concat_axis=0, tiled=True)
        s = jnp.sum(got.astype(f32), axis=0).astype(bf16)
        zs = lax.psum_scatter(s, DX, scatter_dimension=0, tiled=True, axis_index_groups=zgroups)
        return lax.all_gather(zs[0], EX, axis=0, tiled=True).astype(f32)

    def dense_simple(g):
        p = lax.psum_scatter(g, DX, scatter_dimension=0, tiled=True)
        return lax.psum(p, EX).astype(f32)

    if (qkv_weight.shape[0] // DP) % (8 * G) == 0 and parts == 2:
        dn = dense
    else:
        dn = dense_simple
    dsh = [dn(g) for g in dense_shared]
    dq, dk, dv, dwo = [dn(g) for g in (gq, gk, gv, gwo)]
    gains = lax.psum(jnp.stack([agg[0], fgg[0]]), (DX, EX))
    gs = D // DP
    gains = lax.dynamic_slice_in_dim(gains, dpi * gs, gs, 1)

    def finish(t):
        a = [egr[l][t] for l in range(LP)]
        if parts == 1:
            return jnp.stack(a).astype(f32)
        b = jnp.stack(a)
        h = b.reshape(LP, 2, b.shape[1] // 2, b.shape[2])
        mine = lax.dynamic_index_in_dim(h, core, 1, keepdims=False)
        other = swap(lax.dynamic_index_in_dim(h, 1 - core, 1, keepdims=False))
        return jnp.concatenate([jnp.where(core == 0, mine, other), jnp.where(core == 0, other, mine)], axis=0).astype(f32)

    return (block_out, tokens_grad, gains[0], jnp.concatenate([dq, dk, dv], axis=1), dwo, gains[1],
            dsh[0], dsh[1], dsh[2], finish(0), finish(1), finish(2))


def shards_fast(tokens, cotangent, expert_ids, route_gates, slot_order, prefix_len, attention_gain, qkv_weight,
                output_weight, feedforward_gain, shared_gate, shared_up, shared_down, expert_gate, expert_up, expert_down):
    T, D = tokens.shape
    FF = expert_gate.shape[2]
    dpi = lax.axis_index(DX).astype(jnp.int32)
    ei = lax.axis_index(EX).astype(jnp.int32)
    core = lax.rem(dpi, 2)
    zi = lax.div(dpi, 2)
    outer = (zi == 0) | (zi == 3)
    low = zi < 2

    def swap(x):
        return lax.ppermute(x, DX, [(i, i ^ 1) for i in range(8)])

    def across(x):
        return lax.ppermute(x, DX, [(2, 4), (3, 5), (4, 2), (5, 3)])

    def add(*xs):
        t = xs[0].astype(f32)
        for x in xs[1:]:
            t = t + x.astype(f32)
        return t.astype(bf16)

    cosw, sinw = rope_wide(T)
    rows, cols, (s_out,) = route(slot_order, expert_ids, route_gates, cotangent, core[None], 4, 4, 1, True)
    q, k, v, att, lse, state, ntwo, x_out, sa, sb = attn_fwd(
        tokens, prefix_len, attention_gain, qkv_weight, output_weight, feedforward_gain, cosw, sinw, rows,
        s_out.reshape(2, 8, CAP, D))
    flat = lambda y: y.reshape(8 * CAP, D)
    shared_branch, dshared, sh0, sh1, xa, xb, sx = shared_ffn(ntwo, cotangent, shared_gate, shared_up, shared_down,
                                                              x_out.reshape(2, 8, CAP, D), sa)
    ws = (expert_gate, expert_up, expert_down)
    blocks = lambda y: y.reshape(8, CAP, D)
    dsum = add(sh0, swap(sh1))
    (rb, db), gb0, gb1, wb0, wb1, xx = expert_ffn([], 1, [flat(xb)], [flat(sb)], *ws, 0, 4, inw=(xa, xa), cid=6)
    sa, sx, xa, xx = flat(sa), flat(sx), flat(xa), flat(xx)
    (rx, dx), gx0, gx1, wx0, wx1, db, r0, rf0 = expert_ffn([], 0, [xx], [sx], *ws, 0, 4, carry=blocks(db), dense=(dsum, 0, 1),
                                                           inw=(gb0[0], gb0[0]), cid=2)
    bs0 = add(gb0[0], rf0)
    m_b0 = across(bs0)
    (ra, da), ga0, ga1, wa0, wa1, r1, rf1, dxl = expert_ffn([bs0], 0, [xa], [sa], *ws, 0, 4, dense=(dsum, 1, 2),
                                                            inw=(gb1[0], gb1[0]), ext=blocks(dx),
                                                            gprev=(gx0, gx1, wx0, wx1), cid=3)
    bs1 = add(gb1[0], rf1)
    m_b1 = across(bs1)
    m_a0o = across(ga0[0][:D // 4])
    sgrad, fgg, _, rf2, r2, rxl = mid_bwd_home([bs1], (wb1, wb0), dsum, blocks(rx), cols, blocks(da), dxl, flat(db), dshared,
                                               state, feedforward_gain, cotangent)
    bs2 = add(jnp.where(low, wb1, wb0), rf2)
    mine = lax.dynamic_index_in_dim(dsum, ei, 0, keepdims=False)
    got = jnp.concatenate([r0, r1, r2], axis=1)
    msh = add(mine, got[0], got[1], got[2])
    carried = {
        "cols": cols, "gates": route_gates, "state": state, "shared": shared_branch, "hown": blocks(ra), "rxl": rxl, "rbs": blocks(rb), "fgg": fgg, "msh": msh,
        "m0": m_b0, "ni0": gb0[1], "no0": gb0[2],
        "m1": m_b1, "m2o": m_a0o, "ni1": gb1[1], "no1": gb1[2],
        "far2": ga0[0], "ni2": ga0[1], "no2": ga0[2],
        "far3": ga1[0], "ni3": ga1[1], "no3": ga1[2],
        "wa0": wa0, "wa1": wa1, "wb0": wb0, "wb1": wb1,
        "far5": bs2,
    }
    tail = Tail(carried, T, D, FF)
    tokens_grad, _, *rest = attn_bwd(sgrad, prefix_len, tokens, attention_gain, qkv_weight, output_weight,
                                     cosw, sinw, q, k, v, att, lse, tail)
    o = dict(zip(tail.onames, rest))
    sg = D // 8
    gains = lax.dynamic_slice_in_dim(o["gains"], dpi * sg, sg, 1)
    return (o["block"], tokens_grad, gains[0], o["dqkv"], o["dwo"], gains[1], o["dgate"], o["dup"], o["ddown"],
            o["gate"].astype(f32), o["up"].astype(f32), o["down"].astype(f32))


def shards(*args):
    local = args[13].shape[0]
    if lax.axis_size(DX) == 8 and lax.axis_size(EX) == 4 and local == 4:
        return shards_fast(*args)
    return shards_any(*args)


def solution(mesh):
    row = P((DX, EX), None)
    return jax.shard_map(
        shards,
        mesh=mesh,
        in_specs=(row, row, row, row, row, P((DX, EX)), P(), P(), P(), P(), P(), P(), P(),
                  P(EX, None, None), P(EX, None, None), P(EX, None, None)),
        out_specs=(row, row, P(DX), P(DX, None), P(DX, None), P(DX), P(DX, None), P(DX, None),
                   P(DX, None), P(EX, DX, None), P(EX, DX, None), P(EX, DX, None)),
        check_vma=False,
    )
```

```python
import jax
import jax.numpy as jnp
import numpy as np
from jax import lax
from jax.experimental import pallas as pl
from jax.experimental.pallas import tpu as pltpu
from jax.sharding import PartitionSpec as P

EX = "expert"
DX = "dp"
ARB = "arbitrary"


MESH_ID = pl.DeviceIdType.MESH

def xor4(e,k):
    lo=lax.rem(e,2); hi=lax.div(e,2)
    if k&1: lo=1-lo
    if k&2: hi=1-hi
    return hi*2+lo

def spot():
    d=lax.axis_index(DX); e=lax.axis_index(EX)
    c=lax.rem(d,2)
    return c,lax.div(d,2),e

def shard_of(q):
    c,z,e=spot()
    return jnp.where(z<2,3-q,q).astype(jnp.int32)

def peer(z,kk):
    c,_,e=spot()
    return (2*z+lax.rem(c+(kk>>2),2),xor4(e,kk&3))

def block_of(kk):
    c,_,e=spot()
    return lax.rem(c+(kk>>2),2)*4+xor4(e,kk&3)

def plane_sems(n):
    return [pltpu.SemaphoreType.DMA((n,)),pltpu.SemaphoreType.DMA((n,7)),pltpu.SemaphoreType.DMA((n,7))]

def plane_barrier():
    c,z,e=spot()
    b=pltpu.get_barrier_semaphore()
    for kk in range(1,8):
        pl.semaphore_signal(b,inc=1,device_id=peer(z,kk),device_id_type=MESH_ID)
    pl.semaphore_wait(b,7)

def plane_z_barrier():
    c,z,e=spot()
    b=pltpu.get_barrier_semaphore()
    for kk in range(1,8):
        pl.semaphore_signal(b,inc=1,device_id=peer(z,kk),device_id_type=MESH_ID)
    pl.semaphore_signal(b,inc=1,device_id=(2*side()+c,e),device_id_type=MESH_ID)
    pl.semaphore_wait(b,8)

def side():
    c,z,e=spot()
    return z+1-2*lax.rem(z,2)

def inward_run(srcs, dst, sems, start):
    c,z,e=spot()
    end=(z==0)|(z==3)
    def cp(src): return pltpu.make_async_remote_copy(src_ref=src,dst_ref=dst,send_sem=sems[0].at[0],recv_sem=sems[1].at[0],
        device_id=(2*side()+c,e),device_id_type=MESH_ID)
    if start:
        @pl.when(z==0)
        def _(): cp(srcs[0]).start()
        @pl.when(z==3)
        def _(): cp(srcs[1]).start()
    else:
        @pl.when(end)
        def _(): cp(srcs[0]).wait_send()
        @pl.when(jnp.logical_not(end))
        def _(): cp(srcs[0]).wait_recv()

def plane_copies(pairs, sems):
    local,send,recv=sems
    c,z,e=spot()
    me=block_of(0)
    out=[]
    for i,(src,dst) in enumerate(pairs):
        out.append(pltpu.make_async_copy(src.at[me],dst.at[me],local.at[i]))
        for kk in range(1,8):
            out.append(pltpu.make_async_remote_copy(src_ref=src.at[block_of(kk)],dst_ref=dst.at[me],send_sem=send.at[i,kk-1],
                recv_sem=recv.at[i,kk-1],device_id=peer(z,kk),device_id_type=MESH_ID))
    return out

def home_barrier():
    c,z,e=spot()
    b=pltpu.get_barrier_semaphore()
    inner=(z==1)|(z==2)
    zo=jnp.where(z<2,0,3); zi=jnp.where(z<2,1,2)
    @pl.when(inner)
    def _():
        for kk in range(8):
            pl.semaphore_signal(b,inc=1,device_id=peer(zo,kk),device_id_type=MESH_ID)
            if kk:
                pl.semaphore_signal(b,inc=1,device_id=peer(z,kk),device_id_type=MESH_ID)
        pl.semaphore_wait(b,15)
    @pl.when(jnp.logical_not(inner))
    def _():
        for kk in range(8):
            pl.semaphore_signal(b,inc=1,device_id=peer(zi,kk),device_id_type=MESH_ID)
            if kk:
                pl.semaphore_signal(b,inc=1,device_id=peer(z,kk),device_id_type=MESH_ID)
        pl.semaphore_wait(b,15)

def is_inner():
    c,z,e=spot()
    return (z==1)|(z==2)

def ext_sems():
    return [pltpu.SemaphoreType.DMA((8,)),pltpu.SemaphoreType.DMA((8,))]

def ext_run(src, dst, sems, start):
    send,recv=sems
    me=block_of(0)
    c,z,e=spot()
    def remote(kk,zz):
        return pltpu.make_async_remote_copy(src_ref=src.at[block_of(kk)],dst_ref=dst.at[me],send_sem=send.at[kk],recv_sem=recv.at[kk],
            device_id=peer(zz,kk),device_id_type=MESH_ID)
    @pl.when(is_inner())
    def _():
        for kk in range(8):
            if start: remote(kk,side()).start()
            else: remote(kk,side()).wait_send()
    if not start:
        @pl.when(jnp.logical_not(is_inner()))
        def _():
            for kk in range(8): remote(kk,side()).wait_recv()

def own_run(src, dst, sems, start):
    @pl.when(is_inner())
    def _():
        for cp in plane_copies([(src,dst)],sems):
            if start: cp.start()
            else: cp.wait()

def row_sems():
    return [pltpu.SemaphoreType.DMA((3,)),pltpu.SemaphoreType.DMA((3,))]

def row_copies(src, dst, part, sems):
    send,recv=sems
    c,z,e=spot()
    return [pltpu.make_async_remote_copy(src_ref=src.at[xor4(e,kk),part],dst_ref=dst.at[kk-1],send_sem=send.at[kk-1],recv_sem=recv.at[kk-1],
        device_id=peer(z,kk),device_id_type=MESH_ID) for kk in (1,2,3)]


def add_rows(dst, srcs):
    rows,cols=dst.shape
    step=max(s for s in range(16,rows+1,16) if rows%s==0 and s*cols<=40000)
    @pl.loop(0,dst.shape[0]//step)
    def _(i):
        r=pl.ds(pl.multiple_of(i*step,step),step)
        t=srcs[0][r,:].astype(f32)
        for s in srcs[1:]: t=t+s[r,:].astype(f32)
        dst[r,:]=t.astype(dst.dtype)

class Tail:
    KIND=("g","g","g","g","w","w")
    L2=(1,1,0,0,0,1)
    H=(0,1,0,1,0,0)
    RIN=(0,1,5)
    MID=((3,"o"),(4,"o"),(5,"o"),(2,"i"),(3,"i"),(4,"i"),(5,"i"))
    def __init__(self, arrays, T, D, FF):
        self.names=list(arrays); self.arrays=[arrays[n] for n in self.names]
        self.T,self.D,self.FF=T,D,FF
        SG=D//8; self.SG=SG; self.SD=FF//32
        R2=2*SG; self.R2=R2; HW=FF//4
        self.gs=(R2,FF); self.ws=(HW,D)
        self.NR=arrays["msh"].shape[1]
        an=pl.BlockSpec(memory_space=pl.ANY)
        S=jax.ShapeDtypeStruct
        outs={"gate":S((4,SG,FF),bf16),"up":S((4,SG,FF),bf16),"down":S((4,FF//8,D),bf16),
              "dgate":S((SG,FF),f32),"dup":S((SG,FF),f32),"ddown":S((FF//8,D),f32),
              "dqkv":S((SG,3*D),f32),"dwo":S((SG,D),f32),"gains":S((8,D),f32),
              "ra":S((8,CAP,D),bf16),"rb":S((8,CAP,D),bf16),"block":S((T,D),bf16)}
        for i,w in self.MID:
            outs[f"m{i}{w}"]=S(self.shape(i),bf16)
        for i in self.RIN:
            outs[f"rin{i}"]=S(self.shape(i),bf16)
        for i in range(6):
            outs[f"ro{i}"]=S(self.shape(i),bf16)
        self.onames=list(outs); self.oshape=[outs[n] for n in self.onames]
        self.in_specs=[pl.BlockSpec(memory_space=pltpu.VMEM) if n in ("cols","gates") else an for n in self.names]; self.out_specs=[an]*len(self.onames)
        V=pltpu.VMEM; DM=pltpu.SemaphoreType.DMA
        scr={"ga":V((2,3)+self.gs,bf16),"wa":V((2,3)+self.ws,bf16),
             "gto":V((3,)+self.gs,bf16),"wto":V((1,)+self.ws,bf16),
             "gfin":V((2,)+self.gs,bf16),"wfin":V((1,)+self.ws,bf16),
             "gsw":V((4,SG,FF),bf16),"wsw":V((2,FF//8,D),bf16),
             "atr":V((4,4,SG,D),bf16),"sv":V((4,4,SG,D),bf16),"xr":V((3,4,SG,D),bf16),
             "za":V((4,SG,D),bf16),"zb":V((4,self.NR,128),bf16),
             "gn":V((8,8,D),f32),
             "s_x":DM((7,)),"r_x":DM((7,)),"lra":DM((1,)),"cb":DM((18,)),"s_o":DM((6,)),"r_o":DM((6,)),"s_w":DM((6,)),"r_w":DM((6,)),
             "ld":DM((2,2,3)),"st":DM((8,)),"so":DM((6,2)),"s_r":DM((3,)),"r_r":DM((3,)),"s_at":DM((16,)),"r_at":DM((16,)),"s_xr":DM((3,)),"r_xr":DM((3,)),
             "s_gn":DM((7,)),"r_gn":DM((7,)),"st2":DM((4,)),"sz":DM((2,3))}
        for nm,sh in (("a",(SG,D)),("b",(self.NR,128))):
            scr.update({"zr"+nm:V((2,)+sh,bf16),"zs"+nm:V((2,)+sh,bf16),"zm"+nm:V((2,)+sh,bf16),"zi"+nm:V(sh,bf16),"zt"+nm:V(sh,bf16),
                "zo"+nm:V(sh,bf16),"fi"+nm:V(sh,bf16),"ag"+nm:V((3,)+sh,bf16),
                "s_z"+nm:DM((4,)),"r_z"+nm:DM((4,)),"s_ag"+nm:DM((3,)),"r_ag"+nm:DM((3,))})
        scr.update({"og":V((2,2,SG,FF//4),f32),"od":V((2,self.SD,D),f32)})
        self.snames=list(scr)+[f"own{i}" for i in range(3)]+[f"plane{i}" for i in range(3)]
        self.scratch=[scr[n] for n in scr]+plane_sems(1)+plane_sems(1)
    def shape(self,i): return self.gs if self.KIND[i]=="g" else self.ws
    def bind(self,ins,outs,scr):
        self.r=dict(zip(self.names,ins)); self.r.update(zip(self.onames,outs)); self.r.update(zip(self.snames,scr))
        c,z,e=spot()
        self.c,self.z,self.e=c,z,e
        self.inner=(z==1)|(z==2); self.outer=jnp.logical_not(self.inner); self.low=z<2
        self.zo=jnp.where(z<2,0,3); self.zi=jnp.where(z<2,1,2); self.zx=3-z
        self.own=[self.r[f"own{i}"] for i in range(3)]
        self.plane=[self.r[f"plane{i}"] for i in range(3)]
    def rcopy(self,src,dst,s,r,dev):
        return pltpu.make_async_remote_copy(src_ref=src,dst_ref=dst,send_sem=s,recv_sem=r,device_id=dev,device_id_type=MESH_ID)
    def barrier(self):
        b=pltpu.get_barrier_semaphore()
        def sig(dev): pl.semaphore_signal(b,inc=1,device_id=dev,device_id_type=MESH_ID)
        for kk in range(1,8): sig(peer(self.z,kk))
        @pl.when(self.inner)
        def _():
            for kk in range(8): sig(peer(self.zo,kk))
            sig(peer(self.zx,0))
            pl.semaphore_wait(b,16)
        @pl.when(self.outer)
        def _():
            for kk in range(8): sig(peer(self.zi,kk))
            pl.semaphore_wait(b,15)
    def across(self,q,high=False):
        i,w=self.MID[q]; n=self.shape(i)[0]
        src={2:self.r["far2"],3:self.r["far3"],4:self.r["wa0" if high else "wa1"],5:self.r["far5"]}[i]
        return self.rcopy(src.at[pl.ds(0 if w=="o" else n,n)],self.r[f"m{i}{w}"],self.r["s_x"].at[q],self.r["r_x"].at[q],peer(self.zx,0))
    def across_start(self,qs):
        @pl.when(self.inner)
        def _():
            for q in qs:
                if self.MID[q][0]==4:
                    @pl.when(self.low)
                    def _(q=q): self.across(q).start()
                    @pl.when(jnp.logical_not(self.low))
                    def _(q=q): self.across(q,True).start()
                else: self.across(q).start()
    def rows_home(self,start):
        own_run(self.r["hown"],self.r["ra"],self.own,start)
        @pl.when(self.outer)
        def _():
            cp=pltpu.make_async_copy(self.r["rxl"],self.r["ra"],self.r["lra"].at[0])
            if start: cp.start()
            else: cp.wait()
    def start(self):
        self.barrier()
        self.across_start((0,1,2))
        self.stage1(0,1)
        ld=pltpu.make_async_copy(self.r["msh"],self.r["zb"],self.r["st2"].at[0])
        ld.start(); ld.wait()
        self.z_inward("b")
        self.rin_start()
        for cp in plane_copies([(self.r["rbs"],self.r["rb"])],self.plane): cp.start()
        self.rows_home(True)
        self.stage1(2)
    def load(self,pairs,kind,slot,go):
        buf=self.r[kind+"a"]; ki=0 if kind=="g" else 1
        for k,s in enumerate(pairs):
            def cp(x,k=k): return pltpu.make_async_copy(x,buf.at[slot,k],self.r["ld"].at[ki,slot,k])
            two=isinstance(s,tuple)
            if not go: cp(s[0] if two else s).wait()
            elif two:
                pl.when(self.low)(lambda cp=cp,s=s: cp(s[0]).start())
                pl.when(jnp.logical_not(self.low))(lambda cp=cp,s=s: cp(s[1]).start())
            else: cp(s).start()
    def near(self,i,which):
        if self.KIND[i]=="g":
            return self.r[f"n{which}{i}"]
        n=self.ws[0]
        x="a" if i==4 else "b"
        return tuple(self.r[f"w{x}{h}"].at[pl.ds(0 if which=="o" else n,n)] for h in (0,1))
    def rin(self,k,src=None):
        i=self.RIN[k]
        src=self.r[f"rin{i}"] if src is None else src
        return self.rcopy(src,self.r[f"rin{i}"],self.r["s_r"].at[k],self.r["r_r"].at[k],peer(self.zi,0))
    def rin_start(self):
        @pl.when(self.outer)
        def _():
            for k,i in enumerate((0,1)): self.rin(k,self.near(i,"i")).start()
            lo,hi=self.near(5,"i")
            @pl.when(self.low)
            def _(): self.rin(2,lo).start()
            @pl.when(jnp.logical_not(self.low))
            def _(): self.rin(2,hi).start()
    def parts_of(self,i):
        k="g" if self.KIND[i]=="g" else "w"
        idx=i if k=="g" else i-4
        return k,idx,self.shape(i)[0],self.L2[i]==1
    def ro(self,i):
        k,idx,n,b=self.parts_of(i)
        return self.rcopy(self.r[k+"to"].at[idx%3 if k=="g" else 0],self.r[f"ro{i}"],self.r["s_o"].at[i],self.r["r_o"].at[i],peer(self.zo,0))
    def view(self,i,w):
        if i<2:
            n=self.shape(i)[0]
            return self.r[f"m{i}"].at[pl.ds(0 if w=="o" else n,n)]
        return self.r[f"m{i}{w}"]
    def outward_load(self,i,go=True):
        k,idx,n,b=self.parts_of(i)
        if go and (i,"o") in self.MID: self.across(self.MID.index((i,"o"))).wait()
        self.load([self.view(i,"o"),self.near(i,"o")],k,idx%2,go)
    def outward_load_start(self,i):
        @pl.when(self.inner)
        def _(): self.outward_load(i)
    def outward_send(self,i):
        k,idx,n,b=self.parts_of(i); buf=self.r[k+"a"]
        @pl.when(self.inner)
        def _():
            self.outward_load(i,False)
            if i==3: self.ro(0).wait_send()
            if i==5: self.ro(4).wait_send()
            add_rows(self.r[k+"to"].at[idx%3 if k=="g" else 0],[buf.at[idx%2,0],buf.at[idx%2,1]])
            self.ro(i).start()
    def stage1(self,*pieces):
        for p,i in enumerate(pieces):
            self.outward_load_start(i)
            if p: self.outward_send(pieces[p-1])
        self.outward_send(pieces[-1])
    def sources(self,i):
        b=self.L2[i]==1
        return ([self.view(i,"i"),self.near(i,"i")]+([self.r[f"rin{i}"]] if b else []),
                [self.r[f"ro{i}"]]+([self.near(i,"o")] if b else []))
    def piece_load(self,i):
        k,idx,n,b=self.parts_of(i); s=self.sources(i)
        @pl.when(self.inner)
        def _():
            if (i,"i") in self.MID: self.across(self.MID.index((i,"i"))).wait()
            if b: self.rin(self.RIN.index(i)).wait_recv()
            self.load(s[0],k,idx%2,True)
        @pl.when(self.outer)
        def _():
            self.ro(i).wait_recv()
            self.load(s[1],k,idx%2,True)
    def fin_of(self,i):
        k,idx,n,b=self.parts_of(i)
        return self.r[k+"fin"].at[idx%2 if k=="g" else 0]
    def piece(self,i):
        k,idx,n,b=self.parts_of(i)
        slot=idx%2; buf=self.r[k+"a"]; fin=self.fin_of(i); s=self.sources(i); hn=n//2
        for who,src in ((self.inner,s[0]),(self.outer,s[1])):
            @pl.when(who)
            def _(src=src):
                self.load(src,k,slot,False)
                add_rows(fin,[buf.at[slot,q] for q in range(len(src))])
        self.swap(i).start()
        for cp in self.store(i,fin.at[pl.ds(pl.multiple_of(self.c*hn,hn),hn)],self.c,False): cp.start()
    def swap(self,i):
        k,idx,n,b=self.parts_of(i); hn=n//2
        return self.rcopy(self.fin_of(i).at[pl.ds(pl.multiple_of((1-self.c)*hn,hn),hn)],self.r[k+"sw"].at[idx],self.r["s_w"].at[i],self.r["r_w"].at[i],peer(self.z,4))
    def store(self,i,src,core,theirs):
        ex=2*core+self.L2[i]; k,idx,n,b=self.parts_of(i); slot=idx%2
        if k=="g":
            hc=self.FF//2; h=self.H[i]
            return [pltpu.make_async_copy(src.at[:,pl.ds(t*hc,hc)],self.r[nm].at[ex,:,pl.ds(h*hc,hc)],self.r["so"].at[i,t] if theirs else self.r["st"].at[2*slot+t])
                    for t,nm in enumerate(("gate","up"))]
        return [pltpu.make_async_copy(src,self.r["down"].at[ex],self.r["so"].at[i,0] if theirs else self.r["st"].at[4+slot])]
    def other_half(self,i):
        k,idx,n,b=self.parts_of(i); hn=n//2
        for cp in self.store(i,self.fin_of(i).at[pl.ds(pl.multiple_of(self.c*hn,hn),hn)],self.c,False): cp.wait()
        self.swap(i).wait()
        for cp in self.store(i,self.r[k+"sw"].at[idx],1-self.c,True): cp.start()
    def stores_end(self):
        for i in range(6):
            k,idx,n,b=self.parts_of(i)
            for cp in self.store(i,self.r[k+"sw"].at[idx],1-self.c,True): cp.wait()
    def zsem(self,nm,k): return self.r["s_z"+nm].at[k],self.r["r_z"+nm].at[k]
    def zc(self,nm,k):
        r=self.r; M=r["z"+nm]
        src,dst,dev={0:(M.at[pl.ds(0,2)],r["zr"+nm],peer(self.zi,0)),1:(M.at[2],r["zi"+nm],peer(self.zi,0)),
            2:(r["zs"+nm],r["zm"+nm],peer(self.zx,0)),3:(r["zt"+nm],r["zo"+nm],peer(self.zo,0))}[k]
        s,v=self.zsem(nm,k)
        return self.rcopy(src,dst,s,v,dev)
    def z_inward(self,nm):
        @pl.when(self.outer)
        def _():
            self.zc(nm,0).start(); self.zc(nm,1).start()
    def z_across(self,nm):
        r=self.r
        @pl.when(self.inner)
        def _():
            self.zrecv(nm,0)
            for k in (0,1): add_rows(r["zs"+nm].at[k],[r["z"+nm].at[k],r["zr"+nm].at[k]])
            self.zc(nm,2).start()
    def zrecv(self,nm,k):
        r=self.r; M=r["z"+nm]
        dst={0:r["zr"+nm],1:r["zi"+nm],2:r["zm"+nm],3:r["zo"+nm]}[k]
        src={0:M.at[pl.ds(0,2)],1:M.at[2],2:r["zs"+nm],3:r["zt"+nm]}[k]
        s,v=self.zsem(nm,k)
        dev={0:peer(self.zo,0),1:peer(self.zo,0),2:peer(self.zx,0),3:peer(self.zi,0)}[k]
        self.rcopy(src,dst,s,v,dev).wait_recv()
    def z_last(self,nm):
        r=self.r; M=r["z"+nm]
        @pl.when(self.inner)
        def _():
            self.zrecv(nm,2)
            add_rows(r["zt"+nm],[M.at[3],r["zm"+nm].at[0]])
            self.zc(nm,3).start()
            self.zrecv(nm,1)
            add_rows(r["fi"+nm],[M.at[2],r["zm"+nm].at[1],r["zi"+nm]])
            self.zc(nm,2).wait_send()
        @pl.when(self.outer)
        def _():
            self.zrecv(nm,3)
            add_rows(r["fi"+nm],[M.at[3],r["zo"+nm]])
            self.zc(nm,0).wait_send(); self.zc(nm,1).wait_send()
        for kk in (1,2,3): self.agc(nm,kk).start()
    def agc(self,nm,kk):
        r=self.r
        return self.rcopy(r["fi"+nm],r["ag"+nm].at[kk-1],r["s_ag"+nm].at[kk-1],r["r_ag"+nm].at[kk-1],peer(self.z,kk))
    def z_out(self,nm):
        r=self.r; SG,SD,Q=self.SG,self.SD,self.FF//4; nb=Q//128
        def stores(kk):
            a=xor4(self.e,kk); s=kk%2
            cols=pl.ds(pl.multiple_of(a*Q,Q),Q)
            return [pltpu.make_async_copy(r["og"].at[s,0],r["dgate"].at[:,cols],r["sz"].at[s,0]),
                    pltpu.make_async_copy(r["og"].at[s,1],r["dup"].at[:,cols],r["sz"].at[s,1]),
                    pltpu.make_async_copy(r["od"].at[s],r["ddown"].at[pl.ds(pl.multiple_of(a*SD,SD),SD),:],r["sz"].at[s,2])]
        def store_a(kk,go):
            a=xor4(self.e,kk); s=kk%2
            cols=pl.ds(pl.multiple_of(jnp.minimum(a,2)*self.D,self.D),self.D)
            one=pltpu.make_async_copy(self.oa.at[pl.ds(kk*self.SG,self.SG)],r["dqkv"].at[:,cols],r["sz"].at[s,0])
            if not go: one.wait(); return
            pl.when(a<3)(lambda: one.start())
            pl.when(a==3)(lambda: pltpu.make_async_copy(self.oa.at[pl.ds(kk*self.SG,self.SG)],r["dwo"],r["sz"].at[s,0]).start())
        def done(kk):
            if nm=="a": store_a(kk,False)
            else:
                for cp in stores(kk): cp.wait()
        for kk in range(4):
            if kk: self.agc(nm,kk).wait()
            if kk>=2: done(kk-2)
            src=r["fi"+nm] if kk==0 else r["ag"+nm].at[kk-1]
            if nm=="a":
                add_rows(self.oa.at[pl.ds(kk*self.SG,self.SG)],[src])
                store_a(kk,True)
            else:
                for t in range(2):
                    for b in range(nb):
                        r["og"][kk%2,t,:,b*128:(b+1)*128]=src[(t*nb+b)*SG:(t*nb+b+1)*SG,:].astype(f32)
                off=2*nb*SG
                for b in range(self.D//128):
                    r["od"][kk%2,:,b*128:(b+1)*128]=src[off+b*SD:off+(b+1)*SD,:].astype(f32)
                for cp in stores(kk): cp.start()
        done(2); done(3)
    def rows_of(self,core,zr):
        return pl.ds(pl.multiple_of(2*self.SG*shard_of(zr)+self.SG*core,self.SG),self.SG)
    def at_swap(self,GS):
        return [self.rcopy(GS.at[i,self.rows_of(1-self.c,zr)],self.r["atr"].at[i,zr],self.r["s_at"].at[4*i+zr],self.r["r_at"].at[4*i+zr],peer(self.z,4))
                for i in range(4) for zr in range(4)]
    def at_xy(self,kk):
        return self.rcopy(self.r["sv"].at[xor4(self.e,kk)],self.r["xr"].at[kk-1],self.r["s_xr"].at[kk-1],self.r["r_xr"].at[kk-1],peer(self.z,kk))
    def combine(self,GS,acc,chunk_in,chunks_out):
        r=self.r; T=self.T; Q=chunk_in.shape[0]; self.oa=acc
        self.rows_home(False)
        for cp in plane_copies([(r["rbs"],r["rb"])],self.plane): cp.wait()
        B=T//128
        cps=[pltpu.make_async_copy((r["ra"] if b<8 else r["rb"]).at[b%8],GS.at[b//B,pl.ds((b%B)*128,CAP)],r["cb"].at[b]) for b in range(16)]
        cps.append(pltpu.make_async_copy(r["state"],acc,r["cb"].at[16]))
        for cp in cps: cp.start()
        for cp in cps: cp.wait()
        for c in range(T//Q):
            rows=slice(c*Q,(c+1)*Q)
            cp=pltpu.make_async_copy(r["shared"].at[pl.ds(c*Q,Q)],chunk_in,r["cb"].at[17]); cp.start(); cp.wait()
            out=acc[rows,:]+chunk_in[...]
            for k in range(2):
                s=r["cols"][rows,k:k+1]
                s=s+8*((s*34953)>>22)
                pk=None
                for g in range(3):
                    w=min(T,16*128-g*T)
                    d=jnp.where(lax.broadcasted_iota(jnp.int32,(Q,w),1)+g*T==s,1.0,0.0).astype(bf16)
                    q=lax.dot_general(d,GS[g,0:w,:],(((1,),(0,)),((),())),preferred_element_type=f32)
                    pk=q if pk is None else pk+q
                out=out+r["gates"][rows,k:k+1]*pk
            chunks_out[rows,:]=out.astype(bf16)
        pltpu.make_async_copy(chunks_out,r["block"],r["cb"].at[17]).start()
    def combine_end(self,chunks_out):
        pltpu.make_async_copy(chunks_out,self.r["block"],self.r["cb"].at[17]).wait()
    def gcopy(self,k,dev):
        return self.rcopy(self.r["gn"].at[0] ,self.r["gn"].at[k+1],self.r["s_gn"].at[k],self.r["r_gn"].at[k],dev)
    def middle(self):
        self.z_across("b")
        self.across_start((3,4,5,6))
        self.stage1(3,4)
    def finish(self,GS,gg,acc,chunk_in,chunks_out):
        r=self.r; gn=r["gn"]
        sw=self.at_swap(GS)
        for cp in sw: cp.start()
        row=lax.broadcasted_iota(jnp.int32,(8,self.D),0)
        ld=pltpu.make_async_copy(r["fgg"],gn.at[7],r["st2"].at[1]); ld.start(); ld.wait()
        gn[0]=jnp.where(row==0,gg,jnp.where(row==1,gn[7],0.0))
        self.gcopy(0,peer(self.z,4)).start()
        self.piece_load(0)
        self.piece_load(1)
        self.outward_load_start(5)
        self.piece(0)
        for cp in sw: cp.wait()
        for i in range(4):
            for zr in range(4):
                add_rows(r["sv"].at[i,zr],[GS.at[i,self.rows_of(self.c,zr)],r["atr"].at[i,zr]])
        for kk in (1,2,3): self.at_xy(kk).start()
        self.outward_send(5)
        self.combine(GS,acc,chunk_in,chunks_out)
        self.gcopy(0,peer(self.z,4)).wait()
        gn[0]=gn[0]+gn[1]
        for kk in (1,2,3): self.gcopy(kk,peer(self.z,kk)).start()
        self.z_last("b")
        self.piece(1)
        self.other_half(0)
        self.piece_load(2)
        self.other_half(1)
        self.piece(2)
        self.piece_load(3)
        for kk in (1,2,3): self.gcopy(kk,peer(self.z,kk)).wait()
        gn[0]=(gn[0]+gn[2])+(gn[3]+gn[4])
        @pl.when(self.outer)
        def _(): self.gcopy(4,peer(self.zi,0)).start()
        self.z_out("b")
        for kk in (1,2,3): self.at_xy(kk).wait()
        for zr in range(4): add_rows(r["za"].at[zr],[r["sv"].at[self.e,zr]]+[r["xr"].at[k,zr] for k in range(3)])
        self.z_inward("a")
        @pl.when(self.inner)
        def _():
            self.gcopy(4,peer(self.zo,0)).wait_recv()
            gn[0]=gn[0]+gn[5]
            self.gcopy(5,peer(self.zx,0)).start()
        self.piece(3)
        self.z_across("a")
        self.other_half(2)
        self.piece_load(4)
        @pl.when(self.inner)
        def _():
            self.gcopy(5,peer(self.zx,0)).wait()
            gn[0]=gn[0]+gn[6]
            self.gcopy(6,peer(self.zo,0)).start()
        self.other_half(3)
        self.z_last("a")
        self.piece(4)
        self.piece_load(5)
        @pl.when(self.outer)
        def _():
            self.gcopy(4,peer(self.zi,0)).wait_send()
            self.gcopy(6,peer(self.zi,0)).wait_recv()
            gn[0]=gn[7]
        gcp=pltpu.make_async_copy(gn.at[0],r["gains"],r["st2"].at[3]); gcp.start()
        self.other_half(4)
        self.piece(5)
        self.z_out("a")
        self.other_half(5)
        self.stores_end()
        gcp.wait()
        @pl.when(self.inner)
        def _():
            self.gcopy(6,peer(self.zo,0)).wait_send()
            for i in (1,2,3,5): self.ro(i).wait_send()
            self.zc("a",3).wait_send(); self.zc("b",3).wait_send()
        @pl.when(self.outer)
        def _():
            for k in range(3): self.rin(k).wait_send()
        self.combine_end(chunks_out)

f32=jnp.float32; bf16=jnp.bfloat16
def nn(a,b): return lax.dot_general(a,b,(((1,),(0,)),((),())),preferred_element_type=f32)
def nt(a,b): return lax.dot_general(a,b,(((1,),(1,)),((),())),preferred_element_type=f32)
def tn(a,b): return lax.dot_general(a,b,(((0,),(0,)),((),())),preferred_element_type=f32)
EPS=1e-6
E=16; CAP=120
HD=64; GH=4; GW=GH*HD; QC=256
def lane_head(shape):
    return lax.broadcasted_iota(jnp.int32,shape,1)//HD
def swap_half(x):
    w=x.shape[1]
    first=(lax.broadcasted_iota(jnp.int32,x.shape,1)%HD)<HD//2
    return jnp.where(first,pltpu.roll(x,w-HD//2,1),pltpu.roll(x,HD//2,1))
def wide(t):
    return jnp.concatenate([t,t],axis=1)
def as_rows(g):
    return g if g.ndim==2 else g[None]

def inv_rms(v):
    return lax.rsqrt(jnp.mean(v*v,axis=1,keepdims=True)+EPS)

def attn_fwd(tokens, prefix, again, wqkv, wo, fgain, cosw, sinw, rows=None, sout=None):
    T,D=tokens.shape
    ng=D//GW; nq=T//QC
    fused=rows is not None
    NS=E*CAP; CH=480
    def kernel(pre,tok,ag,fg,wq,wk,wv,wor,cw,sw,*rest):
        if fused:
            rowr,so,qo,ko,vo,atto,lseo,stateo,ntwoo,xo,sia,sib,normed,bias,q4,k4,vT,OT,acc,*sems=rest
        else:
            qo,ko,vo,atto,lseo,stateo,ntwoo,normed,bias,q4,k4,vT,OT,acc=rest
        g=pl.program_id(0)
        @pl.when(g==0)
        def _():
            if fused:
                plane_barrier()
                for cpy in plane_copies([(so.at[0],sia),(so.at[1],sib)],sems): cpy.start()
            for c in range(nq):
                r=slice(c*QC,(c+1)*QC)
                x=tok[r,:].astype(f32)
                normed[r,:]=(x*inv_rms(x)*ag[0:1,:]).astype(bf16)
                j=lax.broadcasted_iota(jnp.int32,(T,QC),0)
                i=lax.broadcasted_iota(jnp.int32,(T,QC),1)+c*QC
                bias[c]=jnp.where((j<=i)|(j<pre[0]),0.0,-1e30)
        for c in range(nq):
            r=slice(c*QC,(c+1)*QC)
            n=normed[r,:]
            C=wide(cw[r,:]); S=wide(sw[r,:])
            q=nn(n,wq[...]); k=nn(n,wk[...]); v=nn(n,wv[...])
            qb=((q*C+swap_half(q)*S).astype(bf16)).astype(f32)*(HD**-0.5)
            qb=qb.astype(bf16)
            kb=(k*C+swap_half(k)*S).astype(bf16)
            q4[r,:]=qb; qo[r,:]=qb
            k4[r,:]=kb; ko[r,:]=kb
            vo[r,:]=v.astype(bf16)
            vT[:,r]=v.T.astype(bf16)
        lh=lane_head((QC,GW))
        @pl.loop(0,GH)
        def _(h):
            hr=pl.ds(pl.multiple_of(h*HD,HD),HD)
            for c in range(nq):
                r=slice(c*QC,(c+1)*QC)
                qm=jnp.where(lh==h,q4[r,:],jnp.zeros((),bf16))
                st=nt(k4[...],qm)+bias[c]
                m=jnp.max(st,axis=0,keepdims=True)
                p=jnp.exp(st-m)
                l=jnp.sum(p,axis=0,keepdims=True)
                ot=nn(vT[hr,:],p.astype(bf16))
                OT[c,hr,:]=ot*(1.0/l)
                lseo[0,pl.ds(h,1),r]=m+jnp.log(l)
        for c in range(nq):
            r=slice(c*QC,(c+1)*QC)
            a=OT[c].T.astype(bf16)
            atto[r,:]=a
            o=nn(a,wor[...])
            @pl.when(g==0)
            def _(): acc[r,:]=o+tok[r,:].astype(f32)
            @pl.when(g>0)
            def _(): acc[r,:]+=o
        @pl.when(g==ng-1)
        def _():
            for c in range(nq):
                r=slice(c*QC,(c+1)*QC)
                st=acc[r,:]
                stateo[r,:]=st
                ntwoo[r,:]=(st*inv_rms(st)*fg[fg.shape[0]-1:,:]).astype(bf16)
            if fused:
                for i in range(NS//CH):
                    si=lax.broadcasted_iota(jnp.int32,(CH,T),0)+i*CH
                    d=jnp.where((si==rowr[0:1,:])|(si==rowr[1:2,:]),1.0,0.0).astype(bf16)
                    xo[i*CH:(i+1)*CH,:]=nn(d,ntwoo[...]).astype(bf16)
                for cpy in plane_copies([(so.at[0],sia),(so.at[1],sib)],sems): cpy.wait()
    full=lambda s: pl.BlockSpec(s,lambda g:(0,)*len(s))
    col=lambda off: pl.BlockSpec((D,GW),lambda g,off=off:(0,g+off))
    tcol=pl.BlockSpec((T,GW),lambda g:(0,g))
    return pl.pallas_call(kernel,grid=(ng,),
      in_specs=[pl.BlockSpec(memory_space=pltpu.SMEM),full((T,D)),full(as_rows(again).shape),full(as_rows(fgain).shape),col(0),col(ng),col(2*ng),pl.BlockSpec((GW,D),lambda g:(g,0)),full((T,128)),full((T,128))]+([full((8,T)),pl.BlockSpec(memory_space=pl.ANY)] if fused else []),
      out_specs=[tcol,tcol,tcol,tcol,pl.BlockSpec((1,8,T),lambda g:(g,0,0)),full((T,D)),full((T,D))]+([full((NS,D))]+[pl.BlockSpec(memory_space=pl.ANY)]*2 if fused else []),
      out_shape=[jax.ShapeDtypeStruct((T,D),bf16)]*4+[jax.ShapeDtypeStruct((ng,8,T),f32),jax.ShapeDtypeStruct((T,D),f32),jax.ShapeDtypeStruct((T,D),bf16)]+([jax.ShapeDtypeStruct((NS,D),bf16),*[jax.ShapeDtypeStruct((8,CAP,D),bf16)]*2] if fused else []),
      scratch_shapes=[pltpu.VMEM((T,D),bf16),pltpu.VMEM((nq,T,QC),f32),pltpu.VMEM((T,GW),bf16),pltpu.VMEM((T,GW),bf16),pltpu.VMEM((GW,T),bf16),pltpu.VMEM((nq,GW,QC),f32),pltpu.VMEM((T,D),f32)]+(plane_sems(2) if fused else []),
      compiler_params=pltpu.CompilerParams(vmem_limit_bytes=56<<20,dimension_semantics=(ARB,),**(dict(collective_id=0,has_side_effects=True) if fused else {})),
      cost_estimate=pl.CostEstimate(flops=2*T*D*4*D+4*T*T*D,bytes_accessed=16<<20,transcendentals=12*T*T),
      name="attn_fwd")(prefix,tokens,as_rows(again),as_rows(fgain),wqkv,wqkv,wqkv,wo,cosw,sinw,*([rows,sout] if fused else []))

def attn_bwd(sgrad, prefix, tokens, again, wqkv, wo, cosw, sinw, q, k, v, att, lse, tail=None):
    T,D=tokens.shape
    ng=D//GW; nq=T//QC
    fast=tail is not None
    def kernel(pre,sg,tok,ag,wq,wk,wv,wor,cw,sw,qr,kr,vr,attr,lser,*rest):
        if fast:
            ni,no=len(tail.in_specs),len(tail.out_specs)
            tgo,ggo=rest[ni:ni+2]
            tins,touts=rest[:ni],rest[ni+2:ni+2+no]
            normedT,bg,bias,dO,kT,PB,DS,dv,dk,dqT,drow,acc,GS,*tscr=rest[ni+2+no:]
            tail.bind(tins,touts,tscr)
        else:
            tgo,ggo,gq,gk,gv,gwo,normedT,bg,bias,dO,kT,PB,DS,dv,dk,dqT,drow,acc=rest
        g=pl.program_id(0)
        if fast:
            @pl.when(g==0)
            def _():
                tail.start()
            @pl.when(g==ng-1)
            def _():
                tail.middle()
        @pl.when(g==0)
        def _():
            for c in range(nq):
                r=slice(c*QC,(c+1)*QC)
                x=tok[r,:].astype(f32)
                n=x*inv_rms(x)*ag[0:1,:]
                normedT[:,r]=n.T.astype(bf16)
                bg[r,:]=sg[r,:].astype(bf16)
                j=lax.broadcasted_iota(jnp.int32,(T,QC),0)
                i=lax.broadcasted_iota(jnp.int32,(T,QC),1)+c*QC
                bias[c]=jnp.where((j<=i)|(j<pre[0]),0.0,-1e30).astype(bf16)
        hmask=(lax.broadcasted_iota(jnp.int32,(8,GW),0)==lane_head((8,GW))).astype(f32)
        for c in range(nq):
            r=slice(c*QC,(c+1)*QC)
            d=nt(bg[r,:],wor[...]).astype(bf16)
            dO[r,:]=d
            a=attr[r,:].astype(f32)
            drow[:,r]=lax.dot_general(hmask,d.astype(f32)*a,(((1,),(1,)),((),())),preferred_element_type=f32,precision=lax.Precision.HIGHEST)
            kT[:,r]=kr[r,:].astype(f32).T.astype(bf16)
        gwv=tn(attr[...],bg[...]).astype(bf16)
        if fast:
            GS[3,pl.ds(pl.multiple_of(g*GW,GW),GW),:]=gwv
        else:
            gwo[...]=gwv
        dv[...]=jnp.zeros_like(dv); dk[...]=jnp.zeros_like(dk)
        lh=lane_head((QC,GW)); lhT=lane_head((T,GW))
        @pl.loop(0,GH)
        def _(h):
            hr=pl.ds(pl.multiple_of(h*HD,HD),HD)
            zero=jnp.zeros((),bf16)
            for c in range(nq):
                r=slice(c*QC,(c+1)*QC)
                qm=jnp.where(lh==h,qr[r,:],zero)
                dOm=jnp.where(lh==h,dO[r,:],zero)
                st=nt(kr[...],qm)+bias[c].astype(f32)
                p=jnp.exp(st-lser[0,pl.ds(h,1),r])
                PB[:,r]=p.astype(bf16)
                dp=nt(vr[...],dOm)
                DS[:,r]=(p*(dp-drow[pl.ds(h,1),r])).astype(bf16)
            dv[...]+=nn(PB[...],jnp.where(lhT==h,dO[...],zero))
            dk[...]+=nn(DS[...],jnp.where(lhT==h,qr[...],zero))
            dqT[hr,:]=nn(kT[hr,:],DS[...])
        for c in range(nq):
            r=slice(c*QC,(c+1)*QC)
            C=wide(cw[r,:]); S=wide(sw[r,:])
            dq=dqT[:,r].T*(HD**-0.5)
            dq=dq*C-swap_half(dq)*S
            dkk=dk[r,:]
            dkk=dkk*C-swap_half(dkk)*S
            a=dq.astype(bf16); b=dkk.astype(bf16); e=dv[r,:].astype(bf16)
            PB[r,0:GW]=a; PB[r,GW:2*GW]=b; PB[r,2*GW:3*GW]=e
            o=nt(a,wq[...])+nt(b,wk[...])+nt(e,wv[...])
            @pl.when(g==0)
            def _(): acc[r,:]=o
            @pl.when(g>0)
            def _(): acc[r,:]+=o
        for i in range(3):
            gval=nn(normedT[...],PB[:,i*GW:(i+1)*GW]).astype(bf16)
            if fast:
                GS[i,:,pl.ds(pl.multiple_of(g*GW,GW),GW)]=gval
            else:
                (gq,gk,gv)[i][...]=gval
        @pl.when(g==ng-1)
        def _():
            gg=jnp.zeros((1,D),f32)
            for c in range(nq):
                r=slice(c*QC,(c+1)*QC)
                x=tok[r,:].astype(f32)
                inv=inv_rms(x); u=x*inv
                ngd=acc[r,:]
                gg=gg+jnp.sum(ngd*u,axis=0,keepdims=True)
                w=ngd*ag[0:1,:]
                tgo[r,:]=(sg[r,:]+inv*(w-u*jnp.mean(w*u,axis=1,keepdims=True))).astype(bf16)
            ggo[...]=jnp.broadcast_to(gg,(8,D))
            if fast:
                tail.finish(GS,gg,acc,dqT,PB)
    full=lambda s: pl.BlockSpec(s,lambda g:(0,)*len(s),pipeline_mode=pl.Buffered(1))
    col=lambda off: pl.BlockSpec((D,GW),lambda g,off=off:(0,g+off))
    tcol=pl.BlockSpec((T,GW),lambda g:(0,g))
    if fast:
        outs=tail.out_specs; oshape=tail.oshape
        extra=[pltpu.VMEM((4,D,D),bf16)]+tail.scratch
    else:
        outs=[tcol,tcol,tcol,pl.BlockSpec((GW,D),lambda g:(g,0))]
        oshape=[jax.ShapeDtypeStruct((D,D),bf16)]*4
        extra=[]
    rowb=pl.BlockSpec((GW,D),lambda g:(g,0))
    return pl.pallas_call(kernel,grid=(ng,),
      in_specs=[pl.BlockSpec(memory_space=pltpu.SMEM)]+[full((T,D)),full((T,D)),full(as_rows(again).shape),col(0),col(ng),col(2*ng),rowb,full((T,128)),full((T,128)),tcol,tcol,tcol,tcol,pl.BlockSpec((1,8,T),lambda g:(g,0,0))]+(tail.in_specs if fast else []),
      out_specs=[full((T,D)),full((8,D))]+outs,
      out_shape=[jax.ShapeDtypeStruct((T,D),bf16),jax.ShapeDtypeStruct((8,D),f32)]+oshape,
      scratch_shapes=[pltpu.VMEM((D,T),bf16),pltpu.VMEM((T,D),bf16),pltpu.VMEM((nq,T,QC),bf16),pltpu.VMEM((T,GW),bf16),pltpu.VMEM((GW,T),bf16),
        pltpu.VMEM((T,T),bf16),pltpu.VMEM((T,T),bf16),pltpu.VMEM((T,GW),f32),pltpu.VMEM((T,GW),f32),pltpu.VMEM((GW,T),f32),pltpu.VMEM((8,T),f32),pltpu.VMEM((T,D),f32)]+extra,
      compiler_params=pltpu.CompilerParams(vmem_limit_bytes=63<<20,dimension_semantics=(ARB,),**(dict(collective_id=5,has_side_effects=True) if fast else {})),
      cost_estimate=pl.CostEstimate(flops=2*T*D*8*D+10*T*T*D,bytes_accessed=24<<20,transcendentals=12*T*T),
      name="attn_bwd")(prefix,sgrad,tokens,as_rows(again),wqkv,wqkv,wqkv,wo,cosw,sinw,q,k,v,att,lse,*(tail.arrays if fast else ()))


def make_ffn(parts, G, L, cap, D, FF, FB, chunk, out_dt):
    R=parts*G*cap
    nf=FF//FB
    def kernel(*refs):
        xs=refs[:parts]; ss=refs[parts:2*parts]
        wg,wu,wd=refs[2*parts:2*parts+3]
        o=2*parts+3
        res=refs[o:o+parts]; dgr=refs[o+parts:o+2*parts]
        gG,gU,gD=refs[o+2*parts:o+2*parts+3]
        X,S,H,GB,UB,AR,AD=refs[o+2*parts+3:]
        f=pl.program_id(1)
        @pl.when(f==0)
        def _():
            for p in range(parts):
                for g in range(G):
                    r=(p*G+g)*cap
                    X[r:r+cap,:]=xs[p][g,0]
                    S[r:r+cap,:]=ss[p][g,0]
        @pl.loop(0,R//chunk)
        def _(i):
            rows=pl.ds(pl.multiple_of(i*chunk,chunk),chunk)
            x=X[rows,:]; s=S[rows,:]
            gate=nn(x,wg[0]); up=nn(x,wu[0]); hg=nt(s,wd[0])
            sig=1.0/(1.0+jnp.exp(-gate))
            sil=gate*sig
            h=(sil*up).astype(bf16)
            gb=(hg*up*(sig*(1.0+gate*(1.0-sig)))).astype(bf16)
            ub=(hg*sil).astype(bf16)
            H[rows,:]=h; GB[rows,:]=gb; UB[rows,:]=ub
            r=nn(h,wd[0]); d=nt(gb,wg[0])+nt(ub,wu[0])
            @pl.when(f==0)
            def _():
                AR[rows,:]=r; AD[rows,:]=d
            @pl.when(f>0)
            def _():
                AR[rows,:]+=r; AD[rows,:]+=d
        gG[0]=tn(X[...],GB[...]).astype(bf16)
        gU[0]=tn(X[...],UB[...]).astype(bf16)
        gD[0]=tn(H[...],S[...]).astype(bf16)
        @pl.when(f==nf-1)
        def _():
            for p in range(parts):
                for g in range(G):
                    r=(p*G+g)*cap
                    res[p][g,0]=AR[r:r+cap,:].astype(out_dt)
                    dgr[p][g,0]=AD[r:r+cap,:].astype(out_dt)
    rowspec=pl.BlockSpec((G,1,cap,D),lambda l,f:(0,l,0,0))
    wspec=pl.BlockSpec((1,D,FB),lambda l,f:(l,0,f))
    wdspec=pl.BlockSpec((1,FB,D),lambda l,f:(l,f,0))
    call=pl.pallas_call(kernel,
      out_shape=[jax.ShapeDtypeStruct((G,L,cap,D),out_dt)]*(2*parts)+[jax.ShapeDtypeStruct((L,D,FF),bf16)]*2+[jax.ShapeDtypeStruct((L,FF,D),bf16)],
      grid=(L,nf),
      in_specs=[rowspec]*(2*parts)+[wspec,wspec,wdspec],
      out_specs=[rowspec]*(2*parts)+[wspec,wspec,wdspec],
      scratch_shapes=[pltpu.VMEM((R,D),bf16)]*2+[pltpu.VMEM((R,FB),bf16)]*3+[pltpu.VMEM((R,D),f32)]*2,
      compiler_params=pltpu.CompilerParams(vmem_limit_bytes=60<<20,dimension_semantics=(ARB,ARB)),
      cost_estimate=pl.CostEstimate(flops=2*9*R*D*FF*L,bytes_accessed=L*(6*D*FF*2+4*R*D*2),transcendentals=R*FF*L),
      name="ffn")
    return call


def ffn_rows(x,s,wg,wu,wd,H,GB,UB,rows):
    gate=nn(x,wg); up=nn(x,wu); hg=nt(s,wd)
    sig=1.0/(1.0+jnp.exp(-gate))
    sil=gate*sig
    h=(sil*up).astype(bf16)
    gb=(hg*up*(sig*(1.0+gate*(1.0-sig)))).astype(bf16)
    ub=(hg*sil).astype(bf16)
    H[rows,:]=h; GB[rows,:]=gb; UB[rows,:]=ub
    return nn(h,wd),nt(gb,wg)+nt(ub,wu)

def expert_ffn(deps, l2, xs, ss, wg, wu, wd, f0, nf, prev=(), carry=None, dense=None, inw=None, ext=None, gprev=None, cid=None, FB=512, chunk=480):
    n=len(xs); RG,D=xs[0].shape; FF=wg.shape[2]; R=n*RG; HB=2*FB; ng=nf//2
    SR=D//4; np_=len(prev); nc=0 if carry is None else 1; nd=0 if dense is None else 1
    part=pl.ds(dense[1],dense[2]) if nd else None
    nx=len(deps); nz=0 if inw is None else 2; ne=0 if ext is None else 1; ngp=0 if gprev is None else 6*ng+ng
    def kernel(*refs):
        refs=refs[nx:]
        xr=refs[:n]; sr=refs[n:2*n]; wgr,wur,wdr=refs[2*n:2*n+3]; o=2*n+3
        pv=refs[o:o+np_]; o+=np_
        csrc=refs[o:o+nc]; o+=nc
        dsrc=refs[o:o+nd]; o+=nd
        zsrc=refs[o:o+nz]; o+=nz
        esrc=refs[o:o+ne]; o+=ne
        gp=refs[o:o+ngp]; o+=ngp
        res=refs[o:o+n]; dgr=refs[o+n:o+2*n]; o+=2*n
        gus=[refs[o+3*q:o+3*q+3] for q in range(ng)]; o+=3*ng
        dws=refs[o:o+ng]; o+=ng
        cdst=refs[o:o+nc]; o+=nc
        ddst=refs[o:o+nd]; o+=nd
        zdst=refs[o:o+nz//2]; o+=nz//2
        edst=refs[o:o+ne]; o+=ne
        XT,XN,H,GB,UB,AR,AD=refs[o:o+7]; sems=refs[o+7:]
        f=pl.program_id(0)
        def copies():
            return (plane_copies([(csrc[0],cdst[0])],sems[2*nd+nz+2*ne:]) if nc else [])+(row_copies(dsrc[0],ddst[0],part,sems[nz+2*ne:nz+2*ne+2]) if nd else [])
        if nc or nd or nz:
            @pl.when(f==0)
            def _():
                if nz:
                    if ne: home_barrier()
                    else: plane_z_barrier()
                    inward_run(zsrc,zdst[0],sems[:2],True)
                else:
                    plane_barrier()
                if ne: ext_run(esrc[0],edst[0],sems[nz:nz+2],True)
                for cpy in copies(): cpy.start()
        @pl.when(f==0)
        def _():
            for a in range(n):
                for b in range(RG//chunk):
                    XN[...]=xr[a][b*chunk:(b+1)*chunk,:].astype(f32).T.astype(bf16)
                    for q in range(4):
                        XT[a*(RG//chunk)+b,q*SR:(q+1)*SR,:]=XN[pl.ds(pl.multiple_of(shard_of(q)*SR,SR),SR),:]
        for a in range(n):
            @pl.loop(0,RG//chunk)
            def _(i):
                src=pl.ds(pl.multiple_of(i*chunk,chunk),chunk)
                rows=pl.ds(pl.multiple_of(a*RG+i*chunk,chunk),chunk)
                r,d=ffn_rows(xr[a][src,:],sr[a][src,:],wgr[0],wur[0],wdr[0],H,GB,UB,rows)
                @pl.when(f==0)
                def _():
                    if np_:
                        AR[rows,:]=r+pv[a][src,:].astype(f32); AD[rows,:]=d+pv[n+a][src,:].astype(f32)
                    else:
                        AR[rows,:]=r; AD[rows,:]=d
                if nf>2:
                    @pl.when((f>0)&(f<nf-1))
                    def _():
                        AR[rows,:]+=r; AD[rows,:]+=d
                @pl.when(f==nf-1)
                def _():
                    res[a][src,:]=(AR[rows,:]+r).astype(bf16); dgr[a][src,:]=(AD[rows,:]+d).astype(bf16)
        for t,Y in enumerate((GB,UB)):
            gv=None
            for b in range(R//chunk):
                p=nn(XT[b],Y[b*chunk:(b+1)*chunk,:])
                gv=p if gv is None else gv+p
            cols=pl.ds(pl.multiple_of(t*HB+lax.rem(f,2)*FB,FB),FB)
            for q in range(ng):
                def put(q=q,t=t,gv=gv,cols=cols):
                    for s,(ref,lo,hi) in enumerate(zip(gus[q],(0,2*SR,3*SR),(2*SR,3*SR,4*SR))):
                        v=gv[lo:hi]
                        if ngp: v=v+gp[6*q+3*t+s][...].astype(f32)
                        ref[:,cols]=v.astype(bf16)
                if ng==1: put()
                else: pl.when(lax.div(f,2)==q)(put)
        dv=None
        for a in range(n):
            t=tn(H[a*RG:(a+1)*RG,:],sr[a][...])
            dv=t if dv is None else dv+t
        for q in range(ng):
            def put(q=q,dv=dv):
                dws[q][...]=((dv+gp[6*ng+q][...].astype(f32)) if ngp else dv).astype(bf16)
            if ng==1: put()
            else: pl.when(lax.div(f,2)==q)(put)
        if nc or nd or nz:
            @pl.when(f==nf-1)
            def _():
                for cpy in copies(): cpy.wait()
                if nz: inward_run(zsrc,zdst[0],sems[:2],False)
                if ne: ext_run(esrc[0],edst[0],sems[nz:nz+2],False)
    one=pl.Buffered(1)
    rowspec=pl.BlockSpec((RG,D),lambda f:(0,0),pipeline_mode=one)
    wspec=pl.BlockSpec((1,D,FB),lambda f:(2*spot()[0]+l2,0,f+f0))
    wdspec=pl.BlockSpec((1,FB,D),lambda f:(2*spot()[0]+l2,f+f0,0))
    full=lambda r,c: pl.BlockSpec((r,c),lambda f:(0,0),pipeline_mode=one)
    anyspec=pl.BlockSpec(memory_space=pl.ANY)
    wspecs=[pl.BlockSpec((FB,D),lambda f: ((1-f) if f0 else f,0))] if ng==1 else [
        pl.BlockSpec((FB,D),lambda f: (jnp.minimum(f,1),0)),pl.BlockSpec((FB,D),lambda f: (jnp.minimum(3-f,1),0))]
    gpspecs=[]; gpargs=[]
    if ngp:
        for q in range(ng):
            for t in range(2):
                for s,rr in enumerate((2*SR,SR,SR)):
                    gpspecs.append(pl.BlockSpec((rr,FB),lambda f,q=q,t=t: (0,2*t+jnp.clip(f-2*q,0,1))))
                    gpargs.append(gprev[q][s])
        gpspecs+=wspecs; gpargs+=list(gprev[ng:])
    out=pl.pallas_call(kernel,grid=(nf,),
        in_specs=[anyspec]*nx+[rowspec]*(2*n)+[wspec,wspec,wdspec]+[rowspec]*np_+[anyspec]*(nc+nd+nz+ne)+gpspecs,
        out_specs=[rowspec]*(2*n)+[full(2*SR,2*HB),full(SR,2*HB),full(SR,2*HB)]*ng+wspecs+[anyspec]*(nc+nd+nz//2+ne),
        scratch_shapes=[pltpu.VMEM((R//chunk,D,chunk),bf16),pltpu.VMEM((D,chunk),bf16)]+[pltpu.VMEM((R,FB),bf16)]*3+[pltpu.VMEM((R,D),f32)]*2+([pltpu.SemaphoreType.DMA((1,)),pltpu.SemaphoreType.DMA((1,))] if nz else [])+(ext_sems() if ne else [])+(row_sems() if nd else [])+(plane_sems(1) if nc else []),
      out_shape=[jax.ShapeDtypeStruct((RG,D),bf16)]*(2*n)+([jax.ShapeDtypeStruct((2*SR,2*HB),bf16)]+[jax.ShapeDtypeStruct((SR,2*HB),bf16)]*2)*ng+[jax.ShapeDtypeStruct((HB,D),bf16)]*ng+[jax.ShapeDtypeStruct((8,RG//8,D),bf16)]*nc+([jax.ShapeDtypeStruct((3,dense[2])+dense[0].shape[2:],bf16)] if nd else [])+([jax.ShapeDtypeStruct(inw[0].shape,bf16)] if nz else [])+([jax.ShapeDtypeStruct(ext.shape,bf16)] if ne else []),
      compiler_params=pltpu.CompilerParams(vmem_limit_bytes=62<<20,dimension_semantics=(ARB,),**(dict(collective_id=cid,has_side_effects=True) if nc or nd or nz else {})),
      cost_estimate=pl.CostEstimate(flops=9*R*D*FF*ng,bytes_accessed=3*D*FF*2*ng+4*R*D*2,transcendentals=R*FF*ng//2),
      name=f"expert_ffn{n}_{f0}")(*deps,*xs,*ss,wg,wu,wd,*prev,*([carry] if nc else []),*([dense[0]] if nd else []),*(inw if nz else ()),*([ext] if ne else []),*gpargs)
    o=2*n
    return (out[:o],*[out[o+3*q:o+3*q+3] for q in range(ng)],*out[o+3*ng:])

def shared_ffn(x, s, wg, wu, wd, xout, sa, FB=512):
    T,D=x.shape; FF=wg.shape[1]; nf=FF//FB; chunk=T//2
    SG=D//8; SD=FB//8
    NR=2*SG*(FB//128)+SD*(D//128)
    def kernel(xr,sr,wgr,wur,wdr,xo,zs,res,dgr,o0,o1,xia,xib,zd,XT,H,GB,UB,VG,VD,zs0,zs1,*sems):
        f=pl.program_id(0)
        core=spot()[0]
        pairs=[(xo.at[0],xia),(xo.at[1],xib)]
        @pl.when(f==0)
        def _():
            plane_z_barrier()
            for cpy in plane_copies(pairs,sems): cpy.start()
            inward_run((zs,zs),zd,(zs0,zs1),True)
        @pl.when(f==0)
        def _():
            for b in range(2):
                XT[:,b*chunk:(b+1)*chunk]=xr[b*chunk:(b+1)*chunk,:].astype(f32).T.astype(bf16)
        @pl.loop(0,T//chunk)
        def _(i):
            rows=pl.ds(pl.multiple_of(i*chunk,chunk),chunk)
            r,d=ffn_rows(xr[rows,:],sr[rows,:],wgr[...],wur[...],wdr[...],H,GB,UB,rows)
            @pl.when(f==0)
            def _():
                res[rows,:]=r; dgr[rows,:]=d
            @pl.when(f>0)
            def _():
                res[rows,:]+=r; dgr[rows,:]+=d
        for t,Y in enumerate((GB,UB)):
            VG[...]=nn(XT[...],Y[...]).astype(bf16)
            for zr in range(4):
                for cp in range(2):
                    src=pl.ds(pl.multiple_of(2*SG*shard_of(zr)+SG*lax.rem(core+cp,2),SG),SG)
                    for b in range(FB//128):
                        off=(t*(FB//128)+b)*SG
                        (o0,o1)[cp][f,zr,off:off+SG,:]=VG[src,b*128:(b+1)*128]
        VD[...]=tn(H[...],sr[...]).astype(bf16)
        zr=jnp.where(spot()[1]<2,3-f,f)
        for cp in range(2):
            for e in range(4):
                src=pl.ds(pl.multiple_of(lax.rem(core+cp,2)*4*SD+e*SD,SD),SD)
                for b in range(D//128):
                    off=2*SG*(FB//128)+b*SD
                    (o0,o1)[cp][e,zr,off:off+SD,:]=VD[src,b*128:(b+1)*128]
        @pl.when(f==nf-1)
        def _():
            for cpy in plane_copies(pairs,sems): cpy.wait()
            inward_run((zs,zs),zd,(zs0,zs1),False)
    full=lambda sh: pl.BlockSpec(sh,lambda f:(0,)*len(sh))
    return pl.pallas_call(kernel,grid=(nf,),
      in_specs=[full((T,D)),full((T,D)),pl.BlockSpec((D,FB),lambda f:(0,f)),pl.BlockSpec((D,FB),lambda f:(0,f)),pl.BlockSpec((FB,D),lambda f:(f,0))]+[pl.BlockSpec(memory_space=pl.ANY)]*2,
      out_specs=[full((T,D)),full((T,D)),full((4,4,NR,128)),full((4,4,NR,128))]+[pl.BlockSpec(memory_space=pl.ANY)]*3,
      out_shape=[jax.ShapeDtypeStruct((T,D),f32)]*2+[jax.ShapeDtypeStruct((4,4,NR,128),bf16)]*2+[jax.ShapeDtypeStruct(xout.shape[1:],bf16)]*3,
      scratch_shapes=[pltpu.VMEM((D,T),bf16)]+[pltpu.VMEM((T,FB),bf16)]*3+[pltpu.VMEM((D,FB),bf16),pltpu.VMEM((FB,D),bf16)]+[pltpu.SemaphoreType.DMA((1,))]*2+plane_sems(2),
      compiler_params=pltpu.CompilerParams(vmem_limit_bytes=62<<20,dimension_semantics=(ARB,),collective_id=1,has_side_effects=True),
      cost_estimate=pl.CostEstimate(flops=2*9*T*D*FF,bytes_accessed=6*D*FF*2+8*T*D*2,transcendentals=T*FF),
      name="shared_ffn")(x,s,wg,wu,wd,xout,sa)


def route(order, expert_ids, gates, cot, core, G, L, parts, plane=False):
    T,D=cot.shape; P2=2*T
    LP=L//parts; S=G*LP*CAP
    big=E*CAP
    CH=480 if S%480==0 else CAP*4
    def kernel(core_ref,orow,ids,gts,ct,rowo,colo,*rest):
        sgs=rest[:parts]; PT,PG=rest[parts:]
        lane=lax.broadcasted_iota(jnp.int32,(T,128),1)
        e0=ids[:,0:1].astype(f32); e1=ids[:,1:2].astype(f32)
        er=jnp.where(lane==0,e0,jnp.where(lane==1,e1,0.0)).T[0:8,:]
        ecat=jnp.concatenate([er[0:1,:],er[1:2,:]],axis=1)
        eoh=(lax.broadcasted_iota(jnp.int32,(E,P2),0).astype(f32)==ecat)
        eohb=jnp.where(eoh,1.0,0.0).astype(bf16)
        o=orow[...]
        oj=(o&1)*T+(o>>1)
        CB=256
        for c in range(P2//CB):
            jj=lax.broadcasted_iota(jnp.int32,(CB,P2),0)+c*CB
            PT[c*CB:(c+1)*CB,:]=jnp.where(jj==oj,1.0,0.0).astype(bf16)
        soh=nn(eohb,PT[...])
        sohb=soh.astype(bf16)
        tri=jnp.where(lax.broadcasted_iota(jnp.int32,(CB,CB),0)<lax.broadcasted_iota(jnp.int32,(CB,CB),1),1.0,0.0).astype(bf16)
        run=jnp.zeros((E,1),f32)
        pos=[]
        for c in range(P2//CB):
            blk=soh[:,c*CB:(c+1)*CB]
            before=nn(sohb[:,c*CB:(c+1)*CB],tri)+run
            run=run+jnp.sum(blk,axis=1,keepdims=True)
            pos.append(jnp.sum(before*blk,axis=0,keepdims=True))
        posr=jnp.minimum(jnp.concatenate(pos,axis=1),127.0)
        posj=nt(jnp.broadcast_to(posr,(16,P2)).astype(bf16),PT[...])[0:1,:]
        e=ecat.astype(jnp.int32)
        l=lax.rem(e,L); j=lax.div(e,L)
        if plane:
            base=((lax.rem(l,2)*2+lax.div(l,2))*G+j)*CAP
        elif parts==2:
            cc=lax.rem(lax.div(l,LP)+core_ref[0],2)
            base=((cc*G+j)*LP+lax.rem(l,LP))*CAP
        else:
            base=e*CAP
        p=posj.astype(jnp.int32)
        slot=jnp.where(p<CAP,base+p,big)
        s0=slot[:,0:T]; s1=slot[:,T:P2]
        r8=lax.broadcasted_iota(jnp.int32,(8,T),0)
        rows=jnp.where(r8==0,s0,jnp.where(r8==1,s1,big))
        rowo[...]=rows
        rep=jnp.concatenate([rows.astype(f32)]*16,axis=0).T
        colo[...]=rep[:,0:8].astype(jnp.int32)
        ctf=ct[...].astype(f32)
        PG[0:T,:]=(gts[:,0:1]*ctf).astype(bf16)
        PG[T:P2,:]=(gts[:,1:2]*ctf).astype(bf16)
        for pi in range(parts):
            @pl.loop(0,S//CH)
            def _(i):
                si=lax.broadcasted_iota(jnp.int32,(CH,T),0)+(i*CH+pi*S)
                d0=jnp.where(si==rowo[0:1,:],1.0,0.0).astype(bf16)
                d1=jnp.where(si==rowo[1:2,:],1.0,0.0).astype(bf16)
                sgs[pi][pl.ds(pl.multiple_of(i*CH,CH),CH),:]=(nn(d0,PG[0:T,:])+nn(d1,PG[T:P2,:])).astype(bf16)
    vm=pl.BlockSpec(memory_space=pltpu.VMEM)
    out=pl.pallas_call(kernel,
      in_specs=[pl.BlockSpec(memory_space=pltpu.SMEM)]+[vm]*4,out_specs=[vm]*(2+parts),
      out_shape=[jax.ShapeDtypeStruct((8,T),jnp.int32),jax.ShapeDtypeStruct((T,8),jnp.int32)]+[jax.ShapeDtypeStruct((S,D),bf16)]*parts,
      scratch_shapes=[pltpu.VMEM((P2,P2),bf16),pltpu.VMEM((P2,D),bf16)],
      compiler_params=pltpu.CompilerParams(vmem_limit_bytes=50<<20),
      cost_estimate=pl.CostEstimate(flops=4*S*parts*T*D+4*P2*P2*16,bytes_accessed=8<<20,transcendentals=0),
      name="route")(core,order,expert_ids,gates,cot)
    return out[0],out[1],out[2:]

def dispatch(rows, x, parts):
    T,D=x.shape; S=E*CAP//parts; CH=480
    def kernel(rowr,xr,*outs):
        for pi in range(parts):
            @pl.loop(0,S//CH)
            def _(i):
                si=lax.broadcasted_iota(jnp.int32,(CH,T),0)+(i*CH+pi*S)
                d=jnp.where((si==rowr[0:1,:])|(si==rowr[1:2,:]),1.0,0.0).astype(bf16)
                outs[pi][pl.ds(pl.multiple_of(i*CH,CH),CH),:]=nn(d,xr[...]).astype(bf16)
    vm=pl.BlockSpec(memory_space=pltpu.VMEM)
    return pl.pallas_call(kernel,in_specs=[vm]*2,out_specs=[vm]*parts,out_shape=[jax.ShapeDtypeStruct((S,D),bf16)]*parts,
      compiler_params=pltpu.CompilerParams(vmem_limit_bytes=50<<20),
      cost_estimate=pl.CostEstimate(flops=2*S*parts*T*D,bytes_accessed=6<<20,transcendentals=0),name="dispatch")(rows,x)

def combine(cols, gates, ret, state, shared):
    parts=len(ret); T,D=state.shape; S=ret[0].shape[0]
    def kernel(colr,g,*refs):
        rs=refs[:parts]; st,sh,out=refs[parts:]
        @pl.loop(0,T//QC)
        def _(i):
            r=pl.ds(pl.multiple_of(i*QC,QC),QC)
            acc=st[r,:]+sh[r,:]
            for k in range(2):
                pk=None
                for pi in range(parts):
                    si=lax.broadcasted_iota(jnp.int32,(QC,S),1)+pi*S
                    d=jnp.where(si==colr[r,k:k+1],1.0,0.0).astype(bf16)
                    q=nn(d,rs[pi][...])
                    pk=q if pk is None else pk+q
                acc=acc+g[r,k:k+1]*pk
            out[r,:]=acc.astype(bf16)
    vm=pl.BlockSpec(memory_space=pltpu.VMEM)
    return pl.pallas_call(kernel,in_specs=[vm]*(4+parts),out_specs=vm,out_shape=jax.ShapeDtypeStruct((T,D),bf16),
      compiler_params=pltpu.CompilerParams(vmem_limit_bytes=50<<20),
      cost_estimate=pl.CostEstimate(flops=4*S*parts*T*D,bytes_accessed=9<<20,transcendentals=0),name="combine")(cols,gates,*ret,state,shared)

def mid_bwd_home(deps, inw, dsum, rext, cols, own, ext, back_b, dsh, state, fgain, cot):
    T,D=state.shape; S=8*CAP; nx=len(deps)
    def kernel(*refs):
        body(*refs[nx:])
    def body(z0,z1,dsrc,rsrc,colr,hown,hext,bb,ds,st,fg,ct,sgo,fgo,ba,zd,dd,rd,BV,cs,zs0,zs1,rs0,rs1,es0,es1,*osems):
        home_barrier()
        own_run(hown,ba,osems,True)
        ext_run(rsrc,rd,(es0,es1),True)
        inward_run((z0,z1),zd,(zs0,zs1),True)
        rows=lambda: row_copies(dsrc,dd,pl.ds(3,1),(rs0,rs1))
        for cp in rows(): cp.start()
        fgo[...]=jnp.zeros_like(fgo)
        @pl.loop(0,T//QC)
        def _(i):
            r=pl.ds(pl.multiple_of(i*QC,QC),QC)
            si=lax.broadcasted_iota(jnp.int32,(QC,S),1)+S
            d=jnp.where((si==colr[r,0:1])|(si==colr[r,1:2]),1.0,0.0).astype(bf16)
            sgo[r,:]=ds[r,:]+nn(d,bb[...])
        own_run(hown,ba,osems,False)
        def fetch(src):
            cps=[pltpu.make_async_copy(src.at[i],BV.at[i],cs.at[i]) for i in range(8)]
            for cp in cps: cp.start()
            for cp in cps: cp.wait()
        pl.when(is_inner())(lambda: fetch(ba))
        pl.when(jnp.logical_not(is_inner()))(lambda: fetch(hext))
        @pl.loop(0,T//QC)
        def _(i):
            r=pl.ds(pl.multiple_of(i*QC,QC),QC)
            n=sgo[r,:]
            for b in range(8):
                si=lax.broadcasted_iota(jnp.int32,(QC,128),1)
                si=jnp.where(si<CAP,si+b*CAP,-1)
                d=jnp.where((si==colr[r,0:1])|(si==colr[r,1:2]),1.0,0.0).astype(bf16)[:,0:CAP]
                n=n+nn(d,BV[b])
            x=st[r,:]; inv=inv_rms(x); u=x*inv
            fgo[...]+=jnp.broadcast_to(jnp.sum(n*u,axis=0,keepdims=True),(8,D))
            w=n*fg[fg.shape[0]-1:,:]
            sgo[r,:]=ct[r,:].astype(f32)+inv*(w-u*jnp.mean(w*u,axis=1,keepdims=True))
        inward_run((z0,z1),zd,(zs0,zs1),False)
        for cp in rows(): cp.wait()
        ext_run(rsrc,rd,(es0,es1),False)
    vm=pl.BlockSpec(memory_space=pltpu.VMEM); an=pl.BlockSpec(memory_space=pl.ANY)
    SD=jax.ShapeDtypeStruct
    return pl.pallas_call(kernel,in_specs=[an]*(nx+4)+[vm,an,an]+[vm]*5,out_specs=[vm]*2+[an]*4,
      out_shape=[SD((T,D),f32),SD((8,D),f32),SD((8,CAP,D),bf16),SD(inw[0].shape,bf16),SD((3,1)+dsum.shape[2:],bf16),SD((8,CAP,D),bf16)],
      scratch_shapes=[pltpu.VMEM((8,CAP,D),bf16),pltpu.SemaphoreType.DMA((8,))]+[pltpu.SemaphoreType.DMA((1,))]*2+row_sems()+ext_sems()+plane_sems(1),
      compiler_params=pltpu.CompilerParams(vmem_limit_bytes=50<<20,collective_id=4,has_side_effects=True),
      cost_estimate=pl.CostEstimate(flops=4*S*T*D,bytes_accessed=12<<20,transcendentals=0),name="mid_bwd")(*deps,*inw,dsum,rext,cols,own,ext,back_b,dsh,state,as_rows(fgain),cot)

def mid_bwd(cols, back, dsh, state, fgain, cot):
    parts=len(back); T,D=state.shape; S=back[0].shape[0]
    def kernel(colr,*refs):
        bs=refs[:parts]; ds,st,fg,ct,sgo,fgo=refs[parts:]
        fgo[...]=jnp.zeros_like(fgo)
        @pl.loop(0,T//QC)
        def _(i):
            r=pl.ds(pl.multiple_of(i*QC,QC),QC)
            n=ds[r,:]
            for pi in range(parts):
                si=lax.broadcasted_iota(jnp.int32,(QC,S),1)+pi*S
                d=jnp.where((si==colr[r,0:1])|(si==colr[r,1:2]),1.0,0.0).astype(bf16)
                n=n+nn(d,bs[pi][...])
            x=st[r,:]; inv=inv_rms(x); u=x*inv
            fgo[...]+=jnp.broadcast_to(jnp.sum(n*u,axis=0,keepdims=True),(8,D))
            w=n*fg[...]
            sgo[r,:]=ct[r,:].astype(f32)+inv*(w-u*jnp.mean(w*u,axis=1,keepdims=True))
    vm=pl.BlockSpec(memory_space=pltpu.VMEM)
    return pl.pallas_call(kernel,in_specs=[vm]*(5+parts),out_specs=[vm]*2,out_shape=[jax.ShapeDtypeStruct((T,D),f32),jax.ShapeDtypeStruct((8,D),f32)],
      compiler_params=pltpu.CompilerParams(vmem_limit_bytes=50<<20),
      cost_estimate=pl.CostEstimate(flops=2*S*parts*T*D,bytes_accessed=12<<20,transcendentals=0),name="mid_bwd")(cols,*back,dsh,state,fgain[None],cot)

HEADS = 12
HEAD_DIM = 64


def rope_wide(length):
    positions = np.arange(length, dtype=np.float32)
    frequency = (10000.0 ** (-np.arange(HEAD_DIM // 2) * 2.0 / HEAD_DIM)).astype(np.float32)
    angles = (positions[:, None] * frequency[None, :]).astype(np.float64)
    c = np.cos(angles).astype(np.float32)
    s = np.sin(angles).astype(np.float32)
    return np.concatenate([c, c, c, c], axis=1), np.concatenate([-s, s, -s, s], axis=1)


def shards_any(tokens, cotangent, expert_ids, route_gates, slot_order, prefix_len, attention_gain, qkv_weight,
           output_weight, feedforward_gain, shared_gate, shared_up, shared_down, expert_gate, expert_up, expert_down):
    T, D = tokens.shape
    L, _, FF = expert_gate.shape
    G = lax.axis_size(EX)
    DP = lax.axis_size(DX)
    Z = DP // 2
    parts = 2 if L % 2 == 0 else 1
    LP = L // parts
    dpi = lax.axis_index(DX)
    core = lax.rem(dpi, 2)
    swap_perm = [(i, i ^ 1) for i in range(DP)]
    zgroups = [[2 * z + c for z in range(Z)] for c in range(2)]

    def swap(x):
        return lax.ppermute(x, DX, swap_perm)

    def a2a(x):
        return lax.all_to_all(x, EX, split_axis=0, concat_axis=0, tiled=True)

    def to_experts(arrs):
        arrs = [a.reshape(G, LP, CAP, D) for a in arrs]
        if parts == 2:
            arrs = [arrs[0], swap(arrs[1])]
        return [a2a(a) for a in arrs]

    def from_experts(arrs):
        arrs = [a2a(a) for a in arrs]
        if parts == 2:
            arrs = [arrs[0], swap(arrs[1])]
        return [a.reshape(G * LP * CAP, D) for a in arrs]

    cosw, sinw = rope_wide(T)
    rows, cols, sgs = route(slot_order, expert_ids, route_gates, cotangent, core[None].astype(jnp.int32), G, L, parts)
    slot_in = to_experts(sgs)
    q, k, v, att, lse, state, ntwo = attn_fwd(tokens, prefix_len, attention_gain, qkv_weight, output_weight,
                                              feedforward_gain, cosw, sinw)
    xs = dispatch(rows, ntwo, parts)
    x_in = to_experts(xs)
    sh = make_ffn(1, 1, 1, T, D, FF, 512, T // 2, f32)(
        ntwo[None, None], cotangent[None, None], shared_gate[None], shared_up[None], shared_down[None])
    shared_branch = sh[0].reshape(T, D)
    dshared = sh[1].reshape(T, D)
    dense_shared = [sh[2][0], sh[3][0], sh[4][0]]

    res, dgr, eg = [], [], []
    one = make_ffn(parts, G, 1, CAP, D, FF, 512, parts * G * CAP // 2, bf16)
    for l in range(LP):
        o = one(*[a[:, l:l + 1] for a in x_in], *[a[:, l:l + 1] for a in slot_in],
                *[lax.dynamic_slice_in_dim(w, (core * LP if parts == 2 else 0) + l, 1, 0)
                  for w in (expert_gate, expert_up, expert_down)])
        res.append(o[:parts])
        dgr.append(o[parts:2 * parts])
        eg.append(o[2 * parts:])
    cat = lambda xs_: jnp.concatenate(xs_, axis=1) if len(xs_) > 1 else xs_[0]
    res = [cat([r[p] for r in res]) for p in range(parts)]
    dgr = [cat([r[p] for r in dgr]) for p in range(parts)]

    egr = []
    for l in range(LP):
        if parts == 2:
            egr.append([lax.psum_scatter(g[0], DX, scatter_dimension=0, tiled=True, axis_index_groups=zgroups)
                        for g in eg[l]])
        else:
            egr.append([lax.psum_scatter(g[0], DX, scatter_dimension=0, tiled=True) for g in eg[l]])

    back = from_experts(dgr)
    ret = from_experts(res)
    sgrad, fgg = mid_bwd(cols, back, dshared, state, feedforward_gain, cotangent)
    tokens_grad, agg, gq, gk, gv, gwo = attn_bwd(sgrad, prefix_len, tokens, attention_gain, qkv_weight, output_weight,
                                                 cosw, sinw, q, k, v, att, lse)
    block_out = combine(cols, route_gates, ret, state, shared_branch)

    def dense(g):
        r = g.shape[0] // DP
        h = g.reshape(Z, 2, r, g.shape[1])
        mine = lax.dynamic_index_in_dim(h, core, 1, keepdims=False)
        other = lax.dynamic_index_in_dim(h, 1 - core, 1, keepdims=False)
        s = (mine.astype(f32) + swap(other).astype(f32)).astype(bf16)
        quarter = s.reshape(Z, G, r // G, g.shape[1])
        quarter = jnp.swapaxes(quarter, 0, 1)
        got = lax.all_to_all(quarter, EX, split_axis=0, concat_axis=0, tiled=True)
        s = jnp.sum(got.astype(f32), axis=0).astype(bf16)
        zs = lax.psum_scatter(s, DX, scatter_dimension=0, tiled=True, axis_index_groups=zgroups)
        return lax.all_gather(zs[0], EX, axis=0, tiled=True).astype(f32)

    def dense_simple(g):
        p = lax.psum_scatter(g, DX, scatter_dimension=0, tiled=True)
        return lax.psum(p, EX).astype(f32)

    if (qkv_weight.shape[0] // DP) % (8 * G) == 0 and parts == 2:
        dn = dense
    else:
        dn = dense_simple
    dsh = [dn(g) for g in dense_shared]
    dq, dk, dv, dwo = [dn(g) for g in (gq, gk, gv, gwo)]
    gains = lax.psum(jnp.stack([agg[0], fgg[0]]), (DX, EX))
    gs = D // DP
    gains = lax.dynamic_slice_in_dim(gains, dpi * gs, gs, 1)

    def finish(t):
        a = [egr[l][t] for l in range(LP)]
        if parts == 1:
            return jnp.stack(a).astype(f32)
        b = jnp.stack(a)
        h = b.reshape(LP, 2, b.shape[1] // 2, b.shape[2])
        mine = lax.dynamic_index_in_dim(h, core, 1, keepdims=False)
        other = swap(lax.dynamic_index_in_dim(h, 1 - core, 1, keepdims=False))
        return jnp.concatenate([jnp.where(core == 0, mine, other), jnp.where(core == 0, other, mine)], axis=0).astype(f32)

    return (block_out, tokens_grad, gains[0], jnp.concatenate([dq, dk, dv], axis=1), dwo, gains[1],
            dsh[0], dsh[1], dsh[2], finish(0), finish(1), finish(2))


def shards_fast(tokens, cotangent, expert_ids, route_gates, slot_order, prefix_len, attention_gain, qkv_weight,
                output_weight, feedforward_gain, shared_gate, shared_up, shared_down, expert_gate, expert_up, expert_down):
    attention_gain = feedforward_gain = jnp.stack([attention_gain, feedforward_gain])
    T, D = tokens.shape
    FF = expert_gate.shape[2]
    dpi = lax.axis_index(DX).astype(jnp.int32)
    ei = lax.axis_index(EX).astype(jnp.int32)
    core = lax.rem(dpi, 2)
    zi = lax.div(dpi, 2)
    outer = (zi == 0) | (zi == 3)
    low = zi < 2

    def swap(x):
        return lax.ppermute(x, DX, [(i, i ^ 1) for i in range(8)])

    def across(x):
        return lax.ppermute(x, DX, [(2, 4), (3, 5), (4, 2), (5, 3)])

    def add(*xs):
        t = xs[0].astype(f32)
        for x in xs[1:]:
            t = t + x.astype(f32)
        return t.astype(bf16)

    cosw, sinw = rope_wide(T)
    rows, cols, (s_out,) = route(slot_order, expert_ids, route_gates, cotangent, core[None], 4, 4, 1, True)
    q, k, v, att, lse, state, ntwo, x_out, sa, sb = attn_fwd(
        tokens, prefix_len, attention_gain, qkv_weight, output_weight, feedforward_gain, cosw, sinw, rows,
        s_out.reshape(2, 8, CAP, D))
    flat = lambda y: y.reshape(8 * CAP, D)
    shared_branch, dshared, sh0, sh1, xa, xb, sx = shared_ffn(ntwo, cotangent, shared_gate, shared_up, shared_down,
                                                              x_out.reshape(2, 8, CAP, D), sa)
    ws = (expert_gate, expert_up, expert_down)
    blocks = lambda y: y.reshape(8, CAP, D)
    dsum = add(sh0, swap(sh1))
    (rb, db), gb0, gb1, wb0, wb1, xx = expert_ffn([], 1, [flat(xb)], [flat(sb)], *ws, 0, 4, inw=(xa, xa), cid=6)
    sa, sx, xa, xx = flat(sa), flat(sx), flat(xa), flat(xx)
    (rx, dx), gx0, gx1, wx0, wx1, db, r0, rf0 = expert_ffn([], 0, [xx], [sx], *ws, 0, 4, carry=blocks(db), dense=(dsum, 0, 1),
                                                           inw=(gb0[0], gb0[0]), cid=2)
    bs0 = add(gb0[0], rf0)
    m_b0 = across(bs0)
    (ra, da), ga0, ga1, wa0, wa1, r1, rf1, dxl = expert_ffn([bs0], 0, [xa], [sa], *ws, 0, 4, dense=(dsum, 1, 2),
                                                            inw=(gb1[0], gb1[0]), ext=blocks(dx),
                                                            gprev=(gx0, gx1, wx0, wx1), cid=3)
    bs1 = add(gb1[0], rf1)
    m_b1 = across(bs1)
    m_a0o = across(ga0[0][:D // 4])
    sgrad, fgg, _, rf2, r2, rxl = mid_bwd_home([bs1], (wb1, wb0), dsum, blocks(rx), cols, blocks(da), dxl, flat(db), dshared,
                                               state, feedforward_gain, cotangent)
    bs2 = add(jnp.where(low, wb1, wb0), rf2)
    mine = lax.dynamic_index_in_dim(dsum, ei, 0, keepdims=False)
    got = jnp.concatenate([r0, r1, r2], axis=1)
    msh = add(mine, got[0], got[1], got[2])
    carried = {
        "cols": cols, "gates": route_gates, "state": state, "shared": shared_branch, "hown": blocks(ra), "rxl": rxl, "rbs": blocks(rb), "fgg": fgg, "msh": msh,
        "m0": m_b0, "ni0": gb0[1], "no0": gb0[2],
        "m1": m_b1, "m2o": m_a0o, "ni1": gb1[1], "no1": gb1[2],
        "far2": ga0[0], "ni2": ga0[1], "no2": ga0[2],
        "far3": ga1[0], "ni3": ga1[1], "no3": ga1[2],
        "wa0": wa0, "wa1": wa1, "wb0": wb0, "wb1": wb1,
        "far5": bs2,
    }
    tail = Tail(carried, T, D, FF)
    tokens_grad, _, *rest = attn_bwd(sgrad, prefix_len, tokens, attention_gain, qkv_weight, output_weight,
                                     cosw, sinw, q, k, v, att, lse, tail)
    o = dict(zip(tail.onames, rest))
    sg = D // 8
    gains = lax.dynamic_slice_in_dim(o["gains"], dpi * sg, sg, 1)
    return (o["block"], tokens_grad, gains[0], o["dqkv"], o["dwo"], gains[1], o["dgate"], o["dup"], o["ddown"],
            o["gate"].astype(f32), o["up"].astype(f32), o["down"].astype(f32))


def shards(*args):
    local = args[13].shape[0]
    if lax.axis_size(DX) == 8 and lax.axis_size(EX) == 4 and local == 4:
        return shards_fast(*args)
    return shards_any(*args)


def solution(mesh):
    row = P((DX, EX), None)
    return jax.shard_map(
        shards,
        mesh=mesh,
        in_specs=(row, row, row, row, row, P((DX, EX)), P(), P(), P(), P(), P(), P(), P(),
                  P(EX, None, None), P(EX, None, None), P(EX, None, None)),
        out_specs=(row, row, P(DX), P(DX, None), P(DX, None), P(DX), P(DX, None), P(DX, None),
                   P(DX, None), P(EX, DX, None), P(EX, DX, None), P(EX, DX, None)),
        check_vma=False,
    )
```
